32 devices in a mesh: terms: 32 (over z, y, x, core).
Axes of the slice: x: 2, y: 2, z: 4, core: 2. Of those that a mesh axis runs over, the one named last changes fastest.
Arguments:
- wavefunction: float32 [512, 16, 512], replicated
- left_env: bfloat16 [64, 512, 512], P('terms')
- pair_ops: bfloat16 [64, 16, 16], P('terms')
- right_env: bfloat16 [64, 512, 512], P('terms')
- full_term: int32 [64], P('terms')
Outputs:
- output 1: float32 [7, 512, 16, 512], P(None, 'terms')
- output 2: float32 [6], replicated
- output 3: float32 [6], replicated
All inputs are finite; a program needn't handle non-finite values.
Results may differ from the reference program's by a relative error of at most 0.0131262.
Values are sent between devices in bfloat16 or wider.
A program may use at most 1 GiB of HBM per device.

```python
import jax
import jax.numpy as jnp
from jax import lax

BOND_DIM = 512
PHYS_DIM = 4
TERMS_DEV = 2
NUM_DEV = 32
NUM_TERMS = 64
LANCZOS_STEPS = 6

PAIR_DIM = PHYS_DIM * PHYS_DIM
VEC_SIZE = BOND_DIM * PAIR_DIM * BOND_DIM


def normal_sym(rng_key, num_mats, mat_size):
    raw_draw = jax.random.normal(rng_key, (num_mats, mat_size, mat_size), jnp.float32)
    return (raw_draw + jnp.swapaxes(raw_draw, 1, 2)) * (2.0 * mat_size) ** -0.5


def draw_flags(rng_key):
    count_key, pick_key, order_key = jax.random.split(rng_key, 3)
    block_counts = jax.random.randint(count_key, (NUM_DEV,), 0, TERMS_DEV + 1)
    picked = jax.random.permutation(pick_key, NUM_DEV)
    block_counts = block_counts.at[picked[0]].set(TERMS_DEV).at[picked[1]].set(0)
    rank_table = jax.vmap(lambda sub_key: jax.random.permutation(sub_key, TERMS_DEV))(jax.random.split(order_key, NUM_DEV))
    return (rank_table < block_counts[:, None]).astype(jnp.int32).reshape(NUM_TERMS)


def setup_inputs(seed: int = 0) -> dict:
    wave_key, left_key, pair_key, right_key, flag_key = jax.random.split(jax.random.key(seed), 5)
    diag_shift = (2.0 / NUM_TERMS ** 0.5) ** 0.5
    wavefunction = jax.random.normal(wave_key, (BOND_DIM, PAIR_DIM, BOND_DIM), jnp.float32)
    left_env = (normal_sym(left_key, NUM_TERMS, BOND_DIM) + diag_shift * jnp.eye(BOND_DIM, dtype=jnp.float32)).astype(jnp.bfloat16)
    pair_ops = ((normal_sym(pair_key, NUM_TERMS, PAIR_DIM) + diag_shift * jnp.eye(PAIR_DIM, dtype=jnp.float32)) * NUM_TERMS ** -0.5).astype(jnp.bfloat16)
    right_env = normal_sym(right_key, NUM_TERMS, BOND_DIM).astype(jnp.bfloat16)
    full_term = draw_flags(flag_key)
    return {'wavefunction': wavefunction, 'left_env': left_env, 'pair_ops': pair_ops, 'right_env': right_env, 'full_term': full_term}


def apply_term(vec_bf, term_data):
    left_env, pair_op, right_env, flag_val = term_data
    flat_vec = vec_bf.reshape(BOND_DIM * PAIR_DIM, BOND_DIM)
    right_done = jnp.dot(flat_vec, right_env.T, preferred_element_type=jnp.float32).astype(jnp.bfloat16)
    right_done = jnp.where(flag_val == 1, right_done.reshape(BOND_DIM, PAIR_DIM, BOND_DIM), vec_bf)
    pair_in = right_done.transpose(1, 0, 2).reshape(PAIR_DIM, BOND_DIM * BOND_DIM)
    pair_done = jnp.dot(pair_op, pair_in, preferred_element_type=jnp.float32).astype(jnp.bfloat16)
    left_in = pair_done.reshape(PAIR_DIM, BOND_DIM, BOND_DIM).transpose(1, 0, 2).reshape(BOND_DIM, PAIR_DIM * BOND_DIM)
    return jnp.dot(left_env, left_in, preferred_element_type=jnp.float32).reshape(BOND_DIM, PAIR_DIM, BOND_DIM)


def apply_hamiltonian(vector, left_env, pair_ops, right_env, full_term):
    vec_bf = vector.astype(jnp.bfloat16)

    def add_term(running_sum, term_data):
        return running_sum + apply_term(vec_bf, term_data), None

    start_sum = jnp.zeros((BOND_DIM, PAIR_DIM, BOND_DIM), jnp.float32)
    total_sum, unused = lax.scan(add_term, start_sum, (left_env, pair_ops, right_env, full_term))
    return total_sum


def reference(wavefunction, left_env, pair_ops, right_env, full_term):
    first_vec = wavefunction / jnp.sqrt(jnp.sum(wavefunction * wavefunction) / VEC_SIZE)

    def lanczos_step(state_in, unused):
        current, previous, beta_prev = state_in
        sigma_vec = apply_hamiltonian(current, left_env, pair_ops, right_env, full_term)
        alpha_now = jnp.sum(sigma_vec * current) / VEC_SIZE
        residual = sigma_vec - alpha_now * current - beta_prev * previous
        beta_now = jnp.sqrt(jnp.sum(residual * residual) / VEC_SIZE)
        following = residual / beta_now
        return (following, current, beta_now), (following, alpha_now, beta_now)

    start_state = (first_vec, jnp.zeros_like(first_vec), jnp.zeros((), jnp.float32))
    final_state, outputs = lax.scan(lanczos_step, start_state, None, length=LANCZOS_STEPS)
    vectors, alpha_diag, beta_offdiag = outputs
    krylov = jnp.concatenate([first_vec[None], vectors], axis=0)
    return krylov, alpha_diag, beta_offdiag
```

```python
import functools

import jax
import jax.numpy as jnp
from jax import lax
from jax.experimental import pallas as pl
from jax.experimental.pallas import tpu as pltpu
from jax.sharding import PartitionSpec as P

LANCZOS_STEPS = 6
AXIS_NAME = 'terms'
MESH = pl.DeviceIdType.MESH

CHIPS = 16
CORES = 2
DEVS = 32
CHUNKS = 2
GROUPS = 4
TILE_PARTS = 4


class Dims:
    def __init__(self, bond, pair, terms_dev):
        self.bond = bond
        self.pair = pair
        self.terms_dev = terms_dev
        self.slab = bond // CHIPS
        self.sub = self.slab // 2
        self.half = bond // CORES
        self.chunk = self.half // CHUNKS
        self.rows = self.slab * pair
        self.prod = self.sub * pair
        self.out_rows = bond // DEVS
        self.group_terms = 4 * CORES * terms_dev
        self.vec_size = bond * pair * bond
        self.lane = min(bond, 128)
        self.lane_tiles = bond // self.lane


def lanczos_kernel(d, psi, left, right, wexp, out, info, lv, rv, wv, kw, uv, ps, yst, zst, sig, part, vcur, vprev, tbuf, gbuf, scs, scr, nbuf,
                   loc_sem, psi_sem, d2d_sem, d2d_recv, rw_send, rw_recv, fw_send, fw_recv, l_send, l_recv, u_send, u_recv,
                   p_send, p_recv, s_send, s_recv, k_send, k_recv, n_send, n_recv, o_sem):
    me = lax.axis_index(AXIS_NAME)
    core = me % 2
    xpos = (me // 2) % 2
    ypos = (me // 4) % 2
    zpos = me // 8

    def device(z, y, x, c):
        return ((z * 2 + y) * 2 + x) * 2 + c

    def chip_slot(z, y, x):
        return (x * 2 + y) * 4 + z

    partner = device(zpos, ypos, xpos, 1 - core)
    slot = chip_slot(zpos, ypos, xpos)
    zs = (zpos, zpos + 1 - 2 * (zpos % 2), (zpos + 2) % 4, 3 - zpos)
    y_two = ypos + (1 - core) * (1 - 2 * ypos)
    x_two = xpos + core * (1 - 2 * xpos)
    y_three = ypos + core * (1 - 2 * ypos)
    x_three = xpos + (1 - core) * (1 - 2 * xpos)
    two = device(zpos, y_two, x_two, core)
    three = device(zpos, y_three, x_three, core)

    def remote(src, dst, send, recv, dev):
        return pltpu.make_async_remote_copy(src_ref=src, dst_ref=dst, send_sem=send, recv_sem=recv, device_id=(dev,), device_id_type=MESH)

    class Gather:
        def __init__(self, block, send, recv):
            self.block, self.send_sem, self.recv_sem = block, send, recv

        def send(self, which, dev):
            remote(self.block(which), self.block(which), self.send_sem, self.recv_sem(which), dev).start()

        def wait(self, which):
            remote(self.block(which), self.block(which), self.send_sem, self.recv_sem(which), me).wait_recv()

        def own_along(self):
            for i in (1, 2, 3):
                self.send(slot, device(zs[i], ypos, xpos, core))

        def own_across(self):
            self.send(slot, three)
            self.send(slot, two)

        def event(self, n):
            i = (n + 1) // 2
            if n % 2:
                which = chip_slot(zs[i], ypos, xpos)
                self.wait(which)
                self.send(which, three)
                self.send(which, two)
            else:
                which = chip_slot(zs[i], y_two, x_two)
                self.wait(which)
                self.send(which, three)

        def last(self, diagonal):
            for i in range(4):
                self.wait(chip_slot(zs[i], 1 - ypos, 1 - xpos) if diagonal else chip_slot(zs[i], y_three, x_three))

    l_gather = Gather(lambda s: lv.at[:, s], l_send, lambda s: l_recv.at[s])

    def u_block(ch):
        return lambda s: uv.at[ch, :, pl.ds(pl.multiple_of(s * d.slab, d.slab), d.slab), :]

    u_gather = [Gather(u_block(ch), u_send.at[ch], lambda s, ch=ch: u_recv.at[ch, s]) for ch in range(CHUNKS)]

    for ch in range(CHUNKS):
        for h in range(2):
            mine = left.at[:, pl.ds(pl.multiple_of(core * d.half + ch * d.chunk, d.chunk), d.chunk),
                           pl.ds(pl.multiple_of((core + h) % 2 * d.half, d.half), d.half)]
            theirs = left.at[:, pl.ds(pl.multiple_of((1 - core) * d.half + ch * d.chunk, d.chunk), d.chunk),
                             pl.ds(pl.multiple_of((1 - core + h) % 2 * d.half, d.half), d.half)]
            remote(theirs, lv.at[ch, slot, core, :, h], d2d_sem.at[ch, h], d2d_recv.at[ch, h], partner).start()
            pltpu.make_async_copy(mine, lv.at[ch, slot, core, :, h], loc_sem.at[ch, h]).start()

    psi_rows = d.half * d.pair // 8
    psi_copies = [pltpu.make_async_copy(psi.at[pl.ds(pl.multiple_of(core * d.half * d.pair + n * psi_rows, psi_rows), psi_rows),
                                               pl.ds(c * d.lane, d.lane)],
                                        ps.at[c, pl.ds(n * psi_rows, psi_rows), :], psi_sem.at[n, c])
                  for n in range(8) for c in range(d.lane_tiles)]
    for copy in psi_copies:
        copy.start()

    def right_rows(s):
        return right.at[:, pl.ds(pl.multiple_of(s * d.slab, d.slab), d.slab), :]

    own_right = pltpu.make_async_copy(right_rows(slot), rv.at[slot, core], loc_sem.at[2, 0])
    own_pair = pltpu.make_async_copy(wexp, wv.at[slot, core], loc_sem.at[2, 1])
    own_right.start()
    own_pair.start()
    for n in range(1, CHIPS):
        chip = (me // 2 + n) % CHIPS
        to = chip_slot(chip // 4, chip // 2 % 2, chip % 2)
        remote(right_rows(to), rv.at[slot, core], rw_send.at[0], rw_recv.at[0], chip * 2 + core).start()
        remote(wexp, wv.at[slot, core], rw_send.at[1], rw_recv.at[1], chip * 2 + core).start()

    for ch in range(CHUNKS):
        for h in range(2):
            pltpu.make_async_copy(lv.at[ch, slot, core, :, h], lv.at[ch, slot, core, :, h], loc_sem.at[ch, h]).wait()
            back = remote(lv.at[ch, slot, 1 - core, :, h], lv.at[ch, slot, 1 - core, :, h], d2d_sem.at[ch, h], d2d_recv.at[ch, h], partner)
            back.wait_recv()
    l_gather.own_along()
    l_gather.own_across()

    total = jnp.zeros((8, d.lane), jnp.float32)
    for n in range(8):
        for copy in psi_copies[n * d.lane_tiles:(n + 1) * d.lane_tiles]:
            copy.wait()

        def add_rows(i, acc, n=n):
            x = ps[:, pl.ds(pl.multiple_of(n * psi_rows + i * (psi_rows // 8), 8), psi_rows // 8), :]
            return acc + jnp.sum((x * x).reshape(d.lane_tiles * psi_rows // 64, 8, d.lane), axis=0)

        total = lax.fori_loop(0, 8, add_rows, total)
    nbuf[0] = jnp.broadcast_to(jnp.sum(total, keepdims=True), (8, 128))
    to_partner = remote(nbuf.at[0], nbuf.at[1], n_send, n_recv, partner)
    to_partner.start()
    to_partner.wait()
    norm = jnp.sqrt((nbuf[0] + nbuf[1])[0:1, :] / d.vec_size)
    info[2] = jnp.broadcast_to(norm, (8, 128))
    norm_one = norm[:, 0:1]

    def place(q):
        tiles = [(ps[c, pl.ds(q, d.half, stride=d.pair), :] / norm_one).T for c in range(d.lane_tiles)]
        xt = jnp.concatenate(tiles, axis=0)
        vprev[...] = xt
        return xt.astype(jnp.bfloat16)

    def start_vector(qb, carry):
        for q2 in range(2):
            q = qb * 2 + q2
            xb = place(q)
            for ch in range(CHUNKS):
                uv[ch, qb, :, q2 * d.chunk:(q2 + 1) * d.chunk] = xb[:, ch * d.chunk:(ch + 1) * d.chunk]
            for bh in range(2):
                rows = vprev[pl.ds(pl.multiple_of(slot * d.slab + bh * d.sub, d.sub), d.sub), :]
                vcur[pl.ds(pl.multiple_of((bh * d.pair + q) * d.sub, d.sub), d.sub), :] = rows
        return carry

    lax.fori_loop(0, d.pair // 4, start_vector, 0)
    own_right.wait()
    own_pair.wait()
    fifteen = rv.at[pl.ds(0, CHIPS - 1), 0]
    fifteen_w = wv.at[pl.ds(0, CHIPS - 1), 0]
    remote(fifteen, fifteen, rw_send.at[0], rw_recv.at[0], me).wait()
    remote(fifteen_w, fifteen_w, rw_send.at[1], rw_recv.at[1], me).wait()
    fw_right = remote(rv.at[:, core], rv.at[:, core], fw_send.at[0], fw_recv.at[0], partner)
    fw_pair = remote(wv.at[:, core], wv.at[:, core], fw_send.at[1], fw_recv.at[1], partner)
    fw_right.start()
    fw_pair.start()
    l_gather.event(0)
    l_gather.event(1)
    lax.fori_loop(d.pair // 4, d.pair // 2, start_vector, 0)
    l_gather.event(2)
    l_gather.event(3)
    fw_right.wait()
    fw_pair.wait()
    lane = lax.broadcasted_iota(jnp.int32, (d.sub, d.prod), 1)
    row = lax.broadcasted_iota(jnp.int32, (d.sub, d.prod), 0)
    diagonal = lane % d.sub == row

    def spread_pair(s, carry):
        for c in range(2):
            for t in range(d.terms_dev):
                w = wv[s, c, t].astype(jnp.float32)
                for q in range(d.pair):
                    full = jnp.where(diagonal, jnp.broadcast_to(w[q:q + 1, :], (d.sub, d.prod)), 0.0)
                    kw[s, c, t, q * d.sub:(q + 1) * d.sub, :] = full.astype(jnp.bfloat16)
        return carry

    lax.fori_loop(0, CHIPS, spread_pair, 0)
    l_gather.event(4)
    l_gather.event(5)
    l_gather.event(6)
    vprev[...] = jnp.zeros_like(vprev)

    def products(ch, grp, is_last):
        r_all = rv[pl.ds(grp * 4, 4)].reshape(d.group_terms * d.slab, d.bond)
        for qb in range(d.pair // 2):
            y = jnp.dot(r_all, uv[ch, qb], preferred_element_type=jnp.float32).astype(jnp.bfloat16)
            y = y.reshape(d.group_terms, 2, d.sub, 2 * d.chunk)
            for q2 in range(2):
                q = qb * 2 + q2
                for bh in range(2):
                    yst[:, q * d.sub:(q + 1) * d.sub, bh * d.chunk:(bh + 1) * d.chunk] = y[:, bh, :, q2 * d.chunk:(q2 + 1) * d.chunk]
        for k in range(d.group_terms):
            w = kw[grp * 4 + k // 4, k // 2 % 2, k % 2]
            z = jnp.dot(w, yst[k], preferred_element_type=jnp.float32).astype(jnp.bfloat16)
            for bh in range(2):
                zst[bh * d.prod:(bh + 1) * d.prod, k * d.chunk:(k + 1) * d.chunk] = z[:, bh * d.chunk:(bh + 1) * d.chunk]
        for h in (1, 0):
            l_all = lv[ch, pl.ds(grp * 4, 4), :, :, h].reshape(d.group_terms * d.chunk, d.half)
            sig[h] += jnp.dot(zst[...], l_all, preferred_element_type=jnp.float32)
            if h == 1:
                @pl.when(is_last)
                def _():
                    remote(sig.at[1], part, p_send, p_recv, partner).start()

    def step(j, beta_prev):
        later = jnp.minimum(j, 1)

        @pl.when(j > 0)
        def _():
            for n in range(7):
                u_gather[0].event(n)
            u_gather[1].own_across()
            for n in range(4):
                u_gather[1].event(n)
            u_gather[0].last(False)
            u_gather[0].last(True)

        sig[...] = jnp.zeros_like(sig)

        def part_step(it, carry):
            ch = (1 - later) * (it % 2) + later * (it // 4)
            n = (1 - later) * (it // 2) + later * (it % 4)
            own = xpos * 2 + ypos
            arrive = jnp.where(n == 0, own, jnp.where(n == 1, x_two * 2 + y_two, jnp.where(n == 2, x_three * 2 + y_three, 3 - own)))
            grp = (1 - later) * arrive + later * n

            @pl.when((j == 0) & (it == 4))
            def _():
                l_gather.last(False)

            @pl.when((j == 0) & (it == 6))
            def _():
                l_gather.last(True)

            for at in range(3):
                @pl.when((j > 0) & (it == at))
                def _():
                    u_gather[1].event(4 + at)

            @pl.when((j > 0) & (it == 4))
            def _():
                u_gather[1].last(False)
                u_gather[1].last(True)

            products(ch, grp, it == 7)
            return carry

        lax.fori_loop(0, 2 * GROUPS, part_step, 0)

        @pl.when(j > 0)
        def _():
            for ch in range(CHUNKS):
                sent = uv.at[ch, :, pl.ds(0, 15 * d.slab), :]
                remote(sent, sent, u_send.at[ch], u_recv.at[ch, 0], me).wait_send()

        remote(sig.at[1], part, p_send, p_recv, partner).wait()
        s = sig[0] + part[...]
        v = vcur[...]
        w = s - beta_prev * vprev[...]
        sv = jnp.sum(s * v, keepdims=True)
        wv_sum = jnp.sum(w * v, keepdims=True)
        vv = jnp.sum(v * v, keepdims=True)
        guess = jnp.where(vv > 0.0, wv_sum / jnp.where(vv > 0.0, vv, 1.0), 0.0)
        t = w - guess * v
        sig[0] = t
        tt = jnp.sum(t * t, keepdims=True)
        tv = jnp.sum(t * v, keepdims=True)
        tile_row = lax.broadcasted_iota(jnp.int32, (8, 128), 0)
        tile = jnp.zeros((8, 128), jnp.float32)
        for n, value in enumerate((sv, vv, tt, tv, guess)):
            tile = jnp.where(tile_row == n, value, tile)
        scs[...] = tile
        scr[me] = tile

        def tell(n, carry):
            remote(scs, scr.at[me], s_send, s_recv, (me + n) % DEVS).start()
            return carry

        lax.fori_loop(1, DEVS, tell, 0)
        heard = scr.at[pl.ds(0, DEVS - 1)]
        remote(heard, heard, s_send, s_recv, me).wait()
        alpha = jnp.sum(scr[:, 0, :], axis=0, keepdims=True) / d.vec_size
        off = alpha - scr[:, 4, :]
        square = scr[:, 2, :] - 2.0 * off * scr[:, 3, :] + off * off * scr[:, 1, :]
        beta = jnp.sqrt(jnp.sum(square, axis=0, keepdims=True) / d.vec_size)
        info[0, pl.ds(j, 1), :] = alpha
        info[1, pl.ds(j, 1), :] = beta
        vnew = (sig[0] - (alpha[:, 0:1] - guess) * vcur[...]) / beta[:, 0:1]
        vprev[...] = vcur[...]
        vcur[...] = vnew
        vb = vnew.astype(jnp.bfloat16)

        @pl.when(j < LANCZOS_STEPS - 1)
        def _():
            for ch in range(CHUNKS):
                for bh in range(2):
                    at = pl.ds(pl.multiple_of(slot * d.slab + bh * d.sub, d.sub), d.sub)
                    for q in range(d.pair):
                        uv[ch, q // 2, at, q % 2 * d.chunk:(q % 2 + 1) * d.chunk] = \
                            vb[(bh * d.pair + q) * d.sub:(bh * d.pair + q + 1) * d.sub, ch * d.chunk:(ch + 1) * d.chunk]
            u_gather[0].own_along()
            u_gather[0].own_across()
            u_gather[1].own_along()

        wide = TILE_PARTS * d.slab
        for n in range(d.pair // TILE_PARTS):
            rows = [vcur[(bh * d.pair + q) * d.sub:(bh * d.pair + q + 1) * d.sub, :]
                    for q in range(n * TILE_PARTS, (n + 1) * TILE_PARTS) for bh in range(2)]
            tbuf[j, :, n * wide:(n + 1) * wide] = jnp.concatenate(rows, axis=0).T

        def hand_out(n, carry):
            to = core * CHIPS + n
            block = tbuf.at[j, pl.ds(pl.multiple_of(n * d.out_rows, d.out_rows), d.out_rows), :]

            @pl.when(to != me)
            def _():
                remote(block, gbuf.at[j, slot], k_send, k_recv, to).start()

            @pl.when(to == me)
            def _():
                gbuf[j, slot] = block[...]
            return carry

        lax.fori_loop(0, CHIPS, hand_out, 0)
        return beta[:, 0:1]

    lax.fori_loop(0, LANCZOS_STEPS, step, jnp.zeros((1, 1), jnp.float32))

    fourteen = lv.at[:, pl.ds(0, 15)]
    remote(fourteen, fourteen, l_send, l_recv.at[0], me).wait_send()
    for ch in range(CHUNKS):
        for h in range(2):
            theirs = left.at[:, pl.ds(0, d.chunk), pl.ds(0, d.half)]
            remote(theirs, lv.at[ch, slot, core, :, h], d2d_sem.at[ch, h], d2d_recv.at[ch, h], partner).wait_send()

    sends_self = me // CHIPS == core

    @pl.when(sends_self)
    def _():
        some = gbuf.at[:, pl.ds(0, CHIPS - 1)]
        remote(some, some, k_send, k_recv, me).wait()

    @pl.when(jnp.logical_not(sends_self))
    def _():
        remote(gbuf, gbuf, k_send, k_recv, me).wait()

    wide = TILE_PARTS * d.slab
    lanes = lax.broadcasted_iota(jnp.int32, (d.out_rows, wide), 1) // d.slab

    def put_out(j, carry):
        for ct in range(CHIPS // TILE_PARTS):
            for qt in range(d.pair // TILE_PARTS):
                src = [gbuf[j, ct * TILE_PARTS + c, :, qt * wide:(qt + 1) * wide] for c in range(TILE_PARTS)]
                for q in range(TILE_PARTS):
                    tile = jnp.zeros((d.out_rows, wide), jnp.float32)
                    for c in range(TILE_PARTS):
                        shift = (c - q) % TILE_PARTS * d.slab
                        moved = pltpu.roll(src[c], shift, 1) if shift else src[c]
                        tile = jnp.where(lanes == c, moved, tile)
                    at = (qt * TILE_PARTS + q) * d.out_rows
                    tbuf[j, at:at + d.out_rows, ct * wide:(ct + 1) * wide] = tile
        pltpu.make_async_copy(tbuf.at[j], out.at[j], o_sem).start()
        return carry

    lax.fori_loop(0, LANCZOS_STEPS, put_out, 0)
    pltpu.make_async_copy(tbuf, out, o_sem).wait()


def solution(mesh):
    def device_body(wavefunction, left_loc, pair_loc, right_loc, flag_loc):
        bond, pair = wavefunction.shape[0], wavefunction.shape[1]
        d = Dims(bond, pair, left_loc.shape[0])
        eye = jnp.eye(bond, dtype=jnp.bfloat16)
        right_used = jnp.where((flag_loc == 1)[:, None, None], right_loc, eye)
        pair_wide = jnp.repeat(pair_loc, d.sub, axis=2)
        bf16, f32 = jnp.bfloat16, jnp.float32
        dma = pltpu.SemaphoreType.DMA
        any_space = pl.BlockSpec(memory_space=pl.ANY)
        rows_out, info = pl.pallas_call(
            functools.partial(lanczos_kernel, d),
            out_shape=(jax.ShapeDtypeStruct((LANCZOS_STEPS, d.half, bond), f32), jax.ShapeDtypeStruct((3, 8, 128), f32)),
            in_specs=[any_space] * 4,
            out_specs=(any_space, pl.BlockSpec(memory_space=pltpu.VMEM)),
            scratch_shapes=[
                pltpu.VMEM((CHUNKS, CHIPS, CORES, d.terms_dev, 2, d.chunk, d.half), bf16),
                pltpu.VMEM((CHIPS, CORES, d.terms_dev, d.slab, bond), bf16),
                pltpu.VMEM((CHIPS, CORES, d.terms_dev, pair, d.prod), bf16),
                pltpu.VMEM((CHIPS, CORES, d.terms_dev, d.prod, d.prod), bf16),
                pltpu.VMEM((CHUNKS, pair // 2, bond, 2 * d.chunk), bf16),
                pltpu.VMEM((d.lane_tiles, d.half * pair, d.lane), f32),
                pltpu.VMEM((d.group_terms, d.prod, 2 * d.chunk), bf16),
                pltpu.VMEM((d.rows, d.group_terms * d.chunk), bf16),
                pltpu.VMEM((2, d.rows, d.half), f32),
                pltpu.VMEM((d.rows, d.half), f32),
                pltpu.VMEM((d.rows, d.half), f32),
                pltpu.VMEM((d.rows, d.half), f32),
                pltpu.VMEM((LANCZOS_STEPS, d.half, bond), f32),
                pltpu.VMEM((LANCZOS_STEPS, CHIPS, d.out_rows, bond), f32),
                pltpu.VMEM((8, 128), f32),
                pltpu.VMEM((DEVS, 8, 128), f32),
                pltpu.VMEM((2, 8, 128), f32),
                dma((3, 2)), dma((8, d.lane_tiles)), dma((CHUNKS, 2)), dma((CHUNKS, 2)), dma((2,)), dma((2,)), dma((2,)), dma((2,)),
                dma, dma((CHIPS,)), dma((CHUNKS,)), dma((CHUNKS, CHIPS)),
                dma, dma, dma, dma, dma, dma, dma, dma, dma,
            ],
            compiler_params=pltpu.CompilerParams(has_side_effects=True, vmem_limit_bytes=67043328),
            name='lanczos',
        )(wavefunction.reshape(bond * pair, bond), left_loc, right_used, pair_wide)
        row_start = lax.axis_index(AXIS_NAME) * d.out_rows
        first = lax.dynamic_slice_in_dim(wavefunction, row_start, d.out_rows, axis=0) / info[2, 0, 0]
        later = rows_out.reshape(LANCZOS_STEPS, pair, d.out_rows, bond).transpose(0, 2, 1, 3)
        return jnp.concatenate([first[None], later]), info[0, :LANCZOS_STEPS, 0], info[1, :LANCZOS_STEPS, 0]

    return jax.shard_map(device_body, mesh=mesh, in_specs=(P(), P(AXIS_NAME), P(AXIS_NAME), P(AXIS_NAME), P(AXIS_NAME)),
                         out_specs=(P(None, AXIS_NAME), P(), P()), check_vma=False)
```

```python
import functools

import jax
import jax.numpy as jnp
from jax import lax
from jax.experimental import pallas as pl
from jax.experimental.pallas import tpu as pltpu
from jax.sharding import PartitionSpec as P

LANCZOS_STEPS = 6
AXIS_NAME = 'terms'
MESH = pl.DeviceIdType.MESH

CHIPS = 16
CORES = 2
DEVS = 32
CHUNKS = 2
GROUPS = 4
TILE_PARTS = 4


class Dims:
    def __init__(self, bond, pair, terms_dev):
        self.bond = bond
        self.pair = pair
        self.terms_dev = terms_dev
        self.slab = bond // CHIPS
        self.sub = self.slab // 2
        self.half = bond // CORES
        self.chunk = self.half // CHUNKS
        self.rows = self.slab * pair
        self.prod = self.sub * pair
        self.out_rows = bond // DEVS
        self.group_terms = 4 * CORES * terms_dev
        self.vec_size = bond * pair * bond
        self.lane = min(bond, 128)
        self.lane_tiles = bond // self.lane


def lanczos_kernel(d, psi, left, right, wexp, out, info, lv, rv, wv, kw, uv, ps, yst, zst, sig, part, vcur, vprev, tbuf, gbuf, scs, scr, nbuf,
                   loc_sem, psi_sem, d2d_sem, d2d_recv, rw_send, rw_recv, fw_send, fw_recv, l_send, l_recv, u_send, u_recv,
                   p_send, p_recv, s_send, s_recv, k_send, k_recv, n_send, n_recv, o_sem):
    me = lax.axis_index(AXIS_NAME)
    core = me % 2
    xpos = (me // 2) % 2
    ypos = (me // 4) % 2
    zpos = me // 8

    def device(z, y, x, c):
        return ((z * 2 + y) * 2 + x) * 2 + c

    def chip_slot(z, y, x):
        return (x * 2 + y) * 4 + z

    partner = device(zpos, ypos, xpos, 1 - core)
    slot = chip_slot(zpos, ypos, xpos)
    zs = (zpos, zpos + 1 - 2 * (zpos % 2), (zpos + 2) % 4, 3 - zpos)
    y_two = ypos + (1 - core) * (1 - 2 * ypos)
    x_two = xpos + core * (1 - 2 * xpos)
    y_three = ypos + core * (1 - 2 * ypos)
    x_three = xpos + (1 - core) * (1 - 2 * xpos)
    two = device(zpos, y_two, x_two, core)
    three = device(zpos, y_three, x_three, core)

    def remote(src, dst, send, recv, dev):
        return pltpu.make_async_remote_copy(src_ref=src, dst_ref=dst, send_sem=send, recv_sem=recv, device_id=(dev,), device_id_type=MESH)

    class Gather:
        def __init__(self, block, send, recv):
            self.block, self.send_sem, self.recv_sem = block, send, recv

        def send(self, which, dev):
            remote(self.block(which), self.block(which), self.send_sem, self.recv_sem(which), dev).start()

        def wait(self, which):
            remote(self.block(which), self.block(which), self.send_sem, self.recv_sem(which), me).wait_recv()

        def own_along(self):
            for i in (1, 2, 3):
                self.send(slot, device(zs[i], ypos, xpos, core))

        def own_across(self):
            self.send(slot, three)
            self.send(slot, two)

        def event(self, n):
            i = (n + 1) // 2
            if n % 2:
                which = chip_slot(zs[i], ypos, xpos)
                self.wait(which)
                self.send(which, three)
                self.send(which, two)
            else:
                which = chip_slot(zs[i], y_two, x_two)
                self.wait(which)
                self.send(which, three)

        def last(self, diagonal):
            for i in range(4):
                self.wait(chip_slot(zs[i], 1 - ypos, 1 - xpos) if diagonal else chip_slot(zs[i], y_three, x_three))

    l_gather = Gather(lambda s: lv.at[:, s], l_send, lambda s: l_recv.at[s])

    def u_block(ch):
        return lambda s: uv.at[ch, :, pl.ds(pl.multiple_of(s * d.slab, d.slab), d.slab), :]

    u_gather = [Gather(u_block(ch), u_send.at[ch], lambda s, ch=ch: u_recv.at[ch, s]) for ch in range(CHUNKS)]

    for ch in range(CHUNKS):
        for h in range(2):
            mine = left.at[:, pl.ds(pl.multiple_of(core * d.half + ch * d.chunk, d.chunk), d.chunk),
                           pl.ds(pl.multiple_of((core + h) % 2 * d.half, d.half), d.half)]
            theirs = left.at[:, pl.ds(pl.multiple_of((1 - core) * d.half + ch * d.chunk, d.chunk), d.chunk),
                             pl.ds(pl.multiple_of((1 - core + h) % 2 * d.half, d.half), d.half)]
            remote(theirs, lv.at[ch, slot, core, :, :, pl.ds(h * d.half, d.half)], d2d_sem.at[ch, h], d2d_recv.at[ch, h], partner).start()
            pltpu.make_async_copy(mine, lv.at[ch, slot, core, :, :, pl.ds(h * d.half, d.half)], loc_sem.at[ch, h]).start()

    psi_rows = d.half * d.pair // 8
    psi_copies = [pltpu.make_async_copy(psi.at[pl.ds(pl.multiple_of(core * d.half * d.pair + n * psi_rows, psi_rows), psi_rows),
                                               pl.ds(c * d.lane, d.lane)],
                                        ps.at[c, pl.ds(n * psi_rows, psi_rows), :], psi_sem.at[n, c])
                  for n in range(8) for c in range(d.lane_tiles)]
    for copy in psi_copies:
        copy.start()

    def right_rows(s):
        return right.at[:, pl.ds(pl.multiple_of(s * d.slab, d.slab), d.slab), :]

    own_right = pltpu.make_async_copy(right_rows(slot), rv.at[slot, core], loc_sem.at[2, 0])
    own_pair = pltpu.make_async_copy(wexp, wv.at[slot, core], loc_sem.at[2, 1])
    own_right.start()
    own_pair.start()
    for n in range(1, CHIPS):
        chip = (me // 2 + n) % CHIPS
        to = chip_slot(chip // 4, chip // 2 % 2, chip % 2)
        remote(right_rows(to), rv.at[slot, core], rw_send.at[0], rw_recv.at[0], chip * 2 + core).start()
        remote(wexp, wv.at[slot, core], rw_send.at[1], rw_recv.at[1], chip * 2 + core).start()

    for ch in range(CHUNKS):
        for h in range(2):
            pltpu.make_async_copy(lv.at[ch, slot, core, :, :, pl.ds(h * d.half, d.half)], lv.at[ch, slot, core, :, :, pl.ds(h * d.half, d.half)], loc_sem.at[ch, h]).wait()
            back = remote(lv.at[ch, slot, 1 - core, :, :, pl.ds(h * d.half, d.half)], lv.at[ch, slot, 1 - core, :, :, pl.ds(h * d.half, d.half)], d2d_sem.at[ch, h], d2d_recv.at[ch, h], partner)
            back.wait_recv()
    l_gather.own_along()
    l_gather.own_across()

    total = jnp.zeros((8, d.lane), jnp.float32)
    for n in range(8):
        for copy in psi_copies[n * d.lane_tiles:(n + 1) * d.lane_tiles]:
            copy.wait()

        def add_rows(i, acc, n=n):
            x = ps[:, pl.ds(pl.multiple_of(n * psi_rows + i * (psi_rows // 8), 8), psi_rows // 8), :]
            return acc + jnp.sum((x * x).reshape(d.lane_tiles * psi_rows // 64, 8, d.lane), axis=0)

        total = lax.fori_loop(0, 8, add_rows, total)
    nbuf[0] = jnp.broadcast_to(jnp.sum(total, keepdims=True), (8, 128))
    to_partner = remote(nbuf.at[0], nbuf.at[1], n_send, n_recv, partner)
    to_partner.start()
    to_partner.wait()
    norm = jnp.sqrt((nbuf[0] + nbuf[1])[0:1, :] / d.vec_size)
    info[2] = jnp.broadcast_to(norm, (8, 128))
    norm_one = norm[:, 0:1]

    def place(q):
        tiles = [(ps[c, pl.ds(q, d.half, stride=d.pair), :] / norm_one).T for c in range(d.lane_tiles)]
        xt = jnp.concatenate(tiles, axis=0)
        vprev[...] = xt
        return xt.astype(jnp.bfloat16)

    def start_vector(qb, carry):
        for q2 in range(2):
            q = qb * 2 + q2
            xb = place(q)
            for ch in range(CHUNKS):
                uv[ch, qb, :, q2 * d.chunk:(q2 + 1) * d.chunk] = xb[:, ch * d.chunk:(ch + 1) * d.chunk]
            for bh in range(2):
                rows = vprev[pl.ds(pl.multiple_of(slot * d.slab + bh * d.sub, d.sub), d.sub), :]
                vcur[pl.ds(pl.multiple_of((bh * d.pair + q) * d.sub, d.sub), d.sub), :] = rows
        return carry

    lax.fori_loop(0, d.pair // 4, start_vector, 0)
    own_right.wait()
    own_pair.wait()
    fifteen = rv.at[pl.ds(0, CHIPS - 1), 0]
    fifteen_w = wv.at[pl.ds(0, CHIPS - 1), 0]
    remote(fifteen, fifteen, rw_send.at[0], rw_recv.at[0], me).wait()
    remote(fifteen_w, fifteen_w, rw_send.at[1], rw_recv.at[1], me).wait()
    fw_right = remote(rv.at[:, core], rv.at[:, core], fw_send.at[0], fw_recv.at[0], partner)
    fw_pair = remote(wv.at[:, core], wv.at[:, core], fw_send.at[1], fw_recv.at[1], partner)
    fw_right.start()
    fw_pair.start()
    l_gather.event(0)
    l_gather.event(1)
    lax.fori_loop(d.pair // 4, d.pair // 2, start_vector, 0)
    l_gather.event(2)
    l_gather.event(3)
    fw_right.wait()
    fw_pair.wait()
    lane = lax.broadcasted_iota(jnp.int32, (d.sub, d.prod), 1)
    row = lax.broadcasted_iota(jnp.int32, (d.sub, d.prod), 0)
    diagonal = lane % d.sub == row

    def spread_pair(s, carry):
        for c in range(2):
            for t in range(d.terms_dev):
                w = wv[s, c, t].astype(jnp.float32)
                for q in range(d.pair):
                    full = jnp.where(diagonal, jnp.broadcast_to(w[q:q + 1, :], (d.sub, d.prod)), 0.0)
                    kw[s, c, t, q * d.sub:(q + 1) * d.sub, :] = full.astype(jnp.bfloat16)
        return carry

    lax.fori_loop(0, CHIPS, spread_pair, 0)
    l_gather.event(4)
    l_gather.event(5)
    l_gather.event(6)
    vprev[...] = jnp.zeros_like(vprev)

    def products(ch, grp):
        r_all = rv[pl.ds(grp * 4, 4)].reshape(d.group_terms * d.slab, d.bond)
        for qb in range(d.pair // 2):
            y = jnp.dot(r_all, uv[ch, qb], preferred_element_type=jnp.float32).astype(jnp.bfloat16)
            y = y.reshape(d.group_terms, 2, d.sub, 2 * d.chunk)
            for q2 in range(2):
                q = qb * 2 + q2
                for bh in range(2):
                    yst[:, q * d.sub:(q + 1) * d.sub, bh * d.chunk:(bh + 1) * d.chunk] = y[:, bh, :, q2 * d.chunk:(q2 + 1) * d.chunk]
        for k in range(d.group_terms):
            w = kw[grp * 4 + k // 4, k // 2 % 2, k % 2]
            z = jnp.dot(w, yst[k], preferred_element_type=jnp.float32).astype(jnp.bfloat16)
            for bh in range(2):
                zst[bh * d.prod:(bh + 1) * d.prod, k * d.chunk:(k + 1) * d.chunk] = z[:, bh * d.chunk:(bh + 1) * d.chunk]
        l_all = lv[ch, pl.ds(grp * 4, 4)].reshape(d.group_terms * d.chunk, d.bond)
        sig[...] += jnp.dot(zst[...], l_all, preferred_element_type=jnp.float32)

    def hand_out(j):
        def one(n, carry):
            to = core * CHIPS + n
            block = tbuf.at[j, pl.ds(pl.multiple_of(n * d.out_rows, d.out_rows), d.out_rows), :]

            @pl.when(to != me)
            def _():
                remote(block, gbuf.at[j, slot], k_send, k_recv, to).start()

            @pl.when(to == me)
            def _():
                gbuf[j, slot] = block[...]
            return carry

        lax.fori_loop(0, CHIPS, one, 0)

    def step(j, beta_prev):
        later = jnp.minimum(j, 1)

        @pl.when(j > 0)
        def _():
            for n in range(7):
                u_gather[0].event(n)
            u_gather[1].own_across()
            for n in range(4):
                u_gather[1].event(n)
            u_gather[0].last(False)
            u_gather[0].last(True)

        sig[...] = jnp.zeros_like(sig)

        def part_step(it, carry):
            ch = (1 - later) * (it % 2) + later * (it // 4)
            n = (1 - later) * (it // 2) + later * (it % 4)
            own = xpos * 2 + ypos
            arrive = jnp.where(n == 0, own, jnp.where(n == 1, x_two * 2 + y_two, jnp.where(n == 2, x_three * 2 + y_three, 3 - own)))
            grp = (1 - later) * arrive + later * n

            @pl.when((j == 0) & (it == 4))
            def _():
                l_gather.last(False)

            @pl.when((j == 0) & (it == 6))
            def _():
                l_gather.last(True)

            for at in range(3):
                @pl.when((j > 0) & (it == at))
                def _():
                    u_gather[1].event(4 + at)

            @pl.when((j > 0) & (it == 4))
            def _():
                u_gather[1].last(False)
                u_gather[1].last(True)
                hand_out(j - 1)

            products(ch, grp)
            return carry

        lax.fori_loop(0, 2 * GROUPS, part_step, 0)

        @pl.when(j > 0)
        def _():
            for ch in range(CHUNKS):
                sent = uv.at[ch, :, pl.ds(0, 15 * d.slab), :]
                remote(sent, sent, u_send.at[ch], u_recv.at[ch, 0], me).wait_send()

        other = sig.at[:, pl.ds(d.half, d.half)]
        to_other = remote(other, part, p_send, p_recv, partner)
        to_other.start()
        to_other.wait()
        s = sig[:, :d.half] + part[...]
        v = vcur[...]
        w = s - beta_prev * vprev[...]
        sv = jnp.sum(s * v, keepdims=True)
        wv_sum = jnp.sum(w * v, keepdims=True)
        vv = jnp.sum(v * v, keepdims=True)
        guess = jnp.where(vv > 0.0, wv_sum / jnp.where(vv > 0.0, vv, 1.0), 0.0)
        t = w - guess * v
        sig[:, :d.half] = t
        tt = jnp.sum(t * t, keepdims=True)
        tv = jnp.sum(t * v, keepdims=True)
        tile_row = lax.broadcasted_iota(jnp.int32, (8, 128), 0)
        tile = jnp.zeros((8, 128), jnp.float32)
        for n, value in enumerate((sv, vv, tt, tv, guess)):
            tile = jnp.where(tile_row == n, value, tile)
        scs[...] = tile
        scr[me] = tile

        def tell(n, carry):
            remote(scs, scr.at[me], s_send, s_recv, (me + n) % DEVS).start()
            return carry

        lax.fori_loop(1, DEVS, tell, 0)
        heard = scr.at[pl.ds(0, DEVS - 1)]
        remote(heard, heard, s_send, s_recv, me).wait()
        alpha = jnp.sum(scr[:, 0, :], axis=0, keepdims=True) / d.vec_size
        off = alpha - scr[:, 4, :]
        square = scr[:, 2, :] - 2.0 * off * scr[:, 3, :] + off * off * scr[:, 1, :]
        beta = jnp.sqrt(jnp.sum(square, axis=0, keepdims=True) / d.vec_size)
        info[0, pl.ds(j, 1), :] = alpha
        info[1, pl.ds(j, 1), :] = beta
        vnew = (sig[:, :d.half] - (alpha[:, 0:1] - guess) * vcur[...]) / beta[:, 0:1]
        vprev[...] = vcur[...]
        vcur[...] = vnew
        vb = vnew.astype(jnp.bfloat16)

        @pl.when(j < LANCZOS_STEPS - 1)
        def _():
            for ch in range(CHUNKS):
                for bh in range(2):
                    at = pl.ds(pl.multiple_of(slot * d.slab + bh * d.sub, d.sub), d.sub)
                    for q in range(d.pair):
                        uv[ch, q // 2, at, q % 2 * d.chunk:(q % 2 + 1) * d.chunk] = \
                            vb[(bh * d.pair + q) * d.sub:(bh * d.pair + q + 1) * d.sub, ch * d.chunk:(ch + 1) * d.chunk]
            u_gather[0].own_along()
            u_gather[0].own_across()
            u_gather[1].own_along()

        wide = TILE_PARTS * d.slab
        for n in range(d.pair // TILE_PARTS):
            rows = [vcur[(bh * d.pair + q) * d.sub:(bh * d.pair + q + 1) * d.sub, :]
                    for q in range(n * TILE_PARTS, (n + 1) * TILE_PARTS) for bh in range(2)]
            tbuf[j, :, n * wide:(n + 1) * wide] = jnp.concatenate(rows, axis=0).T

        return beta[:, 0:1]

    lax.fori_loop(0, LANCZOS_STEPS, step, jnp.zeros((1, 1), jnp.float32))

    hand_out(LANCZOS_STEPS - 1)
    fourteen = lv.at[:, pl.ds(0, 15)]
    remote(fourteen, fourteen, l_send, l_recv.at[0], me).wait_send()
    for ch in range(CHUNKS):
        for h in range(2):
            theirs = left.at[:, pl.ds(0, d.chunk), pl.ds(0, d.half)]
            remote(theirs, lv.at[ch, slot, core, :, :, pl.ds(h * d.half, d.half)], d2d_sem.at[ch, h], d2d_recv.at[ch, h], partner).wait_send()

    sends_self = me // CHIPS == core

    @pl.when(sends_self)
    def _():
        some = gbuf.at[:, pl.ds(0, CHIPS - 1)]
        remote(some, some, k_send, k_recv, me).wait()

    @pl.when(jnp.logical_not(sends_self))
    def _():
        remote(gbuf, gbuf, k_send, k_recv, me).wait()

    wide = TILE_PARTS * d.slab
    lanes = lax.broadcasted_iota(jnp.int32, (d.out_rows, wide), 1) // d.slab

    def put_out(j, carry):
        for ct in range(CHIPS // TILE_PARTS):
            for qt in range(d.pair // TILE_PARTS):
                src = [gbuf[j, ct * TILE_PARTS + c, :, qt * wide:(qt + 1) * wide] for c in range(TILE_PARTS)]
                for q in range(TILE_PARTS):
                    tile = jnp.zeros((d.out_rows, wide), jnp.float32)
                    for c in range(TILE_PARTS):
                        shift = (c - q) % TILE_PARTS * d.slab
                        moved = pltpu.roll(src[c], shift, 1) if shift else src[c]
                        tile = jnp.where(lanes == c, moved, tile)
                    at = (qt * TILE_PARTS + q) * d.out_rows
                    tbuf[j, at:at + d.out_rows, ct * wide:(ct + 1) * wide] = tile
        pltpu.make_async_copy(tbuf.at[j], out.at[j], o_sem).start()
        return carry

    lax.fori_loop(0, LANCZOS_STEPS, put_out, 0)
    pltpu.make_async_copy(tbuf, out, o_sem).wait()


def solution(mesh):
    def device_body(wavefunction, left_loc, pair_loc, right_loc, flag_loc):
        bond, pair = wavefunction.shape[0], wavefunction.shape[1]
        d = Dims(bond, pair, left_loc.shape[0])
        eye = jnp.eye(bond, dtype=jnp.bfloat16)
        right_used = jnp.where((flag_loc == 1)[:, None, None], right_loc, eye)
        pair_wide = jnp.repeat(pair_loc, d.sub, axis=2)
        bf16, f32 = jnp.bfloat16, jnp.float32
        dma = pltpu.SemaphoreType.DMA
        any_space = pl.BlockSpec(memory_space=pl.ANY)
        rows_out, info = pl.pallas_call(
            functools.partial(lanczos_kernel, d),
            out_shape=(jax.ShapeDtypeStruct((LANCZOS_STEPS, d.half, bond), f32), jax.ShapeDtypeStruct((3, 8, 128), f32)),
            in_specs=[any_space] * 4,
            out_specs=(any_space, pl.BlockSpec(memory_space=pltpu.VMEM)),
            scratch_shapes=[
                pltpu.VMEM((CHUNKS, CHIPS, CORES, d.terms_dev, d.chunk, bond), bf16),
                pltpu.VMEM((CHIPS, CORES, d.terms_dev, d.slab, bond), bf16),
                pltpu.VMEM((CHIPS, CORES, d.terms_dev, pair, d.prod), bf16),
                pltpu.VMEM((CHIPS, CORES, d.terms_dev, d.prod, d.prod), bf16),
                pltpu.VMEM((CHUNKS, pair // 2, bond, 2 * d.chunk), bf16),
                pltpu.VMEM((d.lane_tiles, d.half * pair, d.lane), f32),
                pltpu.VMEM((d.group_terms, d.prod, 2 * d.chunk), bf16),
                pltpu.VMEM((d.rows, d.group_terms * d.chunk), bf16),
                pltpu.VMEM((d.rows, bond), f32),
                pltpu.VMEM((d.rows, d.half), f32),
                pltpu.VMEM((d.rows, d.half), f32),
                pltpu.VMEM((d.rows, d.half), f32),
                pltpu.VMEM((LANCZOS_STEPS, d.half, bond), f32),
                pltpu.VMEM((LANCZOS_STEPS, CHIPS, d.out_rows, bond), f32),
                pltpu.VMEM((8, 128), f32),
                pltpu.VMEM((DEVS, 8, 128), f32),
                pltpu.VMEM((2, 8, 128), f32),
                dma((3, 2)), dma((8, d.lane_tiles)), dma((CHUNKS, 2)), dma((CHUNKS, 2)), dma((2,)), dma((2,)), dma((2,)), dma((2,)),
                dma, dma((CHIPS,)), dma((CHUNKS,)), dma((CHUNKS, CHIPS)),
                dma, dma, dma, dma, dma, dma, dma, dma, dma,
            ],
            compiler_params=pltpu.CompilerParams(has_side_effects=True, vmem_limit_bytes=67043328),
            name='lanczos',
        )(wavefunction.reshape(bond * pair, bond), left_loc, right_used, pair_wide)
        row_start = lax.axis_index(AXIS_NAME) * d.out_rows
        first = lax.dynamic_slice_in_dim(wavefunction, row_start, d.out_rows, axis=0) / info[2, 0, 0]
        later = rows_out.reshape(LANCZOS_STEPS, pair, d.out_rows, bond).transpose(0, 2, 1, 3)
        return jnp.concatenate([first[None], later]), info[0, :LANCZOS_STEPS, 0], info[1, :LANCZOS_STEPS, 0]

    return jax.shard_map(device_body, mesh=mesh, in_specs=(P(), P(AXIS_NAME), P(AXIS_NAME), P(AXIS_NAME), P(AXIS_NAME)),
                         out_specs=(P(None, AXIS_NAME), P(), P()), check_vma=False)
```

```python
import functools

import jax
import jax.numpy as jnp
from jax import lax
from jax.experimental import pallas as pl
from jax.experimental.pallas import tpu as pltpu
from jax.sharding import PartitionSpec as P

LANCZOS_STEPS = 6
AXIS_NAME = 'terms'
MESH = pl.DeviceIdType.MESH

CHIPS = 16
CORES = 2
DEVS = 32
CHUNKS = 2
GROUPS = 4
TILE_PARTS = 4


class Dims:
    def __init__(self, bond, pair, terms_dev):
        self.bond = bond
        self.pair = pair
        self.terms_dev = terms_dev
        self.slab = bond // CHIPS
        self.sub = self.slab // 2
        self.half = bond // CORES
        self.chunk = self.half // CHUNKS
        self.rows = self.slab * pair
        self.prod = self.sub * pair
        self.out_rows = bond // DEVS
        self.group_terms = 4 * CORES * terms_dev
        self.vec_size = bond * pair * bond
        self.lane = min(bond, 128)
        self.lane_tiles = bond // self.lane


def lanczos_kernel(d, psi, left, right, wexp, out, info, lv, rv, wv, kw, uv, ps, yst, zst, sig, part, vcur, vprev, tbuf, gbuf, scs, scr, nbuf,
                   loc_sem, psi_sem, d2d_sem, d2d_recv, rw_send, rw_recv, fw_send, fw_recv, l_send, l_recv, f_send, f_recv, u_send, u_recv,
                   p_send, p_recv, s_send, s_recv, k_send, k_recv, n_send, n_recv, o_sem):
    me = lax.axis_index(AXIS_NAME)
    core = me % 2
    xpos = (me // 2) % 2
    ypos = (me // 4) % 2
    zpos = me // 8

    def device(z, y, x, c):
        return ((z * 2 + y) * 2 + x) * 2 + c

    def chip_slot(z, y, x):
        return (x * 2 + y) * 4 + z

    partner = device(zpos, ypos, xpos, 1 - core)
    slot = chip_slot(zpos, ypos, xpos)
    zs = (zpos, zpos + 1 - 2 * (zpos % 2), (zpos + 2) % 4, 3 - zpos)
    y_two = ypos + (1 - core) * (1 - 2 * ypos)
    x_two = xpos + core * (1 - 2 * xpos)
    y_three = ypos + core * (1 - 2 * ypos)
    x_three = xpos + (1 - core) * (1 - 2 * xpos)
    two = device(zpos, y_two, x_two, core)
    three = device(zpos, y_three, x_three, core)

    def remote(src, dst, send, recv, dev):
        return pltpu.make_async_remote_copy(src_ref=src, dst_ref=dst, send_sem=send, recv_sem=recv, device_id=(dev,), device_id_type=MESH)

    class Gather:
        def __init__(self, block, send, recv):
            self.block, self.send_sem, self.recv_sem = block, send, recv

        def send(self, which, dev):
            remote(self.block(which), self.block(which), self.send_sem, self.recv_sem(which), dev).start()

        def wait(self, which):
            remote(self.block(which), self.block(which), self.send_sem, self.recv_sem(which), me).wait_recv()

        def own_along(self):
            for i in (1, 2, 3):
                self.send(slot, device(zs[i], ypos, xpos, core))

        def own_across(self):
            self.send(slot, three)
            self.send(slot, two)

        def event(self, n):
            i = (n + 1) // 2
            if n % 2:
                which = chip_slot(zs[i], ypos, xpos)
                self.wait(which)
                self.send(which, three)
                self.send(which, two)
            else:
                which = chip_slot(zs[i], y_two, x_two)
                self.wait(which)
                self.send(which, three)

        def last(self, diagonal):
            for i in range(4):
                self.wait(chip_slot(zs[i], 1 - ypos, 1 - xpos) if diagonal else chip_slot(zs[i], y_three, x_three))

    edge = d.chunk
    l_parts = (
        (lambda s: lv.at[0, s, :, core], 0),
        (lambda s: lv.at[1, s, :, core, :, pl.ds(edge, d.bond - edge)], 1),
        (lambda s: lv.at[0, s, :, 1 - core, :, pl.ds(0, d.half)], 2),
        (lambda s: lv.at[1, s, :, 1 - core, :, pl.ds(edge, d.half - edge)], 3),
    )
    l_gathers = [Gather(block, l_send.at[n], lambda s, n=n: l_recv.at[n, s]) for block, n in l_parts]

    def l_swap(s, term):
        part = lv.at[:, s, :, term, :, pl.ds(d.half, d.half)]
        return remote(part, part, f_send, f_recv.at[s], partner)

    def l_event(n):
        i = (n + 1) // 2
        for g in l_gathers:
            g.event(n)
        l_swap(chip_slot(zs[i], ypos, xpos) if n % 2 else chip_slot(zs[i], y_two, x_two), core).start()

    def l_last(diagonal):
        for i in range(4):
            which = chip_slot(zs[i], 1 - ypos, 1 - xpos) if diagonal else chip_slot(zs[i], y_three, x_three)
            for g in l_gathers:
                g.wait(which)
            l_swap(which, core).start()

    def l_fill(n, grp):
        s = grp * 4 + n

        @pl.when(s != slot)
        def _():
            l_swap(s, 1 - core).wait_recv()
            for c in range(CORES):
                tile = lv[:, s, c, 1 - core, :, d.half:].reshape(d.half, d.half).T
                lv[:, s, c, 1 - core, :, d.half:] = tile.reshape(CHUNKS, d.chunk, d.half)
                for t in range(d.terms_dev):
                    lv[1, s, c, t, :, :edge] = lv[0, s, c, t, :, edge:d.half].T
        return grp

    def l_along():
        for i in (1, 2, 3):
            for g in l_gathers:
                g.send(slot, device(zs[i], ypos, xpos, core))

    def u_block(ch):
        return lambda s: uv.at[ch, :, pl.ds(pl.multiple_of(s * d.slab, d.slab), d.slab), :]

    u_gather = [Gather(u_block(ch), u_send.at[ch], lambda s, ch=ch: u_recv.at[ch, s]) for ch in range(CHUNKS)]

    for ch in range(CHUNKS):
        for h in range(2):
            mine = left.at[:, pl.ds(pl.multiple_of(core * d.half + ch * d.chunk, d.chunk), d.chunk),
                           pl.ds(pl.multiple_of((core + h) % 2 * d.half, d.half), d.half)]
            theirs = left.at[:, pl.ds(pl.multiple_of((1 - core) * d.half + ch * d.chunk, d.chunk), d.chunk),
                             pl.ds(pl.multiple_of((1 - core + h) % 2 * d.half, d.half), d.half)]
            remote(theirs, lv.at[ch, slot, core, :, :, pl.ds(h * d.half, d.half)], d2d_sem.at[ch, h], d2d_recv.at[ch, h], partner).start()
            pltpu.make_async_copy(mine, lv.at[ch, slot, core, :, :, pl.ds(h * d.half, d.half)], loc_sem.at[ch, h]).start()

    psi_rows = d.half * d.pair // 8
    psi_copies = [pltpu.make_async_copy(psi.at[pl.ds(pl.multiple_of(core * d.half * d.pair + n * psi_rows, psi_rows), psi_rows),
                                               pl.ds(c * d.lane, d.lane)],
                                        ps.at[c, pl.ds(n * psi_rows, psi_rows), :], psi_sem.at[n, c])
                  for n in range(8) for c in range(d.lane_tiles)]
    for copy in psi_copies:
        copy.start()

    def right_rows(s):
        return right.at[:, pl.ds(pl.multiple_of(s * d.slab, d.slab), d.slab), :]

    own_right = pltpu.make_async_copy(right_rows(slot), rv.at[slot, core], loc_sem.at[2, 0])
    own_pair = pltpu.make_async_copy(wexp, wv.at[slot, core], loc_sem.at[2, 1])
    own_right.start()
    own_pair.start()
    for n in range(1, CHIPS):
        chip = (me // 2 + n) % CHIPS
        to = chip_slot(chip // 4, chip // 2 % 2, chip % 2)
        remote(right_rows(to), rv.at[slot, core], rw_send.at[0], rw_recv.at[0], chip * 2 + core).start()
        remote(wexp, wv.at[slot, core], rw_send.at[1], rw_recv.at[1], chip * 2 + core).start()

    for ch in range(CHUNKS):
        for h in range(2):
            pltpu.make_async_copy(lv.at[ch, slot, core, :, :, pl.ds(h * d.half, d.half)], lv.at[ch, slot, core, :, :, pl.ds(h * d.half, d.half)], loc_sem.at[ch, h]).wait()
            back = remote(lv.at[ch, slot, 1 - core, :, :, pl.ds(h * d.half, d.half)], lv.at[ch, slot, 1 - core, :, :, pl.ds(h * d.half, d.half)], d2d_sem.at[ch, h], d2d_recv.at[ch, h], partner)
            back.wait_recv()
    l_along()
    for g in l_gathers:
        g.own_across()

    total = jnp.zeros((8, d.lane), jnp.float32)
    for n in range(8):
        for copy in psi_copies[n * d.lane_tiles:(n + 1) * d.lane_tiles]:
            copy.wait()

        def add_rows(i, acc, n=n):
            x = ps[:, pl.ds(pl.multiple_of(n * psi_rows + i * (psi_rows // 8), 8), psi_rows // 8), :]
            return acc + jnp.sum((x * x).reshape(d.lane_tiles * psi_rows // 64, 8, d.lane), axis=0)

        total = lax.fori_loop(0, 8, add_rows, total)
    nbuf[0] = jnp.broadcast_to(jnp.sum(total, keepdims=True), (8, 128))
    to_partner = remote(nbuf.at[0], nbuf.at[1], n_send, n_recv, partner)
    to_partner.start()
    to_partner.wait()
    norm = jnp.sqrt((nbuf[0] + nbuf[1])[0:1, :] / d.vec_size)
    info[2] = jnp.broadcast_to(norm, (8, 128))
    norm_one = norm[:, 0:1]

    def place(q):
        tiles = [(ps[c, pl.ds(q, d.half, stride=d.pair), :] / norm_one).T for c in range(d.lane_tiles)]
        xt = jnp.concatenate(tiles, axis=0)
        vprev[...] = xt
        return xt.astype(jnp.bfloat16)

    def start_vector(qb, carry):
        for q2 in range(2):
            q = qb * 2 + q2
            xb = place(q)
            for ch in range(CHUNKS):
                uv[ch, qb, :, q2 * d.chunk:(q2 + 1) * d.chunk] = xb[:, ch * d.chunk:(ch + 1) * d.chunk]
            for bh in range(2):
                rows = vprev[pl.ds(pl.multiple_of(slot * d.slab + bh * d.sub, d.sub), d.sub), :]
                vcur[pl.ds(pl.multiple_of((bh * d.pair + q) * d.sub, d.sub), d.sub), :] = rows
        return carry

    lax.fori_loop(0, d.pair // 4, start_vector, 0)
    own_right.wait()
    own_pair.wait()
    fifteen = rv.at[pl.ds(0, CHIPS - 1), 0]
    fifteen_w = wv.at[pl.ds(0, CHIPS - 1), 0]
    remote(fifteen, fifteen, rw_send.at[0], rw_recv.at[0], me).wait()
    remote(fifteen_w, fifteen_w, rw_send.at[1], rw_recv.at[1], me).wait()
    fw_right = remote(rv.at[:, core], rv.at[:, core], fw_send.at[0], fw_recv.at[0], partner)
    fw_pair = remote(wv.at[:, core], wv.at[:, core], fw_send.at[1], fw_recv.at[1], partner)
    fw_right.start()
    fw_pair.start()
    l_event(0)
    l_event(1)
    lax.fori_loop(d.pair // 4, d.pair // 2, start_vector, 0)
    l_event(2)
    l_event(3)
    fw_right.wait()
    fw_pair.wait()
    lane = lax.broadcasted_iota(jnp.int32, (d.sub, d.prod), 1)
    row = lax.broadcasted_iota(jnp.int32, (d.sub, d.prod), 0)
    diagonal = lane % d.sub == row

    def spread_pair(s, carry):
        for c in range(2):
            for t in range(d.terms_dev):
                w = wv[s, c, t].astype(jnp.float32)
                for q in range(d.pair):
                    full = jnp.where(diagonal, jnp.broadcast_to(w[q:q + 1, :], (d.sub, d.prod)), 0.0)
                    kw[s, c, t, q * d.sub:(q + 1) * d.sub, :] = full.astype(jnp.bfloat16)
        return carry

    lax.fori_loop(0, CHIPS, spread_pair, 0)
    l_event(4)
    l_event(5)
    l_event(6)
    vprev[...] = jnp.zeros_like(vprev)

    def products(ch, grp):
        r_all = rv[pl.ds(grp * 4, 4)].reshape(d.group_terms * d.slab, d.bond)
        for qb in range(d.pair // 2):
            y = jnp.dot(r_all, uv[ch, qb], preferred_element_type=jnp.float32).astype(jnp.bfloat16)
            y = y.reshape(d.group_terms, 2, d.sub, 2 * d.chunk)
            for q2 in range(2):
                q = qb * 2 + q2
                for bh in range(2):
                    yst[:, q * d.sub:(q + 1) * d.sub, bh * d.chunk:(bh + 1) * d.chunk] = y[:, bh, :, q2 * d.chunk:(q2 + 1) * d.chunk]
        for k in range(d.group_terms):
            w = kw[grp * 4 + k // 4, k // 2 % 2, k % 2]
            z = jnp.dot(w, yst[k], preferred_element_type=jnp.float32).astype(jnp.bfloat16)
            for bh in range(2):
                zst[bh * d.prod:(bh + 1) * d.prod, k * d.chunk:(k + 1) * d.chunk] = z[:, bh * d.chunk:(bh + 1) * d.chunk]
        l_all = lv[ch, pl.ds(grp * 4, 4)].reshape(d.group_terms * d.chunk, d.bond)
        sig[...] += jnp.dot(zst[...], l_all, preferred_element_type=jnp.float32)

    def hand_out(j):
        def one(n, carry):
            to = core * CHIPS + n
            block = tbuf.at[j, pl.ds(pl.multiple_of(n * d.out_rows, d.out_rows), d.out_rows), :]

            @pl.when(to != me)
            def _():
                remote(block, gbuf.at[j, slot], k_send, k_recv, to).start()

            @pl.when(to == me)
            def _():
                gbuf[j, slot] = block[...]
            return carry

        lax.fori_loop(0, CHIPS, one, 0)

    def step(j, beta_prev):
        later = jnp.minimum(j, 1)

        @pl.when(j > 0)
        def _():
            for n in range(7):
                u_gather[0].event(n)
            u_gather[1].own_across()
            for n in range(4):
                u_gather[1].event(n)
            u_gather[0].last(False)
            u_gather[0].last(True)

        sig[...] = jnp.zeros_like(sig)

        def part_step(it, carry):
            ch = (1 - later) * (it % 2) + later * (it // 4)
            n = (1 - later) * (it // 2) + later * (it % 4)
            own = xpos * 2 + ypos
            arrive = jnp.where(n == 0, own, jnp.where(n == 1, x_two * 2 + y_two, jnp.where(n == 2, x_three * 2 + y_three, 3 - own)))
            grp = (1 - later) * arrive + later * n

            @pl.when((j == 0) & (it == 2))
            def _():
                l_last(False)

            @pl.when((j == 0) & (it == 6))
            def _():
                l_last(True)

            @pl.when((j == 0) & (it % 2 == 0))
            def _():
                lax.fori_loop(0, 4, l_fill, grp)

            for at in range(3):
                @pl.when((j > 0) & (it == at))
                def _():
                    u_gather[1].event(4 + at)

            @pl.when((j > 0) & (it == 4))
            def _():
                u_gather[1].last(False)
                u_gather[1].last(True)
                hand_out(j - 1)

            products(ch, grp)
            return carry

        lax.fori_loop(0, 2 * GROUPS, part_step, 0)

        @pl.when(j > 0)
        def _():
            for ch in range(CHUNKS):
                sent = uv.at[ch, :, pl.ds(0, 15 * d.slab), :]
                remote(sent, sent, u_send.at[ch], u_recv.at[ch, 0], me).wait_send()

        other = sig.at[:, pl.ds(d.half, d.half)]
        to_other = remote(other, part, p_send, p_recv, partner)
        to_other.start()
        to_other.wait()
        s = sig[:, :d.half] + part[...]
        v = vcur[...]
        w = s - beta_prev * vprev[...]
        sv = jnp.sum(s * v, keepdims=True)
        wv_sum = jnp.sum(w * v, keepdims=True)
        vv = jnp.sum(v * v, keepdims=True)
        guess = jnp.where(vv > 0.0, wv_sum / jnp.where(vv > 0.0, vv, 1.0), 0.0)
        t = w - guess * v
        sig[:, :d.half] = t
        tt = jnp.sum(t * t, keepdims=True)
        tv = jnp.sum(t * v, keepdims=True)
        tile_row = lax.broadcasted_iota(jnp.int32, (8, 128), 0)
        tile = jnp.zeros((8, 128), jnp.float32)
        for n, value in enumerate((sv, vv, tt, tv, guess)):
            tile = jnp.where(tile_row == n, value, tile)
        scs[...] = tile
        scr[me] = tile

        def tell(n, carry):
            remote(scs, scr.at[me], s_send, s_recv, (me + n) % DEVS).start()
            return carry

        lax.fori_loop(1, DEVS, tell, 0)
        heard = scr.at[pl.ds(0, DEVS - 1)]
        remote(heard, heard, s_send, s_recv, me).wait()
        alpha = jnp.sum(scr[:, 0, :], axis=0, keepdims=True) / d.vec_size
        off = alpha - scr[:, 4, :]
        square = scr[:, 2, :] - 2.0 * off * scr[:, 3, :] + off * off * scr[:, 1, :]
        beta = jnp.sqrt(jnp.sum(square, axis=0, keepdims=True) / d.vec_size)
        info[0, pl.ds(j, 1), :] = alpha
        info[1, pl.ds(j, 1), :] = beta
        vnew = (sig[:, :d.half] - (alpha[:, 0:1] - guess) * vcur[...]) / beta[:, 0:1]
        vprev[...] = vcur[...]
        vcur[...] = vnew
        vb = vnew.astype(jnp.bfloat16)

        @pl.when(j < LANCZOS_STEPS - 1)
        def _():
            for ch in range(CHUNKS):
                for bh in range(2):
                    at = pl.ds(pl.multiple_of(slot * d.slab + bh * d.sub, d.sub), d.sub)
                    for q in range(d.pair):
                        uv[ch, q // 2, at, q % 2 * d.chunk:(q % 2 + 1) * d.chunk] = \
                            vb[(bh * d.pair + q) * d.sub:(bh * d.pair + q + 1) * d.sub, ch * d.chunk:(ch + 1) * d.chunk]
            u_gather[0].own_along()
            u_gather[0].own_across()
            u_gather[1].own_along()

        wide = TILE_PARTS * d.slab
        for n in range(d.pair // TILE_PARTS):
            rows = [vcur[(bh * d.pair + q) * d.sub:(bh * d.pair + q + 1) * d.sub, :]
                    for q in range(n * TILE_PARTS, (n + 1) * TILE_PARTS) for bh in range(2)]
            tbuf[j, :, n * wide:(n + 1) * wide] = jnp.concatenate(rows, axis=0).T

        return beta[:, 0:1]

    lax.fori_loop(0, LANCZOS_STEPS, step, jnp.zeros((1, 1), jnp.float32))

    hand_out(LANCZOS_STEPS - 1)
    for n, part in enumerate((lv.at[0, pl.ds(0, 15), :, 0], lv.at[1, pl.ds(0, 15), :, 0, :, pl.ds(edge, d.bond - edge)],
                              lv.at[0, pl.ds(0, 15), :, 0, :, pl.ds(0, d.half)], lv.at[1, pl.ds(0, 15), :, 0, :, pl.ds(edge, d.half - edge)])):
        remote(part, part, l_send.at[n], l_recv.at[n, 0], me).wait_send()
    swapped = lv.at[:, pl.ds(0, 15), :, 0, :, pl.ds(d.half, d.half)]
    remote(swapped, swapped, f_send, f_recv.at[0], me).wait_send()
    for ch in range(CHUNKS):
        for h in range(2):
            theirs = left.at[:, pl.ds(0, d.chunk), pl.ds(0, d.half)]
            remote(theirs, lv.at[ch, slot, core, :, :, pl.ds(h * d.half, d.half)], d2d_sem.at[ch, h], d2d_recv.at[ch, h], partner).wait_send()

    sends_self = me // CHIPS == core

    @pl.when(sends_self)
    def _():
        some = gbuf.at[:, pl.ds(0, CHIPS - 1)]
        remote(some, some, k_send, k_recv, me).wait()

    @pl.when(jnp.logical_not(sends_self))
    def _():
        remote(gbuf, gbuf, k_send, k_recv, me).wait()

    wide = TILE_PARTS * d.slab
    lanes = lax.broadcasted_iota(jnp.int32, (d.out_rows, wide), 1) // d.slab

    def put_out(j, carry):
        for ct in range(CHIPS // TILE_PARTS):
            for qt in range(d.pair // TILE_PARTS):
                src = [gbuf[j, ct * TILE_PARTS + c, :, qt * wide:(qt + 1) * wide] for c in range(TILE_PARTS)]
                for q in range(TILE_PARTS):
                    tile = jnp.zeros((d.out_rows, wide), jnp.float32)
                    for c in range(TILE_PARTS):
                        shift = (c - q) % TILE_PARTS * d.slab
                        moved = pltpu.roll(src[c], shift, 1) if shift else src[c]
                        tile = jnp.where(lanes == c, moved, tile)
                    at = (qt * TILE_PARTS + q) * d.out_rows
                    tbuf[j, at:at + d.out_rows, ct * wide:(ct + 1) * wide] = tile
        pltpu.make_async_copy(tbuf.at[j], out.at[j], o_sem).start()
        return carry

    lax.fori_loop(0, LANCZOS_STEPS, put_out, 0)
    pltpu.make_async_copy(tbuf, out, o_sem).wait()


def solution(mesh):
    def device_body(wavefunction, left_loc, pair_loc, right_loc, flag_loc):
        bond, pair = wavefunction.shape[0], wavefunction.shape[1]
        d = Dims(bond, pair, left_loc.shape[0])
        eye = jnp.eye(bond, dtype=jnp.bfloat16)
        right_used = jnp.where((flag_loc == 1)[:, None, None], right_loc, eye)
        pair_wide = jnp.repeat(pair_loc, d.sub, axis=2)
        bf16, f32 = jnp.bfloat16, jnp.float32
        dma = pltpu.SemaphoreType.DMA
        any_space = pl.BlockSpec(memory_space=pl.ANY)
        rows_out, info = pl.pallas_call(
            functools.partial(lanczos_kernel, d),
            out_shape=(jax.ShapeDtypeStruct((LANCZOS_STEPS, d.half, bond), f32), jax.ShapeDtypeStruct((3, 8, 128), f32)),
            in_specs=[any_space] * 4,
            out_specs=(any_space, pl.BlockSpec(memory_space=pltpu.VMEM)),
            scratch_shapes=[
                pltpu.VMEM((CHUNKS, CHIPS, CORES, d.terms_dev, d.chunk, bond), bf16),
                pltpu.VMEM((CHIPS, CORES, d.terms_dev, d.slab, bond), bf16),
                pltpu.VMEM((CHIPS, CORES, d.terms_dev, pair, d.prod), bf16),
                pltpu.VMEM((CHIPS, CORES, d.terms_dev, d.prod, d.prod), bf16),
                pltpu.VMEM((CHUNKS, pair // 2, bond, 2 * d.chunk), bf16),
                pltpu.VMEM((d.lane_tiles, d.half * pair, d.lane), f32),
                pltpu.VMEM((d.group_terms, d.prod, 2 * d.chunk), bf16),
                pltpu.VMEM((d.rows, d.group_terms * d.chunk), bf16),
                pltpu.VMEM((d.rows, bond), f32),
                pltpu.VMEM((d.rows, d.half), f32),
                pltpu.VMEM((d.rows, d.half), f32),
                pltpu.VMEM((d.rows, d.half), f32),
                pltpu.VMEM((LANCZOS_STEPS, d.half, bond), f32),
                pltpu.VMEM((LANCZOS_STEPS, CHIPS, d.out_rows, bond), f32),
                pltpu.VMEM((8, 128), f32),
                pltpu.VMEM((DEVS, 8, 128), f32),
                pltpu.VMEM((2, 8, 128), f32),
                dma((3, 2)), dma((8, d.lane_tiles)), dma((CHUNKS, 2)), dma((CHUNKS, 2)), dma((2,)), dma((2,)), dma((2,)), dma((2,)),
                dma((4,)), dma((4, CHIPS)), dma, dma((CHIPS,)), dma((CHUNKS,)), dma((CHUNKS, CHIPS)),
                dma, dma, dma, dma, dma, dma, dma, dma, dma,
            ],
            compiler_params=pltpu.CompilerParams(has_side_effects=True, vmem_limit_bytes=67043328),
            name='lanczos',
        )(wavefunction.reshape(bond * pair, bond), left_loc, right_used, pair_wide)
        row_start = lax.axis_index(AXIS_NAME) * d.out_rows
        first = lax.dynamic_slice_in_dim(wavefunction, row_start, d.out_rows, axis=0) / info[2, 0, 0]
        later = rows_out.reshape(LANCZOS_STEPS, pair, d.out_rows, bond).transpose(0, 2, 1, 3)
        return jnp.concatenate([first[None], later]), info[0, :LANCZOS_STEPS, 0], info[1, :LANCZOS_STEPS, 0]

    return jax.shard_map(device_body, mesh=mesh, in_specs=(P(), P(AXIS_NAME), P(AXIS_NAME), P(AXIS_NAME), P(AXIS_NAME)),
                         out_specs=(P(None, AXIS_NAME), P(), P()), check_vma=False)
```

```python
import functools

import jax
import jax.numpy as jnp
from jax import lax
from jax.experimental import pallas as pl
from jax.experimental.pallas import tpu as pltpu
from jax.sharding import PartitionSpec as P

LANCZOS_STEPS = 6
AXIS_NAME = 'terms'
MESH = pl.DeviceIdType.MESH

CHIPS = 16
CORES = 2
DEVS = 32
CHUNKS = 2
GROUPS = 4
TILE_PARTS = 4
QUARTERS = 4
PIECES = CHUNKS * QUARTERS

ALONG, ACROSS, FROM_COLUMN, FROM_SECOND, THIRD, DIAGONAL, RESULT, RESULT_OUT = range(8)
RIGHT_SLOTS = (0, 1, 2, 3, 8, 9, 10, 11)
SLOTS = (
    ((1, 0, 1), (1, 0, 6), (0, 1, 1), (1, 0, 2), (1, 0, 3), (0, 1, 2), (1, 0, 4), (1, 0, 7), (0, 2, 2), (1, 0, 5), (0, 1, 3), (0, 1, 0), (0, 2, 0), (0, 3, 0), (0, 3, 1), (0, 2, 1), (0, 3, 2), (1, 0, 0), (3, 0, 3), (3, 0, 2), (2, 1, 2), (2, 1, 1), (0, 3, 3), (2, 1, 0), (2, 2, 0), (3, 0, 0), (2, 2, 1), (3, 1, 1), (0, 2, 3), (2, 2, 2), (3, 1, 0), (2, 3, 0), (3, 2, 0), (3, 0, 1), (2, 2, 3), (0, 3, 4), (2, 3, 1), (2, 3, 2), (0, 3, 5), (3, 3, 0), (0, 1, 4), (0, 2, 4), (0, 1, 5), (2, 1, 3), (3, 2, 1), (3, 2, 3), (3, 3, 1), (0, 2, 5), (0, 1, 6), (2, 3, 3), (0, 3, 7), (3, 3, 2), (3, 1, 3), (0, 3, 6), (3, 2, 2), (0, 2, 6), (3, 1, 2), (0, 2, 7), (3, 3, 3), (5, 0, 0), (3, 0, 4), (4, 0, 1), (4, 0, 0), (3, 0, 5),),
    ((6, 0, 0), (2, 3, 4), (4, 0, 2), (3, 0, 6), (5, 0, 1),),
    ((2, 2, 4), (2, 1, 4), (2, 1, 5), (5, 0, 2), (2, 2, 5),),
    ((5, 0, 3), (0, 1, 7), (3, 3, 4), (4, 0, 3), (2, 3, 5), (2, 1, 6), (2, 2, 6),),
    (),
    ((4, 0, 4), (2, 3, 6), (3, 1, 4), (2, 2, 7), (3, 2, 4),),
    ((3, 3, 5), (3, 2, 5), (3, 1, 5), (2, 3, 7), (2, 1, 7),),
    ((3, 1, 6), (3, 3, 6),),
    ((4, 0, 5), (3, 2, 6), (3, 0, 7), (4, 0, 6), (5, 0, 4), (3, 3, 7), (3, 2, 7),),
    ((5, 0, 5), (3, 1, 7),),
    ((4, 0, 7), (5, 0, 6),),
    ((5, 0, 7), (7, 0, 0),),
    (),
    (),
    (),
    (),
)


class Dims:
    def __init__(self, bond, pair, terms_dev):
        self.bond = bond
        self.pair = pair
        self.terms_dev = terms_dev
        self.slab = bond // CHIPS
        self.sub = self.slab // 2
        self.half = bond // CORES
        self.chunk = self.half // CHUNKS
        self.rows = self.slab * pair
        self.prod = self.sub * pair
        self.out_rows = bond // DEVS
        self.group_terms = 4 * CORES * terms_dev
        self.vec_size = bond * pair * bond
        self.lane = min(bond, 128)
        self.lane_tiles = bond // self.lane


def lanczos_kernel(d, psi, left, right, wexp, out, info, lv, rv, wv, kw, uv, ps, yst, zst, sig, part, vcur, vprev, tbuf, gbuf, scs, scr, nbuf,
                   loc_sem, psi_sem, d2d_sem, d2d_recv, rw_send, rw_recv, fw_send, fw_recv, l_send, l_recv, f_send, f_recv, u_send, u_recv,
                   p_send, p_recv, s_send, s_recv, k_send, k_recv, n_send, n_recv, o_sem):
    me = lax.axis_index(AXIS_NAME)
    core = me % 2
    xpos = (me // 2) % 2
    ypos = (me // 4) % 2
    zpos = me // 8

    def device(z, y, x, c):
        return ((z * 2 + y) * 2 + x) * 2 + c

    def chip_slot(z, y, x):
        return (x * 2 + y) * 4 + z

    partner = device(zpos, ypos, xpos, 1 - core)
    slot = chip_slot(zpos, ypos, xpos)
    zs = (zpos, zpos + 1 - 2 * (zpos % 2), (zpos + 2) % 4, 3 - zpos)
    inner = (zpos + 1) // 2 % 2
    zn = (zpos, (1 - inner) * (zpos + 1 - zpos // 3 * 2) + inner * (zpos - 1), (1 - inner) * ((zpos + 2) % 4) + inner * (zpos + 1),
          (1 - inner) * (3 - zpos) + inner * ((zpos + 2) % 4))
    y_two = ypos + (1 - core) * (1 - 2 * ypos)
    x_two = xpos + core * (1 - 2 * xpos)
    y_three = ypos + core * (1 - 2 * ypos)
    x_three = xpos + (1 - core) * (1 - 2 * xpos)
    two = device(zpos, y_two, x_two, core)
    three = device(zpos, y_three, x_three, core)

    def remote(src, dst, send, recv, dev):
        return pltpu.make_async_remote_copy(src_ref=src, dst_ref=dst, send_sem=send, recv_sem=recv, device_id=(dev,), device_id_type=MESH)

    class Gather:
        def __init__(self, block, send, recv):
            self.block, self.send_sem, self.recv_sem = block, send, recv

        def send(self, which, dev):
            remote(self.block(which), self.block(which), self.send_sem, self.recv_sem(which), dev).start()

        def wait(self, which):
            remote(self.block(which), self.block(which), self.send_sem, self.recv_sem(which), me).wait_recv()

        def own_along(self):
            for i in (1, 2, 3):
                self.send(slot, device(zs[i], ypos, xpos, core))

        def own_across(self):
            self.send(slot, three)
            self.send(slot, two)

        def event(self, n):
            i = (n + 1) // 2
            if n % 2:
                which = chip_slot(zs[i], ypos, xpos)
                self.wait(which)
                self.send(which, three)
                self.send(which, two)
            else:
                which = chip_slot(zs[i], y_two, x_two)
                self.wait(which)
                self.send(which, three)

        def last(self, diagonal):
            for i in range(4):
                self.wait(chip_slot(zs[i], 1 - ypos, 1 - xpos) if diagonal else chip_slot(zs[i], y_three, x_three))

    edge = d.chunk
    l_parts = (
        (lambda s: lv.at[0, s, :, core], 0),
        (lambda s: lv.at[1, s, :, core, :, pl.ds(edge, d.bond - edge)], 1),
        (lambda s: lv.at[0, s, :, 1 - core, :, pl.ds(0, d.half)], 2),
        (lambda s: lv.at[1, s, :, 1 - core, :, pl.ds(edge, d.half - edge)], 3),
    )
    l_gathers = [Gather(block, l_send.at[n], lambda s, n=n: l_recv.at[n, s]) for block, n in l_parts]

    def l_swap(s, term):
        part = lv.at[:, s, :, term, :, pl.ds(d.half, d.half)]
        return remote(part, part, f_send, f_recv.at[s], partner)

    def l_event(n):
        i = (n + 1) // 2
        for g in l_gathers:
            g.event(n)
        l_swap(chip_slot(zs[i], ypos, xpos) if n % 2 else chip_slot(zs[i], y_two, x_two), core).start()

    def l_last(diagonal):
        for i in range(4):
            which = chip_slot(zs[i], 1 - ypos, 1 - xpos) if diagonal else chip_slot(zs[i], y_three, x_three)
            for g in l_gathers:
                g.wait(which)
            l_swap(which, core).start()

    def l_fill(n, grp):
        s = grp * 4 + n

        @pl.when(s != slot)
        def _():
            l_swap(s, 1 - core).wait_recv()
            for c in range(CORES):
                tile = lv[:, s, c, 1 - core, :, d.half:].reshape(d.half, d.half).T
                lv[:, s, c, 1 - core, :, d.half:] = tile.reshape(CHUNKS, d.chunk, d.half)
                for t in range(d.terms_dev):
                    lv[1, s, c, t, :, :edge] = lv[0, s, c, t, :, edge:d.half].T
        return grp

    def l_along():
        for i in (1, 2, 3):
            for g in l_gathers:
                g.send(slot, device(zs[i], ypos, xpos, core))

    def u_block(p):
        return lambda s: uv.at[p // QUARTERS, pl.ds(p % QUARTERS * 2, 2), pl.ds(pl.multiple_of(s * d.slab, d.slab), d.slab), :]

    u_gathers = [Gather(u_block(p), u_send.at[p], lambda s, p=p: u_recv.at[p, s]) for p in range(PIECES)]

    def act(kind, i, p, j):
        g = u_gathers[p]
        if kind == ALONG:
            g.send(slot, device(zn[i], ypos, xpos, core))
        elif kind == ACROSS:
            g.own_across()
        elif kind == FROM_COLUMN:
            which = chip_slot(zn[i], ypos, xpos)
            g.wait(which)
            g.send(which, three)
            g.send(which, two)
        elif kind == FROM_SECOND:
            which = chip_slot(zn[i], y_two, x_two)
            g.wait(which)
            g.send(which, three)
        elif kind == THIRD:
            g.last(False)
        elif kind == DIAGONAL:
            g.last(True)
        elif kind == RESULT:
            turn_result(j - 1)
        elif kind == RESULT_OUT:
            hand_out(j - 1)

    for ch in range(CHUNKS):
        for h in range(2):
            mine = left.at[:, pl.ds(pl.multiple_of(core * d.half + ch * d.chunk, d.chunk), d.chunk),
                           pl.ds(pl.multiple_of((core + h) % 2 * d.half, d.half), d.half)]
            theirs = left.at[:, pl.ds(pl.multiple_of((1 - core) * d.half + ch * d.chunk, d.chunk), d.chunk),
                             pl.ds(pl.multiple_of((1 - core + h) % 2 * d.half, d.half), d.half)]
            remote(theirs, lv.at[ch, slot, core, :, :, pl.ds(h * d.half, d.half)], d2d_sem.at[ch, h], d2d_recv.at[ch, h], partner).start()
            pltpu.make_async_copy(mine, lv.at[ch, slot, core, :, :, pl.ds(h * d.half, d.half)], loc_sem.at[ch, h]).start()

    psi_rows = d.half * d.pair // 8
    psi_copies = [pltpu.make_async_copy(psi.at[pl.ds(pl.multiple_of(core * d.half * d.pair + n * psi_rows, psi_rows), psi_rows),
                                               pl.ds(c * d.lane, d.lane)],
                                        ps.at[c, pl.ds(n * psi_rows, psi_rows), :], psi_sem.at[n, c])
                  for n in range(8) for c in range(d.lane_tiles)]
    for copy in psi_copies:
        copy.start()

    def right_rows(s):
        return right.at[:, pl.ds(pl.multiple_of(s * d.slab, d.slab), d.slab), :]

    own_right = pltpu.make_async_copy(right_rows(slot), rv.at[slot, core], loc_sem.at[2, 0])
    own_pair = pltpu.make_async_copy(wexp, wv.at[slot, core], loc_sem.at[2, 1])
    own_right.start()
    own_pair.start()
    for n in range(1, CHIPS):
        chip = (me // 2 + n) % CHIPS
        to = chip_slot(chip // 4, chip // 2 % 2, chip % 2)
        remote(right_rows(to), rv.at[slot, core], rw_send.at[0], rw_recv.at[0], chip * 2 + core).start()
        remote(wexp, wv.at[slot, core], rw_send.at[1], rw_recv.at[1], chip * 2 + core).start()

    for ch in range(CHUNKS):
        for h in range(2):
            pltpu.make_async_copy(lv.at[ch, slot, core, :, :, pl.ds(h * d.half, d.half)], lv.at[ch, slot, core, :, :, pl.ds(h * d.half, d.half)], loc_sem.at[ch, h]).wait()
            back = remote(lv.at[ch, slot, 1 - core, :, :, pl.ds(h * d.half, d.half)], lv.at[ch, slot, 1 - core, :, :, pl.ds(h * d.half, d.half)], d2d_sem.at[ch, h], d2d_recv.at[ch, h], partner)
            back.wait_recv()
    l_along()
    for g in l_gathers:
        g.own_across()

    total = jnp.zeros((8, d.lane), jnp.float32)
    for n in range(8):
        for copy in psi_copies[n * d.lane_tiles:(n + 1) * d.lane_tiles]:
            copy.wait()

        def add_rows(i, acc, n=n):
            x = ps[:, pl.ds(pl.multiple_of(n * psi_rows + i * (psi_rows // 8), 8), psi_rows // 8), :]
            return acc + jnp.sum((x * x).reshape(d.lane_tiles * psi_rows // 64, 8, d.lane), axis=0)

        total = lax.fori_loop(0, 8, add_rows, total)
    nbuf[0] = jnp.broadcast_to(jnp.sum(total, keepdims=True), (8, 128))
    to_partner = remote(nbuf.at[0], nbuf.at[1], n_send, n_recv, partner)
    to_partner.start()
    to_partner.wait()
    norm = jnp.sqrt((nbuf[0] + nbuf[1])[0:1, :] / d.vec_size)
    info[2] = jnp.broadcast_to(norm, (8, 128))
    norm_one = norm[:, 0:1]

    def place(q):
        tiles = [(ps[c, pl.ds(q, d.half, stride=d.pair), :] / norm_one).T for c in range(d.lane_tiles)]
        xt = jnp.concatenate(tiles, axis=0)
        vprev[...] = xt
        return xt.astype(jnp.bfloat16)

    def start_vector(qb, carry):
        for q2 in range(2):
            q = qb * 2 + q2
            xb = place(q)
            for ch in range(CHUNKS):
                uv[ch, qb, :, q2 * d.chunk:(q2 + 1) * d.chunk] = xb[:, ch * d.chunk:(ch + 1) * d.chunk]
            for bh in range(2):
                rows = vprev[pl.ds(pl.multiple_of(slot * d.slab + bh * d.sub, d.sub), d.sub), :]
                vcur[pl.ds(pl.multiple_of((bh * d.pair + q) * d.sub, d.sub), d.sub), :] = rows
        return carry

    lax.fori_loop(0, d.pair // 4, start_vector, 0)
    own_right.wait()
    own_pair.wait()
    fifteen = rv.at[pl.ds(0, CHIPS - 1), 0]
    fifteen_w = wv.at[pl.ds(0, CHIPS - 1), 0]
    remote(fifteen, fifteen, rw_send.at[0], rw_recv.at[0], me).wait()
    remote(fifteen_w, fifteen_w, rw_send.at[1], rw_recv.at[1], me).wait()
    fw_right = remote(rv.at[:, core], rv.at[:, core], fw_send.at[0], fw_recv.at[0], partner)
    fw_pair = remote(wv.at[:, core], wv.at[:, core], fw_send.at[1], fw_recv.at[1], partner)
    fw_right.start()
    fw_pair.start()
    l_event(0)
    l_event(1)
    lax.fori_loop(d.pair // 4, d.pair // 2, start_vector, 0)
    l_event(2)
    l_event(3)
    fw_right.wait()
    fw_pair.wait()
    lane = lax.broadcasted_iota(jnp.int32, (d.sub, d.prod), 1)
    row = lax.broadcasted_iota(jnp.int32, (d.sub, d.prod), 0)
    diagonal = lane % d.sub == row

    def spread_pair(s, carry):
        for c in range(2):
            for t in range(d.terms_dev):
                w = wv[s, c, t].astype(jnp.float32)
                for q in range(d.pair):
                    full = jnp.where(diagonal, jnp.broadcast_to(w[q:q + 1, :], (d.sub, d.prod)), 0.0)
                    kw[s, c, t, q * d.sub:(q + 1) * d.sub, :] = full.astype(jnp.bfloat16)
        return carry

    lax.fori_loop(0, CHIPS, spread_pair, 0)
    l_event(4)
    l_event(5)
    l_event(6)
    vprev[...] = jnp.zeros_like(vprev)

    def right_product(grp, ch, qb):
        r_all = rv[pl.ds(grp * 4, 4)].reshape(d.group_terms * d.slab, d.bond)
        y = jnp.dot(r_all, uv[ch, qb], preferred_element_type=jnp.float32).astype(jnp.bfloat16)
        y = y.reshape(d.group_terms, 2, d.sub, 2 * d.chunk)
        for q2 in range(2):
            for bh in range(2):
                yst[pl.ds(grp * d.group_terms, d.group_terms), qb * 2 + q2, :, bh * d.chunk:(bh + 1) * d.chunk] = \
                    y[:, bh, :, q2 * d.chunk:(q2 + 1) * d.chunk]

    def right_of_group(grp, ch):
        for qb in range(d.pair // 2):
            right_product(grp, ch, qb)

    def right_of_piece(ch, part):
        for qb in range(2):
            for grp in range(GROUPS):
                right_product(grp, ch, part * 2 + qb)

    def left_products(ch, grp):
        for k in range(d.group_terms):
            w = kw[grp * 4 + k // 4, k // 2 % 2, k % 2]
            z = jnp.dot(w, yst[grp * d.group_terms + k].reshape(d.prod, 2 * d.chunk), preferred_element_type=jnp.float32).astype(jnp.bfloat16)
            for bh in range(2):
                zst[bh * d.prod:(bh + 1) * d.prod, k * d.chunk:(k + 1) * d.chunk] = z[:, bh * d.chunk:(bh + 1) * d.chunk]
        l_all = lv[ch, pl.ds(grp * 4, 4)].reshape(d.group_terms * d.chunk, d.bond)
        sig[...] += jnp.dot(zst[...], l_all, preferred_element_type=jnp.float32)

    def turn_result(j):
        wide = TILE_PARTS * d.slab
        for n in range(d.pair // TILE_PARTS):
            rows = [vcur[(bh * d.pair + q) * d.sub:(bh * d.pair + q + 1) * d.sub, :]
                    for q in range(n * TILE_PARTS, (n + 1) * TILE_PARTS) for bh in range(2)]
            tbuf[j, :, n * wide:(n + 1) * wide] = jnp.concatenate(rows, axis=0).T

    def hand_out(j):
        def one(n, carry):
            to = core * CHIPS + n
            block = tbuf.at[j, pl.ds(pl.multiple_of(n * d.out_rows, d.out_rows), d.out_rows), :]

            @pl.when(to != me)
            def _():
                remote(block, gbuf.at[j, slot], k_send, k_recv, to).start()

            @pl.when(to == me)
            def _():
                gbuf[j, slot] = block[...]
            return carry

        lax.fori_loop(0, CHIPS, one, 0)

    def step(j, beta_prev):
        later = jnp.minimum(j, 1)
        own = xpos * 2 + ypos
        sig[...] = jnp.zeros_like(sig)

        def slot_step(t, carry):
            n = t // 4
            first_grp = jnp.where(n == 0, own, jnp.where(n == 1, x_two * 2 + y_two, jnp.where(n == 2, x_three * 2 + y_three, 3 - own)))
            first_ch = t // 2 % 2
            done_right = sum((t > r).astype(jnp.int32) for r in RIGHT_SLOTS)
            done_left = t - done_right
            now_right = sum((t == r).astype(jnp.int32) for r in RIGHT_SLOTS)
            is_right = (1 - later) * (1 - t % 2) + later * now_right

            @pl.when(j == 0)
            def _():
                @pl.when(t == 4)
                def _():
                    l_last(False)

                @pl.when(t == 12)
                def _():
                    l_last(True)

                @pl.when(t % 4 == 0)
                def _():
                    lax.fori_loop(0, 4, l_fill, first_grp)

            @pl.when(j > 0)
            def _():
                for four in range(0, len(SLOTS), 4):
                    @pl.when((t >= four) & (t < four + 4))
                    def _():
                        for at in range(four, four + 4):
                            if not SLOTS[at]:
                                continue

                            @pl.when(t == at)
                            def _():
                                for kind, i, p in SLOTS[at]:
                                    act(kind, i, p, j)

            @pl.when((is_right == 1) & (j == 0))
            def _():
                right_of_group(first_grp, first_ch)

            @pl.when((is_right == 1) & (j > 0))
            def _():
                right_of_piece(done_right // QUARTERS, done_right % QUARTERS)

            @pl.when(is_right == 0)
            def _():
                left_products((1 - later) * first_ch + later * (done_left // GROUPS), (1 - later) * first_grp + later * (done_left % GROUPS))
            return carry

        lax.fori_loop(0, len(SLOTS), slot_step, 0)

        @pl.when(j > 0)
        def _():
            for p in range(PIECES):
                sent = uv.at[p // QUARTERS, pl.ds(0, 2), pl.ds(0, 15 * d.slab), :]
                remote(sent, sent, u_send.at[p], u_recv.at[p, 0], me).wait_send()

        other = sig.at[:, pl.ds(d.half, d.half)]
        to_other = remote(other, part, p_send, p_recv, partner)
        to_other.start()
        to_other.wait()
        s = sig[:, :d.half] + part[...]
        v = vcur[...]
        w = s - beta_prev * vprev[...]
        sv = jnp.sum(s * v, keepdims=True)
        wv_sum = jnp.sum(w * v, keepdims=True)
        vv = jnp.sum(v * v, keepdims=True)
        guess = jnp.where(vv > 0.0, wv_sum / jnp.where(vv > 0.0, vv, 1.0), 0.0)
        t = w - guess * v
        sig[:, :d.half] = t
        tt = jnp.sum(t * t, keepdims=True)
        tv = jnp.sum(t * v, keepdims=True)
        tile_row = lax.broadcasted_iota(jnp.int32, (8, 128), 0)
        tile = jnp.zeros((8, 128), jnp.float32)
        for n, value in enumerate((sv, vv, tt, tv, guess)):
            tile = jnp.where(tile_row == n, value, tile)
        scs[...] = tile
        scr[me] = tile

        def tell(n, carry):
            remote(scs, scr.at[me], s_send, s_recv, (me + n) % DEVS).start()
            return carry

        lax.fori_loop(1, DEVS, tell, 0)
        heard = scr.at[pl.ds(0, DEVS - 1)]
        remote(heard, heard, s_send, s_recv, me).wait()
        alpha = jnp.sum(scr[:, 0, :], axis=0, keepdims=True) / d.vec_size
        off = alpha - scr[:, 4, :]
        square = scr[:, 2, :] - 2.0 * off * scr[:, 3, :] + off * off * scr[:, 1, :]
        beta = jnp.sqrt(jnp.sum(square, axis=0, keepdims=True) / d.vec_size)
        info[0, pl.ds(j, 1), :] = alpha
        info[1, pl.ds(j, 1), :] = beta
        vnew = (sig[:, :d.half] - (alpha[:, 0:1] - guess) * vcur[...]) / beta[:, 0:1]
        vprev[...] = vcur[...]
        vcur[...] = vnew
        vb = vnew.astype(jnp.bfloat16)

        @pl.when(j < LANCZOS_STEPS - 1)
        def _():
            for ch in range(CHUNKS):
                for bh in range(2):
                    at = pl.ds(pl.multiple_of(slot * d.slab + bh * d.sub, d.sub), d.sub)
                    for q in range(d.pair):
                        uv[ch, q // 2, at, q % 2 * d.chunk:(q % 2 + 1) * d.chunk] = \
                            vb[(bh * d.pair + q) * d.sub:(bh * d.pair + q + 1) * d.sub, ch * d.chunk:(ch + 1) * d.chunk]
        return beta[:, 0:1]


    lax.fori_loop(0, LANCZOS_STEPS, step, jnp.zeros((1, 1), jnp.float32))

    turn_result(LANCZOS_STEPS - 1)
    hand_out(LANCZOS_STEPS - 1)
    for n, part in enumerate((lv.at[0, pl.ds(0, 15), :, 0], lv.at[1, pl.ds(0, 15), :, 0, :, pl.ds(edge, d.bond - edge)],
                              lv.at[0, pl.ds(0, 15), :, 0, :, pl.ds(0, d.half)], lv.at[1, pl.ds(0, 15), :, 0, :, pl.ds(edge, d.half - edge)])):
        remote(part, part, l_send.at[n], l_recv.at[n, 0], me).wait_send()
    swapped = lv.at[:, pl.ds(0, 15), :, 0, :, pl.ds(d.half, d.half)]
    remote(swapped, swapped, f_send, f_recv.at[0], me).wait_send()
    for ch in range(CHUNKS):
        for h in range(2):
            theirs = left.at[:, pl.ds(0, d.chunk), pl.ds(0, d.half)]
            remote(theirs, lv.at[ch, slot, core, :, :, pl.ds(h * d.half, d.half)], d2d_sem.at[ch, h], d2d_recv.at[ch, h], partner).wait_send()

    sends_self = me // CHIPS == core

    @pl.when(sends_self)
    def _():
        some = gbuf.at[:, pl.ds(0, CHIPS - 1)]
        remote(some, some, k_send, k_recv, me).wait()

    @pl.when(jnp.logical_not(sends_self))
    def _():
        remote(gbuf, gbuf, k_send, k_recv, me).wait()

    wide = TILE_PARTS * d.slab
    lanes = lax.broadcasted_iota(jnp.int32, (d.out_rows, wide), 1) // d.slab

    def put_out(j, carry):
        for ct in range(CHIPS // TILE_PARTS):
            for qt in range(d.pair // TILE_PARTS):
                src = [gbuf[j, ct * TILE_PARTS + c, :, qt * wide:(qt + 1) * wide] for c in range(TILE_PARTS)]
                for q in range(TILE_PARTS):
                    tile = jnp.zeros((d.out_rows, wide), jnp.float32)
                    for c in range(TILE_PARTS):
                        shift = (c - q) % TILE_PARTS * d.slab
                        moved = pltpu.roll(src[c], shift, 1) if shift else src[c]
                        tile = jnp.where(lanes == c, moved, tile)
                    at = (qt * TILE_PARTS + q) * d.out_rows
                    tbuf[j, at:at + d.out_rows, ct * wide:(ct + 1) * wide] = tile
        pltpu.make_async_copy(tbuf.at[j], out.at[j], o_sem).start()
        return carry

    lax.fori_loop(0, LANCZOS_STEPS, put_out, 0)
    pltpu.make_async_copy(tbuf, out, o_sem).wait()


def solution(mesh):
    def device_body(wavefunction, left_loc, pair_loc, right_loc, flag_loc):
        bond, pair = wavefunction.shape[0], wavefunction.shape[1]
        d = Dims(bond, pair, left_loc.shape[0])
        eye = jnp.eye(bond, dtype=jnp.bfloat16)
        right_used = jnp.where((flag_loc == 1)[:, None, None], right_loc, eye)
        pair_wide = jnp.repeat(pair_loc, d.sub, axis=2)
        bf16, f32 = jnp.bfloat16, jnp.float32
        dma = pltpu.SemaphoreType.DMA
        any_space = pl.BlockSpec(memory_space=pl.ANY)
        rows_out, info = pl.pallas_call(
            functools.partial(lanczos_kernel, d),
            out_shape=(jax.ShapeDtypeStruct((LANCZOS_STEPS, d.half, bond), f32), jax.ShapeDtypeStruct((3, 8, 128), f32)),
            in_specs=[any_space] * 4,
            out_specs=(any_space, pl.BlockSpec(memory_space=pltpu.VMEM)),
            scratch_shapes=[
                pltpu.VMEM((CHUNKS, CHIPS, CORES, d.terms_dev, d.chunk, bond), bf16),
                pltpu.VMEM((CHIPS, CORES, d.terms_dev, d.slab, bond), bf16),
                pltpu.VMEM((CHIPS, CORES, d.terms_dev, pair, d.prod), bf16),
                pltpu.VMEM((CHIPS, CORES, d.terms_dev, d.prod, d.prod), bf16),
                pltpu.VMEM((CHUNKS, pair // 2, bond, 2 * d.chunk), bf16),
                pltpu.VMEM((d.lane_tiles, d.half * pair, d.lane), f32),
                pltpu.VMEM((CHIPS * CORES * d.terms_dev, pair, d.sub, 2 * d.chunk), bf16),
                pltpu.VMEM((d.rows, d.group_terms * d.chunk), bf16),
                pltpu.VMEM((d.rows, bond), f32),
                pltpu.VMEM((d.rows, d.half), f32),
                pltpu.VMEM((d.rows, d.half), f32),
                pltpu.VMEM((d.rows, d.half), f32),
                pltpu.VMEM((LANCZOS_STEPS, d.half, bond), f32),
                pltpu.VMEM((LANCZOS_STEPS, CHIPS, d.out_rows, bond), f32),
                pltpu.VMEM((8, 128), f32),
                pltpu.VMEM((DEVS, 8, 128), f32),
                pltpu.VMEM((2, 8, 128), f32),
                dma((3, 2)), dma((8, d.lane_tiles)), dma((CHUNKS, 2)), dma((CHUNKS, 2)), dma((2,)), dma((2,)), dma((2,)), dma((2,)),
                dma((4,)), dma((4, CHIPS)), dma, dma((CHIPS,)), dma((PIECES,)), dma((PIECES, CHIPS)),
                dma, dma, dma, dma, dma, dma, dma, dma, dma,
            ],
            compiler_params=pltpu.CompilerParams(has_side_effects=True, vmem_limit_bytes=67043328),
            name='lanczos',
        )(wavefunction.reshape(bond * pair, bond), left_loc, right_used, pair_wide)
        row_start = lax.axis_index(AXIS_NAME) * d.out_rows
        first = lax.dynamic_slice_in_dim(wavefunction, row_start, d.out_rows, axis=0) / info[2, 0, 0]
        later = rows_out.reshape(LANCZOS_STEPS, pair, d.out_rows, bond).transpose(0, 2, 1, 3)
        return jnp.concatenate([first[None], later]), info[0, :LANCZOS_STEPS, 0], info[1, :LANCZOS_STEPS, 0]

    return jax.shard_map(device_body, mesh=mesh, in_specs=(P(), P(AXIS_NAME), P(AXIS_NAME), P(AXIS_NAME), P(AXIS_NAME)),
                         out_specs=(P(None, AXIS_NAME), P(), P()), check_vma=False)
```

```python
import functools

import jax
import jax.numpy as jnp
from jax import lax
from jax.experimental import pallas as pl
from jax.experimental.pallas import tpu as pltpu
from jax.sharding import PartitionSpec as P

LANCZOS_STEPS = 6
AXIS_NAME = 'terms'
MESH = pl.DeviceIdType.MESH

CHIPS = 16
CORES = 2
DEVS = 32
CHUNKS = 2
GROUPS = 4
TILE_PARTS = 4
QUARTERS = 4
PIECES = CHUNKS * QUARTERS

ALONG, ACROSS, FROM_COLUMN, FROM_SECOND, THIRD, DIAGONAL, RESULT, RESULT_OUT = range(8)
RIGHT_SLOTS = (0, 1, 2, 3, 8, 9, 10, 11)
SLOTS = (
    ((1, 0, 1), (1, 0, 6), (0, 1, 1), (1, 0, 2), (1, 0, 3), (0, 1, 2), (1, 0, 4), (1, 0, 7), (0, 2, 2), (1, 0, 5), (0, 1, 3), (0, 1, 0), (0, 2, 0), (0, 3, 0), (0, 3, 1), (0, 2, 1), (0, 3, 2), (1, 0, 0), (3, 0, 3), (3, 0, 2), (2, 1, 2), (2, 1, 1), (0, 3, 3), (2, 1, 0), (2, 2, 0), (3, 0, 0), (2, 2, 1), (3, 1, 1), (0, 2, 3), (2, 2, 2), (3, 1, 0), (2, 3, 0), (3, 2, 0), (3, 0, 1), (2, 2, 3), (0, 3, 4), (2, 3, 1), (2, 3, 2), (0, 3, 5), (3, 3, 0), (0, 1, 4), (0, 2, 4), (0, 1, 5), (2, 1, 3), (3, 2, 1), (3, 2, 3), (3, 3, 1), (0, 2, 5), (0, 1, 6), (2, 3, 3), (0, 3, 7), (3, 3, 2), (3, 1, 3), (0, 3, 6), (3, 2, 2), (0, 2, 6), (3, 1, 2), (0, 2, 7), (3, 3, 3), (5, 0, 0), (3, 0, 4), (4, 0, 1), (4, 0, 0), (3, 0, 5),),
    ((6, 0, 0), (2, 3, 4), (4, 0, 2), (3, 0, 6), (5, 0, 1),),
    ((2, 2, 4), (2, 1, 4), (2, 1, 5), (5, 0, 2), (2, 2, 5),),
    ((5, 0, 3), (0, 1, 7), (3, 3, 4), (4, 0, 3), (2, 3, 5), (2, 1, 6), (2, 2, 6),),
    (),
    ((4, 0, 4), (2, 3, 6), (3, 1, 4), (2, 2, 7), (3, 2, 4), (7, 0, 0),),
    ((3, 3, 5), (3, 2, 5), (3, 1, 5), (2, 3, 7), (2, 1, 7),),
    ((3, 1, 6), (3, 3, 6),),
    ((4, 0, 5), (3, 2, 6), (3, 0, 7), (4, 0, 6), (5, 0, 4), (3, 3, 7), (3, 2, 7),),
    ((5, 0, 5), (3, 1, 7),),
    ((4, 0, 7), (5, 0, 6),),
    ((5, 0, 7), (7, 1, 0),),
    (),
    (),
    (),
    (),
)


class Dims:
    def __init__(self, bond, pair, terms_dev):
        self.bond = bond
        self.pair = pair
        self.terms_dev = terms_dev
        self.slab = bond // CHIPS
        self.sub = self.slab // 2
        self.half = bond // CORES
        self.chunk = self.half // CHUNKS
        self.rows = self.slab * pair
        self.prod = self.sub * pair
        self.out_rows = bond // DEVS
        self.group_terms = 4 * CORES * terms_dev
        self.vec_size = bond * pair * bond
        self.lane = min(bond, 128)
        self.lane_tiles = bond // self.lane


def lanczos_kernel(d, psi, left, right, wexp, out, info, lv, rv, wv, kw, uv, ps, yst, zst, sig, part, vcur, vprev, tbuf, gbuf, scs, scr, nbuf,
                   loc_sem, psi_sem, d2d_sem, d2d_recv, rw_send, rw_recv, fw_send, fw_recv, l_send, l_recv, f_send, f_recv, u_send, u_recv,
                   p_send, p_recv, s_send, s_recv, k_send, k_recv, n_send, n_recv, o_sem):
    me = lax.axis_index(AXIS_NAME)
    core = me % 2
    xpos = (me // 2) % 2
    ypos = (me // 4) % 2
    zpos = me // 8

    def device(z, y, x, c):
        return ((z * 2 + y) * 2 + x) * 2 + c

    def chip_slot(z, y, x):
        return (x * 2 + y) * 4 + z

    partner = device(zpos, ypos, xpos, 1 - core)
    slot = chip_slot(zpos, ypos, xpos)
    zs = (zpos, zpos + 1 - 2 * (zpos % 2), (zpos + 2) % 4, 3 - zpos)
    inner = (zpos + 1) // 2 % 2
    zn = (zpos, (1 - inner) * (zpos + 1 - zpos // 3 * 2) + inner * (zpos - 1), (1 - inner) * ((zpos + 2) % 4) + inner * (zpos + 1),
          (1 - inner) * (3 - zpos) + inner * ((zpos + 2) % 4))
    y_two = ypos + (1 - core) * (1 - 2 * ypos)
    x_two = xpos + core * (1 - 2 * xpos)
    y_three = ypos + core * (1 - 2 * ypos)
    x_three = xpos + (1 - core) * (1 - 2 * xpos)
    two = device(zpos, y_two, x_two, core)
    three = device(zpos, y_three, x_three, core)

    def remote(src, dst, send, recv, dev):
        return pltpu.make_async_remote_copy(src_ref=src, dst_ref=dst, send_sem=send, recv_sem=recv, device_id=(dev,), device_id_type=MESH)

    class Gather:
        def __init__(self, block, send, recv):
            self.block, self.send_sem, self.recv_sem = block, send, recv

        def send(self, which, dev):
            remote(self.block(which), self.block(which), self.send_sem, self.recv_sem(which), dev).start()

        def wait(self, which):
            remote(self.block(which), self.block(which), self.send_sem, self.recv_sem(which), me).wait_recv()

        def own_along(self):
            for i in (1, 2, 3):
                self.send(slot, device(zs[i], ypos, xpos, core))

        def own_across(self):
            self.send(slot, three)
            self.send(slot, two)

        def event(self, n):
            i = (n + 1) // 2
            if n % 2:
                which = chip_slot(zs[i], ypos, xpos)
                self.wait(which)
                self.send(which, three)
                self.send(which, two)
            else:
                which = chip_slot(zs[i], y_two, x_two)
                self.wait(which)
                self.send(which, three)

        def last(self, diagonal):
            for i in range(4):
                self.wait(chip_slot(zs[i], 1 - ypos, 1 - xpos) if diagonal else chip_slot(zs[i], y_three, x_three))

    edge = d.chunk
    l_parts = (
        (lambda s: lv.at[0, s, :, core], 0),
        (lambda s: lv.at[1, s, :, core, :, pl.ds(edge, d.bond - edge)], 1),
        (lambda s: lv.at[0, s, :, 1 - core, :, pl.ds(0, d.half)], 2),
        (lambda s: lv.at[1, s, :, 1 - core, :, pl.ds(edge, d.half - edge)], 3),
    )
    l_gathers = [Gather(block, l_send.at[n], lambda s, n=n: l_recv.at[n, s]) for block, n in l_parts]

    def l_swap(s, term):
        part = lv.at[:, s, :, term, :, pl.ds(d.half, d.half)]
        return remote(part, part, f_send, f_recv.at[s], partner)

    def l_event(n):
        i = (n + 1) // 2
        for g in l_gathers:
            g.event(n)
        l_swap(chip_slot(zs[i], ypos, xpos) if n % 2 else chip_slot(zs[i], y_two, x_two), core).start()

    def l_last(diagonal):
        for i in range(4):
            which = chip_slot(zs[i], 1 - ypos, 1 - xpos) if diagonal else chip_slot(zs[i], y_three, x_three)
            for g in l_gathers:
                g.wait(which)
            l_swap(which, core).start()

    def l_fill(n, grp):
        s = grp * 4 + n

        @pl.when(s != slot)
        def _():
            l_swap(s, 1 - core).wait_recv()
            for c in range(CORES):
                tile = lv[:, s, c, 1 - core, :, d.half:].reshape(d.half, d.half).T
                lv[:, s, c, 1 - core, :, d.half:] = tile.reshape(CHUNKS, d.chunk, d.half)
                for t in range(d.terms_dev):
                    lv[1, s, c, t, :, :edge] = lv[0, s, c, t, :, edge:d.half].T
        return grp

    def l_along():
        for i in (1, 2, 3):
            for g in l_gathers:
                g.send(slot, device(zs[i], ypos, xpos, core))

    def u_block(p):
        return lambda s: uv.at[p // QUARTERS, pl.ds(p % QUARTERS * 2, 2), pl.ds(pl.multiple_of(s * d.slab, d.slab), d.slab), :]

    u_gathers = [Gather(u_block(p), u_send.at[p], lambda s, p=p: u_recv.at[p, s]) for p in range(PIECES)]

    def act(kind, i, p, j):
        g = u_gathers[p]
        if kind == ALONG:
            g.send(slot, device(zn[i], ypos, xpos, core))
        elif kind == ACROSS:
            g.own_across()
        elif kind == FROM_COLUMN:
            which = chip_slot(zn[i], ypos, xpos)
            g.wait(which)
            g.send(which, three)
            g.send(which, two)
        elif kind == FROM_SECOND:
            which = chip_slot(zn[i], y_two, x_two)
            g.wait(which)
            g.send(which, three)
        elif kind == THIRD:
            g.last(False)
        elif kind == DIAGONAL:
            g.last(True)
        elif kind == RESULT:
            turn_result(j - 1)
        elif kind == RESULT_OUT:
            hand_out(j - 1, ((0,), (3, 1, 2))[i])

    for ch in range(CHUNKS):
        for h in range(2):
            mine = left.at[:, pl.ds(pl.multiple_of(core * d.half + ch * d.chunk, d.chunk), d.chunk),
                           pl.ds(pl.multiple_of((core + h) % 2 * d.half, d.half), d.half)]
            theirs = left.at[:, pl.ds(pl.multiple_of((1 - core) * d.half + ch * d.chunk, d.chunk), d.chunk),
                             pl.ds(pl.multiple_of((1 - core + h) % 2 * d.half, d.half), d.half)]
            remote(theirs, lv.at[ch, slot, core, :, :, pl.ds(h * d.half, d.half)], d2d_sem.at[ch, h], d2d_recv.at[ch, h], partner).start()
            pltpu.make_async_copy(mine, lv.at[ch, slot, core, :, :, pl.ds(h * d.half, d.half)], loc_sem.at[ch, h]).start()

    psi_rows = d.half * d.pair // 8
    psi_copies = [pltpu.make_async_copy(psi.at[pl.ds(pl.multiple_of(core * d.half * d.pair + n * psi_rows, psi_rows), psi_rows),
                                               pl.ds(c * d.lane, d.lane)],
                                        ps.at[c, pl.ds(n * psi_rows, psi_rows), :], psi_sem.at[n, c])
                  for n in range(8) for c in range(d.lane_tiles)]
    for copy in psi_copies:
        copy.start()

    def right_rows(s):
        return right.at[:, pl.ds(pl.multiple_of(s * d.slab, d.slab), d.slab), :]

    own_right = pltpu.make_async_copy(right_rows(slot), rv.at[slot, core], loc_sem.at[2, 0])
    own_pair = pltpu.make_async_copy(wexp, wv.at[slot, core], loc_sem.at[2, 1])
    own_right.start()
    own_pair.start()
    for n in range(1, CHIPS):
        chip = (me // 2 + n) % CHIPS
        to = chip_slot(chip // 4, chip // 2 % 2, chip % 2)
        remote(right_rows(to), rv.at[slot, core], rw_send.at[0], rw_recv.at[0], chip * 2 + core).start()
        remote(wexp, wv.at[slot, core], rw_send.at[1], rw_recv.at[1], chip * 2 + core).start()

    for ch in range(CHUNKS):
        for h in range(2):
            pltpu.make_async_copy(lv.at[ch, slot, core, :, :, pl.ds(h * d.half, d.half)], lv.at[ch, slot, core, :, :, pl.ds(h * d.half, d.half)], loc_sem.at[ch, h]).wait()
            back = remote(lv.at[ch, slot, 1 - core, :, :, pl.ds(h * d.half, d.half)], lv.at[ch, slot, 1 - core, :, :, pl.ds(h * d.half, d.half)], d2d_sem.at[ch, h], d2d_recv.at[ch, h], partner)
            back.wait_recv()
    l_along()
    for g in l_gathers:
        g.own_across()

    total = jnp.zeros((8, d.lane), jnp.float32)
    for n in range(8):
        for copy in psi_copies[n * d.lane_tiles:(n + 1) * d.lane_tiles]:
            copy.wait()

        def add_rows(i, acc, n=n):
            x = ps[:, pl.ds(pl.multiple_of(n * psi_rows + i * (psi_rows // 8), 8), psi_rows // 8), :]
            return acc + jnp.sum((x * x).reshape(d.lane_tiles * psi_rows // 64, 8, d.lane), axis=0)

        total = lax.fori_loop(0, 8, add_rows, total)
    nbuf[0] = jnp.broadcast_to(jnp.sum(total, keepdims=True), (8, 128))
    to_partner = remote(nbuf.at[0], nbuf.at[1], n_send, n_recv, partner)
    to_partner.start()
    to_partner.wait()
    norm = jnp.sqrt((nbuf[0] + nbuf[1])[0:1, :] / d.vec_size)
    info[2] = jnp.broadcast_to(norm, (8, 128))
    norm_one = norm[:, 0:1]

    def place(q):
        tiles = [(ps[c, pl.ds(q, d.half, stride=d.pair), :] / norm_one).T for c in range(d.lane_tiles)]
        xt = jnp.concatenate(tiles, axis=0)
        vprev[...] = xt
        return xt.astype(jnp.bfloat16)

    def start_vector(qb, carry):
        for q2 in range(2):
            q = qb * 2 + q2
            xb = place(q)
            for ch in range(CHUNKS):
                uv[ch, qb, :, q2 * d.chunk:(q2 + 1) * d.chunk] = xb[:, ch * d.chunk:(ch + 1) * d.chunk]
            for bh in range(2):
                rows = vprev[pl.ds(pl.multiple_of(slot * d.slab + bh * d.sub, d.sub), d.sub), :]
                vcur[pl.ds(pl.multiple_of((bh * d.pair + q) * d.sub, d.sub), d.sub), :] = rows
        return carry

    lax.fori_loop(0, d.pair // 4, start_vector, 0)
    own_right.wait()
    own_pair.wait()
    fifteen = rv.at[pl.ds(0, CHIPS - 1), 0]
    fifteen_w = wv.at[pl.ds(0, CHIPS - 1), 0]
    remote(fifteen, fifteen, rw_send.at[0], rw_recv.at[0], me).wait()
    remote(fifteen_w, fifteen_w, rw_send.at[1], rw_recv.at[1], me).wait()
    fw_right = remote(rv.at[:, core], rv.at[:, core], fw_send.at[0], fw_recv.at[0], partner)
    fw_pair = remote(wv.at[:, core], wv.at[:, core], fw_send.at[1], fw_recv.at[1], partner)
    fw_right.start()
    fw_pair.start()
    l_event(0)
    l_event(1)
    lax.fori_loop(d.pair // 4, d.pair // 2, start_vector, 0)
    l_event(2)
    l_event(3)
    fw_right.wait()
    fw_pair.wait()
    lane = lax.broadcasted_iota(jnp.int32, (d.sub, d.prod), 1)
    row = lax.broadcasted_iota(jnp.int32, (d.sub, d.prod), 0)
    diagonal = lane % d.sub == row

    def spread_pair(s, carry):
        for c in range(2):
            for t in range(d.terms_dev):
                w = wv[s, c, t].astype(jnp.float32)
                for q in range(d.pair):
                    full = jnp.where(diagonal, jnp.broadcast_to(w[q:q + 1, :], (d.sub, d.prod)), 0.0)
                    kw[s, c, t, q * d.sub:(q + 1) * d.sub, :] = full.astype(jnp.bfloat16)
        return carry

    lax.fori_loop(0, CHIPS, spread_pair, 0)
    l_event(4)
    l_event(5)
    l_event(6)
    vprev[...] = jnp.zeros_like(vprev)

    def right_product(grp, ch, qb):
        r_all = rv[pl.ds(grp * 4, 4)].reshape(d.group_terms * d.slab, d.bond)
        y = jnp.dot(r_all, uv[ch, qb], preferred_element_type=jnp.float32).astype(jnp.bfloat16)
        y = y.reshape(d.group_terms, 2, d.sub, 2 * d.chunk)
        for q2 in range(2):
            for bh in range(2):
                yst[pl.ds(grp * d.group_terms, d.group_terms), qb * 2 + q2, :, bh * d.chunk:(bh + 1) * d.chunk] = \
                    y[:, bh, :, q2 * d.chunk:(q2 + 1) * d.chunk]

    def right_of_group(grp, ch):
        for qb in range(d.pair // 2):
            right_product(grp, ch, qb)

    def right_of_piece(ch, part):
        for qb in range(2):
            for grp in range(GROUPS):
                right_product(grp, ch, part * 2 + qb)

    def left_products(ch, grp):
        for k in range(d.group_terms):
            w = kw[grp * 4 + k // 4, k // 2 % 2, k % 2]
            z = jnp.dot(w, yst[grp * d.group_terms + k].reshape(d.prod, 2 * d.chunk), preferred_element_type=jnp.float32).astype(jnp.bfloat16)
            for bh in range(2):
                zst[bh * d.prod:(bh + 1) * d.prod, k * d.chunk:(k + 1) * d.chunk] = z[:, bh * d.chunk:(bh + 1) * d.chunk]
        l_all = lv[ch, pl.ds(grp * 4, 4)].reshape(d.group_terms * d.chunk, d.bond)
        sig[...] += jnp.dot(zst[...], l_all, preferred_element_type=jnp.float32)

    def turn_result(j):
        wide = TILE_PARTS * d.slab
        for n in range(d.pair // TILE_PARTS):
            rows = [vcur[(bh * d.pair + q) * d.sub:(bh * d.pair + q + 1) * d.sub, :]
                    for q in range(n * TILE_PARTS, (n + 1) * TILE_PARTS) for bh in range(2)]
            tbuf[j, :, n * wide:(n + 1) * wide] = jnp.concatenate(rows, axis=0).T

    def hand_out(j, planes):
        for plane in planes:
            y, x = (ypos + plane // 2 * (1 - 2 * ypos), xpos + plane % 2 * (1 - 2 * xpos))
            for n in range(4):
                to = device(core * 2 + (zpos + n // 2) % 2, y, x, n % 2)
                block = tbuf.at[j, pl.ds(pl.multiple_of((to - core * CHIPS) * d.out_rows, d.out_rows), d.out_rows), :]

                @pl.when(to != me)
                def _():
                    remote(block, gbuf.at[j, slot], k_send, k_recv, to).start()

                @pl.when(to == me)
                def _():
                    gbuf[j, slot] = block[...]

    def step(j, beta_prev):
        later = jnp.minimum(j, 1)
        own = xpos * 2 + ypos
        sig[...] = jnp.zeros_like(sig)

        def slot_step(t, carry):
            n = t // 4
            first_grp = jnp.where(n == 0, own, jnp.where(n == 1, x_two * 2 + y_two, jnp.where(n == 2, x_three * 2 + y_three, 3 - own)))
            first_ch = t // 2 % 2
            done_right = sum((t > r).astype(jnp.int32) for r in RIGHT_SLOTS)
            done_left = t - done_right
            now_right = sum((t == r).astype(jnp.int32) for r in RIGHT_SLOTS)
            is_right = (1 - later) * (1 - t % 2) + later * now_right

            @pl.when(j == 0)
            def _():
                @pl.when(t == 4)
                def _():
                    l_last(False)

                @pl.when(t == 12)
                def _():
                    l_last(True)

                @pl.when(t % 4 == 0)
                def _():
                    lax.fori_loop(0, 4, l_fill, first_grp)

            @pl.when(j > 0)
            def _():
                for four in range(0, len(SLOTS), 4):
                    @pl.when((t >= four) & (t < four + 4))
                    def _():
                        for at in range(four, four + 4):
                            if not SLOTS[at]:
                                continue

                            @pl.when(t == at)
                            def _():
                                for kind, i, p in SLOTS[at]:
                                    act(kind, i, p, j)

            @pl.when((is_right == 1) & (j == 0))
            def _():
                right_of_group(first_grp, first_ch)

            @pl.when((is_right == 1) & (j > 0))
            def _():
                right_of_piece(done_right // QUARTERS, done_right % QUARTERS)

            @pl.when(is_right == 0)
            def _():
                left_products((1 - later) * first_ch + later * (done_left // GROUPS), (1 - later) * first_grp + later * (done_left % GROUPS))
            return carry

        lax.fori_loop(0, len(SLOTS), slot_step, 0)

        @pl.when(j > 0)
        def _():
            for p in range(PIECES):
                sent = uv.at[p // QUARTERS, pl.ds(0, 2), pl.ds(0, 15 * d.slab), :]
                remote(sent, sent, u_send.at[p], u_recv.at[p, 0], me).wait_send()

        other = sig.at[:, pl.ds(d.half, d.half)]
        to_other = remote(other, part, p_send, p_recv, partner)
        to_other.start()
        to_other.wait()
        s = sig[:, :d.half] + part[...]
        v = vcur[...]
        w = s - beta_prev * vprev[...]
        sv = jnp.sum(s * v, keepdims=True)
        wv_sum = jnp.sum(w * v, keepdims=True)
        vv = jnp.sum(v * v, keepdims=True)
        guess = jnp.where(vv > 0.0, wv_sum / jnp.where(vv > 0.0, vv, 1.0), 0.0)
        t = w - guess * v
        sig[:, :d.half] = t
        tt = jnp.sum(t * t, keepdims=True)
        tv = jnp.sum(t * v, keepdims=True)
        tile_row = lax.broadcasted_iota(jnp.int32, (8, 128), 0)
        tile = jnp.zeros((8, 128), jnp.float32)
        for n, value in enumerate((sv, vv, tt, tv, guess)):
            tile = jnp.where(tile_row == n, value, tile)
        scs[...] = tile
        scr[me] = tile

        def tell(n, carry):
            remote(scs, scr.at[me], s_send, s_recv, (me + n) % DEVS).start()
            return carry

        lax.fori_loop(1, DEVS, tell, 0)
        heard = scr.at[pl.ds(0, DEVS - 1)]
        remote(heard, heard, s_send, s_recv, me).wait()
        alpha = jnp.sum(scr[:, 0, :], axis=0, keepdims=True) / d.vec_size
        off = alpha - scr[:, 4, :]
        square = scr[:, 2, :] - 2.0 * off * scr[:, 3, :] + off * off * scr[:, 1, :]
        beta = jnp.sqrt(jnp.sum(square, axis=0, keepdims=True) / d.vec_size)
        info[0, pl.ds(j, 1), :] = alpha
        info[1, pl.ds(j, 1), :] = beta
        vnew = (sig[:, :d.half] - (alpha[:, 0:1] - guess) * vcur[...]) / beta[:, 0:1]
        vprev[...] = vcur[...]
        vcur[...] = vnew
        vb = vnew.astype(jnp.bfloat16)

        @pl.when(j < LANCZOS_STEPS - 1)
        def _():
            for ch in range(CHUNKS):
                for bh in range(2):
                    at = pl.ds(pl.multiple_of(slot * d.slab + bh * d.sub, d.sub), d.sub)
                    for q in range(d.pair):
                        uv[ch, q // 2, at, q % 2 * d.chunk:(q % 2 + 1) * d.chunk] = \
                            vb[(bh * d.pair + q) * d.sub:(bh * d.pair + q + 1) * d.sub, ch * d.chunk:(ch + 1) * d.chunk]
        return beta[:, 0:1]


    lax.fori_loop(0, LANCZOS_STEPS, step, jnp.zeros((1, 1), jnp.float32))

    turn_result(LANCZOS_STEPS - 1)
    hand_out(LANCZOS_STEPS - 1, (3, 1, 2, 0))
    for n, part in enumerate((lv.at[0, pl.ds(0, 15), :, 0], lv.at[1, pl.ds(0, 15), :, 0, :, pl.ds(edge, d.bond - edge)],
                              lv.at[0, pl.ds(0, 15), :, 0, :, pl.ds(0, d.half)], lv.at[1, pl.ds(0, 15), :, 0, :, pl.ds(edge, d.half - edge)])):
        remote(part, part, l_send.at[n], l_recv.at[n, 0], me).wait_send()
    swapped = lv.at[:, pl.ds(0, 15), :, 0, :, pl.ds(d.half, d.half)]
    remote(swapped, swapped, f_send, f_recv.at[0], me).wait_send()
    for ch in range(CHUNKS):
        for h in range(2):
            theirs = left.at[:, pl.ds(0, d.chunk), pl.ds(0, d.half)]
            remote(theirs, lv.at[ch, slot, core, :, :, pl.ds(h * d.half, d.half)], d2d_sem.at[ch, h], d2d_recv.at[ch, h], partner).wait_send()

    sends_self = me // CHIPS == core

    @pl.when(sends_self)
    def _():
        some = gbuf.at[:, pl.ds(0, CHIPS - 1)]
        remote(some, some, k_send, k_recv, me).wait()

    @pl.when(jnp.logical_not(sends_self))
    def _():
        remote(gbuf, gbuf, k_send, k_recv, me).wait()

    wide = TILE_PARTS * d.slab
    lanes = lax.broadcasted_iota(jnp.int32, (d.out_rows, wide), 1) // d.slab

    def put_out(j, carry):
        for ct in range(CHIPS // TILE_PARTS):
            for qt in range(d.pair // TILE_PARTS):
                src = [gbuf[j, ct * TILE_PARTS + c, :, qt * wide:(qt + 1) * wide] for c in range(TILE_PARTS)]
                for q in range(TILE_PARTS):
                    tile = jnp.zeros((d.out_rows, wide), jnp.float32)
                    for c in range(TILE_PARTS):
                        shift = (c - q) % TILE_PARTS * d.slab
                        moved = pltpu.roll(src[c], shift, 1) if shift else src[c]
                        tile = jnp.where(lanes == c, moved, tile)
                    at = (qt * TILE_PARTS + q) * d.out_rows
                    tbuf[j, at:at + d.out_rows, ct * wide:(ct + 1) * wide] = tile
        pltpu.make_async_copy(tbuf.at[j], out.at[j], o_sem).start()
        return carry

    lax.fori_loop(0, LANCZOS_STEPS, put_out, 0)
    pltpu.make_async_copy(tbuf, out, o_sem).wait()


def solution(mesh):
    def device_body(wavefunction, left_loc, pair_loc, right_loc, flag_loc):
        bond, pair = wavefunction.shape[0], wavefunction.shape[1]
        d = Dims(bond, pair, left_loc.shape[0])
        eye = jnp.eye(bond, dtype=jnp.bfloat16)
        right_used = jnp.where((flag_loc == 1)[:, None, None], right_loc, eye)
        pair_wide = jnp.repeat(pair_loc, d.sub, axis=2)
        bf16, f32 = jnp.bfloat16, jnp.float32
        dma = pltpu.SemaphoreType.DMA
        any_space = pl.BlockSpec(memory_space=pl.ANY)
        rows_out, info = pl.pallas_call(
            functools.partial(lanczos_kernel, d),
            out_shape=(jax.ShapeDtypeStruct((LANCZOS_STEPS, d.half, bond), f32), jax.ShapeDtypeStruct((3, 8, 128), f32)),
            in_specs=[any_space] * 4,
            out_specs=(any_space, pl.BlockSpec(memory_space=pltpu.VMEM)),
            scratch_shapes=[
                pltpu.VMEM((CHUNKS, CHIPS, CORES, d.terms_dev, d.chunk, bond), bf16),
                pltpu.VMEM((CHIPS, CORES, d.terms_dev, d.slab, bond), bf16),
                pltpu.VMEM((CHIPS, CORES, d.terms_dev, pair, d.prod), bf16),
                pltpu.VMEM((CHIPS, CORES, d.terms_dev, d.prod, d.prod), bf16),
                pltpu.VMEM((CHUNKS, pair // 2, bond, 2 * d.chunk), bf16),
                pltpu.VMEM((d.lane_tiles, d.half * pair, d.lane), f32),
                pltpu.VMEM((CHIPS * CORES * d.terms_dev, pair, d.sub, 2 * d.chunk), bf16),
                pltpu.VMEM((d.rows, d.group_terms * d.chunk), bf16),
                pltpu.VMEM((d.rows, bond), f32),
                pltpu.VMEM((d.rows, d.half), f32),
                pltpu.VMEM((d.rows, d.half), f32),
                pltpu.VMEM((d.rows, d.half), f32),
                pltpu.VMEM((LANCZOS_STEPS, d.half, bond), f32),
                pltpu.VMEM((LANCZOS_STEPS, CHIPS, d.out_rows, bond), f32),
                pltpu.VMEM((8, 128), f32),
                pltpu.VMEM((DEVS, 8, 128), f32),
                pltpu.VMEM((2, 8, 128), f32),
                dma((3, 2)), dma((8, d.lane_tiles)), dma((CHUNKS, 2)), dma((CHUNKS, 2)), dma((2,)), dma((2,)), dma((2,)), dma((2,)),
                dma((4,)), dma((4, CHIPS)), dma, dma((CHIPS,)), dma((PIECES,)), dma((PIECES, CHIPS)),
                dma, dma, dma, dma, dma, dma, dma, dma, dma,
            ],
            compiler_params=pltpu.CompilerParams(has_side_effects=True, vmem_limit_bytes=67043328),
            name='lanczos',
        )(wavefunction.reshape(bond * pair, bond), left_loc, right_used, pair_wide)
        row_start = lax.axis_index(AXIS_NAME) * d.out_rows
        first = lax.dynamic_slice_in_dim(wavefunction, row_start, d.out_rows, axis=0) / info[2, 0, 0]
        later = rows_out.reshape(LANCZOS_STEPS, pair, d.out_rows, bond).transpose(0, 2, 1, 3)
        return jnp.concatenate([first[None], later]), info[0, :LANCZOS_STEPS, 0], info[1, :LANCZOS_STEPS, 0]

    return jax.shard_map(device_body, mesh=mesh, in_specs=(P(), P(AXIS_NAME), P(AXIS_NAME), P(AXIS_NAME), P(AXIS_NAME)),
                         out_specs=(P(None, AXIS_NAME), P(), P()), check_vma=False)
```

```python
import functools

import jax
import jax.numpy as jnp
from jax import lax
from jax.experimental import pallas as pl
from jax.experimental.pallas import tpu as pltpu
from jax.sharding import PartitionSpec as P

LANCZOS_STEPS = 6
AXIS_NAME = 'terms'
MESH = pl.DeviceIdType.MESH

CHIPS = 16
CORES = 2
DEVS = 32
CHUNKS = 2
GROUPS = 4
TILE_PARTS = 4
QUARTERS = 4
PIECES = CHUNKS * QUARTERS

ALONG, ACROSS, FROM_COLUMN, FROM_SECOND, THIRD, DIAGONAL, RESULT, RESULT_OUT = range(8)
RIGHT_SLOTS = (0, 1, 2, 3, 8, 9, 10, 11)
SLOTS = (
    ((0, 1, 0), (0, 1, 1), (1, 0, 2), (0, 2, 0), (1, 0, 5), (1, 0, 3), (1, 0, 6), (1, 0, 0), (0, 3, 0), (3, 0, 2), (0, 2, 1), (0, 1, 3), (1, 0, 4), (0, 3, 1), (1, 0, 7), (0, 1, 2), (1, 0, 1), (0, 3, 3), (2, 1, 0), (2, 2, 0), (0, 2, 3), (0, 3, 2), (2, 1, 1), (3, 0, 0), (2, 3, 0), (3, 1, 0), (2, 2, 1), (0, 2, 2), (0, 1, 4), (3, 0, 1), (2, 1, 3), (3, 2, 0), (2, 3, 1), (2, 2, 2), (2, 2, 3), (2, 1, 2), (4, 0, 0), (0, 2, 5), (0, 3, 4), (0, 2, 4), (0, 1, 5), (0, 1, 6), (0, 1, 7), (3, 3, 0), (2, 3, 3), (3, 1, 1), (3, 2, 1), (0, 2, 6), (2, 3, 2), (4, 0, 1), (3, 3, 1), (0, 3, 6), (3, 2, 2), (3, 1, 2), (0, 3, 5), (0, 2, 7), (0, 3, 7), (3, 2, 3), (3, 3, 2), (3, 0, 3), (5, 0, 0), (3, 3, 3), (4, 0, 3), (3, 1, 3), (3, 0, 4),),
    ((6, 0, 0), (2, 2, 4), (5, 0, 1), (3, 0, 6), (2, 1, 4), (4, 0, 2),),
    ((2, 2, 6), (5, 0, 2), (2, 1, 6),),
    ((2, 2, 5), (5, 0, 3), (3, 2, 4), (2, 3, 4),),
    ((2, 1, 5), (3, 0, 5), (3, 1, 4),),
    ((2, 3, 5), (3, 2, 5), (2, 3, 6),),
    ((2, 2, 7), (3, 3, 4), (2, 1, 7), (3, 1, 5),),
    ((3, 3, 5), (2, 3, 7), (3, 2, 6), (3, 1, 6), (3, 3, 6),),
    ((3, 0, 7), (3, 1, 7), (3, 2, 7), (4, 0, 5), (5, 0, 4), (4, 0, 4),),
    ((3, 3, 7), (5, 0, 5),),
    ((4, 0, 6), (5, 0, 6),),
    ((4, 0, 7), (5, 0, 7), (7, 0, 0),),
    (),
    (),
    (),
    (),
)
RESULT_EARLY = 9


class Dims:
    def __init__(self, bond, pair, terms_dev):
        self.bond = bond
        self.pair = pair
        self.terms_dev = terms_dev
        self.slab = bond // CHIPS
        self.sub = self.slab // 2
        self.half = bond // CORES
        self.chunk = self.half // CHUNKS
        self.rows = self.slab * pair
        self.prod = self.sub * pair
        self.out_rows = bond // DEVS
        self.group_terms = 4 * CORES * terms_dev
        self.vec_size = bond * pair * bond
        self.lane = min(bond, 128)
        self.lane_tiles = bond // self.lane


def lanczos_kernel(d, psi, left, right, wexp, out, info, lv, rv, wv, kw, uv, ps, yst, zst, sig, part, vcur, vprev, tbuf, gbuf, scs, scr, nbuf,
                   loc_sem, psi_sem, d2d_sem, d2d_recv, rw_send, rw_recv, fw_send, fw_recv, l_send, l_recv, f_send, f_recv, u_send, u_recv,
                   p_send, p_recv, s_send, s_recv, k_send, k_recv, n_send, n_recv, o_sem):
    me = lax.axis_index(AXIS_NAME)
    core = me % 2
    xpos = (me // 2) % 2
    ypos = (me // 4) % 2
    zpos = me // 8

    def device(z, y, x, c):
        return ((z * 2 + y) * 2 + x) * 2 + c

    def chip_slot(z, y, x):
        return (x * 2 + y) * 4 + z

    partner = device(zpos, ypos, xpos, 1 - core)
    slot = chip_slot(zpos, ypos, xpos)
    zs = (zpos, zpos + 1 - 2 * (zpos % 2), (zpos + 2) % 4, 3 - zpos)
    inner = (zpos + 1) // 2 % 2
    zn = (zpos, (1 - inner) * (zpos + 1 - zpos // 3 * 2) + inner * (zpos - 1), (1 - inner) * ((zpos + 2) % 4) + inner * (zpos + 1),
          (1 - inner) * (3 - zpos) + inner * ((zpos + 2) % 4))
    y_two = ypos + (1 - core) * (1 - 2 * ypos)
    x_two = xpos + core * (1 - 2 * xpos)
    y_three = ypos + core * (1 - 2 * ypos)
    x_three = xpos + (1 - core) * (1 - 2 * xpos)
    two = device(zpos, y_two, x_two, core)
    three = device(zpos, y_three, x_three, core)

    def remote(src, dst, send, recv, dev):
        return pltpu.make_async_remote_copy(src_ref=src, dst_ref=dst, send_sem=send, recv_sem=recv, device_id=(dev,), device_id_type=MESH)

    class Gather:
        def __init__(self, block, send, recv):
            self.block, self.send_sem, self.recv_sem = block, send, recv

        def send(self, which, dev):
            remote(self.block(which), self.block(which), self.send_sem, self.recv_sem(which), dev).start()

        def wait(self, which):
            remote(self.block(which), self.block(which), self.send_sem, self.recv_sem(which), me).wait_recv()

        def own_along(self):
            for i in (1, 2, 3):
                self.send(slot, device(zs[i], ypos, xpos, core))

        def own_across(self):
            self.send(slot, three)
            self.send(slot, two)

        def event(self, n):
            i = (n + 1) // 2
            if n % 2:
                which = chip_slot(zs[i], ypos, xpos)
                self.wait(which)
                self.send(which, three)
                self.send(which, two)
            else:
                which = chip_slot(zs[i], y_two, x_two)
                self.wait(which)
                self.send(which, three)

        def last(self, diagonal):
            for i in range(4):
                self.wait(chip_slot(zs[i], 1 - ypos, 1 - xpos) if diagonal else chip_slot(zs[i], y_three, x_three))

    edge = d.chunk
    l_parts = (
        (lambda s: lv.at[0, s, :, core], 0),
        (lambda s: lv.at[1, s, :, core, :, pl.ds(edge, d.bond - edge)], 1),
        (lambda s: lv.at[0, s, :, 1 - core, :, pl.ds(0, d.half)], 2),
        (lambda s: lv.at[1, s, :, 1 - core, :, pl.ds(edge, d.half - edge)], 3),
    )
    l_gathers = [Gather(block, l_send.at[n], lambda s, n=n: l_recv.at[n, s]) for block, n in l_parts]

    def l_swap(s, term):
        part = lv.at[:, s, :, term, :, pl.ds(d.half, d.half)]
        return remote(part, part, f_send, f_recv.at[s], partner)

    def l_event(n):
        i = (n + 1) // 2
        for g in l_gathers:
            g.event(n)
        l_swap(chip_slot(zs[i], ypos, xpos) if n % 2 else chip_slot(zs[i], y_two, x_two), core).start()

    def l_last(diagonal):
        for i in range(4):
            which = chip_slot(zs[i], 1 - ypos, 1 - xpos) if diagonal else chip_slot(zs[i], y_three, x_three)
            for g in l_gathers:
                g.wait(which)
            l_swap(which, core).start()

    def l_fill(n, grp):
        s = grp * 4 + n

        @pl.when(s != slot)
        def _():
            l_swap(s, 1 - core).wait_recv()
            for c in range(CORES):
                tile = lv[:, s, c, 1 - core, :, d.half:].reshape(d.half, d.half).T
                lv[:, s, c, 1 - core, :, d.half:] = tile.reshape(CHUNKS, d.chunk, d.half)
                for t in range(d.terms_dev):
                    lv[1, s, c, t, :, :edge] = lv[0, s, c, t, :, edge:d.half].T
        return grp

    def l_along():
        for i in (1, 2, 3):
            for g in l_gathers:
                g.send(slot, device(zs[i], ypos, xpos, core))

    def u_block(p):
        return lambda s: uv.at[p // QUARTERS, pl.ds(p % QUARTERS * 2, 2), pl.ds(pl.multiple_of(s * d.slab, d.slab), d.slab), :]

    u_gathers = [Gather(u_block(p), u_send.at[p], lambda s, p=p: u_recv.at[p, s]) for p in range(PIECES)]

    def act(kind, i, p, j):
        g = u_gathers[p]
        if kind == ALONG:
            g.send(slot, device(zn[i], ypos, xpos, core))
        elif kind == ACROSS:
            g.own_across()
        elif kind == FROM_COLUMN:
            which = chip_slot(zn[i], ypos, xpos)
            g.wait(which)
            g.send(which, three)
            g.send(which, two)
        elif kind == FROM_SECOND:
            which = chip_slot(zn[i], y_two, x_two)
            g.wait(which)
            g.send(which, three)
        elif kind == THIRD:
            g.last(False)
        elif kind == DIAGONAL:
            g.last(True)
        elif kind == RESULT:
            turn_result(j - 1)
        elif kind == RESULT_OUT:
            hand_out(j - 1, 0, RESULT_EARLY)

    for ch in range(CHUNKS):
        for h in range(2):
            mine = left.at[:, pl.ds(pl.multiple_of(core * d.half + ch * d.chunk, d.chunk), d.chunk),
                           pl.ds(pl.multiple_of((core + h) % 2 * d.half, d.half), d.half)]
            theirs = left.at[:, pl.ds(pl.multiple_of((1 - core) * d.half + ch * d.chunk, d.chunk), d.chunk),
                             pl.ds(pl.multiple_of((1 - core + h) % 2 * d.half, d.half), d.half)]
            remote(theirs, lv.at[ch, slot, core, :, :, pl.ds(h * d.half, d.half)], d2d_sem.at[ch, h], d2d_recv.at[ch, h], partner).start()
            pltpu.make_async_copy(mine, lv.at[ch, slot, core, :, :, pl.ds(h * d.half, d.half)], loc_sem.at[ch, h]).start()

    psi_rows = d.half * d.pair // 8
    psi_copies = [pltpu.make_async_copy(psi.at[pl.ds(pl.multiple_of(core * d.half * d.pair + n * psi_rows, psi_rows), psi_rows),
                                               pl.ds(c * d.lane, d.lane)],
                                        ps.at[c, pl.ds(n * psi_rows, psi_rows), :], psi_sem.at[n, c])
                  for n in range(8) for c in range(d.lane_tiles)]
    for copy in psi_copies:
        copy.start()

    def right_rows(s):
        return right.at[:, pl.ds(pl.multiple_of(s * d.slab, d.slab), d.slab), :]

    own_right = pltpu.make_async_copy(right_rows(slot), rv.at[slot, core], loc_sem.at[2, 0])
    own_pair = pltpu.make_async_copy(wexp, wv.at[slot, core], loc_sem.at[2, 1])
    own_right.start()
    own_pair.start()
    for n in range(1, CHIPS):
        chip = (me // 2 + n) % CHIPS
        to = chip_slot(chip // 4, chip // 2 % 2, chip % 2)
        remote(right_rows(to), rv.at[slot, core], rw_send.at[0], rw_recv.at[0], chip * 2 + core).start()
        remote(wexp, wv.at[slot, core], rw_send.at[1], rw_recv.at[1], chip * 2 + core).start()

    for ch in range(CHUNKS):
        for h in range(2):
            pltpu.make_async_copy(lv.at[ch, slot, core, :, :, pl.ds(h * d.half, d.half)], lv.at[ch, slot, core, :, :, pl.ds(h * d.half, d.half)], loc_sem.at[ch, h]).wait()
            back = remote(lv.at[ch, slot, 1 - core, :, :, pl.ds(h * d.half, d.half)], lv.at[ch, slot, 1 - core, :, :, pl.ds(h * d.half, d.half)], d2d_sem.at[ch, h], d2d_recv.at[ch, h], partner)
            back.wait_recv()
    l_along()
    for g in l_gathers:
        g.own_across()

    total = jnp.zeros((8, d.lane), jnp.float32)
    for n in range(8):
        for copy in psi_copies[n * d.lane_tiles:(n + 1) * d.lane_tiles]:
            copy.wait()

        def add_rows(i, acc, n=n):
            x = ps[:, pl.ds(pl.multiple_of(n * psi_rows + i * (psi_rows // 8), 8), psi_rows // 8), :]
            return acc + jnp.sum((x * x).reshape(d.lane_tiles * psi_rows // 64, 8, d.lane), axis=0)

        total = lax.fori_loop(0, 8, add_rows, total)
    nbuf[0] = jnp.broadcast_to(jnp.sum(total, keepdims=True), (8, 128))
    to_partner = remote(nbuf.at[0], nbuf.at[1], n_send, n_recv, partner)
    to_partner.start()
    to_partner.wait()
    norm = jnp.sqrt((nbuf[0] + nbuf[1])[0:1, :] / d.vec_size)
    info[2] = jnp.broadcast_to(norm, (8, 128))
    norm_one = norm[:, 0:1]

    def place(q):
        tiles = [(ps[c, pl.ds(q, d.half, stride=d.pair), :] / norm_one).T for c in range(d.lane_tiles)]
        xt = jnp.concatenate(tiles, axis=0)
        vprev[...] = xt
        return xt.astype(jnp.bfloat16)

    def start_vector(qb, carry):
        for q2 in range(2):
            q = qb * 2 + q2
            xb = place(q)
            for ch in range(CHUNKS):
                uv[ch, qb, :, q2 * d.chunk:(q2 + 1) * d.chunk] = xb[:, ch * d.chunk:(ch + 1) * d.chunk]
            for bh in range(2):
                rows = vprev[pl.ds(pl.multiple_of(slot * d.slab + bh * d.sub, d.sub), d.sub), :]
                vcur[pl.ds(pl.multiple_of((bh * d.pair + q) * d.sub, d.sub), d.sub), :] = rows
        return carry

    lax.fori_loop(0, d.pair // 4, start_vector, 0)
    own_right.wait()
    own_pair.wait()
    fifteen = rv.at[pl.ds(0, CHIPS - 1), 0]
    fifteen_w = wv.at[pl.ds(0, CHIPS - 1), 0]
    remote(fifteen, fifteen, rw_send.at[0], rw_recv.at[0], me).wait()
    remote(fifteen_w, fifteen_w, rw_send.at[1], rw_recv.at[1], me).wait()
    fw_right = remote(rv.at[:, core], rv.at[:, core], fw_send.at[0], fw_recv.at[0], partner)
    fw_pair = remote(wv.at[:, core], wv.at[:, core], fw_send.at[1], fw_recv.at[1], partner)
    fw_right.start()
    fw_pair.start()
    l_event(0)
    l_event(1)
    lax.fori_loop(d.pair // 4, d.pair // 2, start_vector, 0)
    l_event(2)
    l_event(3)
    fw_right.wait()
    fw_pair.wait()
    lane = lax.broadcasted_iota(jnp.int32, (d.sub, d.prod), 1)
    row = lax.broadcasted_iota(jnp.int32, (d.sub, d.prod), 0)
    diagonal = lane % d.sub == row

    def spread_pair(s, carry):
        for c in range(2):
            for t in range(d.terms_dev):
                w = wv[s, c, t].astype(jnp.float32)
                for q in range(d.pair):
                    full = jnp.where(diagonal, jnp.broadcast_to(w[q:q + 1, :], (d.sub, d.prod)), 0.0)
                    kw[s, c, t, q * d.sub:(q + 1) * d.sub, :] = full.astype(jnp.bfloat16)
        return carry

    lax.fori_loop(0, CHIPS, spread_pair, 0)
    l_event(4)
    l_event(5)
    l_event(6)
    vprev[...] = jnp.zeros_like(vprev)

    def right_product(grp, ch, qb):
        r_all = rv[pl.ds(grp * 4, 4)].reshape(d.group_terms * d.slab, d.bond)
        y = jnp.dot(r_all, uv[ch, qb], preferred_element_type=jnp.float32).astype(jnp.bfloat16)
        y = y.reshape(d.group_terms, 2, d.sub, 2 * d.chunk)
        for q2 in range(2):
            for bh in range(2):
                yst[pl.ds(grp * d.group_terms, d.group_terms), qb * 2 + q2, :, bh * d.chunk:(bh + 1) * d.chunk] = \
                    y[:, bh, :, q2 * d.chunk:(q2 + 1) * d.chunk]

    def right_of_group(grp, ch):
        for qb in range(d.pair // 2):
            right_product(grp, ch, qb)

    def right_of_piece(ch, part):
        for qb in range(2):
            for grp in range(GROUPS):
                right_product(grp, ch, part * 2 + qb)

    def left_products(ch, grp):
        for k in range(d.group_terms):
            w = kw[grp * 4 + k // 4, k // 2 % 2, k % 2]
            z = jnp.dot(w, yst[grp * d.group_terms + k].reshape(d.prod, 2 * d.chunk), preferred_element_type=jnp.float32).astype(jnp.bfloat16)
            for bh in range(2):
                zst[bh * d.prod:(bh + 1) * d.prod, k * d.chunk:(k + 1) * d.chunk] = z[:, bh * d.chunk:(bh + 1) * d.chunk]
        l_all = lv[ch, pl.ds(grp * 4, 4)].reshape(d.group_terms * d.chunk, d.bond)
        sig[...] += jnp.dot(zst[...], l_all, preferred_element_type=jnp.float32)

    def turn_result(j):
        wide = TILE_PARTS * d.slab
        for n in range(d.pair // TILE_PARTS):
            rows = [vcur[(bh * d.pair + q) * d.sub:(bh * d.pair + q + 1) * d.sub, :]
                    for q in range(n * TILE_PARTS, (n + 1) * TILE_PARTS) for bh in range(2)]
            tbuf[j, :, n * wide:(n + 1) * wide] = jnp.concatenate(rows, axis=0).T

    def hand_out(j, first, last):
        for n in range(first, last):
            to = core * CHIPS + n
            block = tbuf.at[j, n * d.out_rows:(n + 1) * d.out_rows, :]

            @pl.when(to != me)
            def _():
                remote(block, gbuf.at[j, slot], k_send, k_recv, to).start()

            @pl.when(to == me)
            def _():
                gbuf[j, slot] = block[...]

    def step(j, beta_prev):
        later = jnp.minimum(j, 1)
        own = xpos * 2 + ypos
        sig[...] = jnp.zeros_like(sig)

        def slot_step(t, carry):
            n = t // 4
            first_grp = jnp.where(n == 0, own, jnp.where(n == 1, x_two * 2 + y_two, jnp.where(n == 2, x_three * 2 + y_three, 3 - own)))
            first_ch = t // 2 % 2
            done_right = sum((t > r).astype(jnp.int32) for r in RIGHT_SLOTS)
            done_left = t - done_right
            now_right = sum((t == r).astype(jnp.int32) for r in RIGHT_SLOTS)
            is_right = (1 - later) * (1 - t % 2) + later * now_right

            @pl.when(j == 0)
            def _():
                @pl.when(t == 5)
                def _():
                    l_last(False)

                @pl.when(t == 13)
                def _():
                    l_last(True)

                @pl.when(t % 4 == 1)
                def _():
                    lax.fori_loop(0, 4, l_fill, first_grp)

            @pl.when(j > 0)
            def _():
                for four in range(0, len(SLOTS), 4):
                    @pl.when((t >= four) & (t < four + 4))
                    def _():
                        for at in range(four, four + 4):
                            if not SLOTS[at]:
                                continue

                            @pl.when(t == at)
                            def _():
                                for kind, i, p in SLOTS[at]:
                                    act(kind, i, p, j)

            @pl.when((is_right == 1) & (j == 0))
            def _():
                right_of_group(first_grp, first_ch)

            @pl.when((is_right == 1) & (j > 0))
            def _():
                right_of_piece(done_right // QUARTERS, done_right % QUARTERS)

            @pl.when(is_right == 0)
            def _():
                left_products((1 - later) * first_ch + later * (done_left // GROUPS), (1 - later) * first_grp + later * (done_left % GROUPS))
            return carry

        lax.fori_loop(0, len(SLOTS), slot_step, 0)

        @pl.when(j > 0)
        def _():
            for p in range(PIECES):
                sent = uv.at[p // QUARTERS, pl.ds(0, 2), pl.ds(0, 15 * d.slab), :]
                remote(sent, sent, u_send.at[p], u_recv.at[p, 0], me).wait_send()

        other = sig.at[:, pl.ds(d.half, d.half)]
        to_other = remote(other, part, p_send, p_recv, partner)
        to_other.start()
        to_other.wait()
        s = sig[:, :d.half] + part[...]
        v = vcur[...]
        w = s - beta_prev * vprev[...]
        sv = jnp.sum(s * v, keepdims=True)
        wv_sum = jnp.sum(w * v, keepdims=True)
        vv = jnp.sum(v * v, keepdims=True)
        guess = jnp.where(vv > 0.0, wv_sum / jnp.where(vv > 0.0, vv, 1.0), 0.0)
        t = w - guess * v
        sig[:, :d.half] = t
        tt = jnp.sum(t * t, keepdims=True)
        tv = jnp.sum(t * v, keepdims=True)
        at_lane = lax.broadcasted_iota(jnp.int32, (1, 128), 1)
        line = jnp.zeros((1, 128), jnp.float32)
        for n, value in enumerate((sv, vv, tt, tv, guess)):
            line = jnp.where(at_lane == n, value, line)
        scs[...] = line
        scr[me] = line

        def tell(n, carry):
            remote(scs, scr.at[me], s_send, s_recv, (me + n) % DEVS).start()
            return carry

        lax.fori_loop(1, DEVS, tell, 0)

        @pl.when(j > 0)
        def _():
            hand_out(j - 1, RESULT_EARLY, CHIPS)

        heard = scr.at[pl.ds(0, DEVS - 1)]
        remote(heard, heard, s_send, s_recv, me).wait()
        told = scr[:, 0, :]
        alpha = jnp.sum(told[:, 0:1], axis=0, keepdims=True) / d.vec_size
        off = alpha - told[:, 4:5]
        square = told[:, 2:3] - 2.0 * off * told[:, 3:4] + off * off * told[:, 1:2]
        beta = jnp.sqrt(jnp.sum(square, axis=0, keepdims=True) / d.vec_size)
        info[0, pl.ds(j, 1), :] = jnp.broadcast_to(alpha, (1, 128))
        info[1, pl.ds(j, 1), :] = jnp.broadcast_to(beta, (1, 128))
        vnew = (sig[:, :d.half] - (alpha - guess) * vcur[...]) / beta
        vprev[...] = vcur[...]
        vcur[...] = vnew
        vb = vnew.astype(jnp.bfloat16)

        @pl.when(j < LANCZOS_STEPS - 1)
        def _():
            for ch in range(CHUNKS):
                for bh in range(2):
                    at = pl.ds(pl.multiple_of(slot * d.slab + bh * d.sub, d.sub), d.sub)
                    for q in range(d.pair):
                        uv[ch, q // 2, at, q % 2 * d.chunk:(q % 2 + 1) * d.chunk] = \
                            vb[(bh * d.pair + q) * d.sub:(bh * d.pair + q + 1) * d.sub, ch * d.chunk:(ch + 1) * d.chunk]
        return beta


    lax.fori_loop(0, LANCZOS_STEPS, step, jnp.zeros((1, 1), jnp.float32))

    turn_result(LANCZOS_STEPS - 1)
    hand_out(LANCZOS_STEPS - 1, 0, CHIPS)
    for n, part in enumerate((lv.at[0, pl.ds(0, 15), :, 0], lv.at[1, pl.ds(0, 15), :, 0, :, pl.ds(edge, d.bond - edge)],
                              lv.at[0, pl.ds(0, 15), :, 0, :, pl.ds(0, d.half)], lv.at[1, pl.ds(0, 15), :, 0, :, pl.ds(edge, d.half - edge)])):
        remote(part, part, l_send.at[n], l_recv.at[n, 0], me).wait_send()
    swapped = lv.at[:, pl.ds(0, 15), :, 0, :, pl.ds(d.half, d.half)]
    remote(swapped, swapped, f_send, f_recv.at[0], me).wait_send()
    for ch in range(CHUNKS):
        for h in range(2):
            theirs = left.at[:, pl.ds(0, d.chunk), pl.ds(0, d.half)]
            remote(theirs, lv.at[ch, slot, core, :, :, pl.ds(h * d.half, d.half)], d2d_sem.at[ch, h], d2d_recv.at[ch, h], partner).wait_send()

    sends_self = me // CHIPS == core

    @pl.when(sends_self)
    def _():
        some = gbuf.at[:, pl.ds(0, CHIPS - 1)]
        remote(some, some, k_send, k_recv, me).wait()

    @pl.when(jnp.logical_not(sends_self))
    def _():
        remote(gbuf, gbuf, k_send, k_recv, me).wait()

    wide = TILE_PARTS * d.slab
    lanes = lax.broadcasted_iota(jnp.int32, (d.out_rows, wide), 1) // d.slab

    def put_out(j, carry):
        for ct in range(CHIPS // TILE_PARTS):
            for qt in range(d.pair // TILE_PARTS):
                src = [gbuf[j, ct * TILE_PARTS + c, :, qt * wide:(qt + 1) * wide] for c in range(TILE_PARTS)]
                for q in range(TILE_PARTS):
                    tile = jnp.zeros((d.out_rows, wide), jnp.float32)
                    for c in range(TILE_PARTS):
                        shift = (c - q) % TILE_PARTS * d.slab
                        moved = pltpu.roll(src[c], shift, 1) if shift else src[c]
                        tile = jnp.where(lanes == c, moved, tile)
                    at = (qt * TILE_PARTS + q) * d.out_rows
                    tbuf[j, at:at + d.out_rows, ct * wide:(ct + 1) * wide] = tile
        pltpu.make_async_copy(tbuf.at[j], out.at[j], o_sem).start()
        return carry

    lax.fori_loop(0, LANCZOS_STEPS, put_out, 0)
    pltpu.make_async_copy(tbuf, out, o_sem).wait()


def solution(mesh):
    def device_body(wavefunction, left_loc, pair_loc, right_loc, flag_loc):
        bond, pair = wavefunction.shape[0], wavefunction.shape[1]
        d = Dims(bond, pair, left_loc.shape[0])
        eye = jnp.eye(bond, dtype=jnp.bfloat16)
        right_used = jnp.where((flag_loc == 1)[:, None, None], right_loc, eye)
        pair_wide = jnp.repeat(pair_loc, d.sub, axis=2)
        bf16, f32 = jnp.bfloat16, jnp.float32
        dma = pltpu.SemaphoreType.DMA
        any_space = pl.BlockSpec(memory_space=pl.ANY)
        rows_out, info = pl.pallas_call(
            functools.partial(lanczos_kernel, d),
            out_shape=(jax.ShapeDtypeStruct((LANCZOS_STEPS, d.half, bond), f32), jax.ShapeDtypeStruct((3, 8, 128), f32)),
            in_specs=[any_space] * 4,
            out_specs=(any_space, pl.BlockSpec(memory_space=pltpu.VMEM)),
            scratch_shapes=[
                pltpu.VMEM((CHUNKS, CHIPS, CORES, d.terms_dev, d.chunk, bond), bf16),
                pltpu.VMEM((CHIPS, CORES, d.terms_dev, d.slab, bond), bf16),
                pltpu.VMEM((CHIPS, CORES, d.terms_dev, pair, d.prod), bf16),
                pltpu.VMEM((CHIPS, CORES, d.terms_dev, d.prod, d.prod), bf16),
                pltpu.VMEM((CHUNKS, pair // 2, bond, 2 * d.chunk), bf16),
                pltpu.VMEM((d.lane_tiles, d.half * pair, d.lane), f32),
                pltpu.VMEM((CHIPS * CORES * d.terms_dev, pair, d.sub, 2 * d.chunk), bf16),
                pltpu.VMEM((d.rows, d.group_terms * d.chunk), bf16),
                pltpu.VMEM((d.rows, bond), f32),
                pltpu.VMEM((d.rows, d.half), f32),
                pltpu.VMEM((d.rows, d.half), f32),
                pltpu.VMEM((d.rows, d.half), f32),
                pltpu.VMEM((LANCZOS_STEPS, d.half, bond), f32),
                pltpu.VMEM((LANCZOS_STEPS, CHIPS, d.out_rows, bond), f32),
                pltpu.VMEM((1, 128), f32),
                pltpu.VMEM((DEVS, 1, 128), f32),
                pltpu.VMEM((2, 8, 128), f32),
                dma((3, 2)), dma((8, d.lane_tiles)), dma((CHUNKS, 2)), dma((CHUNKS, 2)), dma((2,)), dma((2,)), dma((2,)), dma((2,)),
                dma((4,)), dma((4, CHIPS)), dma, dma((CHIPS,)), dma((PIECES,)), dma((PIECES, CHIPS)),
                dma, dma, dma, dma, dma, dma, dma, dma, dma,
            ],
            compiler_params=pltpu.CompilerParams(has_side_effects=True, vmem_limit_bytes=67043328),
            name='lanczos',
        )(wavefunction.reshape(bond * pair, bond), left_loc, right_used, pair_wide)
        row_start = lax.axis_index(AXIS_NAME) * d.out_rows
        first = lax.dynamic_slice_in_dim(wavefunction, row_start, d.out_rows, axis=0) / info[2, 0, 0]
        later = rows_out.reshape(LANCZOS_STEPS, pair, d.out_rows, bond).transpose(0, 2, 1, 3)
        return jnp.concatenate([first[None], later]), info[0, :LANCZOS_STEPS, 0], info[1, :LANCZOS_STEPS, 0]

    return jax.shard_map(device_body, mesh=mesh, in_specs=(P(), P(AXIS_NAME), P(AXIS_NAME), P(AXIS_NAME), P(AXIS_NAME)),
                         out_specs=(P(None, AXIS_NAME), P(), P()), check_vma=False)
```

```python
import functools

import jax
import jax.numpy as jnp
from jax import lax
from jax.experimental import pallas as pl
from jax.experimental.pallas import tpu as pltpu
from jax.sharding import PartitionSpec as P

LANCZOS_STEPS = 6
AXIS_NAME = 'terms'
MESH = pl.DeviceIdType.MESH

CHIPS = 16
CORES = 2
DEVS = 32
CHUNKS = 2
GROUPS = 4
TILE_PARTS = 4
QUARTERS = 4
PIECES = CHUNKS * QUARTERS

ALONG, ACROSS, FROM_COLUMN, FROM_SECOND, THIRD, DIAGONAL, RESULT, RESULT_OUT, RESULT_PUT = range(9)
RIGHT_SLOTS = (0, 1, 2, 3, 8, 9, 10, 11)
SLOTS = (
    ((0, 1, 0), (0, 1, 1), (1, 0, 2), (0, 2, 0), (1, 0, 5), (1, 0, 3), (1, 0, 6), (1, 0, 0), (0, 3, 0), (3, 0, 2), (0, 2, 1), (0, 1, 3), (1, 0, 4), (0, 3, 1), (1, 0, 7), (0, 1, 2), (1, 0, 1), (0, 3, 3), (2, 1, 0), (2, 2, 0), (0, 2, 3), (0, 3, 2), (2, 1, 1), (3, 0, 0), (2, 3, 0), (3, 1, 0), (2, 2, 1), (0, 2, 2), (0, 1, 4), (3, 0, 1), (2, 1, 3), (3, 2, 0), (2, 3, 1), (2, 2, 2), (2, 2, 3), (2, 1, 2), (4, 0, 0), (0, 2, 5), (0, 3, 4), (0, 2, 4), (0, 1, 5), (0, 1, 6), (0, 1, 7), (3, 3, 0), (2, 3, 3), (3, 1, 1), (3, 2, 1), (0, 2, 6), (2, 3, 2), (4, 0, 1), (3, 3, 1), (0, 3, 6), (3, 2, 2), (3, 1, 2), (0, 3, 5), (0, 2, 7), (0, 3, 7), (3, 2, 3), (3, 3, 2), (3, 0, 3), (5, 0, 0), (3, 3, 3), (4, 0, 3), (3, 1, 3), (3, 0, 4),),
    ((6, 0, 0), (2, 2, 4), (5, 0, 1), (3, 0, 6), (2, 1, 4), (4, 0, 2),),
    ((2, 2, 6), (5, 0, 2), (2, 1, 6),),
    ((2, 2, 5), (5, 0, 3), (3, 2, 4), (2, 3, 4),),
    ((2, 1, 5), (3, 0, 5), (3, 1, 4),),
    ((2, 3, 5), (3, 2, 5), (2, 3, 6),),
    ((2, 2, 7), (3, 3, 4), (2, 1, 7), (3, 1, 5), (8, 0, 0),),
    ((3, 3, 5), (2, 3, 7), (3, 2, 6), (3, 1, 6), (3, 3, 6),),
    ((3, 0, 7), (3, 1, 7), (3, 2, 7), (4, 0, 5), (5, 0, 4), (4, 0, 4),),
    ((3, 3, 7), (5, 0, 5),),
    ((4, 0, 6), (5, 0, 6),),
    ((4, 0, 7), (5, 0, 7), (7, 0, 0),),
    (),
    (),
    (),
    (),
)
RESULT_EARLY = 9


class Dims:
    def __init__(self, bond, pair, terms_dev):
        self.bond = bond
        self.pair = pair
        self.terms_dev = terms_dev
        self.slab = bond // CHIPS
        self.sub = self.slab // 2
        self.half = bond // CORES
        self.chunk = self.half // CHUNKS
        self.rows = self.slab * pair
        self.prod = self.sub * pair
        self.out_rows = bond // DEVS
        self.group_terms = 4 * CORES * terms_dev
        self.vec_size = bond * pair * bond
        self.lane = min(bond, 128)
        self.wide = TILE_PARTS * self.slab
        self.lane_tiles = bond // self.lane


def lanczos_kernel(d, psi, left, right, pair_ops, flags, out, alphas, betas, lv, rv, rs, wv, kw, uv, ps, yst, zst, sig, part, vcur, vprev, tbuf, gbuf,
                   scs, scr, nbuf,
                   loc_sem, psi_sem, d2d_sem, d2d_recv, rw_send, rw_recv, fw_send, fw_recv, l_send, l_recv, f_send, f_recv, u_send, u_recv,
                   p_send, p_recv, s_send, s_recv, k_send, k_recv, n_send, n_recv, o_sem, first_sem):
    me = lax.axis_index(AXIS_NAME)
    core = me % 2
    xpos = (me // 2) % 2
    ypos = (me // 4) % 2
    zpos = me // 8

    def device(z, y, x, c):
        return ((z * 2 + y) * 2 + x) * 2 + c

    def chip_slot(z, y, x):
        return (x * 2 + y) * 4 + z

    partner = device(zpos, ypos, xpos, 1 - core)
    slot = chip_slot(zpos, ypos, xpos)
    zs = (zpos, zpos + 1 - 2 * (zpos % 2), (zpos + 2) % 4, 3 - zpos)
    inner = (zpos + 1) // 2 % 2
    zn = (zpos, (1 - inner) * (zpos + 1 - zpos // 3 * 2) + inner * (zpos - 1), (1 - inner) * ((zpos + 2) % 4) + inner * (zpos + 1),
          (1 - inner) * (3 - zpos) + inner * ((zpos + 2) % 4))
    y_two = ypos + (1 - core) * (1 - 2 * ypos)
    x_two = xpos + core * (1 - 2 * xpos)
    y_three = ypos + core * (1 - 2 * ypos)
    x_three = xpos + (1 - core) * (1 - 2 * xpos)
    two = device(zpos, y_two, x_two, core)
    three = device(zpos, y_three, x_three, core)

    def remote(src, dst, send, recv, dev):
        return pltpu.make_async_remote_copy(src_ref=src, dst_ref=dst, send_sem=send, recv_sem=recv, device_id=(dev,), device_id_type=MESH)

    class Gather:
        def __init__(self, block, send, recv):
            self.block, self.send_sem, self.recv_sem = block, send, recv

        def send(self, which, dev):
            remote(self.block(which), self.block(which), self.send_sem, self.recv_sem(which), dev).start()

        def wait(self, which):
            remote(self.block(which), self.block(which), self.send_sem, self.recv_sem(which), me).wait_recv()

        def own_along(self):
            for i in (1, 2, 3):
                self.send(slot, device(zs[i], ypos, xpos, core))

        def own_across(self):
            self.send(slot, three)
            self.send(slot, two)

        def event(self, n):
            i = (n + 1) // 2
            if n % 2:
                which = chip_slot(zs[i], ypos, xpos)
                self.wait(which)
                self.send(which, three)
                self.send(which, two)
            else:
                which = chip_slot(zs[i], y_two, x_two)
                self.wait(which)
                self.send(which, three)

        def last(self, diagonal):
            for i in range(4):
                self.wait(chip_slot(zs[i], 1 - ypos, 1 - xpos) if diagonal else chip_slot(zs[i], y_three, x_three))

    edge = d.chunk
    l_parts = (
        (lambda s: lv.at[0, s, :, core], 0),
        (lambda s: lv.at[1, s, :, core, :, pl.ds(edge, d.bond - edge)], 1),
        (lambda s: lv.at[0, s, :, 1 - core, :, pl.ds(0, d.half)], 2),
        (lambda s: lv.at[1, s, :, 1 - core, :, pl.ds(edge, d.half - edge)], 3),
    )
    l_gathers = [Gather(block, l_send.at[n], lambda s, n=n: l_recv.at[n, s]) for block, n in l_parts]

    def l_swap(s, term):
        part = lv.at[:, s, :, term, :, pl.ds(d.half, d.half)]
        return remote(part, part, f_send, f_recv.at[s], partner)

    def l_event(n):
        i = (n + 1) // 2
        for g in l_gathers:
            g.event(n)
        l_swap(chip_slot(zs[i], ypos, xpos) if n % 2 else chip_slot(zs[i], y_two, x_two), core).start()

    def l_last(diagonal):
        for i in range(4):
            which = chip_slot(zs[i], 1 - ypos, 1 - xpos) if diagonal else chip_slot(zs[i], y_three, x_three)
            for g in l_gathers:
                g.wait(which)
            l_swap(which, core).start()

    def l_fill(n, grp):
        s = grp * 4 + n

        @pl.when(s != slot)
        def _():
            l_swap(s, 1 - core).wait_recv()
            for c in range(CORES):
                tile = lv[:, s, c, 1 - core, :, d.half:].reshape(d.half, d.half).T
                lv[:, s, c, 1 - core, :, d.half:] = tile.reshape(CHUNKS, d.chunk, d.half)
                for t in range(d.terms_dev):
                    lv[1, s, c, t, :, :edge] = lv[0, s, c, t, :, edge:d.half].T
        return grp

    def l_along():
        for i in (1, 2, 3):
            for g in l_gathers:
                g.send(slot, device(zs[i], ypos, xpos, core))

    def u_block(p):
        return lambda s: uv.at[p // QUARTERS, pl.ds(p % QUARTERS * 2, 2), pl.ds(pl.multiple_of(s * d.slab, d.slab), d.slab), :]

    u_gathers = [Gather(u_block(p), u_send.at[p], lambda s, p=p: u_recv.at[p, s]) for p in range(PIECES)]

    def act(kind, i, p, j):
        g = u_gathers[p]
        if kind == ALONG:
            g.send(slot, device(zn[i], ypos, xpos, core))
        elif kind == ACROSS:
            g.own_across()
        elif kind == FROM_COLUMN:
            which = chip_slot(zn[i], ypos, xpos)
            g.wait(which)
            g.send(which, three)
            g.send(which, two)
        elif kind == FROM_SECOND:
            which = chip_slot(zn[i], y_two, x_two)
            g.wait(which)
            g.send(which, three)
        elif kind == THIRD:
            g.last(False)
        elif kind == DIAGONAL:
            g.last(True)
        elif kind == RESULT:
            turn_result(j - 1)
        elif kind == RESULT_OUT:
            hand_out(j - 1, 0, RESULT_EARLY)
        elif kind == RESULT_PUT:
            @pl.when(j > 1)
            def _():
                put_out(j - 2)

    for ch in range(CHUNKS):
        for h in range(2):
            mine = left.at[:, pl.ds(pl.multiple_of(core * d.half + ch * d.chunk, d.chunk), d.chunk),
                           pl.ds(pl.multiple_of((core + h) % 2 * d.half, d.half), d.half)]
            theirs = left.at[:, pl.ds(pl.multiple_of((1 - core) * d.half + ch * d.chunk, d.chunk), d.chunk),
                             pl.ds(pl.multiple_of((1 - core + h) % 2 * d.half, d.half), d.half)]
            remote(theirs, lv.at[ch, slot, core, :, :, pl.ds(h * d.half, d.half)], d2d_sem.at[ch, h], d2d_recv.at[ch, h], partner).start()
            pltpu.make_async_copy(mine, lv.at[ch, slot, core, :, :, pl.ds(h * d.half, d.half)], loc_sem.at[ch, h]).start()

    all_right = pltpu.make_async_copy(right, rs, loc_sem.at[2, 0])
    all_right.start()
    psi_rows = d.half * d.pair // 8
    psi_copies = [pltpu.make_async_copy(psi.at[pl.ds(pl.multiple_of(core * d.half * d.pair + n * psi_rows, psi_rows), psi_rows),
                                               pl.ds(c * d.lane, d.lane)],
                                        ps.at[c, pl.ds(n * psi_rows, psi_rows), :], psi_sem.at[n, c])
                  for n in range(8) for c in range(d.lane_tiles)]
    for copy in psi_copies:
        copy.start()

    first_rows = d.out_rows * d.pair
    first_copies = [pltpu.make_async_copy(psi.at[pl.ds(pl.multiple_of(me * first_rows, first_rows), first_rows), pl.ds(c * d.wide, d.wide)],
                                          tbuf.at[LANCZOS_STEPS - 1, c], first_sem.at[c]) for c in range(d.bond // d.wide)]
    for copy in first_copies:
        copy.start()

    spread = (lax.broadcasted_iota(jnp.int32, (d.pair, d.prod), 1) // d.sub == lax.broadcasted_iota(jnp.int32, (d.pair, d.prod), 0))
    spread = spread.astype(jnp.float32).astype(jnp.bfloat16)
    for t in range(d.terms_dev):
        wv[slot, core, t] = jnp.dot(pair_ops[t], spread, preferred_element_type=jnp.float32).astype(jnp.bfloat16)
    all_right.wait()
    some_rows = d.bond // 8

    def one_sided(i, carry):
        at = pl.ds(pl.multiple_of(i * some_rows, some_rows), some_rows)
        row = lax.broadcasted_iota(jnp.int32, (some_rows, d.bond), 0) + i * some_rows
        one = jnp.where(row == lax.broadcasted_iota(jnp.int32, (some_rows, d.bond), 1), 1.0, 0.0)
        for t in range(d.terms_dev):
            rs[t, at, :] = jnp.where(flags[t] == 1, rs[t, at, :].astype(jnp.float32), one).astype(jnp.bfloat16)
        return carry

    lax.fori_loop(0, 8, one_sided, 0)

    def right_rows(s):
        return rs.at[:, pl.ds(pl.multiple_of(s * d.slab, d.slab), d.slab), :]

    rv[slot, core] = rs[:, pl.ds(pl.multiple_of(slot * d.slab, d.slab), d.slab), :]
    for n in range(1, CHIPS):
        chip = (me // 2 + n) % CHIPS
        to = chip_slot(chip // 4, chip // 2 % 2, chip % 2)
        remote(right_rows(to), rv.at[slot, core], rw_send.at[0], rw_recv.at[0], chip * 2 + core).start()
        remote(wv.at[slot, core], wv.at[slot, core], rw_send.at[1], rw_recv.at[1], chip * 2 + core).start()

    for ch in range(CHUNKS):
        for h in range(2):
            pltpu.make_async_copy(lv.at[ch, slot, core, :, :, pl.ds(h * d.half, d.half)], lv.at[ch, slot, core, :, :, pl.ds(h * d.half, d.half)], loc_sem.at[ch, h]).wait()
            back = remote(lv.at[ch, slot, 1 - core, :, :, pl.ds(h * d.half, d.half)], lv.at[ch, slot, 1 - core, :, :, pl.ds(h * d.half, d.half)], d2d_sem.at[ch, h], d2d_recv.at[ch, h], partner)
            back.wait_recv()
    l_along()
    for g in l_gathers:
        g.own_across()

    total = jnp.zeros((8, d.lane), jnp.float32)
    for n in range(8):
        for copy in psi_copies[n * d.lane_tiles:(n + 1) * d.lane_tiles]:
            copy.wait()

        def add_rows(i, acc, n=n):
            x = ps[:, pl.ds(pl.multiple_of(n * psi_rows + i * (psi_rows // 8), 8), psi_rows // 8), :]
            return acc + jnp.sum((x * x).reshape(d.lane_tiles * psi_rows // 64, 8, d.lane), axis=0)

        total = lax.fori_loop(0, 8, add_rows, total)
    nbuf[0] = jnp.broadcast_to(jnp.sum(total, keepdims=True), (8, 128))
    to_partner = remote(nbuf.at[0], nbuf.at[1], n_send, n_recv, partner)
    to_partner.start()
    to_partner.wait()
    norm = jnp.sqrt((nbuf[0] + nbuf[1])[0:1, :] / d.vec_size)
    norm_one = norm[:, 0:1]
    for copy in first_copies:
        copy.wait()
    tbuf[LANCZOS_STEPS - 1] = tbuf[LANCZOS_STEPS - 1] / norm_one[None]
    first_out = [pltpu.make_async_copy(tbuf.at[LANCZOS_STEPS - 1, c], out.at[0, :, pl.ds(c * d.wide, d.wide)], first_sem.at[c])
                 for c in range(d.bond // d.wide)]
    for copy in first_out:
        copy.start()

    def place(q):
        tiles = [(ps[c, pl.ds(q, d.half, stride=d.pair), :] / norm_one).T for c in range(d.lane_tiles)]
        xt = jnp.concatenate(tiles, axis=0)
        vprev[...] = xt
        return xt.astype(jnp.bfloat16)

    def start_vector(qb, carry):
        for q2 in range(2):
            q = qb * 2 + q2
            xb = place(q)
            for ch in range(CHUNKS):
                uv[ch, qb, :, q2 * d.chunk:(q2 + 1) * d.chunk] = xb[:, ch * d.chunk:(ch + 1) * d.chunk]
            for bh in range(2):
                rows = vprev[pl.ds(pl.multiple_of(slot * d.slab + bh * d.sub, d.sub), d.sub), :]
                vcur[pl.ds(pl.multiple_of((bh * d.pair + q) * d.sub, d.sub), d.sub), :] = rows
        return carry

    lax.fori_loop(0, d.pair // 4, start_vector, 0)
    fifteen = rv.at[pl.ds(0, CHIPS - 1), 0]
    fifteen_w = wv.at[pl.ds(0, CHIPS - 1), 0]
    remote(fifteen, fifteen, rw_send.at[0], rw_recv.at[0], me).wait()
    remote(fifteen_w, fifteen_w, rw_send.at[1], rw_recv.at[1], me).wait()
    fw_right = remote(rv.at[:, core], rv.at[:, core], fw_send.at[0], fw_recv.at[0], partner)
    fw_pair = remote(wv.at[:, core], wv.at[:, core], fw_send.at[1], fw_recv.at[1], partner)
    fw_right.start()
    fw_pair.start()
    l_event(0)
    l_event(1)
    lax.fori_loop(d.pair // 4, d.pair // 2, start_vector, 0)
    l_event(2)
    l_event(3)
    fw_right.wait()
    fw_pair.wait()
    lane = lax.broadcasted_iota(jnp.int32, (d.sub, d.prod), 1)
    row = lax.broadcasted_iota(jnp.int32, (d.sub, d.prod), 0)
    diagonal = lane % d.sub == row

    def spread_pair(s, carry):
        for c in range(2):
            for t in range(d.terms_dev):
                w = wv[s, c, t].astype(jnp.float32)
                for q in range(d.pair):
                    full = jnp.where(diagonal, jnp.broadcast_to(w[q:q + 1, :], (d.sub, d.prod)), 0.0)
                    kw[s, c, t, q * d.sub:(q + 1) * d.sub, :] = full.astype(jnp.bfloat16)
        return carry

    lax.fori_loop(0, CHIPS, spread_pair, 0)
    l_event(4)
    l_event(5)
    l_event(6)
    vprev[...] = jnp.zeros_like(vprev)
    for copy in first_out:
        copy.wait()

    def right_product(grp, ch, qb):
        r_all = rv[pl.ds(grp * 4, 4)].reshape(d.group_terms * d.slab, d.bond)
        y = jnp.dot(r_all, uv[ch, qb], preferred_element_type=jnp.float32).astype(jnp.bfloat16)
        y = y.reshape(d.group_terms, 2, d.sub, 2 * d.chunk)
        for q2 in range(2):
            for bh in range(2):
                yst[pl.ds(grp * d.group_terms, d.group_terms), qb * 2 + q2, :, bh * d.chunk:(bh + 1) * d.chunk] = \
                    y[:, bh, :, q2 * d.chunk:(q2 + 1) * d.chunk]

    def right_of_group(grp, ch):
        for qb in range(d.pair // 2):
            right_product(grp, ch, qb)

    def right_of_piece(ch, part):
        for qb in range(2):
            for grp in range(GROUPS):
                right_product(grp, ch, part * 2 + qb)

    def left_products(ch, grp):
        for k in range(d.group_terms):
            w = kw[grp * 4 + k // 4, k // 2 % 2, k % 2]
            z = jnp.dot(w, yst[grp * d.group_terms + k].reshape(d.prod, 2 * d.chunk), preferred_element_type=jnp.float32).astype(jnp.bfloat16)
            for bh in range(2):
                zst[bh * d.prod:(bh + 1) * d.prod, k * d.chunk:(k + 1) * d.chunk] = z[:, bh * d.chunk:(bh + 1) * d.chunk]
        l_all = lv[ch, pl.ds(grp * 4, 4)].reshape(d.group_terms * d.chunk, d.bond)
        sig[...] += jnp.dot(zst[...], l_all, preferred_element_type=jnp.float32)

    def turn_result(j):
        for n in range(d.pair // TILE_PARTS):
            rows = [vcur[(bh * d.pair + q) * d.sub:(bh * d.pair + q + 1) * d.sub, :]
                    for q in range(n * TILE_PARTS, (n + 1) * TILE_PARTS) for bh in range(2)]
            tbuf[j, n] = jnp.concatenate(rows, axis=0).T

    def hand_out(j, first, last):
        for n in range(first, last):
            to = core * CHIPS + n
            block = tbuf.at[j, :, pl.ds(n * d.out_rows, d.out_rows), :]

            @pl.when(to != me)
            def _():
                remote(block, gbuf.at[j, slot], k_send.at[j], k_recv.at[j], to).start()

            @pl.when(to == me)
            def _():
                gbuf[j, slot] = block[...]

    sends_self = me // CHIPS == core
    lanes = lax.broadcasted_iota(jnp.int32, (d.out_rows, d.wide), 1) // d.slab

    def put_out(j):
        @pl.when(sends_self)
        def _():
            some = gbuf.at[j, pl.ds(0, CHIPS - 1)]
            remote(some, some, k_send.at[j], k_recv.at[j], me).wait()

        @pl.when(jnp.logical_not(sends_self))
        def _():
            remote(gbuf.at[j], gbuf.at[j], k_send.at[j], k_recv.at[j], me).wait()

        for ct in range(CHIPS // TILE_PARTS):
            for qt in range(d.pair // TILE_PARTS):
                src = [gbuf[j, ct * TILE_PARTS + c, qt] for c in range(TILE_PARTS)]
                for q in range(TILE_PARTS):
                    tile = jnp.zeros((d.out_rows, d.wide), jnp.float32)
                    for c in range(TILE_PARTS):
                        shift = (c - q) % TILE_PARTS * d.slab
                        moved = pltpu.roll(src[c], shift, 1) if shift else src[c]
                        tile = jnp.where(lanes == c, moved, tile)
                    tbuf[j, ct, pl.ds(qt * TILE_PARTS + q, d.out_rows, stride=d.pair), :] = tile
            pltpu.make_async_copy(tbuf.at[j, ct], out.at[1 + j, :, pl.ds(ct * d.wide, d.wide)], o_sem.at[j, ct]).start()

    def step(j, beta_prev):
        later = jnp.minimum(j, 1)
        own = xpos * 2 + ypos
        sig[...] = jnp.zeros_like(sig)

        def slot_step(t, carry):
            n = t // 4
            first_grp = jnp.where(n == 0, own, jnp.where(n == 1, x_two * 2 + y_two, jnp.where(n == 2, x_three * 2 + y_three, 3 - own)))
            first_ch = t // 2 % 2
            done_right = sum((t > r).astype(jnp.int32) for r in RIGHT_SLOTS)
            done_left = t - done_right
            now_right = sum((t == r).astype(jnp.int32) for r in RIGHT_SLOTS)
            is_right = (1 - later) * (1 - t % 2) + later * now_right

            @pl.when(j == 0)
            def _():
                @pl.when(t == 5)
                def _():
                    l_last(False)

                @pl.when(t == 13)
                def _():
                    l_last(True)

                @pl.when(t % 4 == 1)
                def _():
                    lax.fori_loop(0, 4, l_fill, first_grp)

            @pl.when(j > 0)
            def _():
                for four in range(0, len(SLOTS), 4):
                    @pl.when((t >= four) & (t < four + 4))
                    def _():
                        for at in range(four, four + 4):
                            if not SLOTS[at]:
                                continue

                            @pl.when(t == at)
                            def _():
                                for kind, i, p in SLOTS[at]:
                                    act(kind, i, p, j)

            @pl.when((is_right == 1) & (j == 0))
            def _():
                right_of_group(first_grp, first_ch)

            @pl.when((is_right == 1) & (j > 0))
            def _():
                right_of_piece(done_right // QUARTERS, done_right % QUARTERS)

            @pl.when(is_right == 0)
            def _():
                left_products((1 - later) * first_ch + later * (done_left // GROUPS), (1 - later) * first_grp + later * (done_left % GROUPS))
            return carry

        lax.fori_loop(0, len(SLOTS), slot_step, 0)

        @pl.when(j > 0)
        def _():
            for p in range(PIECES):
                sent = uv.at[p // QUARTERS, pl.ds(0, 2), pl.ds(0, 15 * d.slab), :]
                remote(sent, sent, u_send.at[p], u_recv.at[p, 0], me).wait_send()

        other = sig.at[:, pl.ds(d.half, d.half)]
        to_other = remote(other, part, p_send, p_recv, partner)
        to_other.start()
        to_other.wait()
        s = sig[:, :d.half] + part[...]
        v = vcur[...]
        w = s - beta_prev * vprev[...]
        sv = jnp.sum(s * v, keepdims=True)
        wv_sum = jnp.sum(w * v, keepdims=True)
        vv = jnp.sum(v * v, keepdims=True)
        guess = jnp.where(vv > 0.0, wv_sum / jnp.where(vv > 0.0, vv, 1.0), 0.0)
        t = w - guess * v
        sig[:, :d.half] = t
        tt = jnp.sum(t * t, keepdims=True)
        tv = jnp.sum(t * v, keepdims=True)
        at_lane = lax.broadcasted_iota(jnp.int32, (1, 128), 1)
        line = jnp.zeros((1, 128), jnp.float32)
        for n, value in enumerate((sv, vv, tt, tv, guess)):
            line = jnp.where(at_lane == n, value, line)
        scs[...] = line
        scr[me] = line

        def tell(n, carry):
            remote(scs, scr.at[me], s_send, s_recv, (me + n) % DEVS).start()
            return carry

        lax.fori_loop(1, DEVS, tell, 0)

        @pl.when(j > 0)
        def _():
            hand_out(j - 1, RESULT_EARLY, CHIPS)

        heard = scr.at[pl.ds(0, DEVS - 1)]
        remote(heard, heard, s_send, s_recv, me).wait()
        told = scr[:, 0, :]
        alpha = jnp.sum(told[:, 0:1], axis=0, keepdims=True) / d.vec_size
        off = alpha - told[:, 4:5]
        square = told[:, 2:3] - 2.0 * off * told[:, 3:4] + off * off * told[:, 1:2]
        beta = jnp.sqrt(jnp.sum(square, axis=0, keepdims=True) / d.vec_size)
        vnew = (sig[:, :d.half] - (alpha - guess) * vcur[...]) / beta
        vprev[...] = vcur[...]
        vcur[...] = vnew
        vb = vnew.astype(jnp.bfloat16)

        @pl.when(j < LANCZOS_STEPS - 1)
        def _():
            for ch in range(CHUNKS):
                for bh in range(2):
                    at = pl.ds(pl.multiple_of(slot * d.slab + bh * d.sub, d.sub), d.sub)
                    for q in range(d.pair):
                        uv[ch, q // 2, at, q % 2 * d.chunk:(q % 2 + 1) * d.chunk] = \
                            vb[(bh * d.pair + q) * d.sub:(bh * d.pair + q + 1) * d.sub, ch * d.chunk:(ch + 1) * d.chunk]
        alphas[j] = alpha[0, 0]
        betas[j] = beta[0, 0]
        return beta


    lax.fori_loop(0, LANCZOS_STEPS, step, jnp.zeros((1, 1), jnp.float32))

    turn_result(LANCZOS_STEPS - 1)
    hand_out(LANCZOS_STEPS - 1, 0, CHIPS)
    for n, part in enumerate((lv.at[0, pl.ds(0, 15), :, 0], lv.at[1, pl.ds(0, 15), :, 0, :, pl.ds(edge, d.bond - edge)],
                              lv.at[0, pl.ds(0, 15), :, 0, :, pl.ds(0, d.half)], lv.at[1, pl.ds(0, 15), :, 0, :, pl.ds(edge, d.half - edge)])):
        remote(part, part, l_send.at[n], l_recv.at[n, 0], me).wait_send()
    swapped = lv.at[:, pl.ds(0, 15), :, 0, :, pl.ds(d.half, d.half)]
    remote(swapped, swapped, f_send, f_recv.at[0], me).wait_send()
    for ch in range(CHUNKS):
        for h in range(2):
            theirs = left.at[:, pl.ds(0, d.chunk), pl.ds(0, d.half)]
            remote(theirs, lv.at[ch, slot, core, :, :, pl.ds(h * d.half, d.half)], d2d_sem.at[ch, h], d2d_recv.at[ch, h], partner).wait_send()
    put_out(LANCZOS_STEPS - 2)
    put_out(LANCZOS_STEPS - 1)
    for j in range(LANCZOS_STEPS):
        for c in range(d.bond // d.wide):
            pltpu.make_async_copy(tbuf.at[j, c], out.at[1 + j, :, pl.ds(c * d.wide, d.wide)], o_sem.at[j, c]).wait()


def solution(mesh):
    def device_body(wavefunction, left_loc, pair_loc, right_loc, flag_loc):
        bond, pair = wavefunction.shape[0], wavefunction.shape[1]
        d = Dims(bond, pair, left_loc.shape[0])
        bf16, f32 = jnp.bfloat16, jnp.float32
        dma = pltpu.SemaphoreType.DMA
        any_space = pl.BlockSpec(memory_space=pl.ANY)
        smem = pl.BlockSpec(memory_space=pltpu.SMEM)
        scalars = jax.ShapeDtypeStruct((LANCZOS_STEPS,), f32)
        krylov, alphas, betas = pl.pallas_call(
            functools.partial(lanczos_kernel, d),
            out_shape=(jax.ShapeDtypeStruct((LANCZOS_STEPS + 1, d.out_rows * pair, bond), f32), scalars, scalars),
            in_specs=[any_space] * 3 + [pl.BlockSpec(memory_space=pltpu.VMEM), smem],
            out_specs=(any_space, smem, smem),
            scratch_shapes=[
                pltpu.VMEM((CHUNKS, CHIPS, CORES, d.terms_dev, d.chunk, bond), bf16),
                pltpu.VMEM((CHIPS, CORES, d.terms_dev, d.slab, bond), bf16),
                pltpu.VMEM((d.terms_dev, bond, bond), bf16),
                pltpu.VMEM((CHIPS, CORES, d.terms_dev, pair, d.prod), bf16),
                pltpu.VMEM((CHIPS, CORES, d.terms_dev, d.prod, d.prod), bf16),
                pltpu.VMEM((CHUNKS, pair // 2, bond, 2 * d.chunk), bf16),
                pltpu.VMEM((d.lane_tiles, d.half * pair, d.lane), f32),
                pltpu.VMEM((CHIPS * CORES * d.terms_dev, pair, d.sub, 2 * d.chunk), bf16),
                pltpu.VMEM((d.rows, d.group_terms * d.chunk), bf16),
                pltpu.VMEM((d.rows, bond), f32),
                pltpu.VMEM((d.rows, d.half), f32),
                pltpu.VMEM((d.rows, d.half), f32),
                pltpu.VMEM((d.rows, d.half), f32),
                pltpu.VMEM((LANCZOS_STEPS, bond // d.wide, d.half, d.wide), f32),
                pltpu.VMEM((LANCZOS_STEPS, CHIPS, bond // d.wide, d.out_rows, d.wide), f32),
                pltpu.VMEM((1, 128), f32),
                pltpu.VMEM((DEVS, 1, 128), f32),
                pltpu.VMEM((2, 8, 128), f32),
                dma((3, 2)), dma((8, d.lane_tiles)), dma((CHUNKS, 2)), dma((CHUNKS, 2)), dma((2,)), dma((2,)), dma((2,)), dma((2,)),
                dma((4,)), dma((4, CHIPS)), dma, dma((CHIPS,)), dma((PIECES,)), dma((PIECES, CHIPS)),
                dma, dma, dma, dma, dma((LANCZOS_STEPS,)), dma((LANCZOS_STEPS,)), dma, dma, dma((LANCZOS_STEPS, bond // d.wide)), dma((bond // d.wide,)),
            ],
            compiler_params=pltpu.CompilerParams(has_side_effects=True, vmem_limit_bytes=67043328),
            name='lanczos',
        )(wavefunction.reshape(bond * pair, bond), left_loc, right_loc, pair_loc, flag_loc)
        return krylov.reshape(LANCZOS_STEPS + 1, d.out_rows, pair, bond), alphas, betas

    return jax.shard_map(device_body, mesh=mesh, in_specs=(P(), P(AXIS_NAME), P(AXIS_NAME), P(AXIS_NAME), P(AXIS_NAME)),
                         out_specs=(P(None, AXIS_NAME), P(), P()), check_vma=False)
```

```python
import functools

import jax
import jax.numpy as jnp
from jax import lax
from jax.experimental import pallas as pl
from jax.experimental.pallas import tpu as pltpu
from jax.sharding import PartitionSpec as P

LANCZOS_STEPS = 6
AXIS_NAME = 'terms'
MESH = pl.DeviceIdType.MESH

CHIPS = 16
CORES = 2
DEVS = 32
CHUNKS = 2
GROUPS = 4
TILE_PARTS = 4
QUARTERS = 4
PIECES = CHUNKS * QUARTERS

ALONG, ACROSS, FROM_COLUMN, FROM_SECOND, THIRD, DIAGONAL, RESULT, RESULT_OUT, RESULT_PUT = range(9)
RIGHT_SLOTS = (0, 1, 2, 3, 8, 9, 10, 11)
SLOTS = (
    ((0, 1, 0), (0, 1, 1), (1, 0, 2), (0, 2, 0), (1, 0, 5), (1, 0, 3), (1, 0, 6), (1, 0, 0), (0, 3, 0), (3, 0, 2), (0, 2, 1), (0, 1, 3), (1, 0, 4), (0, 3, 1), (1, 0, 7), (0, 1, 2), (1, 0, 1), (0, 3, 3), (2, 1, 0), (2, 2, 0), (0, 2, 3), (0, 3, 2), (2, 1, 1), (3, 0, 0), (2, 3, 0), (3, 1, 0), (2, 2, 1), (0, 2, 2), (0, 1, 4), (3, 0, 1), (2, 1, 3), (3, 2, 0), (2, 3, 1), (2, 2, 2), (2, 2, 3), (2, 1, 2), (4, 0, 0), (0, 2, 5), (0, 3, 4), (0, 2, 4), (0, 1, 5), (0, 1, 6), (0, 1, 7), (3, 3, 0), (2, 3, 3), (3, 1, 1), (3, 2, 1), (0, 2, 6), (2, 3, 2), (4, 0, 1), (3, 3, 1), (0, 3, 6), (3, 2, 2), (3, 1, 2), (0, 3, 5), (0, 2, 7), (0, 3, 7), (3, 2, 3), (3, 3, 2), (3, 0, 3), (5, 0, 0), (3, 3, 3), (4, 0, 3), (3, 1, 3), (3, 0, 4),),
    ((6, 0, 0), (2, 2, 4), (5, 0, 1), (3, 0, 6), (2, 1, 4), (4, 0, 2),),
    ((2, 2, 6), (5, 0, 2), (2, 1, 6),),
    ((2, 2, 5), (5, 0, 3), (3, 2, 4), (2, 3, 4),),
    ((2, 1, 5), (3, 0, 5), (3, 1, 4),),
    ((2, 3, 5), (3, 2, 5), (2, 3, 6),),
    ((2, 2, 7), (3, 3, 4), (2, 1, 7), (3, 1, 5), (8, 0, 0),),
    ((3, 3, 5), (2, 3, 7), (3, 2, 6), (3, 1, 6), (3, 3, 6),),
    ((3, 0, 7), (3, 1, 7), (3, 2, 7), (4, 0, 5), (5, 0, 4), (4, 0, 4),),
    ((3, 3, 7), (5, 0, 5),),
    ((4, 0, 6), (5, 0, 6),),
    ((4, 0, 7), (5, 0, 7), (7, 0, 0),),
    (),
    (),
    (),
    (),
)
RESULT_EARLY, RESULT_LATE = (3, 1, 2), (0,)


class Dims:
    def __init__(self, bond, pair, terms_dev):
        self.bond = bond
        self.pair = pair
        self.terms_dev = terms_dev
        self.slab = bond // CHIPS
        self.sub = self.slab // 2
        self.half = bond // CORES
        self.chunk = self.half // CHUNKS
        self.rows = self.slab * pair
        self.prod = self.sub * pair
        self.out_rows = bond // DEVS
        self.group_terms = 4 * CORES * terms_dev
        self.vec_size = bond * pair * bond
        self.lane = min(bond, 128)
        self.wide = TILE_PARTS * self.slab
        self.lane_tiles = bond // self.lane


def lanczos_kernel(d, psi, left, right, pair_ops, flags, out, first, alphas, betas, lv, rv, rs, wv, kw, uv, ps, yst, zst, sig, part, vcur, vprev, tbuf, gbuf,
                   scs, scr, nbuf,
                   loc_sem, psi_sem, d2d_sem, d2d_recv, rw_send, rw_recv, fw_send, fw_recv, l_send, l_recv, f_send, f_recv, u_send, u_recv,
                   p_send, p_recv, s_send, s_recv, k_send, k_recv, n_send, n_recv, o_sem, first_sem):
    me = lax.axis_index(AXIS_NAME)
    core = me % 2
    xpos = (me // 2) % 2
    ypos = (me // 4) % 2
    zpos = me // 8

    def device(z, y, x, c):
        return ((z * 2 + y) * 2 + x) * 2 + c

    def chip_slot(z, y, x):
        return (x * 2 + y) * 4 + z

    partner = device(zpos, ypos, xpos, 1 - core)
    slot = chip_slot(zpos, ypos, xpos)
    zs = (zpos, zpos + 1 - 2 * (zpos % 2), (zpos + 2) % 4, 3 - zpos)
    inner = (zpos + 1) // 2 % 2
    zn = (zpos, (1 - inner) * (zpos + 1 - zpos // 3 * 2) + inner * (zpos - 1), (1 - inner) * ((zpos + 2) % 4) + inner * (zpos + 1),
          (1 - inner) * (3 - zpos) + inner * ((zpos + 2) % 4))
    y_two = ypos + (1 - core) * (1 - 2 * ypos)
    x_two = xpos + core * (1 - 2 * xpos)
    y_three = ypos + core * (1 - 2 * ypos)
    x_three = xpos + (1 - core) * (1 - 2 * xpos)
    two = device(zpos, y_two, x_two, core)
    three = device(zpos, y_three, x_three, core)

    def remote(src, dst, send, recv, dev):
        return pltpu.make_async_remote_copy(src_ref=src, dst_ref=dst, send_sem=send, recv_sem=recv, device_id=(dev,), device_id_type=MESH)

    class Gather:
        def __init__(self, block, send, recv):
            self.block, self.send_sem, self.recv_sem = block, send, recv

        def send(self, which, dev):
            remote(self.block(which), self.block(which), self.send_sem, self.recv_sem(which), dev).start()

        def wait(self, which):
            remote(self.block(which), self.block(which), self.send_sem, self.recv_sem(which), me).wait_recv()

        def own_along(self):
            for i in (1, 2, 3):
                self.send(slot, device(zs[i], ypos, xpos, core))

        def own_across(self):
            self.send(slot, three)
            self.send(slot, two)

        def event(self, n):
            i = (n + 1) // 2
            if n % 2:
                which = chip_slot(zs[i], ypos, xpos)
                self.wait(which)
                self.send(which, three)
                self.send(which, two)
            else:
                which = chip_slot(zs[i], y_two, x_two)
                self.wait(which)
                self.send(which, three)

        def last(self, diagonal):
            for i in range(4):
                self.wait(chip_slot(zs[i], 1 - ypos, 1 - xpos) if diagonal else chip_slot(zs[i], y_three, x_three))

    edge = d.chunk
    l_parts = (
        (lambda s: lv.at[0, s, :, core], 0),
        (lambda s: lv.at[1, s, :, core, :, pl.ds(edge, d.bond - edge)], 1),
        (lambda s: lv.at[0, s, :, 1 - core, :, pl.ds(0, d.half)], 2),
        (lambda s: lv.at[1, s, :, 1 - core, :, pl.ds(edge, d.half - edge)], 3),
    )
    l_gathers = [Gather(block, l_send.at[n], lambda s, n=n: l_recv.at[n, s]) for block, n in l_parts]

    def l_swap(s, term):
        part = lv.at[:, s, :, term, :, pl.ds(d.half, d.half)]
        return remote(part, part, f_send, f_recv.at[s], partner)

    def l_event(n):
        i = (n + 1) // 2
        for g in l_gathers:
            g.event(n)
        l_swap(chip_slot(zs[i], ypos, xpos) if n % 2 else chip_slot(zs[i], y_two, x_two), core).start()

    def l_last(diagonal):
        for i in range(4):
            which = chip_slot(zs[i], 1 - ypos, 1 - xpos) if diagonal else chip_slot(zs[i], y_three, x_three)
            for g in l_gathers:
                g.wait(which)
            l_swap(which, core).start()

    def l_fill(n, grp):
        s = grp * 4 + n

        @pl.when(s != slot)
        def _():
            l_swap(s, 1 - core).wait_recv()
            for c in range(CORES):
                tile = lv[:, s, c, 1 - core, :, d.half:].reshape(d.half, d.half).T
                lv[:, s, c, 1 - core, :, d.half:] = tile.reshape(CHUNKS, d.chunk, d.half)
                for t in range(d.terms_dev):
                    lv[1, s, c, t, :, :edge] = lv[0, s, c, t, :, edge:d.half].T
        return grp

    def l_along():
        for i in (1, 2, 3):
            for g in l_gathers:
                g.send(slot, device(zs[i], ypos, xpos, core))

    def u_block(p):
        return lambda s: uv.at[p // QUARTERS, pl.ds(p % QUARTERS * 2, 2), pl.ds(pl.multiple_of(s * d.slab, d.slab), d.slab), :]

    u_gathers = [Gather(u_block(p), u_send.at[p], lambda s, p=p: u_recv.at[p, s]) for p in range(PIECES)]

    def act(kind, i, p, j):
        g = u_gathers[p]
        if kind == ALONG:
            g.send(slot, device(zn[i], ypos, xpos, core))
        elif kind == ACROSS:
            g.own_across()
        elif kind == FROM_COLUMN:
            which = chip_slot(zn[i], ypos, xpos)
            g.wait(which)
            g.send(which, three)
            g.send(which, two)
        elif kind == FROM_SECOND:
            which = chip_slot(zn[i], y_two, x_two)
            g.wait(which)
            g.send(which, three)
        elif kind == THIRD:
            g.last(False)
        elif kind == DIAGONAL:
            g.last(True)
        elif kind == RESULT:
            turn_result(j - 1, vcur)
        elif kind == RESULT_OUT:
            hand_out(j - 1, RESULT_EARLY)
        elif kind == RESULT_PUT:
            @pl.when(j > 1)
            def _():
                put_out(j - 2)

    for ch in range(CHUNKS):
        for h in range(2):
            mine = left.at[:, pl.ds(pl.multiple_of(core * d.half + ch * d.chunk, d.chunk), d.chunk),
                           pl.ds(pl.multiple_of((core + h) % 2 * d.half, d.half), d.half)]
            theirs = left.at[:, pl.ds(pl.multiple_of((1 - core) * d.half + ch * d.chunk, d.chunk), d.chunk),
                             pl.ds(pl.multiple_of((1 - core + h) % 2 * d.half, d.half), d.half)]
            remote(theirs, lv.at[ch, slot, core, :, :, pl.ds(h * d.half, d.half)], d2d_sem.at[ch, h], d2d_recv.at[ch, h], partner).start()
            pltpu.make_async_copy(mine, lv.at[ch, slot, core, :, :, pl.ds(h * d.half, d.half)], loc_sem.at[ch, h]).start()

    all_right = pltpu.make_async_copy(right, rs, loc_sem.at[2, 0])
    all_right.start()
    psi_rows = d.half * d.pair // 8
    psi_copies = [pltpu.make_async_copy(psi.at[pl.ds(pl.multiple_of(core * d.half * d.pair + n * psi_rows, psi_rows), psi_rows),
                                               pl.ds(c * d.lane, d.lane)],
                                        ps.at[c, pl.ds(n * psi_rows, psi_rows), :], psi_sem.at[n, c])
                  for n in range(8) for c in range(d.lane_tiles)]
    for copy in psi_copies:
        copy.start()

    first_rows = d.out_rows * d.pair
    first_copies = [pltpu.make_async_copy(psi.at[pl.ds(pl.multiple_of(me * first_rows, first_rows), first_rows), pl.ds(c * d.wide, d.wide)],
                                          tbuf.at[LANCZOS_STEPS - 1, c], first_sem.at[c]) for c in range(d.bond // d.wide)]
    for copy in first_copies:
        copy.start()

    for ch in range(CHUNKS):
        for h in range(2):
            pltpu.make_async_copy(lv.at[ch, slot, core, :, :, pl.ds(h * d.half, d.half)], lv.at[ch, slot, core, :, :, pl.ds(h * d.half, d.half)], loc_sem.at[ch, h]).wait()
            back = remote(lv.at[ch, slot, 1 - core, :, :, pl.ds(h * d.half, d.half)], lv.at[ch, slot, 1 - core, :, :, pl.ds(h * d.half, d.half)], d2d_sem.at[ch, h], d2d_recv.at[ch, h], partner)
            back.wait_recv()
    l_along()
    for g in l_gathers:
        g.own_across()

    spread = (lax.broadcasted_iota(jnp.int32, (d.pair, d.prod), 1) // d.sub == lax.broadcasted_iota(jnp.int32, (d.pair, d.prod), 0))
    spread = spread.astype(jnp.float32).astype(jnp.bfloat16)
    for t in range(d.terms_dev):
        wv[slot, core, t] = jnp.dot(pair_ops[t], spread, preferred_element_type=jnp.float32).astype(jnp.bfloat16)
    all_right.wait()
    some_rows = d.bond // 8

    def one_sided(i, carry):
        at = pl.ds(pl.multiple_of(i * some_rows, some_rows), some_rows)
        row = lax.broadcasted_iota(jnp.int32, (some_rows, d.bond), 0) + i * some_rows
        one = jnp.where(row == lax.broadcasted_iota(jnp.int32, (some_rows, d.bond), 1), 1.0, 0.0)
        for t in range(d.terms_dev):
            rs[t, at, :] = jnp.where(flags[t] == 1, rs[t, at, :].astype(jnp.float32), one).astype(jnp.bfloat16)
        return carry

    lax.fori_loop(0, 8, one_sided, 0)

    def right_rows(s):
        return rs.at[:, pl.ds(pl.multiple_of(s * d.slab, d.slab), d.slab), :]

    rv[slot, core] = rs[:, pl.ds(pl.multiple_of(slot * d.slab, d.slab), d.slab), :]
    for n in range(1, CHIPS):
        chip = (me // 2 + n) % CHIPS
        to = chip_slot(chip // 4, chip // 2 % 2, chip % 2)
        remote(right_rows(to), rv.at[slot, core], rw_send.at[0], rw_recv.at[0], chip * 2 + core).start()
        remote(wv.at[slot, core], wv.at[slot, core], rw_send.at[1], rw_recv.at[1], chip * 2 + core).start()

    total = jnp.zeros((8, d.lane), jnp.float32)
    for n in range(8):
        for copy in psi_copies[n * d.lane_tiles:(n + 1) * d.lane_tiles]:
            copy.wait()

        def add_rows(i, acc, n=n):
            x = ps[:, pl.ds(pl.multiple_of(n * psi_rows + i * (psi_rows // 8), 8), psi_rows // 8), :]
            return acc + jnp.sum((x * x).reshape(d.lane_tiles * psi_rows // 64, 8, d.lane), axis=0)

        total = lax.fori_loop(0, 8, add_rows, total)
    nbuf[0] = jnp.broadcast_to(jnp.sum(total, keepdims=True), (8, 128))
    to_partner = remote(nbuf.at[0], nbuf.at[1], n_send, n_recv, partner)
    to_partner.start()
    to_partner.wait()
    norm = jnp.sqrt((nbuf[0] + nbuf[1])[0:1, :] / d.vec_size)
    norm_one = norm[:, 0:1]
    for copy in first_copies:
        copy.wait()
    tbuf[LANCZOS_STEPS - 1] = tbuf[LANCZOS_STEPS - 1] / norm_one[None]
    first_out = [pltpu.make_async_copy(tbuf.at[LANCZOS_STEPS - 1, c], first.at[:, pl.ds(c * d.wide, d.wide)], first_sem.at[c])
                 for c in range(d.bond // d.wide)]
    for copy in first_out:
        copy.start()

    def place(q):
        tiles = [(ps[c, pl.ds(q, d.half, stride=d.pair), :] / norm_one).T for c in range(d.lane_tiles)]
        xt = jnp.concatenate(tiles, axis=0)
        vprev[...] = xt
        return xt.astype(jnp.bfloat16)

    def start_vector(qb, carry):
        for q2 in range(2):
            q = qb * 2 + q2
            xb = place(q)
            for ch in range(CHUNKS):
                uv[ch, qb, :, q2 * d.chunk:(q2 + 1) * d.chunk] = xb[:, ch * d.chunk:(ch + 1) * d.chunk]
            for bh in range(2):
                rows = vprev[pl.ds(pl.multiple_of(slot * d.slab + bh * d.sub, d.sub), d.sub), :]
                vcur[pl.ds(pl.multiple_of((bh * d.pair + q) * d.sub, d.sub), d.sub), :] = rows
        return carry

    lax.fori_loop(0, d.pair // 4, start_vector, 0)
    fifteen = rv.at[pl.ds(0, CHIPS - 1), 0]
    fifteen_w = wv.at[pl.ds(0, CHIPS - 1), 0]
    remote(fifteen, fifteen, rw_send.at[0], rw_recv.at[0], me).wait()
    remote(fifteen_w, fifteen_w, rw_send.at[1], rw_recv.at[1], me).wait()
    fw_right = remote(rv.at[:, core], rv.at[:, core], fw_send.at[0], fw_recv.at[0], partner)
    fw_pair = remote(wv.at[:, core], wv.at[:, core], fw_send.at[1], fw_recv.at[1], partner)
    fw_right.start()
    fw_pair.start()
    l_event(0)
    l_event(1)
    lax.fori_loop(d.pair // 4, d.pair // 2, start_vector, 0)
    l_event(2)
    l_event(3)
    fw_right.wait()
    fw_pair.wait()
    lane = lax.broadcasted_iota(jnp.int32, (d.sub, d.prod), 1)
    row = lax.broadcasted_iota(jnp.int32, (d.sub, d.prod), 0)
    diagonal = lane % d.sub == row

    def spread_pair(s, carry):
        for c in range(2):
            for t in range(d.terms_dev):
                w = wv[s, c, t].astype(jnp.float32)
                for q in range(d.pair):
                    full = jnp.where(diagonal, jnp.broadcast_to(w[q:q + 1, :], (d.sub, d.prod)), 0.0)
                    kw[s, c, t, q * d.sub:(q + 1) * d.sub, :] = full.astype(jnp.bfloat16)
        return carry

    lax.fori_loop(0, CHIPS, spread_pair, 0)
    l_event(4)
    l_event(5)
    l_event(6)
    vprev[...] = jnp.zeros_like(vprev)
    for copy in first_out:
        copy.wait()

    def right_product(grp, ch, qb):
        r_all = rv[pl.ds(grp * 4, 4)].reshape(d.group_terms * d.slab, d.bond)
        y = jnp.dot(r_all, uv[ch, qb], preferred_element_type=jnp.float32).astype(jnp.bfloat16)
        y = y.reshape(d.group_terms, 2, d.sub, 2 * d.chunk)
        for q2 in range(2):
            for bh in range(2):
                yst[pl.ds(grp * d.group_terms, d.group_terms), qb * 2 + q2, :, bh * d.chunk:(bh + 1) * d.chunk] = \
                    y[:, bh, :, q2 * d.chunk:(q2 + 1) * d.chunk]

    def right_of_group(grp, ch):
        for qb in range(d.pair // 2):
            right_product(grp, ch, qb)

    def right_of_piece(ch, part):
        for qb in range(2):
            for grp in range(GROUPS):
                right_product(grp, ch, part * 2 + qb)

    def left_products(ch, grp):
        for k in range(d.group_terms):
            w = kw[grp * 4 + k // 4, k // 2 % 2, k % 2]
            z = jnp.dot(w, yst[grp * d.group_terms + k].reshape(d.prod, 2 * d.chunk), preferred_element_type=jnp.float32).astype(jnp.bfloat16)
            for bh in range(2):
                zst[bh * d.prod:(bh + 1) * d.prod, k * d.chunk:(k + 1) * d.chunk] = z[:, bh * d.chunk:(bh + 1) * d.chunk]
        l_all = lv[ch, pl.ds(grp * 4, 4)].reshape(d.group_terms * d.chunk, d.bond)
        sig[...] += jnp.dot(zst[...], l_all, preferred_element_type=jnp.float32)

    def turn_result(j, vector):
        for n in range(d.pair // TILE_PARTS):
            rows = [vector[(bh * d.pair + q) * d.sub:(bh * d.pair + q + 1) * d.sub, :d.half]
                    for q in range(n * TILE_PARTS, (n + 1) * TILE_PARTS) for bh in range(2)]
            tbuf[j, n] = jnp.concatenate(rows, axis=0).T

    def hand_out(j, planes):
        for plane in planes:
            y, x = (ypos + plane // 2 * (1 - 2 * ypos), xpos + plane % 2 * (1 - 2 * xpos))
            for n in range(4):
                to = device(core * 2 + (zpos + n // 2) % 2, y, x, n % 2)
                block = tbuf.at[j, :, pl.ds(pl.multiple_of((to - core * CHIPS) * d.out_rows, d.out_rows), d.out_rows), :]

                @pl.when(to != me)
                def _():
                    remote(block, gbuf.at[j, slot], k_send.at[j], k_recv.at[j], to).start()

                @pl.when(to == me)
                def _():
                    gbuf[j, slot] = block[...]

    sends_self = me // CHIPS == core
    lanes = lax.broadcasted_iota(jnp.int32, (d.out_rows, d.wide), 1) // d.slab

    def put_out(j, finish=None):
        @pl.when(sends_self)
        def _():
            some = gbuf.at[j, pl.ds(0, CHIPS - 1)]
            remote(some, some, k_send.at[j], k_recv.at[j], me).wait()

        @pl.when(jnp.logical_not(sends_self))
        def _():
            remote(gbuf.at[j], gbuf.at[j], k_send.at[j], k_recv.at[j], me).wait()

        for ct in range(CHIPS // TILE_PARTS):
            for qt in range(d.pair // TILE_PARTS):
                src = [gbuf[j, ct * TILE_PARTS + c, qt] for c in range(TILE_PARTS)]
                if finish is not None:
                    src = [finish(x, gbuf[j - 1, ct * TILE_PARTS + c, qt], ct * TILE_PARTS + c) for c, x in enumerate(src)]
                for q in range(TILE_PARTS):
                    tile = jnp.zeros((d.out_rows, d.wide), jnp.float32)
                    for c in range(TILE_PARTS):
                        shift = (c - q) % TILE_PARTS * d.slab
                        moved = pltpu.roll(src[c], shift, 1) if shift else src[c]
                        tile = jnp.where(lanes == c, moved, tile)
                    tbuf[j, ct, pl.ds(qt * TILE_PARTS + q, d.out_rows, stride=d.pair), :] = tile
            pltpu.make_async_copy(tbuf.at[j, ct], out.at[j, :, pl.ds(ct * d.wide, d.wide)], o_sem.at[j, ct]).start()

    def step(j, carried):
        beta_prev = carried[0]
        later = jnp.minimum(j, 1)
        own = xpos * 2 + ypos
        sig[...] = jnp.zeros_like(sig)

        def slot_step(t, carry):
            n = t // 4
            first_grp = jnp.where(n == 0, own, jnp.where(n == 1, x_two * 2 + y_two, jnp.where(n == 2, x_three * 2 + y_three, 3 - own)))
            first_ch = t // 2 % 2
            done_right = sum((t > r).astype(jnp.int32) for r in RIGHT_SLOTS)
            done_left = t - done_right
            now_right = sum((t == r).astype(jnp.int32) for r in RIGHT_SLOTS)
            is_right = (1 - later) * (1 - t % 2) + later * now_right

            @pl.when(j == 0)
            def _():
                @pl.when(t == 5)
                def _():
                    l_last(False)

                @pl.when(t == 13)
                def _():
                    l_last(True)

                @pl.when(t % 4 == 1)
                def _():
                    lax.fori_loop(0, 4, l_fill, first_grp)

            @pl.when(j > 0)
            def _():
                for four in range(0, len(SLOTS), 4):
                    @pl.when((t >= four) & (t < four + 4))
                    def _():
                        for at in range(four, four + 4):
                            if not SLOTS[at]:
                                continue

                            @pl.when(t == at)
                            def _():
                                for kind, i, p in SLOTS[at]:
                                    act(kind, i, p, j)

            @pl.when((is_right == 1) & (j == 0))
            def _():
                right_of_group(first_grp, first_ch)

            @pl.when((is_right == 1) & (j > 0))
            def _():
                right_of_piece(done_right // QUARTERS, done_right % QUARTERS)

            @pl.when(is_right == 0)
            def _():
                left_products((1 - later) * first_ch + later * (done_left // GROUPS), (1 - later) * first_grp + later * (done_left % GROUPS))
            return carry

        lax.fori_loop(0, len(SLOTS), slot_step, 0)

        @pl.when(j > 0)
        def _():
            for p in range(PIECES):
                sent = uv.at[p // QUARTERS, pl.ds(0, 2), pl.ds(0, 15 * d.slab), :]
                remote(sent, sent, u_send.at[p], u_recv.at[p, 0], me).wait_send()

        other = sig.at[:, pl.ds(d.half, d.half)]
        to_other = remote(other, part, p_send, p_recv, partner)
        to_other.start()
        to_other.wait()
        s = sig[:, :d.half] + part[...]
        v = vcur[...]
        w = s - beta_prev * vprev[...]
        sv = jnp.sum(s * v, keepdims=True)
        wv_sum = jnp.sum(w * v, keepdims=True)
        vv = jnp.sum(v * v, keepdims=True)
        guess = jnp.where(vv > 0.0, wv_sum / jnp.where(vv > 0.0, vv, 1.0), 0.0)
        t = w - guess * v
        sig[:, :d.half] = t
        tt = jnp.sum(t * t, keepdims=True)
        tv = jnp.sum(t * v, keepdims=True)
        at_lane = lax.broadcasted_iota(jnp.int32, (1, 128), 1)
        line = jnp.zeros((1, 128), jnp.float32)
        for n, value in enumerate((sv, vv, tt, tv, guess)):
            line = jnp.where(at_lane == n, value, line)
        scs[...] = line
        scr[me] = line

        def tell(n, carry):
            remote(scs, scr.at[me], s_send, s_recv, (me + n) % DEVS).start()
            return carry

        lax.fori_loop(1, DEVS, tell, 0)

        @pl.when(j > 0)
        def _():
            hand_out(j - 1, RESULT_LATE)

        @pl.when(j == LANCZOS_STEPS - 1)
        def _():
            turn_result(LANCZOS_STEPS - 1, sig)
            hand_out(LANCZOS_STEPS - 1, (3, 1, 2, 0))

        heard = scr.at[pl.ds(0, DEVS - 1)]
        remote(heard, heard, s_send, s_recv, me).wait()
        told = scr[:, 0, :]
        alpha = jnp.sum(told[:, 0:1], axis=0, keepdims=True) / d.vec_size
        off = alpha - told[:, 4:5]
        square = told[:, 2:3] - 2.0 * off * told[:, 3:4] + off * off * told[:, 1:2]
        beta = jnp.sqrt(jnp.sum(square, axis=0, keepdims=True) / d.vec_size)
        vnew = (sig[:, :d.half] - (alpha - guess) * vcur[...]) / beta
        vprev[...] = vcur[...]
        vcur[...] = vnew
        vb = vnew.astype(jnp.bfloat16)

        @pl.when(j < LANCZOS_STEPS - 1)
        def _():
            for ch in range(CHUNKS):
                for bh in range(2):
                    at = pl.ds(pl.multiple_of(slot * d.slab + bh * d.sub, d.sub), d.sub)
                    for q in range(d.pair):
                        uv[ch, q // 2, at, q % 2 * d.chunk:(q % 2 + 1) * d.chunk] = \
                            vb[(bh * d.pair + q) * d.sub:(bh * d.pair + q + 1) * d.sub, ch * d.chunk:(ch + 1) * d.chunk]
        alphas[j] = alpha[0, 0]
        betas[j] = beta[0, 0]
        return beta, alpha


    zero = jnp.zeros((1, 1), jnp.float32)
    last_beta, last_alpha = lax.fori_loop(0, LANCZOS_STEPS, step, (zero, zero))

    for n, part in enumerate((lv.at[0, pl.ds(0, 15), :, 0], lv.at[1, pl.ds(0, 15), :, 0, :, pl.ds(edge, d.bond - edge)],
                              lv.at[0, pl.ds(0, 15), :, 0, :, pl.ds(0, d.half)], lv.at[1, pl.ds(0, 15), :, 0, :, pl.ds(edge, d.half - edge)])):
        remote(part, part, l_send.at[n], l_recv.at[n, 0], me).wait_send()
    swapped = lv.at[:, pl.ds(0, 15), :, 0, :, pl.ds(d.half, d.half)]
    remote(swapped, swapped, f_send, f_recv.at[0], me).wait_send()
    for ch in range(CHUNKS):
        for h in range(2):
            theirs = left.at[:, pl.ds(0, d.chunk), pl.ds(0, d.half)]
            remote(theirs, lv.at[ch, slot, core, :, :, pl.ds(h * d.half, d.half)], d2d_sem.at[ch, h], d2d_recv.at[ch, h], partner).wait_send()
    put_out(LANCZOS_STEPS - 2)

    def finish(block, before, s):
        owner = device(s % 4, s // 4 % 2, s // 8, me // CHIPS)
        return (block - (last_alpha - scr[owner][:, 4:5]) * before) / last_beta

    put_out(LANCZOS_STEPS - 1, finish)
    for j in range(LANCZOS_STEPS):
        for c in range(d.bond // d.wide):
            pltpu.make_async_copy(tbuf.at[j, c], out.at[j, :, pl.ds(c * d.wide, d.wide)], o_sem.at[j, c]).wait()


def solution(mesh):
    def device_body(wavefunction, left_loc, pair_loc, right_loc, flag_loc):
        bond, pair = wavefunction.shape[0], wavefunction.shape[1]
        d = Dims(bond, pair, left_loc.shape[0])
        bf16, f32 = jnp.bfloat16, jnp.float32
        dma = pltpu.SemaphoreType.DMA
        any_space = pl.BlockSpec(memory_space=pl.ANY)
        smem = pl.BlockSpec(memory_space=pltpu.SMEM)
        scalars = jax.ShapeDtypeStruct((LANCZOS_STEPS,), f32)
        later, first, alphas, betas = pl.pallas_call(
            functools.partial(lanczos_kernel, d),
            out_shape=(jax.ShapeDtypeStruct((LANCZOS_STEPS, d.out_rows * pair, bond), f32),
                       jax.ShapeDtypeStruct((d.out_rows * pair, bond), f32), scalars, scalars),
            in_specs=[any_space] * 3 + [pl.BlockSpec(memory_space=pltpu.VMEM), smem],
            out_specs=(any_space, any_space, smem, smem),
            scratch_shapes=[
                pltpu.VMEM((CHUNKS, CHIPS, CORES, d.terms_dev, d.chunk, bond), bf16),
                pltpu.VMEM((CHIPS, CORES, d.terms_dev, d.slab, bond), bf16),
                pltpu.VMEM((d.terms_dev, bond, bond), bf16),
                pltpu.VMEM((CHIPS, CORES, d.terms_dev, pair, d.prod), bf16),
                pltpu.VMEM((CHIPS, CORES, d.terms_dev, d.prod, d.prod), bf16),
                pltpu.VMEM((CHUNKS, pair // 2, bond, 2 * d.chunk), bf16),
                pltpu.VMEM((d.lane_tiles, d.half * pair, d.lane), f32),
                pltpu.VMEM((CHIPS * CORES * d.terms_dev, pair, d.sub, 2 * d.chunk), bf16),
                pltpu.VMEM((d.rows, d.group_terms * d.chunk), bf16),
                pltpu.VMEM((d.rows, bond), f32),
                pltpu.VMEM((d.rows, d.half), f32),
                pltpu.VMEM((d.rows, d.half), f32),
                pltpu.VMEM((d.rows, d.half), f32),
                pltpu.VMEM((LANCZOS_STEPS, bond // d.wide, d.half, d.wide), f32),
                pltpu.VMEM((LANCZOS_STEPS, CHIPS, bond // d.wide, d.out_rows, d.wide), f32),
                pltpu.VMEM((1, 128), f32),
                pltpu.VMEM((DEVS, 1, 128), f32),
                pltpu.VMEM((2, 8, 128), f32),
                dma((3, 2)), dma((8, d.lane_tiles)), dma((CHUNKS, 2)), dma((CHUNKS, 2)), dma((2,)), dma((2,)), dma((2,)), dma((2,)),
                dma((4,)), dma((4, CHIPS)), dma, dma((CHIPS,)), dma((PIECES,)), dma((PIECES, CHIPS)),
                dma, dma, dma, dma, dma((LANCZOS_STEPS,)), dma((LANCZOS_STEPS,)), dma, dma, dma((LANCZOS_STEPS, bond // d.wide)), dma((bond // d.wide,)),
            ],
            compiler_params=pltpu.CompilerParams(has_side_effects=True, vmem_limit_bytes=67043328),
            name='lanczos',
        )(wavefunction.reshape(bond * pair, bond), left_loc, right_loc, pair_loc, flag_loc)
        krylov = jnp.concatenate([first[None], later])
        return krylov.reshape(LANCZOS_STEPS + 1, d.out_rows, pair, bond), alphas, betas

    return jax.shard_map(device_body, mesh=mesh, in_specs=(P(), P(AXIS_NAME), P(AXIS_NAME), P(AXIS_NAME), P(AXIS_NAME)),
                         out_specs=(P(None, AXIS_NAME), P(), P()), check_vma=False)
```

```python
import functools

import jax
import jax.numpy as jnp
from jax import lax
from jax.experimental import pallas as pl
from jax.experimental.pallas import tpu as pltpu
from jax.sharding import PartitionSpec as P

LANCZOS_STEPS = 6
AXIS_NAME = 'terms'
MESH = pl.DeviceIdType.MESH

CHIPS = 16
CORES = 2
DEVS = 32
CHUNKS = 2
GROUPS = 4
TILE_PARTS = 4
QUARTERS = 4
PIECES = CHUNKS * QUARTERS

ALONG, ACROSS, FROM_COLUMN, FROM_SECOND, THIRD, DIAGONAL, RESULT, RESULT_OUT, RESULT_PUT = range(9)
RIGHT_SLOTS = (0, 1, 2, 3, 8, 9, 10, 11)
SLOTS = (
    ((0, 1, 0), (0, 1, 1), (1, 0, 2), (0, 2, 0), (1, 0, 5), (1, 0, 3), (1, 0, 6), (1, 0, 0), (0, 3, 0), (3, 0, 2), (0, 2, 1), (0, 1, 3), (1, 0, 4), (0, 3, 1), (1, 0, 7), (0, 1, 2), (1, 0, 1), (0, 3, 3), (2, 1, 0), (2, 2, 0), (0, 2, 3), (0, 3, 2), (2, 1, 1), (3, 0, 0), (2, 3, 0), (3, 1, 0), (2, 2, 1), (0, 2, 2), (0, 1, 4), (3, 0, 1), (2, 1, 3), (3, 2, 0), (2, 3, 1), (2, 2, 2), (2, 2, 3), (2, 1, 2), (4, 0, 0), (0, 2, 5), (0, 3, 4), (0, 2, 4), (0, 1, 5), (0, 1, 6), (0, 1, 7), (3, 3, 0), (2, 3, 3), (3, 1, 1), (3, 2, 1), (0, 2, 6), (2, 3, 2), (4, 0, 1), (3, 3, 1), (0, 3, 6), (3, 2, 2), (3, 1, 2), (0, 3, 5), (0, 2, 7), (0, 3, 7), (3, 2, 3), (3, 3, 2), (3, 0, 3), (5, 0, 0), (3, 3, 3), (4, 0, 3), (3, 1, 3), (3, 0, 4),),
    ((6, 0, 0), (2, 2, 4), (5, 0, 1), (3, 0, 6), (2, 1, 4), (4, 0, 2),),
    ((2, 2, 6), (5, 0, 2), (2, 1, 6),),
    ((2, 2, 5), (5, 0, 3), (3, 2, 4), (2, 3, 4),),
    ((2, 1, 5), (3, 0, 5), (3, 1, 4),),
    ((2, 3, 5), (3, 2, 5), (2, 3, 6),),
    ((2, 2, 7), (3, 3, 4), (2, 1, 7), (3, 1, 5), (8, 0, 0),),
    ((3, 3, 5), (2, 3, 7), (3, 2, 6), (3, 1, 6), (3, 3, 6),),
    ((3, 0, 7), (3, 1, 7), (3, 2, 7), (4, 0, 5), (5, 0, 4), (4, 0, 4),),
    ((3, 3, 7), (5, 0, 5),),
    ((4, 0, 6), (5, 0, 6),),
    ((4, 0, 7), (5, 0, 7), (7, 0, 0),),
    (),
    (),
    (),
    (),
)
RESULT_EARLY = 9


class Dims:
    def __init__(self, bond, pair, terms_dev):
        self.bond = bond
        self.pair = pair
        self.terms_dev = terms_dev
        self.slab = bond // CHIPS
        self.sub = self.slab // 2
        self.half = bond // CORES
        self.chunk = self.half // CHUNKS
        self.rows = self.slab * pair
        self.prod = self.sub * pair
        self.out_rows = bond // DEVS
        self.group_terms = 4 * CORES * terms_dev
        self.vec_size = bond * pair * bond
        self.lane = min(bond, 128)
        self.wide = TILE_PARTS * self.slab
        self.lane_tiles = bond // self.lane


def lanczos_kernel(d, psi, left, right, pair_ops, flags, out, first, alphas, betas, lv, rv, rs, wv, kw, uv, ps, yst, zst, sig, part, vcur, vprev, tbuf, gbuf,
                   scs, scr, nbuf,
                   loc_sem, psi_sem, d2d_sem, d2d_recv, rw_send, rw_recv, fw_send, fw_recv, l_send, l_recv, f_send, f_recv, u_send, u_recv,
                   p_send, p_recv, s_send, s_recv, k_send, k_recv, n_send, n_recv, o_sem, first_sem):
    me = lax.axis_index(AXIS_NAME)
    core = me % 2
    xpos = (me // 2) % 2
    ypos = (me // 4) % 2
    zpos = me // 8

    def device(z, y, x, c):
        return ((z * 2 + y) * 2 + x) * 2 + c

    def chip_slot(z, y, x):
        return (x * 2 + y) * 4 + z

    partner = device(zpos, ypos, xpos, 1 - core)
    slot = chip_slot(zpos, ypos, xpos)
    zs = (zpos, zpos + 1 - 2 * (zpos % 2), (zpos + 2) % 4, 3 - zpos)
    inner = (zpos + 1) // 2 % 2
    zn = (zpos, (1 - inner) * (zpos + 1 - zpos // 3 * 2) + inner * (zpos - 1), (1 - inner) * ((zpos + 2) % 4) + inner * (zpos + 1),
          (1 - inner) * (3 - zpos) + inner * ((zpos + 2) % 4))
    y_two = ypos + (1 - core) * (1 - 2 * ypos)
    x_two = xpos + core * (1 - 2 * xpos)
    y_three = ypos + core * (1 - 2 * ypos)
    x_three = xpos + (1 - core) * (1 - 2 * xpos)
    two = device(zpos, y_two, x_two, core)
    three = device(zpos, y_three, x_three, core)

    def remote(src, dst, send, recv, dev):
        return pltpu.make_async_remote_copy(src_ref=src, dst_ref=dst, send_sem=send, recv_sem=recv, device_id=(dev,), device_id_type=MESH)

    class Gather:
        def __init__(self, block, send, recv):
            self.block, self.send_sem, self.recv_sem = block, send, recv

        def send(self, which, dev):
            remote(self.block(which), self.block(which), self.send_sem, self.recv_sem(which), dev).start()

        def wait(self, which):
            remote(self.block(which), self.block(which), self.send_sem, self.recv_sem(which), me).wait_recv()

        def own_along(self):
            for i in (1, 2, 3):
                self.send(slot, device(zs[i], ypos, xpos, core))

        def own_across(self):
            self.send(slot, three)
            self.send(slot, two)

        def event(self, n):
            i = (n + 1) // 2
            if n % 2:
                which = chip_slot(zs[i], ypos, xpos)
                self.wait(which)
                self.send(which, three)
                self.send(which, two)
            else:
                which = chip_slot(zs[i], y_two, x_two)
                self.wait(which)
                self.send(which, three)

        def last(self, diagonal):
            for i in range(4):
                self.wait(chip_slot(zs[i], 1 - ypos, 1 - xpos) if diagonal else chip_slot(zs[i], y_three, x_three))

    edge = d.chunk
    l_parts = (
        (lambda s: lv.at[0, s, :, core], 0),
        (lambda s: lv.at[1, s, :, core, :, pl.ds(edge, d.bond - edge)], 1),
        (lambda s: lv.at[0, s, :, 1 - core, :, pl.ds(0, d.half)], 2),
        (lambda s: lv.at[1, s, :, 1 - core, :, pl.ds(edge, d.half - edge)], 3),
    )
    l_gathers = [Gather(block, l_send.at[n], lambda s, n=n: l_recv.at[n, s]) for block, n in l_parts]

    def l_swap(s, term):
        part = lv.at[:, s, :, term, :, pl.ds(d.half, d.half)]
        return remote(part, part, f_send, f_recv.at[s], partner)

    def l_event(n):
        i = (n + 1) // 2
        for g in l_gathers:
            g.event(n)
        l_swap(chip_slot(zs[i], ypos, xpos) if n % 2 else chip_slot(zs[i], y_two, x_two), core).start()

    def l_last(diagonal):
        for i in range(4):
            which = chip_slot(zs[i], 1 - ypos, 1 - xpos) if diagonal else chip_slot(zs[i], y_three, x_three)
            for g in l_gathers:
                g.wait(which)
            l_swap(which, core).start()

    def l_fill(n, grp):
        s = grp * 4 + n

        @pl.when(s != slot)
        def _():
            l_swap(s, 1 - core).wait_recv()
            for c in range(CORES):
                tile = lv[:, s, c, 1 - core, :, d.half:].reshape(d.half, d.half).T
                lv[:, s, c, 1 - core, :, d.half:] = tile.reshape(CHUNKS, d.chunk, d.half)
                for t in range(d.terms_dev):
                    lv[1, s, c, t, :, :edge] = lv[0, s, c, t, :, edge:d.half].T
        return grp

    def l_along():
        for i in (1, 2, 3):
            for g in l_gathers:
                g.send(slot, device(zs[i], ypos, xpos, core))

    def u_block(p):
        return lambda s: uv.at[p // QUARTERS, pl.ds(p % QUARTERS * 2, 2), pl.ds(pl.multiple_of(s * d.slab, d.slab), d.slab), :]

    u_gathers = [Gather(u_block(p), u_send.at[p], lambda s, p=p: u_recv.at[p, s]) for p in range(PIECES)]

    def act(kind, i, p, j):
        g = u_gathers[p]
        if kind == ALONG:
            g.send(slot, device(zn[i], ypos, xpos, core))
        elif kind == ACROSS:
            g.own_across()
        elif kind == FROM_COLUMN:
            which = chip_slot(zn[i], ypos, xpos)
            g.wait(which)
            g.send(which, three)
            g.send(which, two)
        elif kind == FROM_SECOND:
            which = chip_slot(zn[i], y_two, x_two)
            g.wait(which)
            g.send(which, three)
        elif kind == THIRD:
            g.last(False)
        elif kind == DIAGONAL:
            g.last(True)
        elif kind == RESULT:
            turn_result(j - 1, vcur)
        elif kind == RESULT_OUT:
            hand_out(j - 1, 0, RESULT_EARLY)
        elif kind == RESULT_PUT:
            @pl.when(j > 1)
            def _():
                put_out(j - 2)

    all_right = pltpu.make_async_copy(right, rs, loc_sem.at[2, 0])
    all_right.start()

    for ch in range(CHUNKS):
        for h in range(2):
            mine = left.at[:, pl.ds(pl.multiple_of(core * d.half + ch * d.chunk, d.chunk), d.chunk),
                           pl.ds(pl.multiple_of((core + h) % 2 * d.half, d.half), d.half)]
            theirs = left.at[:, pl.ds(pl.multiple_of((1 - core) * d.half + ch * d.chunk, d.chunk), d.chunk),
                             pl.ds(pl.multiple_of((1 - core + h) % 2 * d.half, d.half), d.half)]
            remote(theirs, lv.at[ch, slot, core, :, :, pl.ds(h * d.half, d.half)], d2d_sem.at[ch, h], d2d_recv.at[ch, h], partner).start()
            pltpu.make_async_copy(mine, lv.at[ch, slot, core, :, :, pl.ds(h * d.half, d.half)], loc_sem.at[ch, h]).start()

    psi_rows = d.half * d.pair // 8
    psi_copies = [pltpu.make_async_copy(psi.at[pl.ds(pl.multiple_of(core * d.half * d.pair + n * psi_rows, psi_rows), psi_rows),
                                               pl.ds(c * d.lane, d.lane)],
                                        ps.at[c, pl.ds(n * psi_rows, psi_rows), :], psi_sem.at[n, c])
                  for n in range(8) for c in range(d.lane_tiles)]
    for copy in psi_copies:
        copy.start()

    first_rows = d.out_rows * d.pair
    first_copies = [pltpu.make_async_copy(psi.at[pl.ds(pl.multiple_of(me * first_rows, first_rows), first_rows), pl.ds(c * d.wide, d.wide)],
                                          tbuf.at[LANCZOS_STEPS - 1, c], first_sem.at[c]) for c in range(d.bond // d.wide)]
    for copy in first_copies:
        copy.start()

    spread = (lax.broadcasted_iota(jnp.int32, (d.pair, d.prod), 1) // d.sub == lax.broadcasted_iota(jnp.int32, (d.pair, d.prod), 0))
    spread = spread.astype(jnp.float32).astype(jnp.bfloat16)
    for t in range(d.terms_dev):
        wv[slot, core, t] = jnp.dot(pair_ops[t], spread, preferred_element_type=jnp.float32).astype(jnp.bfloat16)
    all_right.wait()
    some_rows = d.bond // 8

    def one_sided(i, carry):
        at = pl.ds(pl.multiple_of(i * some_rows, some_rows), some_rows)
        row = lax.broadcasted_iota(jnp.int32, (some_rows, d.bond), 0) + i * some_rows
        one = jnp.where(row == lax.broadcasted_iota(jnp.int32, (some_rows, d.bond), 1), 1.0, 0.0)
        for t in range(d.terms_dev):
            rs[t, at, :] = jnp.where(flags[t] == 1, rs[t, at, :].astype(jnp.float32), one).astype(jnp.bfloat16)
        return carry

    lax.fori_loop(0, 8, one_sided, 0)

    def right_rows(s):
        return rs.at[:, pl.ds(pl.multiple_of(s * d.slab, d.slab), d.slab), :]

    rv[slot, core] = rs[:, pl.ds(pl.multiple_of(slot * d.slab, d.slab), d.slab), :]
    for n in range(1, CHIPS):
        chip = (me // 2 + n) % CHIPS
        to = chip_slot(chip // 4, chip // 2 % 2, chip % 2)
        remote(right_rows(to), rv.at[slot, core], rw_send.at[0], rw_recv.at[0], chip * 2 + core).start()
        remote(wv.at[slot, core], wv.at[slot, core], rw_send.at[1], rw_recv.at[1], chip * 2 + core).start()

    for ch in range(CHUNKS):
        for h in range(2):
            pltpu.make_async_copy(lv.at[ch, slot, core, :, :, pl.ds(h * d.half, d.half)], lv.at[ch, slot, core, :, :, pl.ds(h * d.half, d.half)], loc_sem.at[ch, h]).wait()
            back = remote(lv.at[ch, slot, 1 - core, :, :, pl.ds(h * d.half, d.half)], lv.at[ch, slot, 1 - core, :, :, pl.ds(h * d.half, d.half)], d2d_sem.at[ch, h], d2d_recv.at[ch, h], partner)
            back.wait_recv()
    l_along()
    for g in l_gathers:
        g.own_across()

    total = jnp.zeros((8, d.lane), jnp.float32)
    for n in range(8):
        for copy in psi_copies[n * d.lane_tiles:(n + 1) * d.lane_tiles]:
            copy.wait()

        def add_rows(i, acc, n=n):
            x = ps[:, pl.ds(pl.multiple_of(n * psi_rows + i * (psi_rows // 8), 8), psi_rows // 8), :]
            return acc + jnp.sum((x * x).reshape(d.lane_tiles * psi_rows // 64, 8, d.lane), axis=0)

        total = lax.fori_loop(0, 8, add_rows, total)
    nbuf[0] = jnp.broadcast_to(jnp.sum(total, keepdims=True), (8, 128))
    to_partner = remote(nbuf.at[0], nbuf.at[1], n_send, n_recv, partner)
    to_partner.start()
    to_partner.wait()
    norm = jnp.sqrt((nbuf[0] + nbuf[1])[0:1, :] / d.vec_size)
    norm_one = norm[:, 0:1]
    for copy in first_copies:
        copy.wait()
    tbuf[LANCZOS_STEPS - 1] = tbuf[LANCZOS_STEPS - 1] / norm_one[None]
    first_out = [pltpu.make_async_copy(tbuf.at[LANCZOS_STEPS - 1, c], first.at[:, pl.ds(c * d.wide, d.wide)], first_sem.at[c])
                 for c in range(d.bond // d.wide)]
    for copy in first_out:
        copy.start()

    def place(q):
        tiles = [(ps[c, pl.ds(q, d.half, stride=d.pair), :] / norm_one).T for c in range(d.lane_tiles)]
        xt = jnp.concatenate(tiles, axis=0)
        vprev[...] = xt
        return xt.astype(jnp.bfloat16)

    def start_vector(qb, carry):
        for q2 in range(2):
            q = qb * 2 + q2
            xb = place(q)
            for ch in range(CHUNKS):
                uv[ch, qb, :, q2 * d.chunk:(q2 + 1) * d.chunk] = xb[:, ch * d.chunk:(ch + 1) * d.chunk]
            for bh in range(2):
                rows = vprev[pl.ds(pl.multiple_of(slot * d.slab + bh * d.sub, d.sub), d.sub), :]
                vcur[pl.ds(pl.multiple_of((bh * d.pair + q) * d.sub, d.sub), d.sub), :] = rows
        return carry

    lax.fori_loop(0, d.pair // 4, start_vector, 0)
    fifteen = rv.at[pl.ds(0, CHIPS - 1), 0]
    fifteen_w = wv.at[pl.ds(0, CHIPS - 1), 0]
    remote(fifteen, fifteen, rw_send.at[0], rw_recv.at[0], me).wait()
    remote(fifteen_w, fifteen_w, rw_send.at[1], rw_recv.at[1], me).wait()
    fw_right = remote(rv.at[:, core], rv.at[:, core], fw_send.at[0], fw_recv.at[0], partner)
    fw_pair = remote(wv.at[:, core], wv.at[:, core], fw_send.at[1], fw_recv.at[1], partner)
    fw_right.start()
    fw_pair.start()
    l_event(0)
    l_event(1)
    lax.fori_loop(d.pair // 4, d.pair // 2, start_vector, 0)
    l_event(2)
    l_event(3)
    fw_right.wait()
    fw_pair.wait()
    lane = lax.broadcasted_iota(jnp.int32, (d.sub, d.prod), 1)
    row = lax.broadcasted_iota(jnp.int32, (d.sub, d.prod), 0)
    diagonal = lane % d.sub == row

    def spread_pair(s, carry):
        for c in range(2):
            for t in range(d.terms_dev):
                w = wv[s, c, t].astype(jnp.float32)
                for q in range(d.pair):
                    full = jnp.where(diagonal, jnp.broadcast_to(w[q:q + 1, :], (d.sub, d.prod)), 0.0)
                    kw[s, c, t, q * d.sub:(q + 1) * d.sub, :] = full.astype(jnp.bfloat16)
        return carry

    lax.fori_loop(0, CHIPS, spread_pair, 0)
    l_event(4)
    l_event(5)
    l_event(6)
    vprev[...] = jnp.zeros_like(vprev)
    for copy in first_out:
        copy.wait()

    def right_product(grp, ch, qb):
        r_all = rv[pl.ds(grp * 4, 4)].reshape(d.group_terms * d.slab, d.bond)
        y = jnp.dot(r_all, uv[ch, qb], preferred_element_type=jnp.float32).astype(jnp.bfloat16)
        y = y.reshape(d.group_terms, 2, d.sub, 2 * d.chunk)
        for q2 in range(2):
            for bh in range(2):
                yst[pl.ds(grp * d.group_terms, d.group_terms), qb * 2 + q2, :, bh * d.chunk:(bh + 1) * d.chunk] = \
                    y[:, bh, :, q2 * d.chunk:(q2 + 1) * d.chunk]

    def right_of_group(grp, ch):
        for qb in range(d.pair // 2):
            right_product(grp, ch, qb)

    def right_of_piece(ch, part):
        for qb in range(2):
            for grp in range(GROUPS):
                right_product(grp, ch, part * 2 + qb)

    def left_products(ch, grp):
        for k in range(d.group_terms):
            w = kw[grp * 4 + k // 4, k // 2 % 2, k % 2]
            z = jnp.dot(w, yst[grp * d.group_terms + k].reshape(d.prod, 2 * d.chunk), preferred_element_type=jnp.float32).astype(jnp.bfloat16)
            for bh in range(2):
                zst[bh * d.prod:(bh + 1) * d.prod, k * d.chunk:(k + 1) * d.chunk] = z[:, bh * d.chunk:(bh + 1) * d.chunk]
        l_all = lv[ch, pl.ds(grp * 4, 4)].reshape(d.group_terms * d.chunk, d.bond)
        sig[...] += jnp.dot(zst[...], l_all, preferred_element_type=jnp.float32)

    def turn_result(j, vector):
        for n in range(d.pair // TILE_PARTS):
            rows = [vector[(bh * d.pair + q) * d.sub:(bh * d.pair + q + 1) * d.sub, :d.half]
                    for q in range(n * TILE_PARTS, (n + 1) * TILE_PARTS) for bh in range(2)]
            tbuf[j, n] = jnp.concatenate(rows, axis=0).T

    def hand_out(j, begin, end):
        for n in range(begin, end):
            to = core * CHIPS + n
            block = tbuf.at[j, :, pl.ds(n * d.out_rows, d.out_rows), :]

            @pl.when(to != me)
            def _():
                remote(block, gbuf.at[j, slot], k_send.at[j], k_recv.at[j], to).start()

            @pl.when(to == me)
            def _():
                gbuf[j, slot] = block[...]

    sends_self = me // CHIPS == core
    lanes = lax.broadcasted_iota(jnp.int32, (d.out_rows, d.wide), 1) // d.slab

    def put_out(j, finish=None):
        @pl.when(sends_self)
        def _():
            some = gbuf.at[j, pl.ds(0, CHIPS - 1)]
            remote(some, some, k_send.at[j], k_recv.at[j], me).wait()

        @pl.when(jnp.logical_not(sends_self))
        def _():
            remote(gbuf.at[j], gbuf.at[j], k_send.at[j], k_recv.at[j], me).wait()

        for ct in range(CHIPS // TILE_PARTS):
            for qt in range(d.pair // TILE_PARTS):
                src = [gbuf[j, ct * TILE_PARTS + c, qt] for c in range(TILE_PARTS)]
                if finish is not None:
                    src = [finish(x, gbuf[j - 1, ct * TILE_PARTS + c, qt], ct * TILE_PARTS + c) for c, x in enumerate(src)]
                for q in range(TILE_PARTS):
                    tile = jnp.zeros((d.out_rows, d.wide), jnp.float32)
                    for c in range(TILE_PARTS):
                        shift = (c - q) % TILE_PARTS * d.slab
                        moved = pltpu.roll(src[c], shift, 1) if shift else src[c]
                        tile = jnp.where(lanes == c, moved, tile)
                    tbuf[j, ct, pl.ds(qt * TILE_PARTS + q, d.out_rows, stride=d.pair), :] = tile
            pltpu.make_async_copy(tbuf.at[j, ct], out.at[j, :, pl.ds(ct * d.wide, d.wide)], o_sem.at[j, ct]).start()

    def step(j, carried):
        beta_prev = carried[0]
        later = jnp.minimum(j, 1)
        own = xpos * 2 + ypos
        sig[...] = jnp.zeros_like(sig)

        def slot_step(t, carry):
            n = t // 4
            first_grp = jnp.where(n == 0, own, jnp.where(n == 1, x_two * 2 + y_two, jnp.where(n == 2, x_three * 2 + y_three, 3 - own)))
            first_ch = t // 2 % 2
            done_right = sum((t > r).astype(jnp.int32) for r in RIGHT_SLOTS)
            done_left = t - done_right
            now_right = sum((t == r).astype(jnp.int32) for r in RIGHT_SLOTS)
            is_right = (1 - later) * (1 - t % 2) + later * now_right

            @pl.when(j == 0)
            def _():
                @pl.when(t == 5)
                def _():
                    l_last(False)

                @pl.when(t == 13)
                def _():
                    l_last(True)

                @pl.when(t % 4 == 1)
                def _():
                    lax.fori_loop(0, 4, l_fill, first_grp)

            @pl.when(j > 0)
            def _():
                for four in range(0, len(SLOTS), 4):
                    @pl.when((t >= four) & (t < four + 4))
                    def _():
                        for at in range(four, four + 4):
                            if not SLOTS[at]:
                                continue

                            @pl.when(t == at)
                            def _():
                                for kind, i, p in SLOTS[at]:
                                    act(kind, i, p, j)

            @pl.when((is_right == 1) & (j == 0))
            def _():
                right_of_group(first_grp, first_ch)

            @pl.when((is_right == 1) & (j > 0))
            def _():
                right_of_piece(done_right // QUARTERS, done_right % QUARTERS)

            @pl.when(is_right == 0)
            def _():
                left_products((1 - later) * first_ch + later * (done_left // GROUPS), (1 - later) * first_grp + later * (done_left % GROUPS))
            return carry

        lax.fori_loop(0, len(SLOTS), slot_step, 0)

        @pl.when(j > 0)
        def _():
            for p in range(PIECES):
                sent = uv.at[p // QUARTERS, pl.ds(0, 2), pl.ds(0, 15 * d.slab), :]
                remote(sent, sent, u_send.at[p], u_recv.at[p, 0], me).wait_send()

        other = sig.at[:, pl.ds(d.half, d.half)]
        to_other = remote(other, part, p_send, p_recv, partner)
        to_other.start()
        to_other.wait()
        s = sig[:, :d.half] + part[...]
        v = vcur[...]
        w = s - beta_prev * vprev[...]
        sv = jnp.sum(s * v, keepdims=True)
        wv_sum = jnp.sum(w * v, keepdims=True)
        vv = jnp.sum(v * v, keepdims=True)
        guess = jnp.where(vv > 0.0, wv_sum / jnp.where(vv > 0.0, vv, 1.0), 0.0)
        t = w - guess * v
        sig[:, :d.half] = t
        tt = jnp.sum(t * t, keepdims=True)
        tv = jnp.sum(t * v, keepdims=True)
        at_lane = lax.broadcasted_iota(jnp.int32, (1, 128), 1)
        line = jnp.zeros((1, 128), jnp.float32)
        for n, value in enumerate((sv, vv, tt, tv, guess)):
            line = jnp.where(at_lane == n, value, line)
        scs[...] = line
        scr[me] = line

        def tell(n, carry):
            remote(scs, scr.at[me], s_send, s_recv, (me + n) % DEVS).start()
            return carry

        lax.fori_loop(1, DEVS, tell, 0)

        @pl.when(j > 0)
        def _():
            hand_out(j - 1, RESULT_EARLY, CHIPS)

        @pl.when(j == LANCZOS_STEPS - 1)
        def _():
            turn_result(LANCZOS_STEPS - 1, sig)
            hand_out(LANCZOS_STEPS - 1, 0, CHIPS)

        heard = scr.at[pl.ds(0, DEVS - 1)]
        remote(heard, heard, s_send, s_recv, me).wait()
        told = scr[:, 0, :]
        alpha = jnp.sum(told[:, 0:1], axis=0, keepdims=True) / d.vec_size
        off = alpha - told[:, 4:5]
        square = told[:, 2:3] - 2.0 * off * told[:, 3:4] + off * off * told[:, 1:2]
        beta = jnp.sqrt(jnp.sum(square, axis=0, keepdims=True) / d.vec_size)
        vnew = (sig[:, :d.half] - (alpha - guess) * vcur[...]) / beta
        vprev[...] = vcur[...]
        vcur[...] = vnew
        vb = vnew.astype(jnp.bfloat16)

        @pl.when(j < LANCZOS_STEPS - 1)
        def _():
            for ch in range(CHUNKS):
                for bh in range(2):
                    at = pl.ds(pl.multiple_of(slot * d.slab + bh * d.sub, d.sub), d.sub)
                    for q in range(d.pair):
                        uv[ch, q // 2, at, q % 2 * d.chunk:(q % 2 + 1) * d.chunk] = \
                            vb[(bh * d.pair + q) * d.sub:(bh * d.pair + q + 1) * d.sub, ch * d.chunk:(ch + 1) * d.chunk]
        alphas[j] = alpha[0, 0]
        betas[j] = beta[0, 0]
        return beta, alpha


    zero = jnp.zeros((1, 1), jnp.float32)
    last_beta, last_alpha = lax.fori_loop(0, LANCZOS_STEPS, step, (zero, zero))

    for n, part in enumerate((lv.at[0, pl.ds(0, 15), :, 0], lv.at[1, pl.ds(0, 15), :, 0, :, pl.ds(edge, d.bond - edge)],
                              lv.at[0, pl.ds(0, 15), :, 0, :, pl.ds(0, d.half)], lv.at[1, pl.ds(0, 15), :, 0, :, pl.ds(edge, d.half - edge)])):
        remote(part, part, l_send.at[n], l_recv.at[n, 0], me).wait_send()
    swapped = lv.at[:, pl.ds(0, 15), :, 0, :, pl.ds(d.half, d.half)]
    remote(swapped, swapped, f_send, f_recv.at[0], me).wait_send()
    for ch in range(CHUNKS):
        for h in range(2):
            theirs = left.at[:, pl.ds(0, d.chunk), pl.ds(0, d.half)]
            remote(theirs, lv.at[ch, slot, core, :, :, pl.ds(h * d.half, d.half)], d2d_sem.at[ch, h], d2d_recv.at[ch, h], partner).wait_send()
    put_out(LANCZOS_STEPS - 2)

    def finish(block, before, s):
        owner = device(s % 4, s // 4 % 2, s // 8, me // CHIPS)
        return (block - (last_alpha - scr[owner][:, 4:5]) * before) / last_beta

    put_out(LANCZOS_STEPS - 1, finish)
    for j in range(LANCZOS_STEPS):
        for c in range(d.bond // d.wide):
            pltpu.make_async_copy(tbuf.at[j, c], out.at[j, :, pl.ds(c * d.wide, d.wide)], o_sem.at[j, c]).wait()


def solution(mesh):
    def device_body(wavefunction, left_loc, pair_loc, right_loc, flag_loc):
        bond, pair = wavefunction.shape[0], wavefunction.shape[1]
        d = Dims(bond, pair, left_loc.shape[0])
        bf16, f32 = jnp.bfloat16, jnp.float32
        dma = pltpu.SemaphoreType.DMA
        any_space = pl.BlockSpec(memory_space=pl.ANY)
        smem = pl.BlockSpec(memory_space=pltpu.SMEM)
        scalars = jax.ShapeDtypeStruct((LANCZOS_STEPS,), f32)
        later, first, alphas, betas = pl.pallas_call(
            functools.partial(lanczos_kernel, d),
            out_shape=(jax.ShapeDtypeStruct((LANCZOS_STEPS, d.out_rows * pair, bond), f32),
                       jax.ShapeDtypeStruct((d.out_rows * pair, bond), f32), scalars, scalars),
            in_specs=[any_space] * 3 + [pl.BlockSpec(memory_space=pltpu.VMEM), smem],
            out_specs=(any_space, any_space, smem, smem),
            scratch_shapes=[
                pltpu.VMEM((CHUNKS, CHIPS, CORES, d.terms_dev, d.chunk, bond), bf16),
                pltpu.VMEM((CHIPS, CORES, d.terms_dev, d.slab, bond), bf16),
                pltpu.VMEM((d.terms_dev, bond, bond), bf16),
                pltpu.VMEM((CHIPS, CORES, d.terms_dev, pair, d.prod), bf16),
                pltpu.VMEM((CHIPS, CORES, d.terms_dev, d.prod, d.prod), bf16),
                pltpu.VMEM((CHUNKS, pair // 2, bond, 2 * d.chunk), bf16),
                pltpu.VMEM((d.lane_tiles, d.half * pair, d.lane), f32),
                pltpu.VMEM((CHIPS * CORES * d.terms_dev, pair, d.sub, 2 * d.chunk), bf16),
                pltpu.VMEM((d.rows, d.group_terms * d.chunk), bf16),
                pltpu.VMEM((d.rows, bond), f32),
                pltpu.VMEM((d.rows, d.half), f32),
                pltpu.VMEM((d.rows, d.half), f32),
                pltpu.VMEM((d.rows, d.half), f32),
                pltpu.VMEM((LANCZOS_STEPS, bond // d.wide, d.half, d.wide), f32),
                pltpu.VMEM((LANCZOS_STEPS, CHIPS, bond // d.wide, d.out_rows, d.wide), f32),
                pltpu.VMEM((1, 128), f32),
                pltpu.VMEM((DEVS, 1, 128), f32),
                pltpu.VMEM((2, 8, 128), f32),
                dma((3, 2)), dma((8, d.lane_tiles)), dma((CHUNKS, 2)), dma((CHUNKS, 2)), dma((2,)), dma((2,)), dma((2,)), dma((2,)),
                dma((4,)), dma((4, CHIPS)), dma, dma((CHIPS,)), dma((PIECES,)), dma((PIECES, CHIPS)),
                dma, dma, dma, dma, dma((LANCZOS_STEPS,)), dma((LANCZOS_STEPS,)), dma, dma, dma((LANCZOS_STEPS, bond // d.wide)), dma((bond // d.wide,)),
            ],
            compiler_params=pltpu.CompilerParams(has_side_effects=True, vmem_limit_bytes=67043328),
            name='lanczos',
        )(wavefunction.reshape(bond * pair, bond), left_loc, right_loc, pair_loc, flag_loc)
        krylov = jnp.concatenate([first[None], later])
        return krylov.reshape(LANCZOS_STEPS + 1, d.out_rows, pair, bond), alphas, betas

    return jax.shard_map(device_body, mesh=mesh, in_specs=(P(), P(AXIS_NAME), P(AXIS_NAME), P(AXIS_NAME), P(AXIS_NAME)),
                         out_specs=(P(None, AXIS_NAME), P(), P()), check_vma=False)
```

```python
import functools

import jax
import jax.numpy as jnp
from jax import lax
from jax.experimental import pallas as pl
from jax.experimental.pallas import tpu as pltpu
from jax.sharding import PartitionSpec as P

LANCZOS_STEPS = 6
AXIS_NAME = 'terms'
MESH = pl.DeviceIdType.MESH

CHIPS = 16
CORES = 2
DEVS = 32
CHUNKS = 2
GROUPS = 4
TILE_PARTS = 4
QUARTERS = 4
PIECES = CHUNKS * QUARTERS

ALONG, ACROSS, FROM_COLUMN, FROM_SECOND, THIRD, DIAGONAL, RESULT, RESULT_OUT, RESULT_PUT = range(9)
RIGHT_SLOTS = (0, 1, 2, 3, 8, 9, 10, 11)
SLOTS = (
    ((0, 1, 0), (0, 1, 1), (1, 0, 2), (0, 2, 0), (1, 0, 5), (1, 0, 3), (1, 0, 6), (1, 0, 0), (0, 3, 0), (3, 0, 2), (0, 2, 1), (0, 1, 3), (1, 0, 4), (0, 3, 1), (1, 0, 7), (0, 1, 2), (1, 0, 1), (0, 3, 3), (2, 1, 0), (2, 2, 0), (0, 2, 3), (0, 3, 2), (2, 1, 1), (3, 0, 0), (2, 3, 0), (3, 1, 0), (2, 2, 1), (0, 2, 2), (0, 1, 4), (3, 0, 1), (2, 1, 3), (3, 2, 0), (2, 3, 1), (2, 2, 2), (2, 2, 3), (2, 1, 2), (4, 0, 0), (0, 2, 5), (0, 3, 4), (0, 2, 4), (0, 1, 5), (0, 1, 6), (0, 1, 7), (3, 3, 0), (2, 3, 3), (3, 1, 1), (3, 2, 1), (0, 2, 6), (2, 3, 2), (4, 0, 1), (3, 3, 1), (0, 3, 6), (3, 2, 2), (3, 1, 2), (0, 3, 5), (0, 2, 7), (0, 3, 7), (3, 2, 3), (3, 3, 2), (3, 0, 3), (5, 0, 0), (3, 3, 3), (4, 0, 3), (3, 1, 3), (3, 0, 4),),
    ((6, 0, 0), (2, 2, 4), (5, 0, 1), (3, 0, 6), (2, 1, 4), (4, 0, 2),),
    ((2, 2, 6), (5, 0, 2), (2, 1, 6),),
    ((2, 2, 5), (5, 0, 3), (3, 2, 4), (2, 3, 4),),
    ((2, 1, 5), (3, 0, 5), (3, 1, 4),),
    ((2, 3, 5), (3, 2, 5), (2, 3, 6),),
    ((2, 2, 7), (3, 3, 4), (2, 1, 7), (3, 1, 5), (8, 0, 0),),
    ((3, 3, 5), (2, 3, 7), (3, 2, 6), (3, 1, 6), (3, 3, 6),),
    ((3, 0, 7), (3, 1, 7), (3, 2, 7), (4, 0, 5), (5, 0, 4), (4, 0, 4),),
    ((3, 3, 7), (5, 0, 5),),
    ((4, 0, 6), (5, 0, 6),),
    ((4, 0, 7), (5, 0, 7), (7, 0, 0),),
    (),
    (),
    (),
    (),
)
RESULT_EARLY = 9


class Dims:
    def __init__(self, bond, pair, terms_dev):
        self.bond = bond
        self.pair = pair
        self.terms_dev = terms_dev
        self.slab = bond // CHIPS
        self.sub = self.slab // 2
        self.half = bond // CORES
        self.chunk = self.half // CHUNKS
        self.rows = self.slab * pair
        self.prod = self.sub * pair
        self.out_rows = bond // DEVS
        self.group_terms = 4 * CORES * terms_dev
        self.vec_size = bond * pair * bond
        self.lane = min(bond, 128)
        self.wide = TILE_PARTS * self.slab
        self.lane_tiles = bond // self.lane


def lanczos_kernel(d, psi, left, right, pair_ops, flags, out, first, alphas, betas, lv, rv, rs, wv, kw, uv, ps, yst, zst, sig, part, vcur, vprev, tbuf, gbuf,
                   scs, scr, nbuf,
                   loc_sem, psi_sem, d2d_sem, d2d_recv, rw_send, rw_recv, fw_send, fw_recv, l_send, l_recv, f_send, f_recv, u_send, u_recv,
                   p_send, p_recv, s_send, s_recv, k_send, k_recv, n_send, n_recv, o_sem, first_sem):
    me = lax.axis_index(AXIS_NAME)
    core = me % 2
    xpos = (me // 2) % 2
    ypos = (me // 4) % 2
    zpos = me // 8

    def device(z, y, x, c):
        return ((z * 2 + y) * 2 + x) * 2 + c

    def chip_slot(z, y, x):
        return (x * 2 + y) * 4 + z

    partner = device(zpos, ypos, xpos, 1 - core)
    slot = chip_slot(zpos, ypos, xpos)
    zs = (zpos, zpos + 1 - 2 * (zpos % 2), (zpos + 2) % 4, 3 - zpos)
    inner = (zpos + 1) // 2 % 2
    zn = (zpos, (1 - inner) * (zpos + 1 - zpos // 3 * 2) + inner * (zpos - 1), (1 - inner) * ((zpos + 2) % 4) + inner * (zpos + 1),
          (1 - inner) * (3 - zpos) + inner * ((zpos + 2) % 4))
    y_two = ypos + (1 - core) * (1 - 2 * ypos)
    x_two = xpos + core * (1 - 2 * xpos)
    y_three = ypos + core * (1 - 2 * ypos)
    x_three = xpos + (1 - core) * (1 - 2 * xpos)
    two = device(zpos, y_two, x_two, core)
    three = device(zpos, y_three, x_three, core)

    def remote(src, dst, send, recv, dev):
        return pltpu.make_async_remote_copy(src_ref=src, dst_ref=dst, send_sem=send, recv_sem=recv, device_id=(dev,), device_id_type=MESH)

    class Gather:
        def __init__(self, block, send, recv):
            self.block, self.send_sem, self.recv_sem = block, send, recv

        def send(self, which, dev):
            remote(self.block(which), self.block(which), self.send_sem, self.recv_sem(which), dev).start()

        def wait(self, which):
            remote(self.block(which), self.block(which), self.send_sem, self.recv_sem(which), me).wait_recv()

        def own_along(self):
            for i in (1, 2, 3):
                self.send(slot, device(zs[i], ypos, xpos, core))

        def own_across(self):
            self.send(slot, three)
            self.send(slot, two)

        def event(self, n):
            i = (n + 1) // 2
            if n % 2:
                which = chip_slot(zs[i], ypos, xpos)
                self.wait(which)
                self.send(which, three)
                self.send(which, two)
            else:
                which = chip_slot(zs[i], y_two, x_two)
                self.wait(which)
                self.send(which, three)

        def last(self, diagonal):
            for i in range(4):
                self.wait(chip_slot(zs[i], 1 - ypos, 1 - xpos) if diagonal else chip_slot(zs[i], y_three, x_three))

    edge = d.chunk
    l_parts = (
        (lambda s: lv.at[0, s, :, core], 0),
        (lambda s: lv.at[1, s, :, core, :, pl.ds(edge, d.bond - edge)], 1),
        (lambda s: lv.at[0, s, :, 1 - core, :, pl.ds(0, d.half)], 2),
        (lambda s: lv.at[1, s, :, 1 - core, :, pl.ds(edge, d.half - edge)], 3),
    )
    l_gathers = [Gather(block, l_send.at[n], lambda s, n=n: l_recv.at[n, s]) for block, n in l_parts]

    def l_swap(s, term):
        part = lv.at[:, s, :, term, :, pl.ds(d.half, d.half)]
        return remote(part, part, f_send, f_recv.at[s], partner)

    def l_event(n):
        i = (n + 1) // 2
        for g in l_gathers:
            g.event(n)
        l_swap(chip_slot(zs[i], ypos, xpos) if n % 2 else chip_slot(zs[i], y_two, x_two), core).start()

    def l_late(s):
        for g in l_gathers:
            g.wait(s)
        l_swap(s, core).start()

    def l_fill(s):
        @pl.when(s != slot)
        def _():
            l_swap(s, 1 - core).wait_recv()
            for c in range(CORES):
                tile = lv[:, s, c, 1 - core, :, d.half:].reshape(d.half, d.half).T
                lv[:, s, c, 1 - core, :, d.half:] = tile.reshape(CHUNKS, d.chunk, d.half)
                for t in range(d.terms_dev):
                    lv[1, s, c, t, :, :edge] = lv[0, s, c, t, :, edge:d.half].T

    def l_along():
        for i in (1, 2, 3):
            for g in l_gathers:
                g.send(slot, device(zs[i], ypos, xpos, core))

    def u_block(p):
        return lambda s: uv.at[p // QUARTERS, pl.ds(p % QUARTERS * 2, 2), pl.ds(pl.multiple_of(s * d.slab, d.slab), d.slab), :]

    u_gathers = [Gather(u_block(p), u_send.at[p], lambda s, p=p: u_recv.at[p, s]) for p in range(PIECES)]

    def act(kind, i, p, j):
        g = u_gathers[p]
        if kind == ALONG:
            g.send(slot, device(zn[i], ypos, xpos, core))
        elif kind == ACROSS:
            g.own_across()
        elif kind == FROM_COLUMN:
            which = chip_slot(zn[i], ypos, xpos)
            g.wait(which)
            g.send(which, three)
            g.send(which, two)
        elif kind == FROM_SECOND:
            which = chip_slot(zn[i], y_two, x_two)
            g.wait(which)
            g.send(which, three)
        elif kind == THIRD:
            g.last(False)
        elif kind == DIAGONAL:
            g.last(True)
        elif kind == RESULT:
            turn_result(j - 1, vcur)
        elif kind == RESULT_OUT:
            hand_out(j - 1, 0, RESULT_EARLY)
        elif kind == RESULT_PUT:
            @pl.when(j > 1)
            def _():
                put_out(j - 2)

    all_right = pltpu.make_async_copy(right, rs, loc_sem.at[2, 0])
    all_right.start()

    barrier = pltpu.get_barrier_semaphore()

    def knock(n, carry):
        pl.semaphore_signal(barrier, inc=1, device_id=((me + n) % DEVS,), device_id_type=MESH)
        return carry

    lax.fori_loop(1, DEVS, knock, 0)

    for ch in range(CHUNKS):
        for h in range(2):
            mine = left.at[:, pl.ds(pl.multiple_of(core * d.half + ch * d.chunk, d.chunk), d.chunk),
                           pl.ds(pl.multiple_of((core + h) % 2 * d.half, d.half), d.half)]
            pltpu.make_async_copy(mine, lv.at[ch, slot, core, :, :, pl.ds(h * d.half, d.half)], loc_sem.at[ch, h]).start()

    psi_rows = d.half * d.pair // 8
    psi_copies = [pltpu.make_async_copy(psi.at[pl.ds(pl.multiple_of(core * d.half * d.pair + n * psi_rows, psi_rows), psi_rows),
                                               pl.ds(c * d.lane, d.lane)],
                                        ps.at[c, pl.ds(n * psi_rows, psi_rows), :], psi_sem.at[n, c])
                  for n in range(8) for c in range(d.lane_tiles)]
    for copy in psi_copies:
        copy.start()

    first_rows = d.out_rows * d.pair
    first_copies = [pltpu.make_async_copy(psi.at[pl.ds(pl.multiple_of(me * first_rows, first_rows), first_rows), pl.ds(c * d.wide, d.wide)],
                                          tbuf.at[LANCZOS_STEPS - 1, c], first_sem.at[c]) for c in range(d.bond // d.wide)]
    for copy in first_copies:
        copy.start()

    spread = (lax.broadcasted_iota(jnp.int32, (d.pair, d.prod), 1) // d.sub == lax.broadcasted_iota(jnp.int32, (d.pair, d.prod), 0))
    spread = spread.astype(jnp.float32).astype(jnp.bfloat16)
    for t in range(d.terms_dev):
        wv[slot, core, t] = jnp.dot(pair_ops[t], spread, preferred_element_type=jnp.float32).astype(jnp.bfloat16)
    all_right.wait()
    some_rows = d.bond // 8

    def one_sided(i, carry):
        at = pl.ds(pl.multiple_of(i * some_rows, some_rows), some_rows)
        row = lax.broadcasted_iota(jnp.int32, (some_rows, d.bond), 0) + i * some_rows
        one = jnp.where(row == lax.broadcasted_iota(jnp.int32, (some_rows, d.bond), 1), 1.0, 0.0)
        for t in range(d.terms_dev):
            rs[t, at, :] = jnp.where(flags[t] == 1, rs[t, at, :].astype(jnp.float32), one).astype(jnp.bfloat16)
        return carry

    lax.fori_loop(0, 8, one_sided, 0)

    def right_rows(s):
        return rs.at[:, pl.ds(pl.multiple_of(s * d.slab, d.slab), d.slab), :]

    rv[slot, core] = rs[:, pl.ds(pl.multiple_of(slot * d.slab, d.slab), d.slab), :]

    pl.semaphore_wait(barrier, DEVS - 1)
    for ch in range(CHUNKS):
        for h in range(2):
            theirs = left.at[:, pl.ds(pl.multiple_of((1 - core) * d.half + ch * d.chunk, d.chunk), d.chunk),
                             pl.ds(pl.multiple_of((1 - core + h) % 2 * d.half, d.half), d.half)]
            remote(theirs, lv.at[ch, slot, core, :, :, pl.ds(h * d.half, d.half)], d2d_sem.at[ch, h], d2d_recv.at[ch, h], partner).start()
    for n in range(1, CHIPS):
        chip = (me // 2 + n) % CHIPS
        to = chip_slot(chip // 4, chip // 2 % 2, chip % 2)
        remote(right_rows(to), rv.at[slot, core], rw_send.at[0], rw_recv.at[0], chip * 2 + core).start()
        remote(wv.at[slot, core], wv.at[slot, core], rw_send.at[1], rw_recv.at[1], chip * 2 + core).start()

    for ch in range(CHUNKS):
        for h in range(2):
            pltpu.make_async_copy(lv.at[ch, slot, core, :, :, pl.ds(h * d.half, d.half)], lv.at[ch, slot, core, :, :, pl.ds(h * d.half, d.half)], loc_sem.at[ch, h]).wait()
            back = remote(lv.at[ch, slot, 1 - core, :, :, pl.ds(h * d.half, d.half)], lv.at[ch, slot, 1 - core, :, :, pl.ds(h * d.half, d.half)], d2d_sem.at[ch, h], d2d_recv.at[ch, h], partner)
            back.wait_recv()
    l_along()
    for g in l_gathers:
        g.own_across()

    total = jnp.zeros((8, d.lane), jnp.float32)
    for n in range(8):
        for copy in psi_copies[n * d.lane_tiles:(n + 1) * d.lane_tiles]:
            copy.wait()

        def add_rows(i, acc, n=n):
            x = ps[:, pl.ds(pl.multiple_of(n * psi_rows + i * (psi_rows // 8), 8), psi_rows // 8), :]
            return acc + jnp.sum((x * x).reshape(d.lane_tiles * psi_rows // 64, 8, d.lane), axis=0)

        total = lax.fori_loop(0, 8, add_rows, total)
    nbuf[0] = jnp.broadcast_to(jnp.sum(total, keepdims=True), (8, 128))
    to_partner = remote(nbuf.at[0], nbuf.at[1], n_send, n_recv, partner)
    to_partner.start()
    to_partner.wait()
    norm = jnp.sqrt((nbuf[0] + nbuf[1])[0:1, :] / d.vec_size)
    norm_one = norm[:, 0:1]
    for copy in first_copies:
        copy.wait()
    tbuf[LANCZOS_STEPS - 1] = tbuf[LANCZOS_STEPS - 1] / norm_one[None]
    first_out = [pltpu.make_async_copy(tbuf.at[LANCZOS_STEPS - 1, c], first.at[:, pl.ds(c * d.wide, d.wide)], first_sem.at[c])
                 for c in range(d.bond // d.wide)]
    for copy in first_out:
        copy.start()

    def place(q):
        tiles = [(ps[c, pl.ds(q, d.half, stride=d.pair), :] / norm_one).T for c in range(d.lane_tiles)]
        xt = jnp.concatenate(tiles, axis=0)
        vprev[...] = xt
        return xt.astype(jnp.bfloat16)

    def start_vector(qb, carry):
        for q2 in range(2):
            q = qb * 2 + q2
            xb = place(q)
            for ch in range(CHUNKS):
                uv[ch, qb, :, q2 * d.chunk:(q2 + 1) * d.chunk] = xb[:, ch * d.chunk:(ch + 1) * d.chunk]
            for bh in range(2):
                rows = vprev[pl.ds(pl.multiple_of(slot * d.slab + bh * d.sub, d.sub), d.sub), :]
                vcur[pl.ds(pl.multiple_of((bh * d.pair + q) * d.sub, d.sub), d.sub), :] = rows
        return carry

    lax.fori_loop(0, d.pair // 4, start_vector, 0)
    fifteen = rv.at[pl.ds(0, CHIPS - 1), 0]
    fifteen_w = wv.at[pl.ds(0, CHIPS - 1), 0]
    remote(fifteen, fifteen, rw_send.at[0], rw_recv.at[0], me).wait()
    remote(fifteen_w, fifteen_w, rw_send.at[1], rw_recv.at[1], me).wait()
    fw_right = remote(rv.at[:, core], rv.at[:, core], fw_send.at[0], fw_recv.at[0], partner)
    fw_pair = remote(wv.at[:, core], wv.at[:, core], fw_send.at[1], fw_recv.at[1], partner)
    fw_right.start()
    fw_pair.start()
    l_event(0)
    l_event(1)
    lax.fori_loop(d.pair // 4, d.pair // 2, start_vector, 0)
    l_event(2)
    l_event(3)
    fw_right.wait()
    fw_pair.wait()
    lane = lax.broadcasted_iota(jnp.int32, (d.sub, d.prod), 1)
    row = lax.broadcasted_iota(jnp.int32, (d.sub, d.prod), 0)
    diagonal = lane % d.sub == row

    def spread_pair(s, carry):
        for c in range(2):
            for t in range(d.terms_dev):
                w = wv[s, c, t].astype(jnp.float32)
                for q in range(d.pair):
                    full = jnp.where(diagonal, jnp.broadcast_to(w[q:q + 1, :], (d.sub, d.prod)), 0.0)
                    kw[s, c, t, q * d.sub:(q + 1) * d.sub, :] = full.astype(jnp.bfloat16)
        return carry

    lax.fori_loop(0, CHIPS, spread_pair, 0)
    l_event(4)
    l_event(5)
    l_event(6)
    vprev[...] = jnp.zeros_like(vprev)
    for copy in first_out:
        copy.wait()

    def right_product(grp, ch, qb, to):
        r_all = rv[pl.ds(grp * 4, 4)].reshape(d.group_terms * d.slab, d.bond)
        y = jnp.dot(r_all, uv[ch, qb], preferred_element_type=jnp.float32).astype(jnp.bfloat16)
        y = y.reshape(d.group_terms, 2, d.sub, 2 * d.chunk)
        for q2 in range(2):
            for bh in range(2):
                yst[pl.ds(to * d.group_terms, d.group_terms), qb * 2 + q2, :, bh * d.chunk:(bh + 1) * d.chunk] = \
                    y[:, bh, :, q2 * d.chunk:(q2 + 1) * d.chunk]

    def right_of_piece(ch, part):
        for qb in range(2):
            for grp in range(GROUPS):
                right_product(grp, ch, part * 2 + qb, grp)

    def first_group(n, carry):
        own, third = xpos * 2 + ypos, x_three * 2 + y_three
        grp = jnp.where(n == 0, own, jnp.where(n == 1, x_two * 2 + y_two, jnp.where(n == 2, third, 3 - own)))
        spare = (grp + 1) % GROUPS

        def right_of_group(ch, carry):
            to = grp + ch * (spare - grp)
            for qb in range(d.pair // 2):
                right_product(grp, ch, qb, to)
            return carry

        lax.fori_loop(0, CHUNKS, right_of_group, 0)

        def one_block(i, carry):
            z = jnp.where(i == 0, zs[0], jnp.where(i == 1, zs[1], jnp.where(i == 2, zs[2], zs[3])))
            s = grp * 4 + z

            @pl.when(n == 1)
            def _():
                l_late(third * 4 + z)

            @pl.when(n == 3)
            def _():
                l_late(s)

            l_fill(s)
            block_terms = CORES * d.terms_dev
            for ch in range(CHUNKS):
                at = (grp + ch * (spare - grp)) * d.group_terms + z * block_terms
                for k in range(block_terms):
                    y = yst[at + k].reshape(d.prod, 2 * d.chunk)
                    w = jnp.dot(kw[s, k // 2, k % 2], y, preferred_element_type=jnp.float32).astype(jnp.bfloat16)
                    for bh in range(2):
                        col = (ch * block_terms + k) * d.chunk
                        zst[bh * d.prod:(bh + 1) * d.prod, col:col + d.chunk] = w[:, bh * d.chunk:(bh + 1) * d.chunk]
            wide = CHUNKS * block_terms * d.chunk
            sig[...] += jnp.dot(zst[:, :wide], lv[:, s].reshape(wide, d.bond), preferred_element_type=jnp.float32)
            return carry

        lax.fori_loop(0, 4, one_block, 0)
        return carry

    def left_products(ch, grp):
        for k in range(d.group_terms):
            w = kw[grp * 4 + k // 4, k // 2 % 2, k % 2]
            z = jnp.dot(w, yst[grp * d.group_terms + k].reshape(d.prod, 2 * d.chunk), preferred_element_type=jnp.float32).astype(jnp.bfloat16)
            for bh in range(2):
                zst[bh * d.prod:(bh + 1) * d.prod, k * d.chunk:(k + 1) * d.chunk] = z[:, bh * d.chunk:(bh + 1) * d.chunk]
        l_all = lv[ch, pl.ds(grp * 4, 4)].reshape(d.group_terms * d.chunk, d.bond)
        sig[...] += jnp.dot(zst[...], l_all, preferred_element_type=jnp.float32)

    def turn_result(j, vector):
        for n in range(d.pair // TILE_PARTS):
            rows = [vector[(bh * d.pair + q) * d.sub:(bh * d.pair + q + 1) * d.sub, :d.half]
                    for q in range(n * TILE_PARTS, (n + 1) * TILE_PARTS) for bh in range(2)]
            tbuf[j, n] = jnp.concatenate(rows, axis=0).T

    def hand_out(j, begin, end):
        for n in range(begin, end):
            to = core * CHIPS + n
            block = tbuf.at[j, :, pl.ds(n * d.out_rows, d.out_rows), :]

            @pl.when(to != me)
            def _():
                remote(block, gbuf.at[j, slot], k_send.at[j], k_recv.at[j], to).start()

            @pl.when(to == me)
            def _():
                gbuf[j, slot] = block[...]

    sends_self = me // CHIPS == core
    lanes = lax.broadcasted_iota(jnp.int32, (d.out_rows, d.wide), 1) // d.slab

    def put_out(j, finish=None):
        @pl.when(sends_self)
        def _():
            some = gbuf.at[j, pl.ds(0, CHIPS - 1)]
            remote(some, some, k_send.at[j], k_recv.at[j], me).wait()

        @pl.when(jnp.logical_not(sends_self))
        def _():
            remote(gbuf.at[j], gbuf.at[j], k_send.at[j], k_recv.at[j], me).wait()

        for ct in range(CHIPS // TILE_PARTS):
            for qt in range(d.pair // TILE_PARTS):
                src = [gbuf[j, ct * TILE_PARTS + c, qt] for c in range(TILE_PARTS)]
                if finish is not None:
                    src = [finish(x, gbuf[j - 1, ct * TILE_PARTS + c, qt], ct * TILE_PARTS + c) for c, x in enumerate(src)]
                for q in range(TILE_PARTS):
                    tile = jnp.zeros((d.out_rows, d.wide), jnp.float32)
                    for c in range(TILE_PARTS):
                        shift = (c - q) % TILE_PARTS * d.slab
                        moved = pltpu.roll(src[c], shift, 1) if shift else src[c]
                        tile = jnp.where(lanes == c, moved, tile)
                    tbuf[j, ct, pl.ds(qt * TILE_PARTS + q, d.out_rows, stride=d.pair), :] = tile
            pltpu.make_async_copy(tbuf.at[j, ct], out.at[j, :, pl.ds(ct * d.wide, d.wide)], o_sem.at[j, ct]).start()

    def step(j, carried):
        beta_prev = carried[0]
        sig[...] = jnp.zeros_like(sig)

        def slot_step(t, carry):
            done_right = sum((t > r).astype(jnp.int32) for r in RIGHT_SLOTS)
            done_left = t - done_right
            is_right = sum((t == r).astype(jnp.int32) for r in RIGHT_SLOTS)
            for four in range(0, len(SLOTS), 4):
                @pl.when((t >= four) & (t < four + 4))
                def _():
                    for at in range(four, four + 4):
                        if not SLOTS[at]:
                            continue

                        @pl.when(t == at)
                        def _():
                            for kind, i, p in SLOTS[at]:
                                act(kind, i, p, j)

            @pl.when(is_right == 1)
            def _():
                right_of_piece(done_right // QUARTERS, done_right % QUARTERS)

            @pl.when(is_right == 0)
            def _():
                left_products(done_left // GROUPS, done_left % GROUPS)
            return carry

        @pl.when(j == 0)
        def _():
            lax.fori_loop(0, GROUPS, first_group, 0)

        @pl.when(j > 0)
        def _():
            lax.fori_loop(0, len(SLOTS), slot_step, 0)
            for p in range(PIECES):
                sent = uv.at[p // QUARTERS, pl.ds(0, 2), pl.ds(0, 15 * d.slab), :]
                remote(sent, sent, u_send.at[p], u_recv.at[p, 0], me).wait_send()

        other = sig.at[:, pl.ds(d.half, d.half)]
        to_other = remote(other, part, p_send, p_recv, partner)
        to_other.start()
        to_other.wait()
        s = sig[:, :d.half] + part[...]
        v = vcur[...]
        w = s - beta_prev * vprev[...]
        sv = jnp.sum(s * v, keepdims=True)
        wv_sum = jnp.sum(w * v, keepdims=True)
        vv = jnp.sum(v * v, keepdims=True)
        guess = jnp.where(vv > 0.0, wv_sum / jnp.where(vv > 0.0, vv, 1.0), 0.0)
        t = w - guess * v
        sig[:, :d.half] = t
        tt = jnp.sum(t * t, keepdims=True)
        tv = jnp.sum(t * v, keepdims=True)
        at_lane = lax.broadcasted_iota(jnp.int32, (1, 128), 1)
        line = jnp.zeros((1, 128), jnp.float32)
        for n, value in enumerate((sv, vv, tt, tv, guess)):
            line = jnp.where(at_lane == n, value, line)
        scs[...] = line
        scr[me] = line

        def tell(n, carry):
            remote(scs, scr.at[me], s_send, s_recv, (me + n) % DEVS).start()
            return carry

        lax.fori_loop(1, DEVS, tell, 0)

        @pl.when(j > 0)
        def _():
            hand_out(j - 1, RESULT_EARLY, CHIPS)

        @pl.when(j == LANCZOS_STEPS - 1)
        def _():
            turn_result(LANCZOS_STEPS - 1, sig)
            hand_out(LANCZOS_STEPS - 1, 0, CHIPS)

        heard = scr.at[pl.ds(0, DEVS - 1)]
        remote(heard, heard, s_send, s_recv, me).wait()
        told = scr[:, 0, :]
        alpha = jnp.sum(told[:, 0:1], axis=0, keepdims=True) / d.vec_size
        off = alpha - told[:, 4:5]
        square = told[:, 2:3] - 2.0 * off * told[:, 3:4] + off * off * told[:, 1:2]
        beta = jnp.sqrt(jnp.sum(square, axis=0, keepdims=True) / d.vec_size)
        vnew = (sig[:, :d.half] - (alpha - guess) * vcur[...]) / beta
        vprev[...] = vcur[...]
        vcur[...] = vnew
        vb = vnew.astype(jnp.bfloat16)

        @pl.when(j < LANCZOS_STEPS - 1)
        def _():
            for ch in range(CHUNKS):
                for bh in range(2):
                    at = pl.ds(pl.multiple_of(slot * d.slab + bh * d.sub, d.sub), d.sub)
                    for q in range(d.pair):
                        uv[ch, q // 2, at, q % 2 * d.chunk:(q % 2 + 1) * d.chunk] = \
                            vb[(bh * d.pair + q) * d.sub:(bh * d.pair + q + 1) * d.sub, ch * d.chunk:(ch + 1) * d.chunk]
        alphas[j] = alpha[0, 0]
        betas[j] = beta[0, 0]
        return beta, alpha


    zero = jnp.zeros((1, 1), jnp.float32)
    last_beta, last_alpha = lax.fori_loop(0, LANCZOS_STEPS, step, (zero, zero))

    for n, part in enumerate((lv.at[0, pl.ds(0, 15), :, 0], lv.at[1, pl.ds(0, 15), :, 0, :, pl.ds(edge, d.bond - edge)],
                              lv.at[0, pl.ds(0, 15), :, 0, :, pl.ds(0, d.half)], lv.at[1, pl.ds(0, 15), :, 0, :, pl.ds(edge, d.half - edge)])):
        remote(part, part, l_send.at[n], l_recv.at[n, 0], me).wait_send()
    swapped = lv.at[:, pl.ds(0, 15), :, 0, :, pl.ds(d.half, d.half)]
    remote(swapped, swapped, f_send, f_recv.at[0], me).wait_send()
    for ch in range(CHUNKS):
        for h in range(2):
            theirs = left.at[:, pl.ds(0, d.chunk), pl.ds(0, d.half)]
            remote(theirs, lv.at[ch, slot, core, :, :, pl.ds(h * d.half, d.half)], d2d_sem.at[ch, h], d2d_recv.at[ch, h], partner).wait_send()
    put_out(LANCZOS_STEPS - 2)

    def finish(block, before, s):
        owner = device(s % 4, s // 4 % 2, s // 8, me // CHIPS)
        return (block - (last_alpha - scr[owner][:, 4:5]) * before) / last_beta

    put_out(LANCZOS_STEPS - 1, finish)
    for j in range(LANCZOS_STEPS):
        for c in range(d.bond // d.wide):
            pltpu.make_async_copy(tbuf.at[j, c], out.at[j, :, pl.ds(c * d.wide, d.wide)], o_sem.at[j, c]).wait()


def solution(mesh):
    def device_body(wavefunction, left_loc, pair_loc, right_loc, flag_loc):
        bond, pair = wavefunction.shape[0], wavefunction.shape[1]
        d = Dims(bond, pair, left_loc.shape[0])
        bf16, f32 = jnp.bfloat16, jnp.float32
        dma = pltpu.SemaphoreType.DMA
        any_space = pl.BlockSpec(memory_space=pl.ANY)
        smem = pl.BlockSpec(memory_space=pltpu.SMEM)
        scalars = jax.ShapeDtypeStruct((LANCZOS_STEPS,), f32)
        later, first, alphas, betas = pl.pallas_call(
            functools.partial(lanczos_kernel, d),
            out_shape=(jax.ShapeDtypeStruct((LANCZOS_STEPS, d.out_rows * pair, bond), f32),
                       jax.ShapeDtypeStruct((d.out_rows * pair, bond), f32), scalars, scalars),
            in_specs=[any_space] * 3 + [pl.BlockSpec(memory_space=pltpu.VMEM), smem],
            out_specs=(any_space, any_space, smem, smem),
            scratch_shapes=[
                pltpu.VMEM((CHUNKS, CHIPS, CORES, d.terms_dev, d.chunk, bond), bf16),
                pltpu.VMEM((CHIPS, CORES, d.terms_dev, d.slab, bond), bf16),
                pltpu.VMEM((d.terms_dev, bond, bond), bf16),
                pltpu.VMEM((CHIPS, CORES, d.terms_dev, pair, d.prod), bf16),
                pltpu.VMEM((CHIPS, CORES, d.terms_dev, d.prod, d.prod), bf16),
                pltpu.VMEM((CHUNKS, pair // 2, bond, 2 * d.chunk), bf16),
                pltpu.VMEM((d.lane_tiles, d.half * pair, d.lane), f32),
                pltpu.VMEM((CHIPS * CORES * d.terms_dev, pair, d.sub, 2 * d.chunk), bf16),
                pltpu.VMEM((d.rows, d.group_terms * d.chunk), bf16),
                pltpu.VMEM((d.rows, bond), f32),
                pltpu.VMEM((d.rows, d.half), f32),
                pltpu.VMEM((d.rows, d.half), f32),
                pltpu.VMEM((d.rows, d.half), f32),
                pltpu.VMEM((LANCZOS_STEPS, bond // d.wide, d.half, d.wide), f32),
                pltpu.VMEM((LANCZOS_STEPS, CHIPS, bond // d.wide, d.out_rows, d.wide), f32),
                pltpu.VMEM((1, 128), f32),
                pltpu.VMEM((DEVS, 1, 128), f32),
                pltpu.VMEM((2, 8, 128), f32),
                dma((3, 2)), dma((8, d.lane_tiles)), dma((CHUNKS, 2)), dma((CHUNKS, 2)), dma((2,)), dma((2,)), dma((2,)), dma((2,)),
                dma((4,)), dma((4, CHIPS)), dma, dma((CHIPS,)), dma((PIECES,)), dma((PIECES, CHIPS)),
                dma, dma, dma, dma, dma((LANCZOS_STEPS,)), dma((LANCZOS_STEPS,)), dma, dma, dma((LANCZOS_STEPS, bond // d.wide)), dma((bond // d.wide,)),
            ],
            compiler_params=pltpu.CompilerParams(has_side_effects=True, collective_id=0, vmem_limit_bytes=67043328),
            name='lanczos',
        )(wavefunction.reshape(bond * pair, bond), left_loc, right_loc, pair_loc, flag_loc)
        krylov = jnp.concatenate([first[None], later])
        return krylov.reshape(LANCZOS_STEPS + 1, d.out_rows, pair, bond), alphas, betas

    return jax.shard_map(device_body, mesh=mesh, in_specs=(P(), P(AXIS_NAME), P(AXIS_NAME), P(AXIS_NAME), P(AXIS_NAME)),
                         out_specs=(P(None, AXIS_NAME), P(), P()), check_vma=False)
```

```python
import functools

import jax
import jax.numpy as jnp
from jax import lax
from jax.experimental import pallas as pl
from jax.experimental.pallas import tpu as pltpu
from jax.sharding import PartitionSpec as P

LANCZOS_STEPS = 6
AXIS_NAME = 'terms'
MESH = pl.DeviceIdType.MESH

CHIPS = 16
CORES = 2
DEVS = 32
CHUNKS = 2
GROUPS = 4
TILE_PARTS = 4
QUARTERS = 4
PIECES = CHUNKS * QUARTERS

ALONG, ACROSS, FROM_COLUMN, FROM_SECOND, THIRD, DIAGONAL, RESULT, RESULT_OUT, RESULT_PUT = range(9)
RIGHT_SLOTS = (0, 1, 2, 3, 8, 9, 10, 11)
SLOTS = (
    ((0, 1, 0), (0, 1, 1), (1, 0, 2), (0, 2, 0), (1, 0, 5), (1, 0, 3), (1, 0, 6), (1, 0, 0), (0, 3, 0), (3, 0, 2), (0, 2, 1), (0, 1, 3), (1, 0, 4), (0, 3, 1), (1, 0, 7), (0, 1, 2), (1, 0, 1), (0, 3, 3), (2, 1, 0), (2, 2, 0), (0, 2, 3), (0, 3, 2), (2, 1, 1), (3, 0, 0), (2, 3, 0), (3, 1, 0), (2, 2, 1), (0, 2, 2), (0, 1, 4), (3, 0, 1), (2, 1, 3), (3, 2, 0), (2, 3, 1), (2, 2, 2), (2, 2, 3), (2, 1, 2), (4, 0, 0), (0, 2, 5), (0, 3, 4), (0, 2, 4), (0, 1, 5), (0, 1, 6), (0, 1, 7), (3, 3, 0), (2, 3, 3), (3, 1, 1), (3, 2, 1), (0, 2, 6), (2, 3, 2), (4, 0, 1), (3, 3, 1), (0, 3, 6), (3, 2, 2), (3, 1, 2), (0, 3, 5), (0, 2, 7), (0, 3, 7), (3, 2, 3), (3, 3, 2), (3, 0, 3), (5, 0, 0), (3, 3, 3), (4, 0, 3), (3, 1, 3), (3, 0, 4),),
    ((6, 0, 0), (2, 2, 4), (5, 0, 1), (3, 0, 6), (2, 1, 4), (4, 0, 2),),
    ((2, 2, 6), (5, 0, 2), (2, 1, 6),),
    ((2, 2, 5), (5, 0, 3), (3, 2, 4), (2, 3, 4),),
    ((2, 1, 5), (3, 0, 5), (3, 1, 4),),
    ((2, 3, 5), (3, 2, 5), (2, 3, 6),),
    ((2, 2, 7), (3, 3, 4), (2, 1, 7), (3, 1, 5), (8, 0, 0),),
    ((3, 3, 5), (2, 3, 7), (3, 2, 6), (3, 1, 6), (3, 3, 6),),
    ((3, 0, 7), (3, 1, 7), (3, 2, 7), (4, 0, 5), (5, 0, 4), (4, 0, 4),),
    ((3, 3, 7), (5, 0, 5),),
    ((4, 0, 6), (5, 0, 6),),
    ((4, 0, 7), (5, 0, 7), (7, 0, 0),),
    (),
    (),
    (),
    (),
)
RESULT_EARLY = 9


class Dims:
    def __init__(self, bond, pair, terms_dev):
        self.bond = bond
        self.pair = pair
        self.terms_dev = terms_dev
        self.slab = bond // CHIPS
        self.sub = self.slab // 2
        self.half = bond // CORES
        self.chunk = self.half // CHUNKS
        self.rows = self.slab * pair
        self.prod = self.sub * pair
        self.out_rows = bond // DEVS
        self.group_terms = 4 * CORES * terms_dev
        self.vec_size = bond * pair * bond
        self.lane = min(bond, 128)
        self.wide = TILE_PARTS * self.slab
        self.lane_tiles = bond // self.lane


def lanczos_kernel(d, psi, left, right, pair_ops, flags, out, first, alphas, betas, lv, rv, rs, wv, kw, uv, ps, yst, zst, sig, part, vcur, vprev, tbuf, gbuf,
                   scs, scr, nbuf,
                   loc_sem, psi_sem, d2d_sem, d2d_recv, rw_send, rw_recv, fw_send, fw_recv, l_send, l_recv, f_send, f_recv, u_send, u_recv,
                   p_send, p_recv, s_send, s_recv, k_send, k_recv, n_send, n_recv, o_sem, first_sem):
    me = lax.axis_index(AXIS_NAME)
    core = me % 2
    xpos = (me // 2) % 2
    ypos = (me // 4) % 2
    zpos = me // 8

    def device(z, y, x, c):
        return ((z * 2 + y) * 2 + x) * 2 + c

    def chip_slot(z, y, x):
        return (x * 2 + y) * 4 + z

    partner = device(zpos, ypos, xpos, 1 - core)
    slot = chip_slot(zpos, ypos, xpos)
    zs = (zpos, zpos + 1 - 2 * (zpos % 2), (zpos + 2) % 4, 3 - zpos)
    inner = (zpos + 1) // 2 % 2
    zn = (zpos, (1 - inner) * (zpos + 1 - zpos // 3 * 2) + inner * (zpos - 1), (1 - inner) * ((zpos + 2) % 4) + inner * (zpos + 1),
          (1 - inner) * (3 - zpos) + inner * ((zpos + 2) % 4))
    y_two = ypos + (1 - core) * (1 - 2 * ypos)
    x_two = xpos + core * (1 - 2 * xpos)
    y_three = ypos + core * (1 - 2 * ypos)
    x_three = xpos + (1 - core) * (1 - 2 * xpos)
    two = device(zpos, y_two, x_two, core)
    three = device(zpos, y_three, x_three, core)

    def remote(src, dst, send, recv, dev):
        return pltpu.make_async_remote_copy(src_ref=src, dst_ref=dst, send_sem=send, recv_sem=recv, device_id=(dev,), device_id_type=MESH)

    class Gather:
        def __init__(self, block, send, recv):
            self.block, self.send_sem, self.recv_sem = block, send, recv

        def send(self, which, dev):
            remote(self.block(which), self.block(which), self.send_sem, self.recv_sem(which), dev).start()

        def wait(self, which):
            remote(self.block(which), self.block(which), self.send_sem, self.recv_sem(which), me).wait_recv()

        def own_along(self):
            for i in (1, 2, 3):
                self.send(slot, device(zs[i], ypos, xpos, core))

        def own_across(self):
            self.send(slot, three)
            self.send(slot, two)

        def event(self, n):
            i = (n + 1) // 2
            if n % 2:
                which = chip_slot(zs[i], ypos, xpos)
                self.wait(which)
                self.send(which, three)
                self.send(which, two)
            else:
                which = chip_slot(zs[i], y_two, x_two)
                self.wait(which)
                self.send(which, three)

        def last(self, diagonal):
            for i in range(4):
                self.wait(chip_slot(zs[i], 1 - ypos, 1 - xpos) if diagonal else chip_slot(zs[i], y_three, x_three))

    edge = d.chunk
    l_parts = (
        (lambda s: lv.at[0, s, :, core], 0),
        (lambda s: lv.at[1, s, :, core, :, pl.ds(edge, d.bond - edge)], 1),
        (lambda s: lv.at[0, s, :, 1 - core, :, pl.ds(0, d.half)], 2),
        (lambda s: lv.at[1, s, :, 1 - core, :, pl.ds(edge, d.half - edge)], 3),
    )
    l_gathers = [Gather(block, l_send.at[n], lambda s, n=n: l_recv.at[n, s]) for block, n in l_parts]

    def l_swap(s, term):
        part = lv.at[:, s, :, term, :, pl.ds(d.half, d.half)]
        return remote(part, part, f_send, f_recv.at[s], partner)

    def l_event(n):
        i = (n + 1) // 2
        for g in l_gathers:
            g.event(n)
        l_swap(chip_slot(zs[i], ypos, xpos) if n % 2 else chip_slot(zs[i], y_two, x_two), core).start()

    def l_last(diagonal):
        for i in range(4):
            which = chip_slot(zs[i], 1 - ypos, 1 - xpos) if diagonal else chip_slot(zs[i], y_three, x_three)
            for g in l_gathers:
                g.wait(which)
            l_swap(which, core).start()

    def l_fill(n, grp):
        s = grp * 4 + n

        @pl.when(s != slot)
        def _():
            l_swap(s, 1 - core).wait_recv()
            for c in range(CORES):
                tile = lv[:, s, c, 1 - core, :, d.half:].reshape(d.half, d.half).T
                lv[:, s, c, 1 - core, :, d.half:] = tile.reshape(CHUNKS, d.chunk, d.half)
                for t in range(d.terms_dev):
                    lv[1, s, c, t, :, :edge] = lv[0, s, c, t, :, edge:d.half].T
        return grp

    def l_along():
        for i in (1, 2, 3):
            for g in l_gathers:
                g.send(slot, device(zs[i], ypos, xpos, core))

    def u_block(p):
        return lambda s: uv.at[p // QUARTERS, pl.ds(p % QUARTERS * 2, 2), pl.ds(pl.multiple_of(s * d.slab, d.slab), d.slab), :]

    u_gathers = [Gather(u_block(p), u_send.at[p], lambda s, p=p: u_recv.at[p, s]) for p in range(PIECES)]

    def act(kind, i, p, j):
        g = u_gathers[p]
        if kind == ALONG:
            g.send(slot, device(zn[i], ypos, xpos, core))
        elif kind == ACROSS:
            g.own_across()
        elif kind == FROM_COLUMN:
            which = chip_slot(zn[i], ypos, xpos)
            g.wait(which)
            g.send(which, three)
            g.send(which, two)
        elif kind == FROM_SECOND:
            which = chip_slot(zn[i], y_two, x_two)
            g.wait(which)
            g.send(which, three)
        elif kind == THIRD:
            g.last(False)
        elif kind == DIAGONAL:
            g.last(True)
        elif kind == RESULT:
            turn_result(j - 1, vcur)
        elif kind == RESULT_OUT:
            hand_out(j - 1, 0, RESULT_EARLY)
        elif kind == RESULT_PUT:
            @pl.when(j > 1)
            def _():
                put_out(j - 2)

    all_right = pltpu.make_async_copy(right, rs, loc_sem.at[2, 0])
    all_right.start()

    barrier = pltpu.get_barrier_semaphore()

    def knock(n, carry):
        pl.semaphore_signal(barrier, inc=1, device_id=((me + n) % DEVS,), device_id_type=MESH)
        return carry

    lax.fori_loop(1, DEVS, knock, 0)

    for ch in range(CHUNKS):
        for h in range(2):
            mine = left.at[:, pl.ds(pl.multiple_of(core * d.half + ch * d.chunk, d.chunk), d.chunk),
                           pl.ds(pl.multiple_of((core + h) % 2 * d.half, d.half), d.half)]
            pltpu.make_async_copy(mine, lv.at[ch, slot, core, :, :, pl.ds(h * d.half, d.half)], loc_sem.at[ch, h]).start()

    psi_rows = d.half * d.pair // 8
    psi_copies = [pltpu.make_async_copy(psi.at[pl.ds(pl.multiple_of(core * d.half * d.pair + n * psi_rows, psi_rows), psi_rows),
                                               pl.ds(c * d.lane, d.lane)],
                                        ps.at[c, pl.ds(n * psi_rows, psi_rows), :], psi_sem.at[n, c])
                  for n in range(8) for c in range(d.lane_tiles)]
    for copy in psi_copies:
        copy.start()

    first_rows = d.out_rows * d.pair
    first_copies = [pltpu.make_async_copy(psi.at[pl.ds(pl.multiple_of(me * first_rows, first_rows), first_rows), pl.ds(c * d.wide, d.wide)],
                                          tbuf.at[LANCZOS_STEPS - 1, c], first_sem.at[c]) for c in range(d.bond // d.wide)]
    for copy in first_copies:
        copy.start()

    spread = (lax.broadcasted_iota(jnp.int32, (d.pair, d.prod), 1) // d.sub == lax.broadcasted_iota(jnp.int32, (d.pair, d.prod), 0))
    spread = spread.astype(jnp.float32).astype(jnp.bfloat16)
    for t in range(d.terms_dev):
        wv[slot, core, t] = jnp.dot(pair_ops[t], spread, preferred_element_type=jnp.float32).astype(jnp.bfloat16)
    all_right.wait()
    some_rows = d.bond // 8

    def one_sided(i, carry):
        at = pl.ds(pl.multiple_of(i * some_rows, some_rows), some_rows)
        row = lax.broadcasted_iota(jnp.int32, (some_rows, d.bond), 0) + i * some_rows
        one = jnp.where(row == lax.broadcasted_iota(jnp.int32, (some_rows, d.bond), 1), 1.0, 0.0)
        for t in range(d.terms_dev):
            rs[t, at, :] = jnp.where(flags[t] == 1, rs[t, at, :].astype(jnp.float32), one).astype(jnp.bfloat16)
        return carry

    lax.fori_loop(0, 8, one_sided, 0)

    def right_rows(s):
        return rs.at[:, pl.ds(pl.multiple_of(s * d.slab, d.slab), d.slab), :]

    rv[slot, core] = rs[:, pl.ds(pl.multiple_of(slot * d.slab, d.slab), d.slab), :]

    pl.semaphore_wait(barrier, DEVS - 1)
    for ch in range(CHUNKS):
        for h in range(2):
            theirs = left.at[:, pl.ds(pl.multiple_of((1 - core) * d.half + ch * d.chunk, d.chunk), d.chunk),
                             pl.ds(pl.multiple_of((1 - core + h) % 2 * d.half, d.half), d.half)]
            remote(theirs, lv.at[ch, slot, core, :, :, pl.ds(h * d.half, d.half)], d2d_sem.at[ch, h], d2d_recv.at[ch, h], partner).start()
    for n in range(1, CHIPS):
        chip = (me // 2 + n) % CHIPS
        to = chip_slot(chip // 4, chip // 2 % 2, chip % 2)
        remote(right_rows(to), rv.at[slot, core], rw_send.at[0], rw_recv.at[0], chip * 2 + core).start()
        remote(wv.at[slot, core], wv.at[slot, core], rw_send.at[1], rw_recv.at[1], chip * 2 + core).start()

    for ch in range(CHUNKS):
        for h in range(2):
            pltpu.make_async_copy(lv.at[ch, slot, core, :, :, pl.ds(h * d.half, d.half)], lv.at[ch, slot, core, :, :, pl.ds(h * d.half, d.half)], loc_sem.at[ch, h]).wait()
            back = remote(lv.at[ch, slot, 1 - core, :, :, pl.ds(h * d.half, d.half)], lv.at[ch, slot, 1 - core, :, :, pl.ds(h * d.half, d.half)], d2d_sem.at[ch, h], d2d_recv.at[ch, h], partner)
            back.wait_recv()
    l_along()
    for g in l_gathers:
        g.own_across()

    total = jnp.zeros((8, d.lane), jnp.float32)
    for n in range(8):
        for copy in psi_copies[n * d.lane_tiles:(n + 1) * d.lane_tiles]:
            copy.wait()

        def add_rows(i, acc, n=n):
            x = ps[:, pl.ds(pl.multiple_of(n * psi_rows + i * (psi_rows // 8), 8), psi_rows // 8), :]
            return acc + jnp.sum((x * x).reshape(d.lane_tiles * psi_rows // 64, 8, d.lane), axis=0)

        total = lax.fori_loop(0, 8, add_rows, total)
    nbuf[0] = jnp.broadcast_to(jnp.sum(total, keepdims=True), (8, 128))
    to_partner = remote(nbuf.at[0], nbuf.at[1], n_send, n_recv, partner)
    to_partner.start()
    to_partner.wait()
    norm = jnp.sqrt((nbuf[0] + nbuf[1])[0:1, :] / d.vec_size)
    norm_one = norm[:, 0:1]
    for copy in first_copies:
        copy.wait()
    tbuf[LANCZOS_STEPS - 1] = tbuf[LANCZOS_STEPS - 1] / norm_one[None]
    first_out = [pltpu.make_async_copy(tbuf.at[LANCZOS_STEPS - 1, c], first.at[:, pl.ds(c * d.wide, d.wide)], first_sem.at[c])
                 for c in range(d.bond // d.wide)]
    for copy in first_out:
        copy.start()

    def place(q):
        tiles = [(ps[c, pl.ds(q, d.half, stride=d.pair), :] / norm_one).T for c in range(d.lane_tiles)]
        xt = jnp.concatenate(tiles, axis=0)
        vprev[...] = xt
        return xt.astype(jnp.bfloat16)

    def start_vector(qb, carry):
        for q2 in range(2):
            q = qb * 2 + q2
            xb = place(q)
            for ch in range(CHUNKS):
                uv[ch, qb, :, q2 * d.chunk:(q2 + 1) * d.chunk] = xb[:, ch * d.chunk:(ch + 1) * d.chunk]
            for bh in range(2):
                rows = vprev[pl.ds(pl.multiple_of(slot * d.slab + bh * d.sub, d.sub), d.sub), :]
                vcur[pl.ds(pl.multiple_of((bh * d.pair + q) * d.sub, d.sub), d.sub), :] = rows
        return carry

    lax.fori_loop(0, d.pair // 4, start_vector, 0)
    fifteen = rv.at[pl.ds(0, CHIPS - 1), 0]
    fifteen_w = wv.at[pl.ds(0, CHIPS - 1), 0]
    remote(fifteen, fifteen, rw_send.at[0], rw_recv.at[0], me).wait()
    remote(fifteen_w, fifteen_w, rw_send.at[1], rw_recv.at[1], me).wait()
    fw_right = remote(rv.at[:, core], rv.at[:, core], fw_send.at[0], fw_recv.at[0], partner)
    fw_pair = remote(wv.at[:, core], wv.at[:, core], fw_send.at[1], fw_recv.at[1], partner)
    fw_right.start()
    fw_pair.start()
    l_event(0)
    l_event(1)
    lax.fori_loop(d.pair // 4, d.pair // 2, start_vector, 0)
    l_event(2)
    l_event(3)
    fw_right.wait()
    fw_pair.wait()
    lane = lax.broadcasted_iota(jnp.int32, (d.sub, d.prod), 1)
    row = lax.broadcasted_iota(jnp.int32, (d.sub, d.prod), 0)
    diagonal = lane % d.sub == row

    def spread_pair(s, carry):
        for c in range(2):
            for t in range(d.terms_dev):
                w = wv[s, c, t].astype(jnp.float32)
                for q in range(d.pair):
                    full = jnp.where(diagonal, jnp.broadcast_to(w[q:q + 1, :], (d.sub, d.prod)), 0.0)
                    kw[s, c, t, q * d.sub:(q + 1) * d.sub, :] = full.astype(jnp.bfloat16)
        return carry

    lax.fori_loop(0, CHIPS, spread_pair, 0)
    l_event(4)
    l_event(5)
    l_event(6)
    vprev[...] = jnp.zeros_like(vprev)
    for copy in first_out:
        copy.wait()

    def right_product(grp, ch, qb):
        r_all = rv[pl.ds(grp * 4, 4)].reshape(d.group_terms * d.slab, d.bond)
        y = jnp.dot(r_all, uv[ch, qb], preferred_element_type=jnp.float32).astype(jnp.bfloat16)
        y = y.reshape(d.group_terms, 2, d.sub, 2 * d.chunk)
        for q2 in range(2):
            for bh in range(2):
                yst[pl.ds(grp * d.group_terms, d.group_terms), qb * 2 + q2, :, bh * d.chunk:(bh + 1) * d.chunk] = \
                    y[:, bh, :, q2 * d.chunk:(q2 + 1) * d.chunk]

    def right_of_group(grp, ch):
        for qb in range(d.pair // 2):
            right_product(grp, ch, qb)

    def right_of_piece(ch, part):
        for qb in range(2):
            for grp in range(GROUPS):
                right_product(grp, ch, part * 2 + qb)

    def left_products(ch, grp):
        for k in range(d.group_terms):
            w = kw[grp * 4 + k // 4, k // 2 % 2, k % 2]
            z = jnp.dot(w, yst[grp * d.group_terms + k].reshape(d.prod, 2 * d.chunk), preferred_element_type=jnp.float32).astype(jnp.bfloat16)
            for bh in range(2):
                zst[bh * d.prod:(bh + 1) * d.prod, k * d.chunk:(k + 1) * d.chunk] = z[:, bh * d.chunk:(bh + 1) * d.chunk]
        l_all = lv[ch, pl.ds(grp * 4, 4)].reshape(d.group_terms * d.chunk, d.bond)
        sig[...] += jnp.dot(zst[...], l_all, preferred_element_type=jnp.float32)

    def turn_result(j, vector):
        for n in range(d.pair // TILE_PARTS):
            rows = [vector[(bh * d.pair + q) * d.sub:(bh * d.pair + q + 1) * d.sub, :d.half]
                    for q in range(n * TILE_PARTS, (n + 1) * TILE_PARTS) for bh in range(2)]
            tbuf[j, n] = jnp.concatenate(rows, axis=0).T

    def hand_out(j, begin, end):
        for n in range(begin, end):
            to = core * CHIPS + n
            block = tbuf.at[j, :, pl.ds(n * d.out_rows, d.out_rows), :]

            @pl.when(to != me)
            def _():
                remote(block, gbuf.at[j, slot], k_send.at[j], k_recv.at[j], to).start()

            @pl.when(to == me)
            def _():
                gbuf[j, slot] = block[...]

    sends_self = me // CHIPS == core
    lanes = lax.broadcasted_iota(jnp.int32, (d.out_rows, d.wide), 1) // d.slab

    def put_out(j, finish=None):
        @pl.when(sends_self)
        def _():
            some = gbuf.at[j, pl.ds(0, CHIPS - 1)]
            remote(some, some, k_send.at[j], k_recv.at[j], me).wait()

        @pl.when(jnp.logical_not(sends_self))
        def _():
            remote(gbuf.at[j], gbuf.at[j], k_send.at[j], k_recv.at[j], me).wait()

        for ct in range(CHIPS // TILE_PARTS):
            for qt in range(d.pair // TILE_PARTS):
                src = [gbuf[j, ct * TILE_PARTS + c, qt] for c in range(TILE_PARTS)]
                if finish is not None:
                    src = [finish(x, gbuf[j - 1, ct * TILE_PARTS + c, qt], ct * TILE_PARTS + c) for c, x in enumerate(src)]
                for q in range(TILE_PARTS):
                    tile = jnp.zeros((d.out_rows, d.wide), jnp.float32)
                    for c in range(TILE_PARTS):
                        shift = (c - q) % TILE_PARTS * d.slab
                        moved = pltpu.roll(src[c], shift, 1) if shift else src[c]
                        tile = jnp.where(lanes == c, moved, tile)
                    tbuf[j, ct, pl.ds(qt * TILE_PARTS + q, d.out_rows, stride=d.pair), :] = tile
            pltpu.make_async_copy(tbuf.at[j, ct], out.at[j, :, pl.ds(ct * d.wide, d.wide)], o_sem.at[j, ct]).start()

    def step(j, carried):
        beta_prev = carried[0]
        later = jnp.minimum(j, 1)
        own = xpos * 2 + ypos
        sig[...] = jnp.zeros_like(sig)

        def slot_step(t, carry):
            n = t // 4
            first_grp = jnp.where(n == 0, own, jnp.where(n == 1, x_two * 2 + y_two, jnp.where(n == 2, x_three * 2 + y_three, 3 - own)))
            first_ch = t // 2 % 2
            done_right = sum((t > r).astype(jnp.int32) for r in RIGHT_SLOTS)
            done_left = t - done_right
            now_right = sum((t == r).astype(jnp.int32) for r in RIGHT_SLOTS)
            is_right = (1 - later) * (1 - t % 2) + later * now_right

            @pl.when(j == 0)
            def _():
                @pl.when(t == 5)
                def _():
                    l_last(False)

                @pl.when(t == 13)
                def _():
                    l_last(True)

                @pl.when(t % 4 == 1)
                def _():
                    lax.fori_loop(0, 4, l_fill, first_grp)

            @pl.when(j > 0)
            def _():
                for four in range(0, len(SLOTS), 4):
                    @pl.when((t >= four) & (t < four + 4))
                    def _():
                        for at in range(four, four + 4):
                            if not SLOTS[at]:
                                continue

                            @pl.when(t == at)
                            def _():
                                for kind, i, p in SLOTS[at]:
                                    act(kind, i, p, j)

            @pl.when((is_right == 1) & (j == 0))
            def _():
                right_of_group(first_grp, first_ch)

            @pl.when((is_right == 1) & (j > 0))
            def _():
                right_of_piece(done_right // QUARTERS, done_right % QUARTERS)

            @pl.when(is_right == 0)
            def _():
                left_products((1 - later) * first_ch + later * (done_left // GROUPS), (1 - later) * first_grp + later * (done_left % GROUPS))
            return carry

        lax.fori_loop(0, len(SLOTS), slot_step, 0)

        @pl.when(j > 0)
        def _():
            for p in range(PIECES):
                sent = uv.at[p // QUARTERS, pl.ds(0, 2), pl.ds(0, 15 * d.slab), :]
                remote(sent, sent, u_send.at[p], u_recv.at[p, 0], me).wait_send()

        other = sig.at[:, pl.ds(d.half, d.half)]
        to_other = remote(other, part, p_send, p_recv, partner)
        to_other.start()
        to_other.wait()
        s = sig[:, :d.half] + part[...]
        v = vcur[...]
        w = s - beta_prev * vprev[...]
        sv = jnp.sum(s * v, keepdims=True)
        wv_sum = jnp.sum(w * v, keepdims=True)
        vv = jnp.sum(v * v, keepdims=True)
        guess = jnp.where(vv > 0.0, wv_sum / jnp.where(vv > 0.0, vv, 1.0), 0.0)
        t = w - guess * v
        sig[:, :d.half] = t
        tt = jnp.sum(t * t, keepdims=True)
        tv = jnp.sum(t * v, keepdims=True)
        at_lane = lax.broadcasted_iota(jnp.int32, (1, 128), 1)
        line = jnp.zeros((1, 128), jnp.float32)
        for n, value in enumerate((sv, vv, tt, tv, guess)):
            line = jnp.where(at_lane == n, value, line)
        scs[...] = line
        scr[me] = line

        def tell(n, carry):
            remote(scs, scr.at[me], s_send, s_recv, (me + n) % DEVS).start()
            return carry

        lax.fori_loop(1, DEVS, tell, 0)

        @pl.when(j > 0)
        def _():
            hand_out(j - 1, RESULT_EARLY, CHIPS)

        @pl.when(j == LANCZOS_STEPS - 1)
        def _():
            turn_result(LANCZOS_STEPS - 1, sig)
            hand_out(LANCZOS_STEPS - 1, 0, CHIPS)

        heard = scr.at[pl.ds(0, DEVS - 1)]
        remote(heard, heard, s_send, s_recv, me).wait()
        told = scr[:, 0, :]
        alpha = jnp.sum(told[:, 0:1], axis=0, keepdims=True) / d.vec_size
        off = alpha - told[:, 4:5]
        square = told[:, 2:3] - 2.0 * off * told[:, 3:4] + off * off * told[:, 1:2]
        beta = jnp.sqrt(jnp.sum(square, axis=0, keepdims=True) / d.vec_size)
        vnew = (sig[:, :d.half] - (alpha - guess) * vcur[...]) / beta
        vprev[...] = vcur[...]
        vcur[...] = vnew
        vb = vnew.astype(jnp.bfloat16)

        @pl.when(j < LANCZOS_STEPS - 1)
        def _():
            for ch in range(CHUNKS):
                for bh in range(2):
                    at = pl.ds(pl.multiple_of(slot * d.slab + bh * d.sub, d.sub), d.sub)
                    for q in range(d.pair):
                        uv[ch, q // 2, at, q % 2 * d.chunk:(q % 2 + 1) * d.chunk] = \
                            vb[(bh * d.pair + q) * d.sub:(bh * d.pair + q + 1) * d.sub, ch * d.chunk:(ch + 1) * d.chunk]
        alphas[j] = alpha[0, 0]
        betas[j] = beta[0, 0]
        return beta, alpha


    zero = jnp.zeros((1, 1), jnp.float32)
    last_beta, last_alpha = lax.fori_loop(0, LANCZOS_STEPS, step, (zero, zero))

    for n, part in enumerate((lv.at[0, pl.ds(0, 15), :, 0], lv.at[1, pl.ds(0, 15), :, 0, :, pl.ds(edge, d.bond - edge)],
                              lv.at[0, pl.ds(0, 15), :, 0, :, pl.ds(0, d.half)], lv.at[1, pl.ds(0, 15), :, 0, :, pl.ds(edge, d.half - edge)])):
        remote(part, part, l_send.at[n], l_recv.at[n, 0], me).wait_send()
    swapped = lv.at[:, pl.ds(0, 15), :, 0, :, pl.ds(d.half, d.half)]
    remote(swapped, swapped, f_send, f_recv.at[0], me).wait_send()
    for ch in range(CHUNKS):
        for h in range(2):
            theirs = left.at[:, pl.ds(0, d.chunk), pl.ds(0, d.half)]
            remote(theirs, lv.at[ch, slot, core, :, :, pl.ds(h * d.half, d.half)], d2d_sem.at[ch, h], d2d_recv.at[ch, h], partner).wait_send()
    put_out(LANCZOS_STEPS - 2)

    def finish(block, before, s):
        owner = device(s % 4, s // 4 % 2, s // 8, me // CHIPS)
        return (block - (last_alpha - scr[owner][:, 4:5]) * before) / last_beta

    put_out(LANCZOS_STEPS - 1, finish)
    for j in range(LANCZOS_STEPS):
        for c in range(d.bond // d.wide):
            pltpu.make_async_copy(tbuf.at[j, c], out.at[j, :, pl.ds(c * d.wide, d.wide)], o_sem.at[j, c]).wait()


def solution(mesh):
    def device_body(wavefunction, left_loc, pair_loc, right_loc, flag_loc):
        bond, pair = wavefunction.shape[0], wavefunction.shape[1]
        d = Dims(bond, pair, left_loc.shape[0])
        bf16, f32 = jnp.bfloat16, jnp.float32
        dma = pltpu.SemaphoreType.DMA
        any_space = pl.BlockSpec(memory_space=pl.ANY)
        smem = pl.BlockSpec(memory_space=pltpu.SMEM)
        scalars = jax.ShapeDtypeStruct((LANCZOS_STEPS,), f32)
        later, first, alphas, betas = pl.pallas_call(
            functools.partial(lanczos_kernel, d),
            out_shape=(jax.ShapeDtypeStruct((LANCZOS_STEPS, d.out_rows * pair, bond), f32),
                       jax.ShapeDtypeStruct((d.out_rows * pair, bond), f32), scalars, scalars),
            in_specs=[any_space] * 3 + [pl.BlockSpec(memory_space=pltpu.VMEM), smem],
            out_specs=(any_space, any_space, smem, smem),
            scratch_shapes=[
                pltpu.VMEM((CHUNKS, CHIPS, CORES, d.terms_dev, d.chunk, bond), bf16),
                pltpu.VMEM((CHIPS, CORES, d.terms_dev, d.slab, bond), bf16),
                pltpu.VMEM((d.terms_dev, bond, bond), bf16),
                pltpu.VMEM((CHIPS, CORES, d.terms_dev, pair, d.prod), bf16),
                pltpu.VMEM((CHIPS, CORES, d.terms_dev, d.prod, d.prod), bf16),
                pltpu.VMEM((CHUNKS, pair // 2, bond, 2 * d.chunk), bf16),
                pltpu.VMEM((d.lane_tiles, d.half * pair, d.lane), f32),
                pltpu.VMEM((CHIPS * CORES * d.terms_dev, pair, d.sub, 2 * d.chunk), bf16),
                pltpu.VMEM((d.rows, d.group_terms * d.chunk), bf16),
                pltpu.VMEM((d.rows, bond), f32),
                pltpu.VMEM((d.rows, d.half), f32),
                pltpu.VMEM((d.rows, d.half), f32),
                pltpu.VMEM((d.rows, d.half), f32),
                pltpu.VMEM((LANCZOS_STEPS, bond // d.wide, d.half, d.wide), f32),
                pltpu.VMEM((LANCZOS_STEPS, CHIPS, bond // d.wide, d.out_rows, d.wide), f32),
                pltpu.VMEM((1, 128), f32),
                pltpu.VMEM((DEVS, 1, 128), f32),
                pltpu.VMEM((2, 8, 128), f32),
                dma((3, 2)), dma((8, d.lane_tiles)), dma((CHUNKS, 2)), dma((CHUNKS, 2)), dma((2,)), dma((2,)), dma((2,)), dma((2,)),
                dma((4,)), dma((4, CHIPS)), dma, dma((CHIPS,)), dma((PIECES,)), dma((PIECES, CHIPS)),
                dma, dma, dma, dma, dma((LANCZOS_STEPS,)), dma((LANCZOS_STEPS,)), dma, dma, dma((LANCZOS_STEPS, bond // d.wide)), dma((bond // d.wide,)),
            ],
            compiler_params=pltpu.CompilerParams(has_side_effects=True, collective_id=0, vmem_limit_bytes=67043328),
            name='lanczos',
        )(wavefunction.reshape(bond * pair, bond), left_loc, right_loc, pair_loc, flag_loc)
        krylov = jnp.concatenate([first[None], later])
        return krylov.reshape(LANCZOS_STEPS + 1, d.out_rows, pair, bond), alphas, betas

    return jax.shard_map(device_body, mesh=mesh, in_specs=(P(), P(AXIS_NAME), P(AXIS_NAME), P(AXIS_NAME), P(AXIS_NAME)),
                         out_specs=(P(None, AXIS_NAME), P(), P()), check_vma=False)
```

```python
import functools

import jax
import jax.numpy as jnp
from jax import lax
from jax.experimental import pallas as pl
from jax.experimental.pallas import tpu as pltpu
from jax.sharding import PartitionSpec as P

LANCZOS_STEPS = 6
AXIS_NAME = 'terms'
MESH = pl.DeviceIdType.MESH

CHIPS = 16
CORES = 2
DEVS = 32
CHUNKS = 2
GROUPS = 4
TILE_PARTS = 4
QUARTERS = 4
PIECES = CHUNKS * QUARTERS

ALONG, ACROSS, FROM_COLUMN, FROM_SECOND, THIRD, DIAGONAL, RESULT, RESULT_OUT, RESULT_PUT = range(9)
RIGHT_SLOTS = (0, 1, 2, 3, 8, 9, 10, 11)
SLOTS = (
    ((0, 1, 0), (0, 1, 1), (1, 0, 2), (0, 2, 0), (1, 0, 5), (1, 0, 3), (1, 0, 6), (1, 0, 0), (0, 3, 0), (3, 0, 2), (0, 2, 1), (0, 1, 3), (1, 0, 4), (0, 3, 1), (1, 0, 7), (0, 1, 2), (1, 0, 1), (0, 3, 3), (2, 1, 0), (2, 2, 0), (0, 2, 3), (0, 3, 2), (2, 1, 1), (3, 0, 0), (2, 3, 0), (3, 1, 0), (2, 2, 1), (0, 2, 2), (0, 1, 4), (3, 0, 1), (2, 1, 3), (3, 2, 0), (2, 3, 1), (2, 2, 2), (2, 2, 3), (2, 1, 2), (4, 0, 0), (0, 2, 5), (0, 3, 4), (0, 2, 4), (0, 1, 5), (0, 1, 6), (0, 1, 7), (3, 3, 0), (2, 3, 3), (3, 1, 1), (3, 2, 1), (0, 2, 6), (2, 3, 2), (4, 0, 1), (3, 3, 1), (0, 3, 6), (3, 2, 2), (3, 1, 2), (0, 3, 5), (0, 2, 7), (0, 3, 7), (3, 2, 3), (3, 3, 2), (3, 0, 3), (5, 0, 0), (3, 3, 3), (4, 0, 3), (3, 1, 3), (3, 0, 4),),
    ((6, 0, 0), (2, 2, 4), (5, 0, 1), (3, 0, 6), (2, 1, 4), (4, 0, 2),),
    ((2, 2, 6), (5, 0, 2), (2, 1, 6),),
    ((2, 2, 5), (5, 0, 3), (3, 2, 4), (2, 3, 4),),
    ((2, 1, 5), (3, 0, 5), (3, 1, 4),),
    ((2, 3, 5), (3, 2, 5), (2, 3, 6),),
    ((2, 2, 7), (3, 3, 4), (2, 1, 7), (3, 1, 5), (8, 0, 0),),
    ((3, 3, 5), (2, 3, 7), (3, 2, 6), (3, 1, 6), (3, 3, 6),),
    ((3, 0, 7), (3, 1, 7), (3, 2, 7), (4, 0, 5), (5, 0, 4), (4, 0, 4),),
    ((3, 3, 7), (5, 0, 5),),
    ((4, 0, 6), (5, 0, 6),),
    ((4, 0, 7), (5, 0, 7), (7, 0, 0),),
    (),
    (),
    (),
    (),
)
RESULT_EARLY = 9


class Dims:
    def __init__(self, bond, pair, terms_dev):
        self.bond = bond
        self.pair = pair
        self.terms_dev = terms_dev
        self.slab = bond // CHIPS
        self.sub = self.slab // 2
        self.half = bond // CORES
        self.chunk = self.half // CHUNKS
        self.rows = self.slab * pair
        self.prod = self.sub * pair
        self.out_rows = bond // DEVS
        self.group_terms = 4 * CORES * terms_dev
        self.vec_size = bond * pair * bond
        self.lane = min(bond, 128)
        self.wide = TILE_PARTS * self.slab
        self.lane_tiles = bond // self.lane


def lanczos_kernel(d, psi, left, right, pair_ops, flags, out, first, alphas, betas, lv, rv, rs, wv, kw, uv, ps, yst, zst, sig, part, vcur, vprev, tbuf, gbuf,
                   scs, scr, nbuf,
                   loc_sem, psi_sem, d2d_sem, d2d_recv, rw_send, rw_recv, fw_send, fw_recv, l_send, l_recv, f_send, f_recv, u_send, u_recv,
                   p_send, p_recv, s_send, s_recv, k_send, k_recv, n_send, n_recv, o_sem, first_sem):
    me = lax.axis_index(AXIS_NAME)
    core = me % 2
    xpos = (me // 2) % 2
    ypos = (me // 4) % 2
    zpos = me // 8

    def device(z, y, x, c):
        return ((z * 2 + y) * 2 + x) * 2 + c

    def chip_slot(z, y, x):
        return (x * 2 + y) * 4 + z

    partner = device(zpos, ypos, xpos, 1 - core)
    slot = chip_slot(zpos, ypos, xpos)
    zs = (zpos, zpos + 1 - 2 * (zpos % 2), (zpos + 2) % 4, 3 - zpos)
    inner = (zpos + 1) // 2 % 2
    zn = (zpos, (1 - inner) * (zpos + 1 - zpos // 3 * 2) + inner * (zpos - 1), (1 - inner) * ((zpos + 2) % 4) + inner * (zpos + 1),
          (1 - inner) * (3 - zpos) + inner * ((zpos + 2) % 4))
    y_two = ypos + (1 - core) * (1 - 2 * ypos)
    x_two = xpos + core * (1 - 2 * xpos)
    y_three = ypos + core * (1 - 2 * ypos)
    x_three = xpos + (1 - core) * (1 - 2 * xpos)
    two = device(zpos, y_two, x_two, core)
    three = device(zpos, y_three, x_three, core)

    def remote(src, dst, send, recv, dev):
        return pltpu.make_async_remote_copy(src_ref=src, dst_ref=dst, send_sem=send, recv_sem=recv, device_id=(dev,), device_id_type=MESH)

    class Gather:
        def __init__(self, block, send, recv):
            self.block, self.send_sem, self.recv_sem = block, send, recv

        def send(self, which, dev):
            remote(self.block(which), self.block(which), self.send_sem, self.recv_sem(which), dev).start()

        def wait(self, which):
            remote(self.block(which), self.block(which), self.send_sem, self.recv_sem(which), me).wait_recv()

        def own_along(self):
            for i in (1, 2, 3):
                self.send(slot, device(zs[i], ypos, xpos, core))

        def own_across(self):
            self.send(slot, three)
            self.send(slot, two)

        def event(self, n):
            i = (n + 1) // 2
            if n % 2:
                which = chip_slot(zs[i], ypos, xpos)
                self.wait(which)
                self.send(which, three)
                self.send(which, two)
            else:
                which = chip_slot(zs[i], y_two, x_two)
                self.wait(which)
                self.send(which, three)

        def last(self, diagonal):
            for i in range(4):
                self.wait(chip_slot(zs[i], 1 - ypos, 1 - xpos) if diagonal else chip_slot(zs[i], y_three, x_three))

    edge = d.chunk
    l_parts = (
        (lambda s: lv.at[0, s, :, core], 0),
        (lambda s: lv.at[1, s, :, core, :, pl.ds(edge, d.bond - edge)], 1),
        (lambda s: lv.at[0, s, :, 1 - core, :, pl.ds(0, d.half)], 2),
        (lambda s: lv.at[1, s, :, 1 - core, :, pl.ds(edge, d.half - edge)], 3),
    )
    l_gathers = [Gather(block, l_send.at[n], lambda s, n=n: l_recv.at[n, s]) for block, n in l_parts]

    def l_swap(s, term):
        part = lv.at[:, s, :, term, :, pl.ds(d.half, d.half)]
        return remote(part, part, f_send, f_recv.at[s], partner)

    def l_event(n):
        i = (n + 1) // 2
        for g in l_gathers:
            g.event(n)
        l_swap(chip_slot(zs[i], ypos, xpos) if n % 2 else chip_slot(zs[i], y_two, x_two), core).start()

    def l_last(diagonal):
        for i in range(4):
            which = chip_slot(zs[i], 1 - ypos, 1 - xpos) if diagonal else chip_slot(zs[i], y_three, x_three)
            for g in l_gathers:
                g.wait(which)
            l_swap(which, core).start()

    def l_fill(s):
        @pl.when(s != slot)
        def _():
            l_swap(s, 1 - core).wait_recv()
            for c in range(CORES):
                tile = lv[:, s, c, 1 - core, :, d.half:].reshape(d.half, d.half).T
                lv[:, s, c, 1 - core, :, d.half:] = tile.reshape(CHUNKS, d.chunk, d.half)
                for t in range(d.terms_dev):
                    lv[1, s, c, t, :, :edge] = lv[0, s, c, t, :, edge:d.half].T

    def l_along():
        for i in (1, 2, 3):
            for g in l_gathers:
                g.send(slot, device(zs[i], ypos, xpos, core))

    def u_block(p):
        return lambda s: uv.at[p // QUARTERS, pl.ds(p % QUARTERS * 2, 2), pl.ds(pl.multiple_of(s * d.slab, d.slab), d.slab), :]

    u_gathers = [Gather(u_block(p), u_send.at[p], lambda s, p=p: u_recv.at[p, s]) for p in range(PIECES)]

    def act(kind, i, p, j):
        g = u_gathers[p]
        if kind == ALONG:
            g.send(slot, device(zn[i], ypos, xpos, core))
        elif kind == ACROSS:
            g.own_across()
        elif kind == FROM_COLUMN:
            which = chip_slot(zn[i], ypos, xpos)
            g.wait(which)
            g.send(which, three)
            g.send(which, two)
        elif kind == FROM_SECOND:
            which = chip_slot(zn[i], y_two, x_two)
            g.wait(which)
            g.send(which, three)
        elif kind == THIRD:
            g.last(False)
        elif kind == DIAGONAL:
            g.last(True)
        elif kind == RESULT:
            turn_result(j - 1, vcur)
        elif kind == RESULT_OUT:
            hand_out(j - 1, 0, RESULT_EARLY)
        elif kind == RESULT_PUT:
            @pl.when(j > 1)
            def _():
                put_out(j - 2)

    all_right = pltpu.make_async_copy(right, rs, loc_sem.at[2, 0])
    all_right.start()

    barrier = pltpu.get_barrier_semaphore()

    def knock(n, carry):
        pl.semaphore_signal(barrier, inc=1, device_id=((me + n) % DEVS,), device_id_type=MESH)
        return carry

    lax.fori_loop(1, DEVS, knock, 0)

    for ch in range(CHUNKS):
        for h in range(2):
            mine = left.at[:, pl.ds(pl.multiple_of(core * d.half + ch * d.chunk, d.chunk), d.chunk),
                           pl.ds(pl.multiple_of((core + h) % 2 * d.half, d.half), d.half)]
            pltpu.make_async_copy(mine, lv.at[ch, slot, core, :, :, pl.ds(h * d.half, d.half)], loc_sem.at[ch, h]).start()

    psi_rows = d.half * d.pair // 8
    psi_copies = [pltpu.make_async_copy(psi.at[pl.ds(pl.multiple_of(core * d.half * d.pair + n * psi_rows, psi_rows), psi_rows),
                                               pl.ds(c * d.lane, d.lane)],
                                        ps.at[c, pl.ds(n * psi_rows, psi_rows), :], psi_sem.at[n, c])
                  for n in range(8) for c in range(d.lane_tiles)]
    for copy in psi_copies:
        copy.start()

    first_rows = d.out_rows * d.pair
    first_copies = [pltpu.make_async_copy(psi.at[pl.ds(pl.multiple_of(me * first_rows, first_rows), first_rows), pl.ds(c * d.wide, d.wide)],
                                          tbuf.at[LANCZOS_STEPS - 1, c], first_sem.at[c]) for c in range(d.bond // d.wide)]
    for copy in first_copies:
        copy.start()

    spread = (lax.broadcasted_iota(jnp.int32, (d.pair, d.prod), 1) // d.sub == lax.broadcasted_iota(jnp.int32, (d.pair, d.prod), 0))
    spread = spread.astype(jnp.float32).astype(jnp.bfloat16)
    for t in range(d.terms_dev):
        wv[slot, core, t] = jnp.dot(pair_ops[t], spread, preferred_element_type=jnp.float32).astype(jnp.bfloat16)
    all_right.wait()
    some_rows = d.bond // 8

    def one_sided(i, carry):
        at = pl.ds(pl.multiple_of(i * some_rows, some_rows), some_rows)
        row = lax.broadcasted_iota(jnp.int32, (some_rows, d.bond), 0) + i * some_rows
        one = jnp.where(row == lax.broadcasted_iota(jnp.int32, (some_rows, d.bond), 1), 1.0, 0.0)
        for t in range(d.terms_dev):
            rs[t, at, :] = jnp.where(flags[t] == 1, rs[t, at, :].astype(jnp.float32), one).astype(jnp.bfloat16)
        return carry

    lax.fori_loop(0, 8, one_sided, 0)

    def right_rows(s):
        return rs.at[:, pl.ds(pl.multiple_of(s * d.slab, d.slab), d.slab), :]

    rv[slot, core] = rs[:, pl.ds(pl.multiple_of(slot * d.slab, d.slab), d.slab), :]

    pl.semaphore_wait(barrier, DEVS - 1)
    for ch in range(CHUNKS):
        for h in range(2):
            theirs = left.at[:, pl.ds(pl.multiple_of((1 - core) * d.half + ch * d.chunk, d.chunk), d.chunk),
                             pl.ds(pl.multiple_of((1 - core + h) % 2 * d.half, d.half), d.half)]
            remote(theirs, lv.at[ch, slot, core, :, :, pl.ds(h * d.half, d.half)], d2d_sem.at[ch, h], d2d_recv.at[ch, h], partner).start()
    for n in range(1, CHIPS):
        chip = (me // 2 + n) % CHIPS
        to = chip_slot(chip // 4, chip // 2 % 2, chip % 2)
        remote(right_rows(to), rv.at[slot, core], rw_send.at[0], rw_recv.at[0], chip * 2 + core).start()
        remote(wv.at[slot, core], wv.at[slot, core], rw_send.at[1], rw_recv.at[1], chip * 2 + core).start()

    for ch in range(CHUNKS):
        for h in range(2):
            pltpu.make_async_copy(lv.at[ch, slot, core, :, :, pl.ds(h * d.half, d.half)], lv.at[ch, slot, core, :, :, pl.ds(h * d.half, d.half)], loc_sem.at[ch, h]).wait()
            back = remote(lv.at[ch, slot, 1 - core, :, :, pl.ds(h * d.half, d.half)], lv.at[ch, slot, 1 - core, :, :, pl.ds(h * d.half, d.half)], d2d_sem.at[ch, h], d2d_recv.at[ch, h], partner)
            back.wait_recv()
    l_along()
    for g in l_gathers:
        g.own_across()

    total = jnp.zeros((8, d.lane), jnp.float32)
    for n in range(8):
        for copy in psi_copies[n * d.lane_tiles:(n + 1) * d.lane_tiles]:
            copy.wait()

        def add_rows(i, acc, n=n):
            x = ps[:, pl.ds(pl.multiple_of(n * psi_rows + i * (psi_rows // 8), 8), psi_rows // 8), :]
            return acc + jnp.sum((x * x).reshape(d.lane_tiles * psi_rows // 64, 8, d.lane), axis=0)

        total = lax.fori_loop(0, 8, add_rows, total)
    nbuf[0] = jnp.broadcast_to(jnp.sum(total, keepdims=True), (8, 128))
    to_partner = remote(nbuf.at[0], nbuf.at[1], n_send, n_recv, partner)
    to_partner.start()
    to_partner.wait()
    norm = jnp.sqrt((nbuf[0] + nbuf[1])[0:1, :] / d.vec_size)
    norm_one = norm[:, 0:1]
    for copy in first_copies:
        copy.wait()
    tbuf[LANCZOS_STEPS - 1] = tbuf[LANCZOS_STEPS - 1] / norm_one[None]
    first_out = [pltpu.make_async_copy(tbuf.at[LANCZOS_STEPS - 1, c], first.at[:, pl.ds(c * d.wide, d.wide)], first_sem.at[c])
                 for c in range(d.bond // d.wide)]
    for copy in first_out:
        copy.start()

    def place(q):
        tiles = [(ps[c, pl.ds(q, d.half, stride=d.pair), :] / norm_one).T for c in range(d.lane_tiles)]
        xt = jnp.concatenate(tiles, axis=0)
        vprev[...] = xt
        return xt.astype(jnp.bfloat16)

    def start_vector(qb, carry):
        for q2 in range(2):
            q = qb * 2 + q2
            xb = place(q)
            for ch in range(CHUNKS):
                uv[ch, qb, :, q2 * d.chunk:(q2 + 1) * d.chunk] = xb[:, ch * d.chunk:(ch + 1) * d.chunk]
            for bh in range(2):
                rows = vprev[pl.ds(pl.multiple_of(slot * d.slab + bh * d.sub, d.sub), d.sub), :]
                vcur[pl.ds(pl.multiple_of((bh * d.pair + q) * d.sub, d.sub), d.sub), :] = rows
        return carry

    lax.fori_loop(0, d.pair // 4, start_vector, 0)
    fifteen = rv.at[pl.ds(0, CHIPS - 1), 0]
    fifteen_w = wv.at[pl.ds(0, CHIPS - 1), 0]
    remote(fifteen, fifteen, rw_send.at[0], rw_recv.at[0], me).wait()
    remote(fifteen_w, fifteen_w, rw_send.at[1], rw_recv.at[1], me).wait()
    fw_right = remote(rv.at[:, core], rv.at[:, core], fw_send.at[0], fw_recv.at[0], partner)
    fw_pair = remote(wv.at[:, core], wv.at[:, core], fw_send.at[1], fw_recv.at[1], partner)
    fw_right.start()
    fw_pair.start()
    l_event(0)
    l_event(1)
    lax.fori_loop(d.pair // 4, d.pair // 2, start_vector, 0)
    l_event(2)
    l_event(3)
    fw_right.wait()
    fw_pair.wait()
    lane = lax.broadcasted_iota(jnp.int32, (d.sub, d.prod), 1)
    row = lax.broadcasted_iota(jnp.int32, (d.sub, d.prod), 0)
    diagonal = lane % d.sub == row

    def spread_pair(s, carry):
        for c in range(2):
            for t in range(d.terms_dev):
                w = wv[s, c, t].astype(jnp.float32)
                for q in range(d.pair):
                    full = jnp.where(diagonal, jnp.broadcast_to(w[q:q + 1, :], (d.sub, d.prod)), 0.0)
                    kw[s, c, t, q * d.sub:(q + 1) * d.sub, :] = full.astype(jnp.bfloat16)
        return carry

    lax.fori_loop(0, CHIPS, spread_pair, 0)
    vprev[...] = jnp.zeros_like(vprev)
    for copy in first_out:
        copy.wait()

    def right_product(grp, ch, qb, to):
        r_all = rv[pl.ds(grp * 4, 4)].reshape(d.group_terms * d.slab, d.bond)
        y = jnp.dot(r_all, uv[ch, qb], preferred_element_type=jnp.float32).astype(jnp.bfloat16)
        y = y.reshape(d.group_terms, 2, d.sub, 2 * d.chunk)
        for q2 in range(2):
            for bh in range(2):
                yst[pl.ds(to * d.group_terms, d.group_terms), qb * 2 + q2, :, bh * d.chunk:(bh + 1) * d.chunk] = \
                    y[:, bh, :, q2 * d.chunk:(q2 + 1) * d.chunk]

    def right_of_piece(ch, part):
        for qb in range(2):
            for grp in range(GROUPS):
                right_product(grp, ch, part * 2 + qb, grp)

    def right_of_group(grp, ch, to):
        for qb in range(d.pair // 2):
            right_product(grp, ch, qb, to)

    def left_products(ch, grp, at=None):
        for k in range(d.group_terms):
            w = kw[grp * 4 + k // 4, k // 2 % 2, k % 2]
            z = jnp.dot(w, yst[(grp if at is None else at) * d.group_terms + k].reshape(d.prod, 2 * d.chunk), preferred_element_type=jnp.float32).astype(jnp.bfloat16)
            for bh in range(2):
                zst[bh * d.prod:(bh + 1) * d.prod, k * d.chunk:(k + 1) * d.chunk] = z[:, bh * d.chunk:(bh + 1) * d.chunk]
        l_all = lv[ch, pl.ds(grp * 4, 4)].reshape(d.group_terms * d.chunk, d.bond)
        sig[...] += jnp.dot(zst[...], l_all, preferred_element_type=jnp.float32)

    def first_right(grp, carry):
        right_of_group(grp, 0, grp)

        @pl.when(grp == 1)
        def _():
            l_event(4)
        return carry

    def first_group(n, carry):
        own, third = xpos * 2 + ypos, x_three * 2 + y_three
        grp = jnp.where(n == 0, own, jnp.where(n == 1, x_two * 2 + y_two, jnp.where(n == 2, third, 3 - own)))
        spare = jnp.where(n == 3, own, grp)

        @pl.when(n == 1)
        def _():
            l_event(6)
            l_last(False)

        @pl.when(n == 3)
        def _():
            right_of_group(grp, 1, spare)
            l_last(True)

        def fill(z, carry):
            l_fill(grp * 4 + z)
            return carry

        lax.fori_loop(0, 4, fill, 0)

        def chunk_products(ch, carry):
            left_products(ch, grp, (1 - ch) * grp + ch * spare)

            @pl.when((ch == 0) & (n < 3))
            def _():
                right_of_group(grp, 1, spare)
            return carry

        lax.fori_loop(0, CHUNKS, chunk_products, 0)
        return carry

    def turn_result(j, vector):
        for n in range(d.pair // TILE_PARTS):
            rows = [vector[(bh * d.pair + q) * d.sub:(bh * d.pair + q + 1) * d.sub, :d.half]
                    for q in range(n * TILE_PARTS, (n + 1) * TILE_PARTS) for bh in range(2)]
            tbuf[j, n] = jnp.concatenate(rows, axis=0).T

    def hand_out(j, begin, end):
        for n in range(begin, end):
            to = core * CHIPS + n
            block = tbuf.at[j, :, pl.ds(n * d.out_rows, d.out_rows), :]

            @pl.when(to != me)
            def _():
                remote(block, gbuf.at[j, slot], k_send.at[j], k_recv.at[j], to).start()

            @pl.when(to == me)
            def _():
                gbuf[j, slot] = block[...]

    sends_self = me // CHIPS == core
    lanes = lax.broadcasted_iota(jnp.int32, (d.out_rows, d.wide), 1) // d.slab

    def put_out(j, finish=None):
        @pl.when(sends_self)
        def _():
            some = gbuf.at[j, pl.ds(0, CHIPS - 1)]
            remote(some, some, k_send.at[j], k_recv.at[j], me).wait()

        @pl.when(jnp.logical_not(sends_self))
        def _():
            remote(gbuf.at[j], gbuf.at[j], k_send.at[j], k_recv.at[j], me).wait()

        for ct in range(CHIPS // TILE_PARTS):
            for qt in range(d.pair // TILE_PARTS):
                src = [gbuf[j, ct * TILE_PARTS + c, qt] for c in range(TILE_PARTS)]
                if finish is not None:
                    src = [finish(x, gbuf[j - 1, ct * TILE_PARTS + c, qt], ct * TILE_PARTS + c) for c, x in enumerate(src)]
                for q in range(TILE_PARTS):
                    tile = jnp.zeros((d.out_rows, d.wide), jnp.float32)
                    for c in range(TILE_PARTS):
                        shift = (c - q) % TILE_PARTS * d.slab
                        moved = pltpu.roll(src[c], shift, 1) if shift else src[c]
                        tile = jnp.where(lanes == c, moved, tile)
                    tbuf[j, ct, pl.ds(qt * TILE_PARTS + q, d.out_rows, stride=d.pair), :] = tile
            pltpu.make_async_copy(tbuf.at[j, ct], out.at[j, :, pl.ds(ct * d.wide, d.wide)], o_sem.at[j, ct]).start()

    def step(j, carried):
        beta_prev = carried[0]
        sig[...] = jnp.zeros_like(sig)

        def slot_step(t, carry):
            done_right = sum((t > r).astype(jnp.int32) for r in RIGHT_SLOTS)
            done_left = t - done_right
            is_right = sum((t == r).astype(jnp.int32) for r in RIGHT_SLOTS)
            for four in range(0, len(SLOTS), 4):
                @pl.when((t >= four) & (t < four + 4))
                def _():
                    for at in range(four, four + 4):
                        if not SLOTS[at]:
                            continue

                        @pl.when(t == at)
                        def _():
                            for kind, i, p in SLOTS[at]:
                                act(kind, i, p, j)

            @pl.when(is_right == 1)
            def _():
                right_of_piece(done_right // QUARTERS, done_right % QUARTERS)

            @pl.when(is_right == 0)
            def _():
                left_products(done_left // GROUPS, done_left % GROUPS)
            return carry

        @pl.when(j == 0)
        def _():
            lax.fori_loop(0, GROUPS, first_right, 0)
            l_event(5)
            lax.fori_loop(0, GROUPS, first_group, 0)

        @pl.when(j > 0)
        def _():
            lax.fori_loop(0, len(SLOTS), slot_step, 0)
            for p in range(PIECES):
                sent = uv.at[p // QUARTERS, pl.ds(0, 2), pl.ds(0, 15 * d.slab), :]
                remote(sent, sent, u_send.at[p], u_recv.at[p, 0], me).wait_send()

        other = sig.at[:, pl.ds(d.half, d.half)]
        to_other = remote(other, part, p_send, p_recv, partner)
        to_other.start()
        to_other.wait()
        s = sig[:, :d.half] + part[...]
        v = vcur[...]
        w = s - beta_prev * vprev[...]
        sv = jnp.sum(s * v, keepdims=True)
        wv_sum = jnp.sum(w * v, keepdims=True)
        vv = jnp.sum(v * v, keepdims=True)
        guess = jnp.where(vv > 0.0, wv_sum / jnp.where(vv > 0.0, vv, 1.0), 0.0)
        t = w - guess * v
        sig[:, :d.half] = t
        tt = jnp.sum(t * t, keepdims=True)
        tv = jnp.sum(t * v, keepdims=True)
        at_lane = lax.broadcasted_iota(jnp.int32, (1, 128), 1)
        line = jnp.zeros((1, 128), jnp.float32)
        for n, value in enumerate((sv, vv, tt, tv, guess)):
            line = jnp.where(at_lane == n, value, line)
        scs[...] = line
        scr[me] = line

        def tell(n, carry):
            remote(scs, scr.at[me], s_send, s_recv, (me + n) % DEVS).start()
            return carry

        lax.fori_loop(1, DEVS, tell, 0)

        @pl.when(j > 0)
        def _():
            hand_out(j - 1, RESULT_EARLY, CHIPS)

        @pl.when(j == LANCZOS_STEPS - 1)
        def _():
            turn_result(LANCZOS_STEPS - 1, sig)
            hand_out(LANCZOS_STEPS - 1, 0, CHIPS)

        heard = scr.at[pl.ds(0, DEVS - 1)]
        remote(heard, heard, s_send, s_recv, me).wait()
        told = scr[:, 0, :]
        alpha = jnp.sum(told[:, 0:1], axis=0, keepdims=True) / d.vec_size
        off = alpha - told[:, 4:5]
        square = told[:, 2:3] - 2.0 * off * told[:, 3:4] + off * off * told[:, 1:2]
        beta = jnp.sqrt(jnp.sum(square, axis=0, keepdims=True) / d.vec_size)
        vnew = (sig[:, :d.half] - (alpha - guess) * vcur[...]) / beta
        vprev[...] = vcur[...]
        vcur[...] = vnew
        vb = vnew.astype(jnp.bfloat16)

        @pl.when(j < LANCZOS_STEPS - 1)
        def _():
            for ch in range(CHUNKS):
                for bh in range(2):
                    at = pl.ds(pl.multiple_of(slot * d.slab + bh * d.sub, d.sub), d.sub)
                    for q in range(d.pair):
                        uv[ch, q // 2, at, q % 2 * d.chunk:(q % 2 + 1) * d.chunk] = \
                            vb[(bh * d.pair + q) * d.sub:(bh * d.pair + q + 1) * d.sub, ch * d.chunk:(ch + 1) * d.chunk]
        alphas[j] = alpha[0, 0]
        betas[j] = beta[0, 0]
        return beta, alpha


    zero = jnp.zeros((1, 1), jnp.float32)
    last_beta, last_alpha = lax.fori_loop(0, LANCZOS_STEPS, step, (zero, zero))

    for n, part in enumerate((lv.at[0, pl.ds(0, 15), :, 0], lv.at[1, pl.ds(0, 15), :, 0, :, pl.ds(edge, d.bond - edge)],
                              lv.at[0, pl.ds(0, 15), :, 0, :, pl.ds(0, d.half)], lv.at[1, pl.ds(0, 15), :, 0, :, pl.ds(edge, d.half - edge)])):
        remote(part, part, l_send.at[n], l_recv.at[n, 0], me).wait_send()
    swapped = lv.at[:, pl.ds(0, 15), :, 0, :, pl.ds(d.half, d.half)]
    remote(swapped, swapped, f_send, f_recv.at[0], me).wait_send()
    for ch in range(CHUNKS):
        for h in range(2):
            theirs = left.at[:, pl.ds(0, d.chunk), pl.ds(0, d.half)]
            remote(theirs, lv.at[ch, slot, core, :, :, pl.ds(h * d.half, d.half)], d2d_sem.at[ch, h], d2d_recv.at[ch, h], partner).wait_send()
    put_out(LANCZOS_STEPS - 2)

    def finish(block, before, s):
        owner = device(s % 4, s // 4 % 2, s // 8, me // CHIPS)
        return (block - (last_alpha - scr[owner][:, 4:5]) * before) / last_beta

    put_out(LANCZOS_STEPS - 1, finish)
    for j in range(LANCZOS_STEPS):
        for c in range(d.bond // d.wide):
            pltpu.make_async_copy(tbuf.at[j, c], out.at[j, :, pl.ds(c * d.wide, d.wide)], o_sem.at[j, c]).wait()


def solution(mesh):
    def device_body(wavefunction, left_loc, pair_loc, right_loc, flag_loc):
        bond, pair = wavefunction.shape[0], wavefunction.shape[1]
        d = Dims(bond, pair, left_loc.shape[0])
        bf16, f32 = jnp.bfloat16, jnp.float32
        dma = pltpu.SemaphoreType.DMA
        any_space = pl.BlockSpec(memory_space=pl.ANY)
        smem = pl.BlockSpec(memory_space=pltpu.SMEM)
        scalars = jax.ShapeDtypeStruct((LANCZOS_STEPS,), f32)
        later, first, alphas, betas = pl.pallas_call(
            functools.partial(lanczos_kernel, d),
            out_shape=(jax.ShapeDtypeStruct((LANCZOS_STEPS, d.out_rows * pair, bond), f32),
                       jax.ShapeDtypeStruct((d.out_rows * pair, bond), f32), scalars, scalars),
            in_specs=[any_space] * 3 + [pl.BlockSpec(memory_space=pltpu.VMEM), smem],
            out_specs=(any_space, any_space, smem, smem),
            scratch_shapes=[
                pltpu.VMEM((CHUNKS, CHIPS, CORES, d.terms_dev, d.chunk, bond), bf16),
                pltpu.VMEM((CHIPS, CORES, d.terms_dev, d.slab, bond), bf16),
                pltpu.VMEM((d.terms_dev, bond, bond), bf16),
                pltpu.VMEM((CHIPS, CORES, d.terms_dev, pair, d.prod), bf16),
                pltpu.VMEM((CHIPS, CORES, d.terms_dev, d.prod, d.prod), bf16),
                pltpu.VMEM((CHUNKS, pair // 2, bond, 2 * d.chunk), bf16),
                pltpu.VMEM((d.lane_tiles, d.half * pair, d.lane), f32),
                pltpu.VMEM((CHIPS * CORES * d.terms_dev, pair, d.sub, 2 * d.chunk), bf16),
                pltpu.VMEM((d.rows, d.group_terms * d.chunk), bf16),
                pltpu.VMEM((d.rows, bond), f32),
                pltpu.VMEM((d.rows, d.half), f32),
                pltpu.VMEM((d.rows, d.half), f32),
                pltpu.VMEM((d.rows, d.half), f32),
                pltpu.VMEM((LANCZOS_STEPS, bond // d.wide, d.half, d.wide), f32),
                pltpu.VMEM((LANCZOS_STEPS, CHIPS, bond // d.wide, d.out_rows, d.wide), f32),
                pltpu.VMEM((1, 128), f32),
                pltpu.VMEM((DEVS, 1, 128), f32),
                pltpu.VMEM((2, 8, 128), f32),
                dma((3, 2)), dma((8, d.lane_tiles)), dma((CHUNKS, 2)), dma((CHUNKS, 2)), dma((2,)), dma((2,)), dma((2,)), dma((2,)),
                dma((4,)), dma((4, CHIPS)), dma, dma((CHIPS,)), dma((PIECES,)), dma((PIECES, CHIPS)),
                dma, dma, dma, dma, dma((LANCZOS_STEPS,)), dma((LANCZOS_STEPS,)), dma, dma, dma((LANCZOS_STEPS, bond // d.wide)), dma((bond // d.wide,)),
            ],
            compiler_params=pltpu.CompilerParams(has_side_effects=True, collective_id=0, vmem_limit_bytes=67043328),
            name='lanczos',
        )(wavefunction.reshape(bond * pair, bond), left_loc, right_loc, pair_loc, flag_loc)
        krylov = jnp.concatenate([first[None], later])
        return krylov.reshape(LANCZOS_STEPS + 1, d.out_rows, pair, bond), alphas, betas

    return jax.shard_map(device_body, mesh=mesh, in_specs=(P(), P(AXIS_NAME), P(AXIS_NAME), P(AXIS_NAME), P(AXIS_NAME)),
                         out_specs=(P(None, AXIS_NAME), P(), P()), check_vma=False)
```

```python
import functools

import jax
import jax.numpy as jnp
from jax import lax
from jax.experimental import pallas as pl
from jax.experimental.pallas import tpu as pltpu
from jax.sharding import PartitionSpec as P

LANCZOS_STEPS = 6
AXIS_NAME = 'terms'
MESH = pl.DeviceIdType.MESH

CHIPS = 16
CORES = 2
DEVS = 32
CHUNKS = 2
GROUPS = 4
TILE_PARTS = 4
QUARTERS = 4
PIECES = CHUNKS * QUARTERS

ALONG, ACROSS, FROM_COLUMN, FROM_SECOND, THIRD, DIAGONAL, RESULT, RESULT_OUT, RESULT_PUT = range(9)
RIGHT_SLOTS = (0, 1, 2, 3, 8, 9, 10, 11)
SLOTS = (
    ((0, 1, 0), (0, 1, 1), (1, 0, 2), (0, 2, 0), (1, 0, 5), (1, 0, 3), (1, 0, 6), (1, 0, 0), (0, 3, 0), (3, 0, 2), (0, 2, 1), (0, 1, 3), (1, 0, 4), (0, 3, 1), (1, 0, 7), (0, 1, 2), (1, 0, 1), (0, 3, 3), (2, 1, 0), (2, 2, 0), (0, 2, 3), (0, 3, 2), (2, 1, 1), (3, 0, 0), (2, 3, 0), (3, 1, 0), (2, 2, 1), (0, 2, 2), (0, 1, 4), (3, 0, 1), (2, 1, 3), (3, 2, 0), (2, 3, 1), (2, 2, 2), (2, 2, 3), (2, 1, 2), (4, 0, 0), (0, 2, 5), (0, 3, 4), (0, 2, 4), (0, 1, 5), (0, 1, 6), (0, 1, 7), (3, 3, 0), (2, 3, 3), (3, 1, 1), (3, 2, 1), (0, 2, 6), (2, 3, 2), (4, 0, 1), (3, 3, 1), (0, 3, 6), (3, 2, 2), (3, 1, 2), (0, 3, 5), (0, 2, 7), (0, 3, 7), (3, 2, 3), (3, 3, 2), (3, 0, 3), (5, 0, 0), (3, 3, 3), (4, 0, 3), (3, 1, 3), (3, 0, 4),),
    ((6, 0, 0), (2, 2, 4), (5, 0, 1), (3, 0, 6), (2, 1, 4), (4, 0, 2),),
    ((2, 2, 6), (5, 0, 2), (2, 1, 6),),
    ((2, 2, 5), (5, 0, 3), (3, 2, 4), (2, 3, 4),),
    ((2, 1, 5), (3, 0, 5), (3, 1, 4),),
    ((2, 3, 5), (3, 2, 5), (2, 3, 6),),
    ((2, 2, 7), (3, 3, 4), (2, 1, 7), (3, 1, 5), (8, 0, 0),),
    ((3, 3, 5), (2, 3, 7), (3, 2, 6), (3, 1, 6), (3, 3, 6),),
    ((3, 0, 7), (3, 1, 7), (3, 2, 7), (4, 0, 5), (5, 0, 4), (4, 0, 4),),
    ((3, 3, 7), (5, 0, 5),),
    ((4, 0, 6), (5, 0, 6),),
    ((4, 0, 7), (5, 0, 7), (7, 0, 0),),
    (),
    (),
    (),
    (),
)
RESULT_EARLY = 9


class Dims:
    def __init__(self, bond, pair, terms_dev):
        self.bond = bond
        self.pair = pair
        self.terms_dev = terms_dev
        self.slab = bond // CHIPS
        self.sub = self.slab // 2
        self.half = bond // CORES
        self.chunk = self.half // CHUNKS
        self.rows = self.slab * pair
        self.prod = self.sub * pair
        self.out_rows = bond // DEVS
        self.group_terms = 4 * CORES * terms_dev
        self.vec_size = bond * pair * bond
        self.lane = min(bond, 128)
        self.wide = TILE_PARTS * self.slab
        self.lane_tiles = bond // self.lane


def lanczos_kernel(d, psi, left, right, pair_ops, flags, out, first, alphas, betas, lv, rv, rs, wv, kw, uv, ps, yst, zst, sig, part, vcur, vprev, tbuf, gbuf,
                   scs, scr, nbuf,
                   loc_sem, psi_sem, d2d_sem, d2d_recv, rw_send, rw_recv, fw_send, fw_recv, l_send, l_recv, f_send, f_recv, u_send, u_recv,
                   p_send, p_recv, s_send, s_recv, k_send, k_recv, n_send, n_recv, o_sem, first_sem):
    me = lax.axis_index(AXIS_NAME)
    core = me % 2
    xpos = (me // 2) % 2
    ypos = (me // 4) % 2
    zpos = me // 8

    def device(z, y, x, c):
        return ((z * 2 + y) * 2 + x) * 2 + c

    def chip_slot(z, y, x):
        return (x * 2 + y) * 4 + z

    partner = device(zpos, ypos, xpos, 1 - core)
    slot = chip_slot(zpos, ypos, xpos)
    inner = (zpos + 1) // 2 % 2
    zn = (zpos, (1 - inner) * (zpos + 1 - zpos // 3 * 2) + inner * (zpos - 1), (1 - inner) * ((zpos + 2) % 4) + inner * (zpos + 1),
          (1 - inner) * (3 - zpos) + inner * ((zpos + 2) % 4))
    y_two = ypos + (1 - core) * (1 - 2 * ypos)
    x_two = xpos + core * (1 - 2 * xpos)
    y_three = ypos + core * (1 - 2 * ypos)
    x_three = xpos + (1 - core) * (1 - 2 * xpos)
    two = device(zpos, y_two, x_two, core)
    three = device(zpos, y_three, x_three, core)

    def remote(src, dst, send, recv, dev):
        return pltpu.make_async_remote_copy(src_ref=src, dst_ref=dst, send_sem=send, recv_sem=recv, device_id=(dev,), device_id_type=MESH)

    class Gather:
        def __init__(self, block, send, recv):
            self.block, self.send_sem, self.recv_sem = block, send, recv

        def send(self, which, dev):
            remote(self.block(which), self.block(which), self.send_sem, self.recv_sem(which), dev).start()

        def wait(self, which):
            remote(self.block(which), self.block(which), self.send_sem, self.recv_sem(which), me).wait_recv()

        def own_along(self):
            for i in (1, 2, 3):
                self.send(slot, device(zn[i], ypos, xpos, core))

        def own_across(self):
            self.send(slot, three)
            self.send(slot, two)

        def event(self, n):
            i = (n + 1) // 2
            if n % 2:
                which = chip_slot(zn[i], ypos, xpos)
                self.wait(which)
                self.send(which, three)
                self.send(which, two)
            else:
                which = chip_slot(zn[i], y_two, x_two)
                self.wait(which)
                self.send(which, three)

        def last(self, diagonal):
            for i in range(4):
                self.wait(chip_slot(zn[i], 1 - ypos, 1 - xpos) if diagonal else chip_slot(zn[i], y_three, x_three))

    edge = d.chunk
    l_parts = (
        (lambda s: lv.at[0, s, :, core], 0),
        (lambda s: lv.at[1, s, :, core, :, pl.ds(edge, d.bond - edge)], 1),
        (lambda s: lv.at[0, s, :, 1 - core, :, pl.ds(0, d.half)], 2),
        (lambda s: lv.at[1, s, :, 1 - core, :, pl.ds(edge, d.half - edge)], 3),
    )
    l_gathers = [Gather(block, l_send.at[n], lambda s, n=n: l_recv.at[n, s]) for block, n in l_parts]

    def l_swap(s, term):
        part = lv.at[:, s, :, term, :, pl.ds(d.half, d.half)]
        return remote(part, part, f_send, f_recv.at[s], partner)

    def l_event(n):
        i = (n + 1) // 2
        for g in l_gathers:
            g.event(n)
        l_swap(chip_slot(zn[i], ypos, xpos) if n % 2 else chip_slot(zn[i], y_two, x_two), core).start()

    def l_last(diagonal):
        for i in range(4):
            which = chip_slot(zn[i], 1 - ypos, 1 - xpos) if diagonal else chip_slot(zn[i], y_three, x_three)
            for g in l_gathers:
                g.wait(which)
            l_swap(which, core).start()

    def l_fill(s):
        @pl.when(s != slot)
        def _():
            l_swap(s, 1 - core).wait_recv()
            for c in range(CORES):
                tile = lv[:, s, c, 1 - core, :, d.half:].reshape(d.half, d.half).T
                lv[:, s, c, 1 - core, :, d.half:] = tile.reshape(CHUNKS, d.chunk, d.half)
                for t in range(d.terms_dev):
                    lv[1, s, c, t, :, :edge] = lv[0, s, c, t, :, edge:d.half].T

    def l_along():
        for i in (1, 2, 3):
            for g in l_gathers:
                g.send(slot, device(zn[i], ypos, xpos, core))

    def u_block(p):
        return lambda s: uv.at[p // QUARTERS, pl.ds(p % QUARTERS * 2, 2), pl.ds(pl.multiple_of(s * d.slab, d.slab), d.slab), :]

    u_gathers = [Gather(u_block(p), u_send.at[p], lambda s, p=p: u_recv.at[p, s]) for p in range(PIECES)]

    def act(kind, i, p, j):
        g = u_gathers[p]
        if kind == ALONG:
            g.send(slot, device(zn[i], ypos, xpos, core))
        elif kind == ACROSS:
            g.own_across()
        elif kind == FROM_COLUMN:
            which = chip_slot(zn[i], ypos, xpos)
            g.wait(which)
            g.send(which, three)
            g.send(which, two)
        elif kind == FROM_SECOND:
            which = chip_slot(zn[i], y_two, x_two)
            g.wait(which)
            g.send(which, three)
        elif kind == THIRD:
            g.last(False)
        elif kind == DIAGONAL:
            g.last(True)
        elif kind == RESULT:
            turn_result(j - 1, vcur)
        elif kind == RESULT_OUT:
            hand_out(j - 1, 0, RESULT_EARLY)
        elif kind == RESULT_PUT:
            @pl.when(j > 1)
            def _():
                put_out(j - 2)

    all_right = pltpu.make_async_copy(right, rs, loc_sem.at[2, 0])
    all_right.start()

    barrier = pltpu.get_barrier_semaphore()

    def knock(n, carry):
        pl.semaphore_signal(barrier, inc=1, device_id=((me + n) % DEVS,), device_id_type=MESH)
        return carry

    lax.fori_loop(1, DEVS, knock, 0)

    for ch in range(CHUNKS):
        for h in range(2):
            mine = left.at[:, pl.ds(pl.multiple_of(core * d.half + ch * d.chunk, d.chunk), d.chunk),
                           pl.ds(pl.multiple_of((core + h) % 2 * d.half, d.half), d.half)]
            pltpu.make_async_copy(mine, lv.at[ch, slot, core, :, :, pl.ds(h * d.half, d.half)], loc_sem.at[ch, h]).start()

    psi_rows = d.half * d.pair // 8
    psi_copies = [pltpu.make_async_copy(psi.at[pl.ds(pl.multiple_of(core * d.half * d.pair + n * psi_rows, psi_rows), psi_rows),
                                               pl.ds(c * d.lane, d.lane)],
                                        ps.at[c, pl.ds(n * psi_rows, psi_rows), :], psi_sem.at[n, c])
                  for n in range(8) for c in range(d.lane_tiles)]
    for copy in psi_copies:
        copy.start()

    first_rows = d.out_rows * d.pair
    first_copies = [pltpu.make_async_copy(psi.at[pl.ds(pl.multiple_of(me * first_rows, first_rows), first_rows), pl.ds(c * d.wide, d.wide)],
                                          tbuf.at[LANCZOS_STEPS - 1, c], first_sem.at[c]) for c in range(d.bond // d.wide)]
    for copy in first_copies:
        copy.start()

    spread = (lax.broadcasted_iota(jnp.int32, (d.pair, d.prod), 1) // d.sub == lax.broadcasted_iota(jnp.int32, (d.pair, d.prod), 0))
    spread = spread.astype(jnp.float32).astype(jnp.bfloat16)
    for t in range(d.terms_dev):
        wv[slot, core, t] = jnp.dot(pair_ops[t], spread, preferred_element_type=jnp.float32).astype(jnp.bfloat16)
    all_right.wait()
    some_rows = d.bond // 8

    def one_sided(i, carry):
        at = pl.ds(pl.multiple_of(i * some_rows, some_rows), some_rows)
        row = lax.broadcasted_iota(jnp.int32, (some_rows, d.bond), 0) + i * some_rows
        one = jnp.where(row == lax.broadcasted_iota(jnp.int32, (some_rows, d.bond), 1), 1.0, 0.0)
        for t in range(d.terms_dev):
            rs[t, at, :] = jnp.where(flags[t] == 1, rs[t, at, :].astype(jnp.float32), one).astype(jnp.bfloat16)
        return carry

    lax.fori_loop(0, 8, one_sided, 0)

    def right_rows(s):
        return rs.at[:, pl.ds(pl.multiple_of(s * d.slab, d.slab), d.slab), :]

    rv[slot, core] = rs[:, pl.ds(pl.multiple_of(slot * d.slab, d.slab), d.slab), :]

    pl.semaphore_wait(barrier, DEVS - 1)
    for ch in range(CHUNKS):
        for h in range(2):
            theirs = left.at[:, pl.ds(pl.multiple_of((1 - core) * d.half + ch * d.chunk, d.chunk), d.chunk),
                             pl.ds(pl.multiple_of((1 - core + h) % 2 * d.half, d.half), d.half)]
            remote(theirs, lv.at[ch, slot, core, :, :, pl.ds(h * d.half, d.half)], d2d_sem.at[ch, h], d2d_recv.at[ch, h], partner).start()
    for n in range(1, CHIPS):
        z, y, x = zn[n // 4], ypos + n % 4 // 2 * (1 - 2 * ypos), xpos + n % 2 * (1 - 2 * xpos)
        to = device(z, y, x, core)
        remote(right_rows(chip_slot(z, y, x)), rv.at[slot, core], rw_send.at[0], rw_recv.at[0], to).start()
        remote(wv.at[slot, core], wv.at[slot, core], rw_send.at[1], rw_recv.at[1], to).start()

    for ch in range(CHUNKS):
        for h in range(2):
            pltpu.make_async_copy(lv.at[ch, slot, core, :, :, pl.ds(h * d.half, d.half)], lv.at[ch, slot, core, :, :, pl.ds(h * d.half, d.half)], loc_sem.at[ch, h]).wait()
            back = remote(lv.at[ch, slot, 1 - core, :, :, pl.ds(h * d.half, d.half)], lv.at[ch, slot, 1 - core, :, :, pl.ds(h * d.half, d.half)], d2d_sem.at[ch, h], d2d_recv.at[ch, h], partner)
            back.wait_recv()
    l_along()
    for g in l_gathers:
        g.own_across()

    total = jnp.zeros((8, d.lane), jnp.float32)
    for n in range(8):
        for copy in psi_copies[n * d.lane_tiles:(n + 1) * d.lane_tiles]:
            copy.wait()

        def add_rows(i, acc, n=n):
            x = ps[:, pl.ds(pl.multiple_of(n * psi_rows + i * (psi_rows // 8), 8), psi_rows // 8), :]
            return acc + jnp.sum((x * x).reshape(d.lane_tiles * psi_rows // 64, 8, d.lane), axis=0)

        total = lax.fori_loop(0, 8, add_rows, total)
    nbuf[0] = jnp.broadcast_to(jnp.sum(total, keepdims=True), (8, 128))
    to_partner = remote(nbuf.at[0], nbuf.at[1], n_send, n_recv, partner)
    to_partner.start()
    to_partner.wait()
    norm = jnp.sqrt((nbuf[0] + nbuf[1])[0:1, :] / d.vec_size)
    norm_one = norm[:, 0:1]
    for copy in first_copies:
        copy.wait()
    tbuf[LANCZOS_STEPS - 1] = tbuf[LANCZOS_STEPS - 1] / norm_one[None]
    first_out = [pltpu.make_async_copy(tbuf.at[LANCZOS_STEPS - 1, c], first.at[:, pl.ds(c * d.wide, d.wide)], first_sem.at[c])
                 for c in range(d.bond // d.wide)]
    for copy in first_out:
        copy.start()

    def place(q):
        tiles = [(ps[c, pl.ds(q, d.half, stride=d.pair), :] / norm_one).T for c in range(d.lane_tiles)]
        xt = jnp.concatenate(tiles, axis=0)
        vprev[...] = xt
        return xt.astype(jnp.bfloat16)

    def start_vector(qb, carry):
        for q2 in range(2):
            q = qb * 2 + q2
            xb = place(q)
            for ch in range(CHUNKS):
                uv[ch, qb, :, q2 * d.chunk:(q2 + 1) * d.chunk] = xb[:, ch * d.chunk:(ch + 1) * d.chunk]
            for bh in range(2):
                rows = vprev[pl.ds(pl.multiple_of(slot * d.slab + bh * d.sub, d.sub), d.sub), :]
                vcur[pl.ds(pl.multiple_of((bh * d.pair + q) * d.sub, d.sub), d.sub), :] = rows
        return carry

    lax.fori_loop(0, d.pair // 4, start_vector, 0)
    l_event(0)
    l_event(1)
    lax.fori_loop(d.pair // 4, d.pair // 2, start_vector, 0)
    l_event(3)
    l_event(2)
    fifteen = rv.at[pl.ds(0, CHIPS - 1), 0]
    fifteen_w = wv.at[pl.ds(0, CHIPS - 1), 0]
    remote(fifteen, fifteen, rw_send.at[0], rw_recv.at[0], me).wait()
    remote(fifteen_w, fifteen_w, rw_send.at[1], rw_recv.at[1], me).wait()
    fw_right = remote(rv.at[:, core], rv.at[:, core], fw_send.at[0], fw_recv.at[0], partner)
    fw_pair = remote(wv.at[:, core], wv.at[:, core], fw_send.at[1], fw_recv.at[1], partner)
    fw_right.start()
    fw_pair.start()
    fw_right.wait()
    fw_pair.wait()
    lane = lax.broadcasted_iota(jnp.int32, (d.sub, d.prod), 1)
    row = lax.broadcasted_iota(jnp.int32, (d.sub, d.prod), 0)
    diagonal = lane % d.sub == row

    def spread_pair(s, carry):
        for c in range(2):
            for t in range(d.terms_dev):
                w = wv[s, c, t].astype(jnp.float32)
                for q in range(d.pair):
                    full = jnp.where(diagonal, jnp.broadcast_to(w[q:q + 1, :], (d.sub, d.prod)), 0.0)
                    kw[s, c, t, q * d.sub:(q + 1) * d.sub, :] = full.astype(jnp.bfloat16)
        return carry

    lax.fori_loop(0, CHIPS, spread_pair, 0)
    vprev[...] = jnp.zeros_like(vprev)
    for copy in first_out:
        copy.wait()

    def right_product(grp, ch, qb, to):
        r_all = rv[pl.ds(grp * 4, 4)].reshape(d.group_terms * d.slab, d.bond)
        y = jnp.dot(r_all, uv[ch, qb], preferred_element_type=jnp.float32).astype(jnp.bfloat16)
        y = y.reshape(d.group_terms, 2, d.sub, 2 * d.chunk)
        for q2 in range(2):
            for bh in range(2):
                yst[pl.ds(to * d.group_terms, d.group_terms), qb * 2 + q2, :, bh * d.chunk:(bh + 1) * d.chunk] = \
                    y[:, bh, :, q2 * d.chunk:(q2 + 1) * d.chunk]

    def right_of_piece(ch, part):
        for qb in range(2):
            for grp in range(GROUPS):
                right_product(grp, ch, part * 2 + qb, grp)

    def right_of_group(grp, ch, to):
        for qb in range(d.pair // 2):
            right_product(grp, ch, qb, to)

    def left_products(ch, grp, at=None):
        for k in range(d.group_terms):
            w = kw[grp * 4 + k // 4, k // 2 % 2, k % 2]
            z = jnp.dot(w, yst[(grp if at is None else at) * d.group_terms + k].reshape(d.prod, 2 * d.chunk), preferred_element_type=jnp.float32).astype(jnp.bfloat16)
            for bh in range(2):
                zst[bh * d.prod:(bh + 1) * d.prod, k * d.chunk:(k + 1) * d.chunk] = z[:, bh * d.chunk:(bh + 1) * d.chunk]
        l_all = lv[ch, pl.ds(grp * 4, 4)].reshape(d.group_terms * d.chunk, d.bond)
        sig[...] += jnp.dot(zst[...], l_all, preferred_element_type=jnp.float32)

    def first_right(grp, carry):
        right_of_group(grp, 0, grp)

        @pl.when(grp == 1)
        def _():
            l_event(5)
        return carry

    def first_group(n, carry):
        own, third = xpos * 2 + ypos, x_three * 2 + y_three
        grp = jnp.where(n == 0, own, jnp.where(n == 1, x_two * 2 + y_two, jnp.where(n == 2, third, 3 - own)))
        spare = jnp.where(n == 3, own, grp)

        @pl.when(n == 1)
        def _():
            l_event(6)
            l_last(False)

        @pl.when(n == 3)
        def _():
            right_of_group(grp, 1, spare)
            l_last(True)

        def fill(z, carry):
            l_fill(grp * 4 + z)
            return carry

        lax.fori_loop(0, 4, fill, 0)

        def chunk_products(ch, carry):
            left_products(ch, grp, (1 - ch) * grp + ch * spare)

            @pl.when((ch == 0) & (n < 3))
            def _():
                right_of_group(grp, 1, spare)
            return carry

        lax.fori_loop(0, CHUNKS, chunk_products, 0)
        return carry

    def turn_result(j, vector):
        for n in range(d.pair // TILE_PARTS):
            rows = [vector[(bh * d.pair + q) * d.sub:(bh * d.pair + q + 1) * d.sub, :d.half]
                    for q in range(n * TILE_PARTS, (n + 1) * TILE_PARTS) for bh in range(2)]
            tbuf[j, n] = jnp.concatenate(rows, axis=0).T

    def hand_out(j, begin, end):
        for n in range(begin, end):
            to = core * CHIPS + n
            block = tbuf.at[j, :, pl.ds(n * d.out_rows, d.out_rows), :]

            @pl.when(to != me)
            def _():
                remote(block, gbuf.at[j, slot], k_send.at[j], k_recv.at[j], to).start()

            @pl.when(to == me)
            def _():
                gbuf[j, slot] = block[...]

    sends_self = me // CHIPS == core
    lanes = lax.broadcasted_iota(jnp.int32, (d.out_rows, d.wide), 1) // d.slab

    def put_out(j, finish=None):
        @pl.when(sends_self)
        def _():
            some = gbuf.at[j, pl.ds(0, CHIPS - 1)]
            remote(some, some, k_send.at[j], k_recv.at[j], me).wait()

        @pl.when(jnp.logical_not(sends_self))
        def _():
            remote(gbuf.at[j], gbuf.at[j], k_send.at[j], k_recv.at[j], me).wait()

        for ct in range(CHIPS // TILE_PARTS):
            for qt in range(d.pair // TILE_PARTS):
                src = [gbuf[j, ct * TILE_PARTS + c, qt] for c in range(TILE_PARTS)]
                if finish is not None:
                    src = [finish(x, gbuf[j - 1, ct * TILE_PARTS + c, qt], ct * TILE_PARTS + c) for c, x in enumerate(src)]
                for q in range(TILE_PARTS):
                    tile = jnp.zeros((d.out_rows, d.wide), jnp.float32)
                    for c in range(TILE_PARTS):
                        shift = (c - q) % TILE_PARTS * d.slab
                        moved = pltpu.roll(src[c], shift, 1) if shift else src[c]
                        tile = jnp.where(lanes == c, moved, tile)
                    tbuf[j, ct, pl.ds(qt * TILE_PARTS + q, d.out_rows, stride=d.pair), :] = tile
            pltpu.make_async_copy(tbuf.at[j, ct], out.at[j, :, pl.ds(ct * d.wide, d.wide)], o_sem.at[j, ct]).start()

    def step(j, carried):
        beta_prev = carried[0]
        sig[...] = jnp.zeros_like(sig)

        def slot_step(t, carry):
            done_right = sum((t > r).astype(jnp.int32) for r in RIGHT_SLOTS)
            done_left = t - done_right
            is_right = sum((t == r).astype(jnp.int32) for r in RIGHT_SLOTS)
            for four in range(0, len(SLOTS), 4):
                @pl.when((t >= four) & (t < four + 4))
                def _():
                    for at in range(four, four + 4):
                        if not SLOTS[at]:
                            continue

                        @pl.when(t == at)
                        def _():
                            for kind, i, p in SLOTS[at]:
                                act(kind, i, p, j)

            @pl.when(is_right == 1)
            def _():
                right_of_piece(done_right // QUARTERS, done_right % QUARTERS)

            @pl.when(is_right == 0)
            def _():
                left_products(done_left // GROUPS, done_left % GROUPS)
            return carry

        @pl.when(j == 0)
        def _():
            lax.fori_loop(0, GROUPS, first_right, 0)
            l_event(4)
            lax.fori_loop(0, GROUPS, first_group, 0)

        @pl.when(j > 0)
        def _():
            lax.fori_loop(0, len(SLOTS), slot_step, 0)
            for p in range(PIECES):
                sent = uv.at[p // QUARTERS, pl.ds(0, 2), pl.ds(0, 15 * d.slab), :]
                remote(sent, sent, u_send.at[p], u_recv.at[p, 0], me).wait_send()

        other = sig.at[:, pl.ds(d.half, d.half)]
        to_other = remote(other, part, p_send, p_recv, partner)
        to_other.start()
        to_other.wait()
        s = sig[:, :d.half] + part[...]
        v = vcur[...]
        w = s - beta_prev * vprev[...]
        sv = jnp.sum(s * v, keepdims=True)
        wv_sum = jnp.sum(w * v, keepdims=True)
        vv = jnp.sum(v * v, keepdims=True)
        guess = jnp.where(vv > 0.0, wv_sum / jnp.where(vv > 0.0, vv, 1.0), 0.0)
        t = w - guess * v
        sig[:, :d.half] = t
        tt = jnp.sum(t * t, keepdims=True)
        tv = jnp.sum(t * v, keepdims=True)
        at_lane = lax.broadcasted_iota(jnp.int32, (1, 128), 1)
        line = jnp.zeros((1, 128), jnp.float32)
        for n, value in enumerate((sv, vv, tt, tv, guess)):
            line = jnp.where(at_lane == n, value, line)
        scs[...] = line
        scr[me] = line

        def tell(n, carry):
            remote(scs, scr.at[me], s_send, s_recv, (me + n) % DEVS).start()
            return carry

        lax.fori_loop(1, DEVS, tell, 0)

        @pl.when(j > 0)
        def _():
            hand_out(j - 1, RESULT_EARLY, CHIPS)

        @pl.when(j == LANCZOS_STEPS - 1)
        def _():
            turn_result(LANCZOS_STEPS - 1, sig)
            hand_out(LANCZOS_STEPS - 1, 0, CHIPS)

        heard = scr.at[pl.ds(0, DEVS - 1)]
        remote(heard, heard, s_send, s_recv, me).wait()
        told = scr[:, 0, :]
        alpha = jnp.sum(told[:, 0:1], axis=0, keepdims=True) / d.vec_size
        off = alpha - told[:, 4:5]
        square = told[:, 2:3] - 2.0 * off * told[:, 3:4] + off * off * told[:, 1:2]
        beta = jnp.sqrt(jnp.sum(square, axis=0, keepdims=True) / d.vec_size)
        vnew = (sig[:, :d.half] - (alpha - guess) * vcur[...]) / beta
        vprev[...] = vcur[...]
        vcur[...] = vnew
        vb = vnew.astype(jnp.bfloat16)

        @pl.when(j < LANCZOS_STEPS - 1)
        def _():
            for ch in range(CHUNKS):
                for bh in range(2):
                    at = pl.ds(pl.multiple_of(slot * d.slab + bh * d.sub, d.sub), d.sub)
                    for q in range(d.pair):
                        uv[ch, q // 2, at, q % 2 * d.chunk:(q % 2 + 1) * d.chunk] = \
                            vb[(bh * d.pair + q) * d.sub:(bh * d.pair + q + 1) * d.sub, ch * d.chunk:(ch + 1) * d.chunk]
        alphas[j] = alpha[0, 0]
        betas[j] = beta[0, 0]
        return beta, alpha


    zero = jnp.zeros((1, 1), jnp.float32)
    last_beta, last_alpha = lax.fori_loop(0, LANCZOS_STEPS, step, (zero, zero))

    for n, part in enumerate((lv.at[0, pl.ds(0, 15), :, 0], lv.at[1, pl.ds(0, 15), :, 0, :, pl.ds(edge, d.bond - edge)],
                              lv.at[0, pl.ds(0, 15), :, 0, :, pl.ds(0, d.half)], lv.at[1, pl.ds(0, 15), :, 0, :, pl.ds(edge, d.half - edge)])):
        remote(part, part, l_send.at[n], l_recv.at[n, 0], me).wait_send()
    swapped = lv.at[:, pl.ds(0, 15), :, 0, :, pl.ds(d.half, d.half)]
    remote(swapped, swapped, f_send, f_recv.at[0], me).wait_send()
    for ch in range(CHUNKS):
        for h in range(2):
            theirs = left.at[:, pl.ds(0, d.chunk), pl.ds(0, d.half)]
            remote(theirs, lv.at[ch, slot, core, :, :, pl.ds(h * d.half, d.half)], d2d_sem.at[ch, h], d2d_recv.at[ch, h], partner).wait_send()
    put_out(LANCZOS_STEPS - 2)

    def finish(block, before, s):
        owner = device(s % 4, s // 4 % 2, s // 8, me // CHIPS)
        return (block - (last_alpha - scr[owner][:, 4:5]) * before) / last_beta

    put_out(LANCZOS_STEPS - 1, finish)
    for j in range(LANCZOS_STEPS):
        for c in range(d.bond // d.wide):
            pltpu.make_async_copy(tbuf.at[j, c], out.at[j, :, pl.ds(c * d.wide, d.wide)], o_sem.at[j, c]).wait()


def solution(mesh):
    def device_body(wavefunction, left_loc, pair_loc, right_loc, flag_loc):
        bond, pair = wavefunction.shape[0], wavefunction.shape[1]
        d = Dims(bond, pair, left_loc.shape[0])
        bf16, f32 = jnp.bfloat16, jnp.float32
        dma = pltpu.SemaphoreType.DMA
        any_space = pl.BlockSpec(memory_space=pl.ANY)
        smem = pl.BlockSpec(memory_space=pltpu.SMEM)
        scalars = jax.ShapeDtypeStruct((LANCZOS_STEPS,), f32)
        later, first, alphas, betas = pl.pallas_call(
            functools.partial(lanczos_kernel, d),
            out_shape=(jax.ShapeDtypeStruct((LANCZOS_STEPS, d.out_rows * pair, bond), f32),
                       jax.ShapeDtypeStruct((d.out_rows * pair, bond), f32), scalars, scalars),
            in_specs=[any_space] * 3 + [pl.BlockSpec(memory_space=pltpu.VMEM), smem],
            out_specs=(any_space, any_space, smem, smem),
            scratch_shapes=[
                pltpu.VMEM((CHUNKS, CHIPS, CORES, d.terms_dev, d.chunk, bond), bf16),
                pltpu.VMEM((CHIPS, CORES, d.terms_dev, d.slab, bond), bf16),
                pltpu.VMEM((d.terms_dev, bond, bond), bf16),
                pltpu.VMEM((CHIPS, CORES, d.terms_dev, pair, d.prod), bf16),
                pltpu.VMEM((CHIPS, CORES, d.terms_dev, d.prod, d.prod), bf16),
                pltpu.VMEM((CHUNKS, pair // 2, bond, 2 * d.chunk), bf16),
                pltpu.VMEM((d.lane_tiles, d.half * pair, d.lane), f32),
                pltpu.VMEM((CHIPS * CORES * d.terms_dev, pair, d.sub, 2 * d.chunk), bf16),
                pltpu.VMEM((d.rows, d.group_terms * d.chunk), bf16),
                pltpu.VMEM((d.rows, bond), f32),
                pltpu.VMEM((d.rows, d.half), f32),
                pltpu.VMEM((d.rows, d.half), f32),
                pltpu.VMEM((d.rows, d.half), f32),
                pltpu.VMEM((LANCZOS_STEPS, bond // d.wide, d.half, d.wide), f32),
                pltpu.VMEM((LANCZOS_STEPS, CHIPS, bond // d.wide, d.out_rows, d.wide), f32),
                pltpu.VMEM((1, 128), f32),
                pltpu.VMEM((DEVS, 1, 128), f32),
                pltpu.VMEM((2, 8, 128), f32),
                dma((3, 2)), dma((8, d.lane_tiles)), dma((CHUNKS, 2)), dma((CHUNKS, 2)), dma((2,)), dma((2,)), dma((2,)), dma((2,)),
                dma((4,)), dma((4, CHIPS)), dma, dma((CHIPS,)), dma((PIECES,)), dma((PIECES, CHIPS)),
                dma, dma, dma, dma, dma((LANCZOS_STEPS,)), dma((LANCZOS_STEPS,)), dma, dma, dma((LANCZOS_STEPS, bond // d.wide)), dma((bond // d.wide,)),
            ],
            compiler_params=pltpu.CompilerParams(has_side_effects=True, collective_id=0, vmem_limit_bytes=67043328),
            name='lanczos',
        )(wavefunction.reshape(bond * pair, bond), left_loc, right_loc, pair_loc, flag_loc)
        krylov = jnp.concatenate([first[None], later])
        return krylov.reshape(LANCZOS_STEPS + 1, d.out_rows, pair, bond), alphas, betas

    return jax.shard_map(device_body, mesh=mesh, in_specs=(P(), P(AXIS_NAME), P(AXIS_NAME), P(AXIS_NAME), P(AXIS_NAME)),
                         out_specs=(P(None, AXIS_NAME), P(), P()), check_vma=False)
```

```python
import functools

import jax
import jax.numpy as jnp
from jax import lax
from jax.experimental import pallas as pl
from jax.experimental.pallas import tpu as pltpu
from jax.sharding import PartitionSpec as P

LANCZOS_STEPS = 6
AXIS_NAME = 'terms'
MESH = pl.DeviceIdType.MESH

CHIPS = 16
CORES = 2
DEVS = 32
CHUNKS = 2
GROUPS = 4
TILE_PARTS = 4
QUARTERS = 4
PIECES = CHUNKS * QUARTERS

ALONG, ACROSS, FROM_COLUMN, FROM_SECOND, THIRD, DIAGONAL, RESULT, RESULT_OUT, RESULT_PUT = range(9)
RIGHT_SLOTS = (0, 1, 2, 3, 8, 9, 10, 11)
SLOTS = (
    ((0, 1, 0), (0, 1, 1), (1, 0, 2), (0, 2, 0), (1, 0, 5), (1, 0, 3), (1, 0, 6), (1, 0, 0), (0, 3, 0), (3, 0, 2), (0, 2, 1), (0, 1, 3), (1, 0, 4), (0, 3, 1), (1, 0, 7), (0, 1, 2), (1, 0, 1), (0, 3, 3), (2, 1, 0), (2, 2, 0), (0, 2, 3), (0, 3, 2), (2, 1, 1), (3, 0, 0), (2, 3, 0), (3, 1, 0), (2, 2, 1), (0, 2, 2), (0, 1, 4), (3, 0, 1), (2, 1, 3), (3, 2, 0), (2, 3, 1), (2, 2, 2), (2, 2, 3), (2, 1, 2), (4, 0, 0), (0, 2, 5), (0, 3, 4), (0, 2, 4), (0, 1, 5), (0, 1, 6), (0, 1, 7), (3, 3, 0), (2, 3, 3), (3, 1, 1), (3, 2, 1), (0, 2, 6), (2, 3, 2), (4, 0, 1), (3, 3, 1), (0, 3, 6), (3, 2, 2), (3, 1, 2), (0, 3, 5), (0, 2, 7), (0, 3, 7), (3, 2, 3), (3, 3, 2), (3, 0, 3), (5, 0, 0), (3, 3, 3), (4, 0, 3), (3, 1, 3), (3, 0, 4),),
    ((6, 0, 0), (2, 2, 4), (5, 0, 1), (3, 0, 6), (2, 1, 4), (4, 0, 2),),
    ((2, 2, 6), (5, 0, 2), (2, 1, 6),),
    ((2, 2, 5), (5, 0, 3), (3, 2, 4), (2, 3, 4),),
    ((2, 1, 5), (3, 0, 5), (3, 1, 4),),
    ((2, 3, 5), (3, 2, 5), (2, 3, 6),),
    ((2, 2, 7), (3, 3, 4), (2, 1, 7), (3, 1, 5), (8, 0, 0),),
    ((3, 3, 5), (2, 3, 7), (3, 2, 6), (3, 1, 6), (3, 3, 6),),
    ((3, 0, 7), (3, 1, 7), (3, 2, 7), (4, 0, 5), (5, 0, 4), (4, 0, 4),),
    ((3, 3, 7), (5, 0, 5),),
    ((4, 0, 6), (5, 0, 6),),
    ((4, 0, 7), (5, 0, 7), (7, 0, 0),),
    (),
    (),
    (),
    (),
)
RESULT_EARLY = 9


class Dims:
    def __init__(self, bond, pair, terms_dev):
        self.bond = bond
        self.pair = pair
        self.terms_dev = terms_dev
        self.slab = bond // CHIPS
        self.sub = self.slab // 2
        self.half = bond // CORES
        self.chunk = self.half // CHUNKS
        self.rows = self.slab * pair
        self.prod = self.sub * pair
        self.out_rows = bond // DEVS
        self.group_terms = 4 * CORES * terms_dev
        self.vec_size = bond * pair * bond
        self.lane = min(bond, 128)
        self.wide = TILE_PARTS * self.slab
        self.lane_tiles = bond // self.lane


def lanczos_kernel(d, psi, left, right, pair_ops, flags, out, first, alphas, betas, lv, rv, rs, wv, kw, uv, ps, yst, zst, sig, part, vcur, vprev, tbuf, gbuf,
                   scs, scr, nbuf,
                   loc_sem, psi_sem, d2d_sem, d2d_recv, rw_send, rw_recv, fw_send, fw_recv, l_send, l_recv, f_send, f_recv, u_send, u_recv,
                   p_send, p_recv, s_send, s_recv, k_send, k_recv, n_send, n_recv, o_sem, first_sem):
    me = lax.axis_index(AXIS_NAME)
    core = me % 2
    xpos = (me // 2) % 2
    ypos = (me // 4) % 2
    zpos = me // 8

    def device(z, y, x, c):
        return ((z * 2 + y) * 2 + x) * 2 + c

    def chip_slot(z, y, x):
        return (x * 2 + y) * 4 + z

    partner = device(zpos, ypos, xpos, 1 - core)
    slot = chip_slot(zpos, ypos, xpos)
    inner = (zpos + 1) // 2 % 2
    zn = (zpos, (1 - inner) * (zpos + 1 - zpos // 3 * 2) + inner * (zpos - 1), (1 - inner) * ((zpos + 2) % 4) + inner * (zpos + 1),
          (1 - inner) * (3 - zpos) + inner * ((zpos + 2) % 4))
    y_two = ypos + (1 - core) * (1 - 2 * ypos)
    x_two = xpos + core * (1 - 2 * xpos)
    y_three = ypos + core * (1 - 2 * ypos)
    x_three = xpos + (1 - core) * (1 - 2 * xpos)
    two = device(zpos, y_two, x_two, core)
    three = device(zpos, y_three, x_three, core)

    def remote(src, dst, send, recv, dev):
        return pltpu.make_async_remote_copy(src_ref=src, dst_ref=dst, send_sem=send, recv_sem=recv, device_id=(dev,), device_id_type=MESH)

    class Gather:
        def __init__(self, block, send, recv):
            self.block, self.send_sem, self.recv_sem = block, send, recv

        def send(self, which, dev):
            remote(self.block(which), self.block(which), self.send_sem, self.recv_sem(which), dev).start()

        def wait(self, which):
            remote(self.block(which), self.block(which), self.send_sem, self.recv_sem(which), me).wait_recv()

        def own_along(self):
            for i in (1, 2, 3):
                self.send(slot, device(zn[i], ypos, xpos, core))

        def own_across(self):
            self.send(slot, three)
            self.send(slot, two)

        def event(self, n):
            i = (n + 1) // 2
            if n % 2:
                which = chip_slot(zn[i], ypos, xpos)
                self.wait(which)
                self.send(which, three)
                self.send(which, two)
            else:
                which = chip_slot(zn[i], y_two, x_two)
                self.wait(which)
                self.send(which, three)

        def last(self, diagonal):
            for i in range(4):
                self.wait(chip_slot(zn[i], 1 - ypos, 1 - xpos) if diagonal else chip_slot(zn[i], y_three, x_three))

    edge = d.chunk
    l_parts = (
        (lambda s: lv.at[0, s, :, core], 0),
        (lambda s: lv.at[1, s, :, core, :, pl.ds(edge, d.bond - edge)], 1),
        (lambda s: lv.at[0, s, :, 1 - core, :, pl.ds(0, d.half)], 2),
        (lambda s: lv.at[1, s, :, 1 - core, :, pl.ds(edge, d.half - edge)], 3),
    )
    l_gathers = [Gather(block, l_send.at[n], lambda s, n=n: l_recv.at[n, s]) for block, n in l_parts]

    def l_swap(s, term):
        part = lv.at[:, s, :, term, :, pl.ds(d.half, d.half)]
        return remote(part, part, f_send, f_recv.at[s], partner)

    def l_event(n):
        i = (n + 1) // 2
        for g in l_gathers:
            g.event(n)
        l_swap(chip_slot(zn[i], ypos, xpos) if n % 2 else chip_slot(zn[i], y_two, x_two), core).start()

    def l_last(diagonal):
        for i in range(4):
            which = chip_slot(zn[i], 1 - ypos, 1 - xpos) if diagonal else chip_slot(zn[i], y_three, x_three)
            for g in l_gathers:
                g.wait(which)
            l_swap(which, core).start()

    def l_fill(s):
        @pl.when(s != slot)
        def _():
            l_swap(s, 1 - core).wait_recv()
            for c in range(CORES):
                tile = lv[:, s, c, 1 - core, :, d.half:].reshape(d.half, d.half).T
                lv[:, s, c, 1 - core, :, d.half:] = tile.reshape(CHUNKS, d.chunk, d.half)
                for t in range(d.terms_dev):
                    lv[1, s, c, t, :, :edge] = lv[0, s, c, t, :, edge:d.half].T

    def l_along():
        for i in (1, 2, 3):
            for g in l_gathers:
                g.send(slot, device(zn[i], ypos, xpos, core))

    def u_block(p):
        return lambda s: uv.at[p // QUARTERS, pl.ds(p % QUARTERS * 2, 2), pl.ds(pl.multiple_of(s * d.slab, d.slab), d.slab), :]

    u_gathers = [Gather(u_block(p), u_send.at[p], lambda s, p=p: u_recv.at[p, s]) for p in range(PIECES)]

    def act(kind, i, p, j):
        g = u_gathers[p]
        if kind == ALONG:
            g.send(slot, device(zn[i], ypos, xpos, core))
        elif kind == ACROSS:
            g.own_across()
        elif kind == FROM_COLUMN:
            which = chip_slot(zn[i], ypos, xpos)
            g.wait(which)
            g.send(which, three)
            g.send(which, two)
        elif kind == FROM_SECOND:
            which = chip_slot(zn[i], y_two, x_two)
            g.wait(which)
            g.send(which, three)
        elif kind == THIRD:
            g.last(False)
        elif kind == DIAGONAL:
            g.last(True)
        elif kind == RESULT:
            turn_result(j - 1, vcur)
        elif kind == RESULT_OUT:
            hand_out(j - 1, 0, RESULT_EARLY)
        elif kind == RESULT_PUT:
            @pl.when(j > 1)
            def _():
                put_out(j - 2)

    all_right = pltpu.make_async_copy(right, rs, loc_sem.at[2, 0])
    all_right.start()

    barrier = pltpu.get_barrier_semaphore()

    def knock(n, carry):
        pl.semaphore_signal(barrier, inc=1, device_id=((me + n) % DEVS,), device_id_type=MESH)
        return carry

    lax.fori_loop(1, DEVS, knock, 0)

    for ch in range(CHUNKS):
        for h in range(2):
            mine = left.at[:, pl.ds(pl.multiple_of(core * d.half + ch * d.chunk, d.chunk), d.chunk),
                           pl.ds(pl.multiple_of((core + h) % 2 * d.half, d.half), d.half)]
            pltpu.make_async_copy(mine, lv.at[ch, slot, core, :, :, pl.ds(h * d.half, d.half)], loc_sem.at[ch, h]).start()

    psi_rows = d.half * d.pair // 8
    psi_copies = [pltpu.make_async_copy(psi.at[pl.ds(pl.multiple_of(core * d.half * d.pair + n * psi_rows, psi_rows), psi_rows),
                                               pl.ds(c * d.lane, d.lane)],
                                        ps.at[c, pl.ds(n * psi_rows, psi_rows), :], psi_sem.at[n, c])
                  for n in range(8) for c in range(d.lane_tiles)]
    for copy in psi_copies:
        copy.start()

    first_rows = d.out_rows * d.pair
    first_copies = [pltpu.make_async_copy(psi.at[pl.ds(pl.multiple_of(me * first_rows, first_rows), first_rows), pl.ds(c * d.wide, d.wide)],
                                          tbuf.at[LANCZOS_STEPS - 1, c], first_sem.at[c]) for c in range(d.bond // d.wide)]
    for copy in first_copies:
        copy.start()

    spread = (lax.broadcasted_iota(jnp.int32, (d.pair, d.prod), 1) // d.sub == lax.broadcasted_iota(jnp.int32, (d.pair, d.prod), 0))
    spread = spread.astype(jnp.float32).astype(jnp.bfloat16)
    for t in range(d.terms_dev):
        wv[slot, core, t] = jnp.dot(pair_ops[t], spread, preferred_element_type=jnp.float32).astype(jnp.bfloat16)
    all_right.wait()
    some_rows = d.bond // 8

    def one_sided(i, carry):
        at = pl.ds(pl.multiple_of(i * some_rows, some_rows), some_rows)
        row = lax.broadcasted_iota(jnp.int32, (some_rows, d.bond), 0) + i * some_rows
        one = jnp.where(row == lax.broadcasted_iota(jnp.int32, (some_rows, d.bond), 1), 1.0, 0.0)
        for t in range(d.terms_dev):
            rs[t, at, :] = jnp.where(flags[t] == 1, rs[t, at, :].astype(jnp.float32), one).astype(jnp.bfloat16)
        return carry

    lax.fori_loop(0, 8, one_sided, 0)

    def right_rows(s):
        return rs.at[:, pl.ds(pl.multiple_of(s * d.slab, d.slab), d.slab), :]

    rv[slot, core] = rs[:, pl.ds(pl.multiple_of(slot * d.slab, d.slab), d.slab), :]

    pl.semaphore_wait(barrier, DEVS - 1)
    for ch in range(CHUNKS):
        for h in range(2):
            theirs = left.at[:, pl.ds(pl.multiple_of((1 - core) * d.half + ch * d.chunk, d.chunk), d.chunk),
                             pl.ds(pl.multiple_of((1 - core + h) % 2 * d.half, d.half), d.half)]
            remote(theirs, lv.at[ch, slot, core, :, :, pl.ds(h * d.half, d.half)], d2d_sem.at[ch, h], d2d_recv.at[ch, h], partner).start()
    for n in range(1, CHIPS):
        chip = (me // 2 + n) % CHIPS
        to = chip_slot(chip // 4, chip // 2 % 2, chip % 2)
        remote(right_rows(to), rv.at[slot, core], rw_send.at[0], rw_recv.at[0], chip * 2 + core).start()
        remote(wv.at[slot, core], wv.at[slot, core], rw_send.at[1], rw_recv.at[1], chip * 2 + core).start()

    for ch in range(CHUNKS):
        for h in range(2):
            pltpu.make_async_copy(lv.at[ch, slot, core, :, :, pl.ds(h * d.half, d.half)], lv.at[ch, slot, core, :, :, pl.ds(h * d.half, d.half)], loc_sem.at[ch, h]).wait()
            back = remote(lv.at[ch, slot, 1 - core, :, :, pl.ds(h * d.half, d.half)], lv.at[ch, slot, 1 - core, :, :, pl.ds(h * d.half, d.half)], d2d_sem.at[ch, h], d2d_recv.at[ch, h], partner)
            back.wait_recv()
    l_along()
    for g in l_gathers:
        g.own_across()

    total = jnp.zeros((8, d.lane), jnp.float32)
    for n in range(8):
        for copy in psi_copies[n * d.lane_tiles:(n + 1) * d.lane_tiles]:
            copy.wait()

        def add_rows(i, acc, n=n):
            x = ps[:, pl.ds(pl.multiple_of(n * psi_rows + i * (psi_rows // 8), 8), psi_rows // 8), :]
            return acc + jnp.sum((x * x).reshape(d.lane_tiles * psi_rows // 64, 8, d.lane), axis=0)

        total = lax.fori_loop(0, 8, add_rows, total)
    nbuf[0] = jnp.broadcast_to(jnp.sum(total, keepdims=True), (8, 128))
    to_partner = remote(nbuf.at[0], nbuf.at[1], n_send, n_recv, partner)
    to_partner.start()
    to_partner.wait()
    norm = jnp.sqrt((nbuf[0] + nbuf[1])[0:1, :] / d.vec_size)
    norm_one = norm[:, 0:1]
    for copy in first_copies:
        copy.wait()
    tbuf[LANCZOS_STEPS - 1] = tbuf[LANCZOS_STEPS - 1] / norm_one[None]
    first_out = [pltpu.make_async_copy(tbuf.at[LANCZOS_STEPS - 1, c], first.at[:, pl.ds(c * d.wide, d.wide)], first_sem.at[c])
                 for c in range(d.bond // d.wide)]
    for copy in first_out:
        copy.start()

    def place(q):
        tiles = [(ps[c, pl.ds(q, d.half, stride=d.pair), :] / norm_one).T for c in range(d.lane_tiles)]
        xt = jnp.concatenate(tiles, axis=0)
        vprev[...] = xt
        return xt.astype(jnp.bfloat16)

    def start_vector(qb, carry):
        for q2 in range(2):
            q = qb * 2 + q2
            xb = place(q)
            for ch in range(CHUNKS):
                uv[ch, qb, :, q2 * d.chunk:(q2 + 1) * d.chunk] = xb[:, ch * d.chunk:(ch + 1) * d.chunk]
            for bh in range(2):
                rows = vprev[pl.ds(pl.multiple_of(slot * d.slab + bh * d.sub, d.sub), d.sub), :]
                vcur[pl.ds(pl.multiple_of((bh * d.pair + q) * d.sub, d.sub), d.sub), :] = rows
        return carry

    lax.fori_loop(0, d.pair // 4, start_vector, 0)
    fifteen = rv.at[pl.ds(0, CHIPS - 1), 0]
    fifteen_w = wv.at[pl.ds(0, CHIPS - 1), 0]
    remote(fifteen, fifteen, rw_send.at[0], rw_recv.at[0], me).wait()
    remote(fifteen_w, fifteen_w, rw_send.at[1], rw_recv.at[1], me).wait()
    fw_right = remote(rv.at[:, core], rv.at[:, core], fw_send.at[0], fw_recv.at[0], partner)
    fw_pair = remote(wv.at[:, core], wv.at[:, core], fw_send.at[1], fw_recv.at[1], partner)
    fw_right.start()
    fw_pair.start()
    l_event(0)
    l_event(1)
    lax.fori_loop(d.pair // 4, d.pair // 2, start_vector, 0)
    l_event(3)
    l_event(2)
    fw_right.wait()
    fw_pair.wait()
    lane = lax.broadcasted_iota(jnp.int32, (d.sub, d.prod), 1)
    row = lax.broadcasted_iota(jnp.int32, (d.sub, d.prod), 0)
    diagonal = lane % d.sub == row

    def spread_pair(s, carry):
        for c in range(2):
            for t in range(d.terms_dev):
                w = wv[s, c, t].astype(jnp.float32)
                for q in range(d.pair):
                    full = jnp.where(diagonal, jnp.broadcast_to(w[q:q + 1, :], (d.sub, d.prod)), 0.0)
                    kw[s, c, t, q * d.sub:(q + 1) * d.sub, :] = full.astype(jnp.bfloat16)
        return carry

    lax.fori_loop(0, CHIPS, spread_pair, 0)
    vprev[...] = jnp.zeros_like(vprev)
    for copy in first_out:
        copy.wait()

    def right_product(grp, ch, qb, to):
        r_all = rv[pl.ds(grp * 4, 4)].reshape(d.group_terms * d.slab, d.bond)
        y = jnp.dot(r_all, uv[ch, qb], preferred_element_type=jnp.float32).astype(jnp.bfloat16)
        y = y.reshape(d.group_terms, 2, d.sub, 2 * d.chunk)
        for q2 in range(2):
            for bh in range(2):
                yst[pl.ds(to * d.group_terms, d.group_terms), qb * 2 + q2, :, bh * d.chunk:(bh + 1) * d.chunk] = \
                    y[:, bh, :, q2 * d.chunk:(q2 + 1) * d.chunk]

    def right_of_piece(ch, part):
        for qb in range(2):
            for grp in range(GROUPS):
                right_product(grp, ch, part * 2 + qb, grp)

    def right_of_group(grp, ch, to):
        for qb in range(d.pair // 2):
            right_product(grp, ch, qb, to)

    def left_products(ch, grp, at=None):
        for k in range(d.group_terms):
            w = kw[grp * 4 + k // 4, k // 2 % 2, k % 2]
            z = jnp.dot(w, yst[(grp if at is None else at) * d.group_terms + k].reshape(d.prod, 2 * d.chunk), preferred_element_type=jnp.float32).astype(jnp.bfloat16)
            for bh in range(2):
                zst[bh * d.prod:(bh + 1) * d.prod, k * d.chunk:(k + 1) * d.chunk] = z[:, bh * d.chunk:(bh + 1) * d.chunk]
        l_all = lv[ch, pl.ds(grp * 4, 4)].reshape(d.group_terms * d.chunk, d.bond)
        sig[...] += jnp.dot(zst[...], l_all, preferred_element_type=jnp.float32)

    def first_right(grp, carry):
        right_of_group(grp, 0, grp)

        @pl.when(grp == 1)
        def _():
            l_event(5)
        return carry

    def first_group(n, carry):
        own, third = xpos * 2 + ypos, x_three * 2 + y_three
        grp = jnp.where(n == 0, own, jnp.where(n == 1, x_two * 2 + y_two, jnp.where(n == 2, third, 3 - own)))
        spare = jnp.where(n == 3, own, grp)

        @pl.when(n == 1)
        def _():
            l_event(6)
            l_last(False)

        @pl.when(n == 3)
        def _():
            right_of_group(grp, 1, spare)
            l_last(True)

        def fill(z, carry):
            l_fill(grp * 4 + z)
            return carry

        lax.fori_loop(0, 4, fill, 0)

        def chunk_products(ch, carry):
            left_products(ch, grp, (1 - ch) * grp + ch * spare)

            @pl.when((ch == 0) & (n < 3))
            def _():
                right_of_group(grp, 1, spare)
            return carry

        lax.fori_loop(0, CHUNKS, chunk_products, 0)
        return carry

    def turn_result(j, vector):
        for n in range(d.pair // TILE_PARTS):
            rows = [vector[(bh * d.pair + q) * d.sub:(bh * d.pair + q + 1) * d.sub, :d.half]
                    for q in range(n * TILE_PARTS, (n + 1) * TILE_PARTS) for bh in range(2)]
            tbuf[j, n] = jnp.concatenate(rows, axis=0).T

    def hand_out(j, begin, end):
        for n in range(begin, end):
            to = core * CHIPS + n
            block = tbuf.at[j, :, pl.ds(n * d.out_rows, d.out_rows), :]

            @pl.when(to != me)
            def _():
                remote(block, gbuf.at[j, slot], k_send.at[j], k_recv.at[j], to).start()

            @pl.when(to == me)
            def _():
                gbuf[j, slot] = block[...]

    sends_self = me // CHIPS == core
    lanes = lax.broadcasted_iota(jnp.int32, (d.out_rows, d.wide), 1) // d.slab

    def put_out(j, finish=None):
        @pl.when(sends_self)
        def _():
            some = gbuf.at[j, pl.ds(0, CHIPS - 1)]
            remote(some, some, k_send.at[j], k_recv.at[j], me).wait()

        @pl.when(jnp.logical_not(sends_self))
        def _():
            remote(gbuf.at[j], gbuf.at[j], k_send.at[j], k_recv.at[j], me).wait()

        for ct in range(CHIPS // TILE_PARTS):
            for qt in range(d.pair // TILE_PARTS):
                src = [gbuf[j, ct * TILE_PARTS + c, qt] for c in range(TILE_PARTS)]
                if finish is not None:
                    src = [finish(x, gbuf[j - 1, ct * TILE_PARTS + c, qt], ct * TILE_PARTS + c) for c, x in enumerate(src)]
                for q in range(TILE_PARTS):
                    tile = jnp.zeros((d.out_rows, d.wide), jnp.float32)
                    for c in range(TILE_PARTS):
                        shift = (c - q) % TILE_PARTS * d.slab
                        moved = pltpu.roll(src[c], shift, 1) if shift else src[c]
                        tile = jnp.where(lanes == c, moved, tile)
                    tbuf[j, ct, pl.ds(qt * TILE_PARTS + q, d.out_rows, stride=d.pair), :] = tile
            pltpu.make_async_copy(tbuf.at[j, ct], out.at[j, :, pl.ds(ct * d.wide, d.wide)], o_sem.at[j, ct]).start()

    def step(j, carried):
        beta_prev = carried[0]
        sig[...] = jnp.zeros_like(sig)

        def slot_step(t, carry):
            done_right = sum((t > r).astype(jnp.int32) for r in RIGHT_SLOTS)
            done_left = t - done_right
            is_right = sum((t == r).astype(jnp.int32) for r in RIGHT_SLOTS)
            for four in range(0, len(SLOTS), 4):
                @pl.when((t >= four) & (t < four + 4))
                def _():
                    for at in range(four, four + 4):
                        if not SLOTS[at]:
                            continue

                        @pl.when(t == at)
                        def _():
                            for kind, i, p in SLOTS[at]:
                                act(kind, i, p, j)

            @pl.when(is_right == 1)
            def _():
                right_of_piece(done_right // QUARTERS, done_right % QUARTERS)

            @pl.when(is_right == 0)
            def _():
                left_products(done_left // GROUPS, done_left % GROUPS)
            return carry

        @pl.when(j == 0)
        def _():
            lax.fori_loop(0, GROUPS, first_right, 0)
            l_event(4)
            lax.fori_loop(0, GROUPS, first_group, 0)

        @pl.when(j > 0)
        def _():
            lax.fori_loop(0, len(SLOTS), slot_step, 0)
            for p in range(PIECES):
                sent = uv.at[p // QUARTERS, pl.ds(0, 2), pl.ds(0, 15 * d.slab), :]
                remote(sent, sent, u_send.at[p], u_recv.at[p, 0], me).wait_send()

        other = sig.at[:, pl.ds(d.half, d.half)]
        to_other = remote(other, part, p_send, p_recv, partner)
        to_other.start()
        to_other.wait()
        s = sig[:, :d.half] + part[...]
        v = vcur[...]
        w = s - beta_prev * vprev[...]
        sv = jnp.sum(s * v, keepdims=True)
        wv_sum = jnp.sum(w * v, keepdims=True)
        vv = jnp.sum(v * v, keepdims=True)
        guess = jnp.where(vv > 0.0, wv_sum / jnp.where(vv > 0.0, vv, 1.0), 0.0)
        t = w - guess * v
        sig[:, :d.half] = t
        tt = jnp.sum(t * t, keepdims=True)
        tv = jnp.sum(t * v, keepdims=True)
        at_lane = lax.broadcasted_iota(jnp.int32, (1, 128), 1)
        line = jnp.zeros((1, 128), jnp.float32)
        for n, value in enumerate((sv, vv, tt, tv, guess)):
            line = jnp.where(at_lane == n, value, line)
        scs[...] = line
        scr[me] = line

        def tell(n, carry):
            remote(scs, scr.at[me], s_send, s_recv, (me + n) % DEVS).start()
            return carry

        lax.fori_loop(1, DEVS, tell, 0)

        @pl.when(j > 0)
        def _():
            hand_out(j - 1, RESULT_EARLY, CHIPS)

        @pl.when(j == LANCZOS_STEPS - 1)
        def _():
            turn_result(LANCZOS_STEPS - 1, sig)
            hand_out(LANCZOS_STEPS - 1, 0, CHIPS)

        heard = scr.at[pl.ds(0, DEVS - 1)]
        remote(heard, heard, s_send, s_recv, me).wait()
        told = scr[:, 0, :]
        alpha = jnp.sum(told[:, 0:1], axis=0, keepdims=True) / d.vec_size
        off = alpha - told[:, 4:5]
        square = told[:, 2:3] - 2.0 * off * told[:, 3:4] + off * off * told[:, 1:2]
        beta = jnp.sqrt(jnp.sum(square, axis=0, keepdims=True) / d.vec_size)
        vnew = (sig[:, :d.half] - (alpha - guess) * vcur[...]) / beta
        vprev[...] = vcur[...]
        vcur[...] = vnew
        vb = vnew.astype(jnp.bfloat16)

        @pl.when(j < LANCZOS_STEPS - 1)
        def _():
            for ch in range(CHUNKS):
                for bh in range(2):
                    at = pl.ds(pl.multiple_of(slot * d.slab + bh * d.sub, d.sub), d.sub)
                    for q in range(d.pair):
                        uv[ch, q // 2, at, q % 2 * d.chunk:(q % 2 + 1) * d.chunk] = \
                            vb[(bh * d.pair + q) * d.sub:(bh * d.pair + q + 1) * d.sub, ch * d.chunk:(ch + 1) * d.chunk]
        alphas[j] = alpha[0, 0]
        betas[j] = beta[0, 0]
        return beta, alpha


    zero = jnp.zeros((1, 1), jnp.float32)
    last_beta, last_alpha = lax.fori_loop(0, LANCZOS_STEPS, step, (zero, zero))

    for n, part in enumerate((lv.at[0, pl.ds(0, 15), :, 0], lv.at[1, pl.ds(0, 15), :, 0, :, pl.ds(edge, d.bond - edge)],
                              lv.at[0, pl.ds(0, 15), :, 0, :, pl.ds(0, d.half)], lv.at[1, pl.ds(0, 15), :, 0, :, pl.ds(edge, d.half - edge)])):
        remote(part, part, l_send.at[n], l_recv.at[n, 0], me).wait_send()
    swapped = lv.at[:, pl.ds(0, 15), :, 0, :, pl.ds(d.half, d.half)]
    remote(swapped, swapped, f_send, f_recv.at[0], me).wait_send()
    for ch in range(CHUNKS):
        for h in range(2):
            theirs = left.at[:, pl.ds(0, d.chunk), pl.ds(0, d.half)]
            remote(theirs, lv.at[ch, slot, core, :, :, pl.ds(h * d.half, d.half)], d2d_sem.at[ch, h], d2d_recv.at[ch, h], partner).wait_send()
    put_out(LANCZOS_STEPS - 2)

    def finish(block, before, s):
        owner = device(s % 4, s // 4 % 2, s // 8, me // CHIPS)
        return (block - (last_alpha - scr[owner][:, 4:5]) * before) / last_beta

    put_out(LANCZOS_STEPS - 1, finish)
    for j in range(LANCZOS_STEPS):
        for c in range(d.bond // d.wide):
            pltpu.make_async_copy(tbuf.at[j, c], out.at[j, :, pl.ds(c * d.wide, d.wide)], o_sem.at[j, c]).wait()


def solution(mesh):
    def device_body(wavefunction, left_loc, pair_loc, right_loc, flag_loc):
        bond, pair = wavefunction.shape[0], wavefunction.shape[1]
        d = Dims(bond, pair, left_loc.shape[0])
        bf16, f32 = jnp.bfloat16, jnp.float32
        dma = pltpu.SemaphoreType.DMA
        any_space = pl.BlockSpec(memory_space=pl.ANY)
        smem = pl.BlockSpec(memory_space=pltpu.SMEM)
        scalars = jax.ShapeDtypeStruct((LANCZOS_STEPS,), f32)
        later, first, alphas, betas = pl.pallas_call(
            functools.partial(lanczos_kernel, d),
            out_shape=(jax.ShapeDtypeStruct((LANCZOS_STEPS, d.out_rows * pair, bond), f32),
                       jax.ShapeDtypeStruct((d.out_rows * pair, bond), f32), scalars, scalars),
            in_specs=[any_space] * 3 + [pl.BlockSpec(memory_space=pltpu.VMEM), smem],
            out_specs=(any_space, any_space, smem, smem),
            scratch_shapes=[
                pltpu.VMEM((CHUNKS, CHIPS, CORES, d.terms_dev, d.chunk, bond), bf16),
                pltpu.VMEM((CHIPS, CORES, d.terms_dev, d.slab, bond), bf16),
                pltpu.VMEM((d.terms_dev, bond, bond), bf16),
                pltpu.VMEM((CHIPS, CORES, d.terms_dev, pair, d.prod), bf16),
                pltpu.VMEM((CHIPS, CORES, d.terms_dev, d.prod, d.prod), bf16),
                pltpu.VMEM((CHUNKS, pair // 2, bond, 2 * d.chunk), bf16),
                pltpu.VMEM((d.lane_tiles, d.half * pair, d.lane), f32),
                pltpu.VMEM((CHIPS * CORES * d.terms_dev, pair, d.sub, 2 * d.chunk), bf16),
                pltpu.VMEM((d.rows, d.group_terms * d.chunk), bf16),
                pltpu.VMEM((d.rows, bond), f32),
                pltpu.VMEM((d.rows, d.half), f32),
                pltpu.VMEM((d.rows, d.half), f32),
                pltpu.VMEM((d.rows, d.half), f32),
                pltpu.VMEM((LANCZOS_STEPS, bond // d.wide, d.half, d.wide), f32),
                pltpu.VMEM((LANCZOS_STEPS, CHIPS, bond // d.wide, d.out_rows, d.wide), f32),
                pltpu.VMEM((1, 128), f32),
                pltpu.VMEM((DEVS, 1, 128), f32),
                pltpu.VMEM((2, 8, 128), f32),
                dma((3, 2)), dma((8, d.lane_tiles)), dma((CHUNKS, 2)), dma((CHUNKS, 2)), dma((2,)), dma((2,)), dma((2,)), dma((2,)),
                dma((4,)), dma((4, CHIPS)), dma, dma((CHIPS,)), dma((PIECES,)), dma((PIECES, CHIPS)),
                dma, dma, dma, dma, dma((LANCZOS_STEPS,)), dma((LANCZOS_STEPS,)), dma, dma, dma((LANCZOS_STEPS, bond // d.wide)), dma((bond // d.wide,)),
            ],
            compiler_params=pltpu.CompilerParams(has_side_effects=True, collective_id=0, vmem_limit_bytes=67043328),
            name='lanczos',
        )(wavefunction.reshape(bond * pair, bond), left_loc, right_loc, pair_loc, flag_loc)
        krylov = jnp.concatenate([first[None], later])
        return krylov.reshape(LANCZOS_STEPS + 1, d.out_rows, pair, bond), alphas, betas

    return jax.shard_map(device_body, mesh=mesh, in_specs=(P(), P(AXIS_NAME), P(AXIS_NAME), P(AXIS_NAME), P(AXIS_NAME)),
                         out_specs=(P(None, AXIS_NAME), P(), P()), check_vma=False)
```

```python
import functools

import jax
import jax.numpy as jnp
from jax import lax
from jax.experimental import pallas as pl
from jax.experimental.pallas import tpu as pltpu
from jax.sharding import PartitionSpec as P

LANCZOS_STEPS = 6
AXIS_NAME = 'terms'
MESH = pl.DeviceIdType.MESH

CHIPS = 16
CORES = 2
DEVS = 32
CHUNKS = 2
GROUPS = 4
TILE_PARTS = 4
QUARTERS = 4
PIECES = CHUNKS * QUARTERS

ALONG, ACROSS, FROM_COLUMN, FROM_SECOND, THIRD, DIAGONAL, RESULT, RESULT_OUT, RESULT_PUT = range(9)
RIGHT_SLOTS = (0, 1, 2, 3, 8, 9, 10, 11)
SLOTS = (
    ((0, 1, 0), (0, 1, 1), (1, 0, 2), (0, 2, 0), (1, 0, 5), (1, 0, 3), (1, 0, 6), (1, 0, 0), (0, 3, 0), (3, 0, 2), (0, 2, 1), (0, 1, 3), (1, 0, 4), (0, 3, 1), (1, 0, 7), (0, 1, 2), (1, 0, 1), (0, 3, 3), (2, 1, 0), (2, 2, 0), (0, 2, 3), (0, 3, 2), (2, 1, 1), (3, 0, 0), (2, 3, 0), (3, 1, 0), (2, 2, 1), (0, 2, 2), (0, 1, 4), (3, 0, 1), (2, 1, 3), (3, 2, 0), (2, 3, 1), (2, 2, 2), (2, 2, 3), (2, 1, 2), (4, 0, 0), (0, 2, 5), (0, 3, 4), (0, 2, 4), (0, 1, 5), (0, 1, 6), (0, 1, 7), (3, 3, 0), (2, 3, 3), (3, 1, 1), (3, 2, 1), (0, 2, 6), (2, 3, 2), (4, 0, 1), (3, 3, 1), (0, 3, 6), (3, 2, 2), (3, 1, 2), (0, 3, 5), (0, 2, 7), (0, 3, 7), (3, 2, 3), (3, 3, 2), (3, 0, 3), (5, 0, 0), (3, 3, 3), (4, 0, 3), (3, 1, 3), (3, 0, 4),),
    ((6, 0, 0), (2, 2, 4), (5, 0, 1), (3, 0, 6), (2, 1, 4), (4, 0, 2),),
    ((2, 2, 6), (5, 0, 2), (2, 1, 6),),
    ((2, 2, 5), (5, 0, 3), (3, 2, 4), (2, 3, 4),),
    ((2, 1, 5), (3, 0, 5), (3, 1, 4),),
    ((2, 3, 5), (3, 2, 5), (2, 3, 6),),
    ((2, 2, 7), (3, 3, 4), (2, 1, 7), (3, 1, 5), (8, 0, 0),),
    ((3, 3, 5), (2, 3, 7), (3, 2, 6), (3, 1, 6), (3, 3, 6),),
    ((3, 0, 7), (3, 1, 7), (3, 2, 7), (4, 0, 5), (5, 0, 4), (4, 0, 4),),
    ((3, 3, 7), (5, 0, 5),),
    ((4, 0, 6), (5, 0, 6),),
    ((4, 0, 7), (5, 0, 7), (7, 0, 0),),
    (),
    (),
    (),
    (),
)
RESULT_EARLY = 5


class Dims:
    def __init__(self, bond, pair, terms_dev):
        self.bond = bond
        self.pair = pair
        self.terms_dev = terms_dev
        self.slab = bond // CHIPS
        self.sub = self.slab // 2
        self.half = bond // CORES
        self.chunk = self.half // CHUNKS
        self.rows = self.slab * pair
        self.prod = self.sub * pair
        self.out_rows = bond // DEVS
        self.group_terms = 4 * CORES * terms_dev
        self.vec_size = bond * pair * bond
        self.lane = min(bond, 128)
        self.wide = TILE_PARTS * self.slab
        self.lane_tiles = bond // self.lane


def lanczos_kernel(d, psi, left, right, pair_ops, flags, out, first, alphas, betas, lv, rv, rs, wv, kw, uv, ps, yst, zst, sig, part, vcur, vprev, tbuf, gbuf,
                   scs, scr, nbuf,
                   loc_sem, psi_sem, d2d_sem, d2d_recv, rw_send, rw_recv, fw_send, fw_recv, l_send, l_recv, f_send, f_recv, u_send, u_recv,
                   p_send, p_recv, s_send, s_recv, k_send, k_recv, n_send, n_recv, o_sem, first_sem):
    me = lax.axis_index(AXIS_NAME)
    core = me % 2
    xpos = (me // 2) % 2
    ypos = (me // 4) % 2
    zpos = me // 8

    def device(z, y, x, c):
        return ((z * 2 + y) * 2 + x) * 2 + c

    def chip_slot(z, y, x):
        return (x * 2 + y) * 4 + z

    partner = device(zpos, ypos, xpos, 1 - core)
    slot = chip_slot(zpos, ypos, xpos)
    zs = (zpos, zpos + 1 - 2 * (zpos % 2), (zpos + 2) % 4, 3 - zpos)
    inner = (zpos + 1) // 2 % 2
    zn = (zpos, (1 - inner) * (zpos + 1 - zpos // 3 * 2) + inner * (zpos - 1), (1 - inner) * ((zpos + 2) % 4) + inner * (zpos + 1),
          (1 - inner) * (3 - zpos) + inner * ((zpos + 2) % 4))
    y_two = ypos + (1 - core) * (1 - 2 * ypos)
    x_two = xpos + core * (1 - 2 * xpos)
    y_three = ypos + core * (1 - 2 * ypos)
    x_three = xpos + (1 - core) * (1 - 2 * xpos)
    two = device(zpos, y_two, x_two, core)
    three = device(zpos, y_three, x_three, core)

    def remote(src, dst, send, recv, dev):
        return pltpu.make_async_remote_copy(src_ref=src, dst_ref=dst, send_sem=send, recv_sem=recv, device_id=(dev,), device_id_type=MESH)

    class Gather:
        def __init__(self, block, send, recv):
            self.block, self.send_sem, self.recv_sem = block, send, recv

        def send(self, which, dev):
            remote(self.block(which), self.block(which), self.send_sem, self.recv_sem(which), dev).start()

        def wait(self, which):
            remote(self.block(which), self.block(which), self.send_sem, self.recv_sem(which), me).wait_recv()

        def own_along(self):
            for i in (1, 2, 3):
                self.send(slot, device(zs[i], ypos, xpos, core))

        def own_across(self):
            self.send(slot, three)
            self.send(slot, two)

        def event(self, n):
            i = (n + 1) // 2
            if n % 2:
                which = chip_slot(zs[i], ypos, xpos)
                self.wait(which)
                self.send(which, three)
                self.send(which, two)
            else:
                which = chip_slot(zs[i], y_two, x_two)
                self.wait(which)
                self.send(which, three)

        def last(self, diagonal):
            for i in range(4):
                self.wait(chip_slot(zs[i], 1 - ypos, 1 - xpos) if diagonal else chip_slot(zs[i], y_three, x_three))

    edge = d.chunk
    l_parts = (
        (lambda s: lv.at[0, s, :, core], 0),
        (lambda s: lv.at[1, s, :, core, :, pl.ds(edge, d.bond - edge)], 1),
        (lambda s: lv.at[0, s, :, 1 - core, :, pl.ds(0, d.half)], 2),
        (lambda s: lv.at[1, s, :, 1 - core, :, pl.ds(edge, d.half - edge)], 3),
    )
    l_gathers = [Gather(block, l_send.at[n], lambda s, n=n: l_recv.at[n, s]) for block, n in l_parts]

    def l_swap(s, term):
        part = lv.at[:, s, :, term, :, pl.ds(d.half, d.half)]
        return remote(part, part, f_send, f_recv.at[s], partner)

    def l_event(n):
        i = (n + 1) // 2
        for g in l_gathers:
            g.event(n)
        l_swap(chip_slot(zs[i], ypos, xpos) if n % 2 else chip_slot(zs[i], y_two, x_two), core).start()

    def l_last(diagonal):
        for i in range(4):
            which = chip_slot(zs[i], 1 - ypos, 1 - xpos) if diagonal else chip_slot(zs[i], y_three, x_three)
            for g in l_gathers:
                g.wait(which)
            l_swap(which, core).start()

    def l_fill(s):
        @pl.when(s != slot)
        def _():
            l_swap(s, 1 - core).wait_recv()
            for c in range(CORES):
                tile = lv[:, s, c, 1 - core, :, d.half:].reshape(d.half, d.half).T
                lv[:, s, c, 1 - core, :, d.half:] = tile.reshape(CHUNKS, d.chunk, d.half)
                for t in range(d.terms_dev):
                    lv[1, s, c, t, :, :edge] = lv[0, s, c, t, :, edge:d.half].T

    def l_along():
        for i in (1, 2, 3):
            for g in l_gathers:
                g.send(slot, device(zs[i], ypos, xpos, core))

    def u_block(p):
        return lambda s: uv.at[p // QUARTERS, pl.ds(p % QUARTERS * 2, 2), pl.ds(pl.multiple_of(s * d.slab, d.slab), d.slab), :]

    u_gathers = [Gather(u_block(p), u_send.at[p], lambda s, p=p: u_recv.at[p, s]) for p in range(PIECES)]

    def act(kind, i, p, j):
        g = u_gathers[p]
        if kind == ALONG:
            g.send(slot, device(zn[i], ypos, xpos, core))
        elif kind == ACROSS:
            g.own_across()
        elif kind == FROM_COLUMN:
            which = chip_slot(zn[i], ypos, xpos)
            g.wait(which)
            g.send(which, three)
            g.send(which, two)
        elif kind == FROM_SECOND:
            which = chip_slot(zn[i], y_two, x_two)
            g.wait(which)
            g.send(which, three)
        elif kind == THIRD:
            g.last(False)
        elif kind == DIAGONAL:
            g.last(True)
        elif kind == RESULT:
            turn_result(j - 1, vcur)
        elif kind == RESULT_OUT:
            hand_out(j - 1, 0, RESULT_EARLY)
        elif kind == RESULT_PUT:
            @pl.when(j > 1)
            def _():
                put_out(j - 2)

    all_right = pltpu.make_async_copy(right, rs, loc_sem.at[2, 0])
    all_right.start()

    barrier = pltpu.get_barrier_semaphore()

    def knock(n, carry):
        pl.semaphore_signal(barrier, inc=1, device_id=((me + n) % DEVS,), device_id_type=MESH)
        return carry

    lax.fori_loop(1, DEVS, knock, 0)

    for ch in range(CHUNKS):
        for h in range(2):
            mine = left.at[:, pl.ds(pl.multiple_of(core * d.half + ch * d.chunk, d.chunk), d.chunk),
                           pl.ds(pl.multiple_of((core + h) % 2 * d.half, d.half), d.half)]
            pltpu.make_async_copy(mine, lv.at[ch, slot, core, :, :, pl.ds(h * d.half, d.half)], loc_sem.at[ch, h]).start()

    psi_rows = d.half * d.pair // 8
    psi_copies = [pltpu.make_async_copy(psi.at[pl.ds(pl.multiple_of(core * d.half * d.pair + n * psi_rows, psi_rows), psi_rows),
                                               pl.ds(c * d.lane, d.lane)],
                                        ps.at[c, pl.ds(n * psi_rows, psi_rows), :], psi_sem.at[n, c])
                  for n in range(8) for c in range(d.lane_tiles)]
    for copy in psi_copies:
        copy.start()

    first_rows = d.out_rows * d.pair
    first_copies = [pltpu.make_async_copy(psi.at[pl.ds(pl.multiple_of(me * first_rows, first_rows), first_rows), pl.ds(c * d.wide, d.wide)],
                                          tbuf.at[LANCZOS_STEPS - 1, c], first_sem.at[c]) for c in range(d.bond // d.wide)]
    for copy in first_copies:
        copy.start()

    spread = (lax.broadcasted_iota(jnp.int32, (d.pair, d.prod), 1) // d.sub == lax.broadcasted_iota(jnp.int32, (d.pair, d.prod), 0))
    spread = spread.astype(jnp.float32).astype(jnp.bfloat16)
    for t in range(d.terms_dev):
        wv[slot, core, t] = jnp.dot(pair_ops[t], spread, preferred_element_type=jnp.float32).astype(jnp.bfloat16)
    all_right.wait()
    some_rows = d.bond // 8

    def one_sided(i, carry):
        at = pl.ds(pl.multiple_of(i * some_rows, some_rows), some_rows)
        row = lax.broadcasted_iota(jnp.int32, (some_rows, d.bond), 0) + i * some_rows
        one = jnp.where(row == lax.broadcasted_iota(jnp.int32, (some_rows, d.bond), 1), 1.0, 0.0)
        for t in range(d.terms_dev):
            rs[t, at, :] = jnp.where(flags[t] == 1, rs[t, at, :].astype(jnp.float32), one).astype(jnp.bfloat16)
        return carry

    lax.fori_loop(0, 8, one_sided, 0)

    def right_rows(s):
        return rs.at[:, pl.ds(pl.multiple_of(s * d.slab, d.slab), d.slab), :]

    rv[slot, core] = rs[:, pl.ds(pl.multiple_of(slot * d.slab, d.slab), d.slab), :]

    pl.semaphore_wait(barrier, DEVS - 1)
    for ch in range(CHUNKS):
        for h in range(2):
            theirs = left.at[:, pl.ds(pl.multiple_of((1 - core) * d.half + ch * d.chunk, d.chunk), d.chunk),
                             pl.ds(pl.multiple_of((1 - core + h) % 2 * d.half, d.half), d.half)]
            remote(theirs, lv.at[ch, slot, core, :, :, pl.ds(h * d.half, d.half)], d2d_sem.at[ch, h], d2d_recv.at[ch, h], partner).start()
    for n in range(1, CHIPS):
        chip = (me // 2 + n) % CHIPS
        to = chip_slot(chip // 4, chip // 2 % 2, chip % 2)
        remote(right_rows(to), rv.at[slot, core], rw_send.at[0], rw_recv.at[0], chip * 2 + core).start()
        remote(wv.at[slot, core], wv.at[slot, core], rw_send.at[1], rw_recv.at[1], chip * 2 + core).start()

    for ch in range(CHUNKS):
        for h in range(2):
            pltpu.make_async_copy(lv.at[ch, slot, core, :, :, pl.ds(h * d.half, d.half)], lv.at[ch, slot, core, :, :, pl.ds(h * d.half, d.half)], loc_sem.at[ch, h]).wait()
            back = remote(lv.at[ch, slot, 1 - core, :, :, pl.ds(h * d.half, d.half)], lv.at[ch, slot, 1 - core, :, :, pl.ds(h * d.half, d.half)], d2d_sem.at[ch, h], d2d_recv.at[ch, h], partner)
            back.wait_recv()
    l_along()
    for g in l_gathers:
        g.own_across()

    total = jnp.zeros((8, d.lane), jnp.float32)
    for n in range(8):
        for copy in psi_copies[n * d.lane_tiles:(n + 1) * d.lane_tiles]:
            copy.wait()

        def add_rows(i, acc, n=n):
            x = ps[:, pl.ds(pl.multiple_of(n * psi_rows + i * (psi_rows // 8), 8), psi_rows // 8), :]
            return acc + jnp.sum((x * x).reshape(d.lane_tiles * psi_rows // 64, 8, d.lane), axis=0)

        total = lax.fori_loop(0, 8, add_rows, total)
    nbuf[0] = jnp.broadcast_to(jnp.sum(total, keepdims=True), (8, 128))
    to_partner = remote(nbuf.at[0], nbuf.at[1], n_send, n_recv, partner)
    to_partner.start()
    to_partner.wait()
    norm = jnp.sqrt((nbuf[0] + nbuf[1])[0:1, :] / d.vec_size)
    norm_one = norm[:, 0:1]
    for copy in first_copies:
        copy.wait()
    tbuf[LANCZOS_STEPS - 1] = tbuf[LANCZOS_STEPS - 1] / norm_one[None]
    first_out = [pltpu.make_async_copy(tbuf.at[LANCZOS_STEPS - 1, c], first.at[:, pl.ds(c * d.wide, d.wide)], first_sem.at[c])
                 for c in range(d.bond // d.wide)]
    for copy in first_out:
        copy.start()

    def place(q):
        tiles = [(ps[c, pl.ds(q, d.half, stride=d.pair), :] / norm_one).T for c in range(d.lane_tiles)]
        xt = jnp.concatenate(tiles, axis=0)
        vprev[...] = xt
        return xt.astype(jnp.bfloat16)

    def start_vector(qb, carry):
        for q2 in range(2):
            q = qb * 2 + q2
            xb = place(q)
            for ch in range(CHUNKS):
                uv[ch, qb, :, q2 * d.chunk:(q2 + 1) * d.chunk] = xb[:, ch * d.chunk:(ch + 1) * d.chunk]
            for bh in range(2):
                rows = vprev[pl.ds(pl.multiple_of(slot * d.slab + bh * d.sub, d.sub), d.sub), :]
                vcur[pl.ds(pl.multiple_of((bh * d.pair + q) * d.sub, d.sub), d.sub), :] = rows
        return carry

    lax.fori_loop(0, d.pair // 4, start_vector, 0)
    fifteen = rv.at[pl.ds(0, CHIPS - 1), 0]
    fifteen_w = wv.at[pl.ds(0, CHIPS - 1), 0]
    remote(fifteen, fifteen, rw_send.at[0], rw_recv.at[0], me).wait()
    remote(fifteen_w, fifteen_w, rw_send.at[1], rw_recv.at[1], me).wait()
    fw_right = remote(rv.at[:, core], rv.at[:, core], fw_send.at[0], fw_recv.at[0], partner)
    fw_pair = remote(wv.at[:, core], wv.at[:, core], fw_send.at[1], fw_recv.at[1], partner)
    fw_right.start()
    fw_pair.start()
    l_event(0)
    l_event(1)
    lax.fori_loop(d.pair // 4, d.pair // 2, start_vector, 0)
    l_event(2)
    l_event(3)
    fw_right.wait()
    fw_pair.wait()
    lane = lax.broadcasted_iota(jnp.int32, (d.sub, d.prod), 1)
    row = lax.broadcasted_iota(jnp.int32, (d.sub, d.prod), 0)
    diagonal = lane % d.sub == row

    def spread_pair(s, carry):
        for c in range(2):
            for t in range(d.terms_dev):
                w = wv[s, c, t].astype(jnp.float32)
                for q in range(d.pair):
                    full = jnp.where(diagonal, jnp.broadcast_to(w[q:q + 1, :], (d.sub, d.prod)), 0.0)
                    kw[s, c, t, q * d.sub:(q + 1) * d.sub, :] = full.astype(jnp.bfloat16)
        return carry

    lax.fori_loop(0, CHIPS, spread_pair, 0)
    vprev[...] = jnp.zeros_like(vprev)
    for copy in first_out:
        copy.wait()

    def right_product(grp, ch, qb, to):
        r_all = rv[pl.ds(grp * 4, 4)].reshape(d.group_terms * d.slab, d.bond)
        y = jnp.dot(r_all, uv[ch, qb], preferred_element_type=jnp.float32).astype(jnp.bfloat16)
        y = y.reshape(d.group_terms, 2, d.sub, 2 * d.chunk)
        for q2 in range(2):
            for bh in range(2):
                yst[pl.ds(to * d.group_terms, d.group_terms), qb * 2 + q2, :, bh * d.chunk:(bh + 1) * d.chunk] = \
                    y[:, bh, :, q2 * d.chunk:(q2 + 1) * d.chunk]

    def right_of_piece(ch, part):
        for qb in range(2):
            for grp in range(GROUPS):
                right_product(grp, ch, part * 2 + qb, grp)

    def right_of_group(grp, ch, to):
        for qb in range(d.pair // 2):
            right_product(grp, ch, qb, to)

    def left_products(ch, grp, at=None):
        for k in range(d.group_terms):
            w = kw[grp * 4 + k // 4, k // 2 % 2, k % 2]
            z = jnp.dot(w, yst[(grp if at is None else at) * d.group_terms + k].reshape(d.prod, 2 * d.chunk), preferred_element_type=jnp.float32).astype(jnp.bfloat16)
            for bh in range(2):
                zst[bh * d.prod:(bh + 1) * d.prod, k * d.chunk:(k + 1) * d.chunk] = z[:, bh * d.chunk:(bh + 1) * d.chunk]
        l_all = lv[ch, pl.ds(grp * 4, 4)].reshape(d.group_terms * d.chunk, d.bond)
        sig[...] += jnp.dot(zst[...], l_all, preferred_element_type=jnp.float32)

    def first_right(grp, carry):
        right_of_group(grp, 0, grp)

        @pl.when(grp == 1)
        def _():
            l_event(4)
        return carry

    def first_group(n, carry):
        own, third = xpos * 2 + ypos, x_three * 2 + y_three
        grp = jnp.where(n == 0, own, jnp.where(n == 1, x_two * 2 + y_two, jnp.where(n == 2, third, 3 - own)))
        spare = jnp.where(n == 3, own, grp)

        @pl.when(n == 1)
        def _():
            l_event(6)
            l_last(False)

        @pl.when(n == 3)
        def _():
            right_of_group(grp, 1, spare)
            l_last(True)

        def fill(z, carry):
            l_fill(grp * 4 + z)
            return carry

        lax.fori_loop(0, 4, fill, 0)

        def chunk_products(ch, carry):
            left_products(ch, grp, (1 - ch) * grp + ch * spare)

            @pl.when((ch == 0) & (n < 3))
            def _():
                right_of_group(grp, 1, spare)
            return carry

        lax.fori_loop(0, CHUNKS, chunk_products, 0)
        return carry

    def turn_result(j, vector):
        for n in range(d.pair // TILE_PARTS):
            rows = [vector[(bh * d.pair + q) * d.sub:(bh * d.pair + q + 1) * d.sub, :d.half]
                    for q in range(n * TILE_PARTS, (n + 1) * TILE_PARTS) for bh in range(2)]
            tbuf[j, n] = jnp.concatenate(rows, axis=0).T

    def hand_out(j, begin, end):
        for n in range(begin, end):
            to = core * CHIPS + n
            block = tbuf.at[j, :, pl.ds(n * d.out_rows, d.out_rows), :]

            @pl.when(to != me)
            def _():
                remote(block, gbuf.at[j, slot], k_send.at[j], k_recv.at[j], to).start()

            @pl.when(to == me)
            def _():
                gbuf[j, slot] = block[...]

    sends_self = me // CHIPS == core
    lanes = lax.broadcasted_iota(jnp.int32, (d.out_rows, d.wide), 1) // d.slab

    def put_out(j, finish=None):
        @pl.when(sends_self)
        def _():
            some = gbuf.at[j, pl.ds(0, CHIPS - 1)]
            remote(some, some, k_send.at[j], k_recv.at[j], me).wait()

        @pl.when(jnp.logical_not(sends_self))
        def _():
            remote(gbuf.at[j], gbuf.at[j], k_send.at[j], k_recv.at[j], me).wait()

        for ct in range(CHIPS // TILE_PARTS):
            for qt in range(d.pair // TILE_PARTS):
                src = [gbuf[j, ct * TILE_PARTS + c, qt] for c in range(TILE_PARTS)]
                if finish is not None:
                    src = [finish(x, gbuf[j - 1, ct * TILE_PARTS + c, qt], ct * TILE_PARTS + c) for c, x in enumerate(src)]
                for q in range(TILE_PARTS):
                    tile = jnp.zeros((d.out_rows, d.wide), jnp.float32)
                    for c in range(TILE_PARTS):
                        shift = (c - q) % TILE_PARTS * d.slab
                        moved = pltpu.roll(src[c], shift, 1) if shift else src[c]
                        tile = jnp.where(lanes == c, moved, tile)
                    tbuf[j, ct, pl.ds(qt * TILE_PARTS + q, d.out_rows, stride=d.pair), :] = tile
            pltpu.make_async_copy(tbuf.at[j, ct], out.at[j, :, pl.ds(ct * d.wide, d.wide)], o_sem.at[j, ct]).start()

    def step(j, carried):
        beta_prev = carried[0]
        sig[...] = jnp.zeros_like(sig)

        def slot_step(t, carry):
            done_right = sum((t > r).astype(jnp.int32) for r in RIGHT_SLOTS)
            done_left = t - done_right
            is_right = sum((t == r).astype(jnp.int32) for r in RIGHT_SLOTS)
            for four in range(0, len(SLOTS), 4):
                @pl.when((t >= four) & (t < four + 4))
                def _():
                    for at in range(four, four + 4):
                        if not SLOTS[at]:
                            continue

                        @pl.when(t == at)
                        def _():
                            for kind, i, p in SLOTS[at]:
                                act(kind, i, p, j)

            @pl.when(is_right == 1)
            def _():
                right_of_piece(done_right // QUARTERS, done_right % QUARTERS)

            @pl.when(is_right == 0)
            def _():
                left_products(done_left // GROUPS, done_left % GROUPS)
            return carry

        @pl.when(j == 0)
        def _():
            lax.fori_loop(0, GROUPS, first_right, 0)
            l_event(5)
            lax.fori_loop(0, GROUPS, first_group, 0)

        @pl.when(j > 0)
        def _():
            lax.fori_loop(0, len(SLOTS), slot_step, 0)
            for p in range(PIECES):
                sent = uv.at[p // QUARTERS, pl.ds(0, 2), pl.ds(0, 15 * d.slab), :]
                remote(sent, sent, u_send.at[p], u_recv.at[p, 0], me).wait_send()

        other = sig.at[:, pl.ds(d.half, d.half)]
        to_other = remote(other, part, p_send, p_recv, partner)
        to_other.start()
        to_other.wait()
        s = sig[:, :d.half] + part[...]
        v = vcur[...]
        w = s - beta_prev * vprev[...]
        sv = jnp.sum(s * v, keepdims=True)
        wv_sum = jnp.sum(w * v, keepdims=True)
        vv = jnp.sum(v * v, keepdims=True)
        guess = jnp.where(vv > 0.0, wv_sum / jnp.where(vv > 0.0, vv, 1.0), 0.0)
        t = w - guess * v
        sig[:, :d.half] = t
        tt = jnp.sum(t * t, keepdims=True)
        tv = jnp.sum(t * v, keepdims=True)
        at_lane = lax.broadcasted_iota(jnp.int32, (1, 128), 1)
        line = jnp.zeros((1, 128), jnp.float32)
        for n, value in enumerate((sv, vv, tt, tv, guess)):
            line = jnp.where(at_lane == n, value, line)
        scs[...] = line
        scr[me] = line

        def tell(n, carry):
            remote(scs, scr.at[me], s_send, s_recv, (me + n) % DEVS).start()
            return carry

        lax.fori_loop(1, DEVS, tell, 0)

        @pl.when(j > 0)
        def _():
            hand_out(j - 1, RESULT_EARLY, CHIPS)

        @pl.when(j == LANCZOS_STEPS - 1)
        def _():
            turn_result(LANCZOS_STEPS - 1, sig)
            hand_out(LANCZOS_STEPS - 1, 0, CHIPS)

        heard = scr.at[pl.ds(0, DEVS - 1)]
        remote(heard, heard, s_send, s_recv, me).wait()
        told = scr[:, 0, :]
        alpha = jnp.sum(told[:, 0:1], axis=0, keepdims=True) / d.vec_size
        off = alpha - told[:, 4:5]
        square = told[:, 2:3] - 2.0 * off * told[:, 3:4] + off * off * told[:, 1:2]
        beta = jnp.sqrt(jnp.sum(square, axis=0, keepdims=True) / d.vec_size)
        vnew = (sig[:, :d.half] - (alpha - guess) * vcur[...]) / beta
        vprev[...] = vcur[...]
        vcur[...] = vnew
        vb = vnew.astype(jnp.bfloat16)

        @pl.when(j < LANCZOS_STEPS - 1)
        def _():
            for ch in range(CHUNKS):
                for bh in range(2):
                    at = pl.ds(pl.multiple_of(slot * d.slab + bh * d.sub, d.sub), d.sub)
                    for q in range(d.pair):
                        uv[ch, q // 2, at, q % 2 * d.chunk:(q % 2 + 1) * d.chunk] = \
                            vb[(bh * d.pair + q) * d.sub:(bh * d.pair + q + 1) * d.sub, ch * d.chunk:(ch + 1) * d.chunk]
        alphas[j] = alpha[0, 0]
        betas[j] = beta[0, 0]
        return beta, alpha


    zero = jnp.zeros((1, 1), jnp.float32)
    last_beta, last_alpha = lax.fori_loop(0, LANCZOS_STEPS, step, (zero, zero))

    for n, part in enumerate((lv.at[0, pl.ds(0, 15), :, 0], lv.at[1, pl.ds(0, 15), :, 0, :, pl.ds(edge, d.bond - edge)],
                              lv.at[0, pl.ds(0, 15), :, 0, :, pl.ds(0, d.half)], lv.at[1, pl.ds(0, 15), :, 0, :, pl.ds(edge, d.half - edge)])):
        remote(part, part, l_send.at[n], l_recv.at[n, 0], me).wait_send()
    swapped = lv.at[:, pl.ds(0, 15), :, 0, :, pl.ds(d.half, d.half)]
    remote(swapped, swapped, f_send, f_recv.at[0], me).wait_send()
    for ch in range(CHUNKS):
        for h in range(2):
            theirs = left.at[:, pl.ds(0, d.chunk), pl.ds(0, d.half)]
            remote(theirs, lv.at[ch, slot, core, :, :, pl.ds(h * d.half, d.half)], d2d_sem.at[ch, h], d2d_recv.at[ch, h], partner).wait_send()
    put_out(LANCZOS_STEPS - 2)

    def finish(block, before, s):
        owner = device(s % 4, s // 4 % 2, s // 8, me // CHIPS)
        return (block - (last_alpha - scr[owner][:, 4:5]) * before) / last_beta

    put_out(LANCZOS_STEPS - 1, finish)
    for j in range(LANCZOS_STEPS):
        for c in range(d.bond // d.wide):
            pltpu.make_async_copy(tbuf.at[j, c], out.at[j, :, pl.ds(c * d.wide, d.wide)], o_sem.at[j, c]).wait()


def solution(mesh):
    def device_body(wavefunction, left_loc, pair_loc, right_loc, flag_loc):
        bond, pair = wavefunction.shape[0], wavefunction.shape[1]
        d = Dims(bond, pair, left_loc.shape[0])
        bf16, f32 = jnp.bfloat16, jnp.float32
        dma = pltpu.SemaphoreType.DMA
        any_space = pl.BlockSpec(memory_space=pl.ANY)
        smem = pl.BlockSpec(memory_space=pltpu.SMEM)
        scalars = jax.ShapeDtypeStruct((LANCZOS_STEPS,), f32)
        later, first, alphas, betas = pl.pallas_call(
            functools.partial(lanczos_kernel, d),
            out_shape=(jax.ShapeDtypeStruct((LANCZOS_STEPS, d.out_rows * pair, bond), f32),
                       jax.ShapeDtypeStruct((d.out_rows * pair, bond), f32), scalars, scalars),
            in_specs=[any_space] * 3 + [pl.BlockSpec(memory_space=pltpu.VMEM), smem],
            out_specs=(any_space, any_space, smem, smem),
            scratch_shapes=[
                pltpu.VMEM((CHUNKS, CHIPS, CORES, d.terms_dev, d.chunk, bond), bf16),
                pltpu.VMEM((CHIPS, CORES, d.terms_dev, d.slab, bond), bf16),
                pltpu.VMEM((d.terms_dev, bond, bond), bf16),
                pltpu.VMEM((CHIPS, CORES, d.terms_dev, pair, d.prod), bf16),
                pltpu.VMEM((CHIPS, CORES, d.terms_dev, d.prod, d.prod), bf16),
                pltpu.VMEM((CHUNKS, pair // 2, bond, 2 * d.chunk), bf16),
                pltpu.VMEM((d.lane_tiles, d.half * pair, d.lane), f32),
                pltpu.VMEM((CHIPS * CORES * d.terms_dev, pair, d.sub, 2 * d.chunk), bf16),
                pltpu.VMEM((d.rows, d.group_terms * d.chunk), bf16),
                pltpu.VMEM((d.rows, bond), f32),
                pltpu.VMEM((d.rows, d.half), f32),
                pltpu.VMEM((d.rows, d.half), f32),
                pltpu.VMEM((d.rows, d.half), f32),
                pltpu.VMEM((LANCZOS_STEPS, bond // d.wide, d.half, d.wide), f32),
                pltpu.VMEM((LANCZOS_STEPS, CHIPS, bond // d.wide, d.out_rows, d.wide), f32),
                pltpu.VMEM((1, 128), f32),
                pltpu.VMEM((DEVS, 1, 128), f32),
                pltpu.VMEM((2, 8, 128), f32),
                dma((3, 2)), dma((8, d.lane_tiles)), dma((CHUNKS, 2)), dma((CHUNKS, 2)), dma((2,)), dma((2,)), dma((2,)), dma((2,)),
                dma((4,)), dma((4, CHIPS)), dma, dma((CHIPS,)), dma((PIECES,)), dma((PIECES, CHIPS)),
                dma, dma, dma, dma, dma((LANCZOS_STEPS,)), dma((LANCZOS_STEPS,)), dma, dma, dma((LANCZOS_STEPS, bond // d.wide)), dma((bond // d.wide,)),
            ],
            compiler_params=pltpu.CompilerParams(has_side_effects=True, collective_id=0, vmem_limit_bytes=67043328),
            name='lanczos',
        )(wavefunction.reshape(bond * pair, bond), left_loc, right_loc, pair_loc, flag_loc)
        krylov = jnp.concatenate([first[None], later])
        return krylov.reshape(LANCZOS_STEPS + 1, d.out_rows, pair, bond), alphas, betas

    return jax.shard_map(device_body, mesh=mesh, in_specs=(P(), P(AXIS_NAME), P(AXIS_NAME), P(AXIS_NAME), P(AXIS_NAME)),
                         out_specs=(P(None, AXIS_NAME), P(), P()), check_vma=False)
```

```python
import functools

import jax
import jax.numpy as jnp
from jax import lax
from jax.experimental import pallas as pl
from jax.experimental.pallas import tpu as pltpu
from jax.sharding import PartitionSpec as P

LANCZOS_STEPS = 6
AXIS_NAME = 'terms'
MESH = pl.DeviceIdType.MESH

CHIPS = 16
CORES = 2
DEVS = 32
CHUNKS = 2
GROUPS = 4
TILE_PARTS = 4
QUARTERS = 4
PIECES = CHUNKS * QUARTERS

ALONG, ACROSS, FROM_COLUMN, FROM_SECOND, THIRD, DIAGONAL, RESULT, RESULT_OUT, RESULT_PUT = range(9)
RIGHT_SLOTS = (0, 1, 2, 3, 8, 9, 10, 11)
SLOTS = (
    ((0, 1, 0), (0, 1, 1), (1, 0, 2), (0, 2, 0), (1, 0, 5), (1, 0, 3), (1, 0, 6), (1, 0, 0), (0, 3, 0), (3, 0, 2), (0, 2, 1), (0, 1, 3), (1, 0, 4), (0, 3, 1), (1, 0, 7), (0, 1, 2), (1, 0, 1), (0, 3, 3), (2, 1, 0), (2, 2, 0), (0, 2, 3), (0, 3, 2), (2, 1, 1), (3, 0, 0), (2, 3, 0), (3, 1, 0), (2, 2, 1), (0, 2, 2), (0, 1, 4), (3, 0, 1), (2, 1, 3), (3, 2, 0), (2, 3, 1), (2, 2, 2), (2, 2, 3), (2, 1, 2), (4, 0, 0), (0, 2, 5), (0, 3, 4), (0, 2, 4), (0, 1, 5), (0, 1, 6), (0, 1, 7), (3, 3, 0), (2, 3, 3), (3, 1, 1), (3, 2, 1), (0, 2, 6), (2, 3, 2), (4, 0, 1), (3, 3, 1), (0, 3, 6), (3, 2, 2), (3, 1, 2), (0, 3, 5), (0, 2, 7), (0, 3, 7), (3, 2, 3), (3, 3, 2), (3, 0, 3), (5, 0, 0), (3, 3, 3), (4, 0, 3), (3, 1, 3), (3, 0, 4),),
    ((6, 0, 0), (2, 2, 4), (5, 0, 1), (3, 0, 6), (2, 1, 4), (4, 0, 2),),
    ((2, 2, 6), (5, 0, 2), (2, 1, 6),),
    ((2, 2, 5), (5, 0, 3), (3, 2, 4), (2, 3, 4),),
    ((2, 1, 5), (3, 0, 5), (3, 1, 4),),
    ((2, 3, 5), (3, 2, 5), (2, 3, 6),),
    ((2, 2, 7), (3, 3, 4), (2, 1, 7), (3, 1, 5), (8, 0, 0),),
    ((3, 3, 5), (2, 3, 7), (3, 2, 6), (3, 1, 6), (3, 3, 6),),
    ((3, 0, 7), (3, 1, 7), (3, 2, 7), (4, 0, 5), (5, 0, 4), (4, 0, 4),),
    ((3, 3, 7), (5, 0, 5),),
    ((4, 0, 6), (5, 0, 6),),
    ((4, 0, 7), (5, 0, 7), (7, 0, 0),),
    (),
    (),
    (),
    (),
)
RESULT_EARLY = 12


class Dims:
    def __init__(self, bond, pair, terms_dev):
        self.bond = bond
        self.pair = pair
        self.terms_dev = terms_dev
        self.slab = bond // CHIPS
        self.sub = self.slab // 2
        self.half = bond // CORES
        self.chunk = self.half // CHUNKS
        self.rows = self.slab * pair
        self.prod = self.sub * pair
        self.out_rows = bond // DEVS
        self.group_terms = 4 * CORES * terms_dev
        self.vec_size = bond * pair * bond
        self.lane = min(bond, 128)
        self.wide = TILE_PARTS * self.slab
        self.lane_tiles = bond // self.lane


def lanczos_kernel(d, psi, left, right, pair_ops, flags, out, first, alphas, betas, lv, rv, rs, wv, kw, uv, ps, yst, zst, sig, part, vcur, vprev, tbuf, gbuf,
                   scs, scr, nbuf,
                   loc_sem, psi_sem, d2d_sem, d2d_recv, rw_send, rw_recv, fw_send, fw_recv, l_send, l_recv, f_send, f_recv, u_send, u_recv,
                   p_send, p_recv, s_send, s_recv, k_send, k_recv, n_send, n_recv, o_sem, first_sem):
    me = lax.axis_index(AXIS_NAME)
    core = me % 2
    xpos = (me // 2) % 2
    ypos = (me // 4) % 2
    zpos = me // 8

    def device(z, y, x, c):
        return ((z * 2 + y) * 2 + x) * 2 + c

    def chip_slot(z, y, x):
        return (x * 2 + y) * 4 + z

    partner = device(zpos, ypos, xpos, 1 - core)
    slot = chip_slot(zpos, ypos, xpos)
    zs = (zpos, zpos + 1 - 2 * (zpos % 2), (zpos + 2) % 4, 3 - zpos)
    inner = (zpos + 1) // 2 % 2
    zn = (zpos, (1 - inner) * (zpos + 1 - zpos // 3 * 2) + inner * (zpos - 1), (1 - inner) * ((zpos + 2) % 4) + inner * (zpos + 1),
          (1 - inner) * (3 - zpos) + inner * ((zpos + 2) % 4))
    y_two = ypos + (1 - core) * (1 - 2 * ypos)
    x_two = xpos + core * (1 - 2 * xpos)
    y_three = ypos + core * (1 - 2 * ypos)
    x_three = xpos + (1 - core) * (1 - 2 * xpos)
    two = device(zpos, y_two, x_two, core)
    three = device(zpos, y_three, x_three, core)

    def remote(src, dst, send, recv, dev):
        return pltpu.make_async_remote_copy(src_ref=src, dst_ref=dst, send_sem=send, recv_sem=recv, device_id=(dev,), device_id_type=MESH)

    class Gather:
        def __init__(self, block, send, recv):
            self.block, self.send_sem, self.recv_sem = block, send, recv

        def send(self, which, dev):
            remote(self.block(which), self.block(which), self.send_sem, self.recv_sem(which), dev).start()

        def wait(self, which):
            remote(self.block(which), self.block(which), self.send_sem, self.recv_sem(which), me).wait_recv()

        def own_along(self):
            for i in (1, 2, 3):
                self.send(slot, device(zs[i], ypos, xpos, core))

        def own_across(self):
            self.send(slot, three)
            self.send(slot, two)

        def event(self, n):
            i = (n + 1) // 2
            if n % 2:
                which = chip_slot(zs[i], ypos, xpos)
                self.wait(which)
                self.send(which, three)
                self.send(which, two)
            else:
                which = chip_slot(zs[i], y_two, x_two)
                self.wait(which)
                self.send(which, three)

        def last(self, diagonal):
            for i in range(4):
                self.wait(chip_slot(zs[i], 1 - ypos, 1 - xpos) if diagonal else chip_slot(zs[i], y_three, x_three))

    edge = d.chunk
    l_parts = (
        (lambda s: lv.at[0, s, :, core], 0),
        (lambda s: lv.at[1, s, :, core, :, pl.ds(edge, d.bond - edge)], 1),
        (lambda s: lv.at[0, s, :, 1 - core, :, pl.ds(0, d.half)], 2),
        (lambda s: lv.at[1, s, :, 1 - core, :, pl.ds(edge, d.half - edge)], 3),
    )
    l_gathers = [Gather(block, l_send.at[n], lambda s, n=n: l_recv.at[n, s]) for block, n in l_parts]

    def l_swap(s, term):
        part = lv.at[:, s, :, term, :, pl.ds(d.half, d.half)]
        return remote(part, part, f_send, f_recv.at[s], partner)

    def l_event(n):
        i = (n + 1) // 2
        for g in l_gathers:
            g.event(n)
        l_swap(chip_slot(zs[i], ypos, xpos) if n % 2 else chip_slot(zs[i], y_two, x_two), core).start()

    def l_last(diagonal):
        for i in range(4):
            which = chip_slot(zs[i], 1 - ypos, 1 - xpos) if diagonal else chip_slot(zs[i], y_three, x_three)
            for g in l_gathers:
                g.wait(which)
            l_swap(which, core).start()

    def l_fill(s):
        @pl.when(s != slot)
        def _():
            l_swap(s, 1 - core).wait_recv()
            for c in range(CORES):
                tile = lv[:, s, c, 1 - core, :, d.half:].reshape(d.half, d.half).T
                lv[:, s, c, 1 - core, :, d.half:] = tile.reshape(CHUNKS, d.chunk, d.half)
                for t in range(d.terms_dev):
                    lv[1, s, c, t, :, :edge] = lv[0, s, c, t, :, edge:d.half].T

    def l_along():
        for i in (1, 2, 3):
            for g in l_gathers:
                g.send(slot, device(zs[i], ypos, xpos, core))

    def u_block(p):
        return lambda s: uv.at[p // QUARTERS, pl.ds(p % QUARTERS * 2, 2), pl.ds(pl.multiple_of(s * d.slab, d.slab), d.slab), :]

    u_gathers = [Gather(u_block(p), u_send.at[p], lambda s, p=p: u_recv.at[p, s]) for p in range(PIECES)]

    def act(kind, i, p, j):
        g = u_gathers[p]
        if kind == ALONG:
            g.send(slot, device(zn[i], ypos, xpos, core))
        elif kind == ACROSS:
            g.own_across()
        elif kind == FROM_COLUMN:
            which = chip_slot(zn[i], ypos, xpos)
            g.wait(which)
            g.send(which, three)
            g.send(which, two)
        elif kind == FROM_SECOND:
            which = chip_slot(zn[i], y_two, x_two)
            g.wait(which)
            g.send(which, three)
        elif kind == THIRD:
            g.last(False)
        elif kind == DIAGONAL:
            g.last(True)
        elif kind == RESULT:
            turn_result(j - 1, vcur)
        elif kind == RESULT_OUT:
            hand_out(j - 1, 0, RESULT_EARLY)
        elif kind == RESULT_PUT:
            @pl.when(j > 1)
            def _():
                put_out(j - 2)

    all_right = pltpu.make_async_copy(right, rs, loc_sem.at[2, 0])
    all_right.start()

    barrier = pltpu.get_barrier_semaphore()

    def knock(n, carry):
        pl.semaphore_signal(barrier, inc=1, device_id=((me + n) % DEVS,), device_id_type=MESH)
        return carry

    lax.fori_loop(1, DEVS, knock, 0)

    for ch in range(CHUNKS):
        for h in range(2):
            mine = left.at[:, pl.ds(pl.multiple_of(core * d.half + ch * d.chunk, d.chunk), d.chunk),
                           pl.ds(pl.multiple_of((core + h) % 2 * d.half, d.half), d.half)]
            pltpu.make_async_copy(mine, lv.at[ch, slot, core, :, :, pl.ds(h * d.half, d.half)], loc_sem.at[ch, h]).start()

    psi_rows = d.half * d.pair // 8
    psi_copies = [pltpu.make_async_copy(psi.at[pl.ds(pl.multiple_of(core * d.half * d.pair + n * psi_rows, psi_rows), psi_rows),
                                               pl.ds(c * d.lane, d.lane)],
                                        ps.at[c, pl.ds(n * psi_rows, psi_rows), :], psi_sem.at[n, c])
                  for n in range(8) for c in range(d.lane_tiles)]
    for copy in psi_copies:
        copy.start()

    first_rows = d.out_rows * d.pair
    first_copies = [pltpu.make_async_copy(psi.at[pl.ds(pl.multiple_of(me * first_rows, first_rows), first_rows), pl.ds(c * d.wide, d.wide)],
                                          tbuf.at[LANCZOS_STEPS - 1, c], first_sem.at[c]) for c in range(d.bond // d.wide)]
    for copy in first_copies:
        copy.start()

    spread = (lax.broadcasted_iota(jnp.int32, (d.pair, d.prod), 1) // d.sub == lax.broadcasted_iota(jnp.int32, (d.pair, d.prod), 0))
    spread = spread.astype(jnp.float32).astype(jnp.bfloat16)
    for t in range(d.terms_dev):
        wv[slot, core, t] = jnp.dot(pair_ops[t], spread, preferred_element_type=jnp.float32).astype(jnp.bfloat16)
    all_right.wait()
    some_rows = d.bond // 8

    def one_sided(i, carry):
        at = pl.ds(pl.multiple_of(i * some_rows, some_rows), some_rows)
        row = lax.broadcasted_iota(jnp.int32, (some_rows, d.bond), 0) + i * some_rows
        one = jnp.where(row == lax.broadcasted_iota(jnp.int32, (some_rows, d.bond), 1), 1.0, 0.0)
        for t in range(d.terms_dev):
            rs[t, at, :] = jnp.where(flags[t] == 1, rs[t, at, :].astype(jnp.float32), one).astype(jnp.bfloat16)
        return carry

    lax.fori_loop(0, 8, one_sided, 0)

    def right_rows(s):
        return rs.at[:, pl.ds(pl.multiple_of(s * d.slab, d.slab), d.slab), :]

    rv[slot, core] = rs[:, pl.ds(pl.multiple_of(slot * d.slab, d.slab), d.slab), :]

    pl.semaphore_wait(barrier, DEVS - 1)
    for ch in range(CHUNKS):
        for h in range(2):
            theirs = left.at[:, pl.ds(pl.multiple_of((1 - core) * d.half + ch * d.chunk, d.chunk), d.chunk),
                             pl.ds(pl.multiple_of((1 - core + h) % 2 * d.half, d.half), d.half)]
            remote(theirs, lv.at[ch, slot, core, :, :, pl.ds(h * d.half, d.half)], d2d_sem.at[ch, h], d2d_recv.at[ch, h], partner).start()
    for n in range(1, CHIPS):
        chip = (me // 2 + n) % CHIPS
        to = chip_slot(chip // 4, chip // 2 % 2, chip % 2)
        remote(right_rows(to), rv.at[slot, core], rw_send.at[0], rw_recv.at[0], chip * 2 + core).start()
        remote(wv.at[slot, core], wv.at[slot, core], rw_send.at[1], rw_recv.at[1], chip * 2 + core).start()

    for ch in range(CHUNKS):
        for h in range(2):
            pltpu.make_async_copy(lv.at[ch, slot, core, :, :, pl.ds(h * d.half, d.half)], lv.at[ch, slot, core, :, :, pl.ds(h * d.half, d.half)], loc_sem.at[ch, h]).wait()
            back = remote(lv.at[ch, slot, 1 - core, :, :, pl.ds(h * d.half, d.half)], lv.at[ch, slot, 1 - core, :, :, pl.ds(h * d.half, d.half)], d2d_sem.at[ch, h], d2d_recv.at[ch, h], partner)
            back.wait_recv()
    l_along()
    for g in l_gathers:
        g.own_across()

    total = jnp.zeros((8, d.lane), jnp.float32)
    for n in range(8):
        for copy in psi_copies[n * d.lane_tiles:(n + 1) * d.lane_tiles]:
            copy.wait()

        def add_rows(i, acc, n=n):
            x = ps[:, pl.ds(pl.multiple_of(n * psi_rows + i * (psi_rows // 8), 8), psi_rows // 8), :]
            return acc + jnp.sum((x * x).reshape(d.lane_tiles * psi_rows // 64, 8, d.lane), axis=0)

        total = lax.fori_loop(0, 8, add_rows, total)
    nbuf[0] = jnp.broadcast_to(jnp.sum(total, keepdims=True), (8, 128))
    to_partner = remote(nbuf.at[0], nbuf.at[1], n_send, n_recv, partner)
    to_partner.start()
    to_partner.wait()
    norm = jnp.sqrt((nbuf[0] + nbuf[1])[0:1, :] / d.vec_size)
    norm_one = norm[:, 0:1]
    for copy in first_copies:
        copy.wait()
    tbuf[LANCZOS_STEPS - 1] = tbuf[LANCZOS_STEPS - 1] / norm_one[None]
    first_out = [pltpu.make_async_copy(tbuf.at[LANCZOS_STEPS - 1, c], first.at[:, pl.ds(c * d.wide, d.wide)], first_sem.at[c])
                 for c in range(d.bond // d.wide)]
    for copy in first_out:
        copy.start()

    def place(q):
        tiles = [(ps[c, pl.ds(q, d.half, stride=d.pair), :] / norm_one).T for c in range(d.lane_tiles)]
        xt = jnp.concatenate(tiles, axis=0)
        vprev[...] = xt
        return xt.astype(jnp.bfloat16)

    def start_vector(qb, carry):
        for q2 in range(2):
            q = qb * 2 + q2
            xb = place(q)
            for ch in range(CHUNKS):
                uv[ch, qb, :, q2 * d.chunk:(q2 + 1) * d.chunk] = xb[:, ch * d.chunk:(ch + 1) * d.chunk]
            for bh in range(2):
                rows = vprev[pl.ds(pl.multiple_of(slot * d.slab + bh * d.sub, d.sub), d.sub), :]
                vcur[pl.ds(pl.multiple_of((bh * d.pair + q) * d.sub, d.sub), d.sub), :] = rows
        return carry

    lax.fori_loop(0, d.pair // 4, start_vector, 0)
    fifteen = rv.at[pl.ds(0, CHIPS - 1), 0]
    fifteen_w = wv.at[pl.ds(0, CHIPS - 1), 0]
    remote(fifteen, fifteen, rw_send.at[0], rw_recv.at[0], me).wait()
    remote(fifteen_w, fifteen_w, rw_send.at[1], rw_recv.at[1], me).wait()
    fw_right = remote(rv.at[:, core], rv.at[:, core], fw_send.at[0], fw_recv.at[0], partner)
    fw_pair = remote(wv.at[:, core], wv.at[:, core], fw_send.at[1], fw_recv.at[1], partner)
    fw_right.start()
    fw_pair.start()
    l_event(0)
    l_event(1)
    lax.fori_loop(d.pair // 4, d.pair // 2, start_vector, 0)
    l_event(2)
    l_event(3)
    fw_right.wait()
    fw_pair.wait()
    lane = lax.broadcasted_iota(jnp.int32, (d.sub, d.prod), 1)
    row = lax.broadcasted_iota(jnp.int32, (d.sub, d.prod), 0)
    diagonal = lane % d.sub == row

    def spread_pair(s, carry):
        for c in range(2):
            for t in range(d.terms_dev):
                w = wv[s, c, t].astype(jnp.float32)
                for q in range(d.pair):
                    full = jnp.where(diagonal, jnp.broadcast_to(w[q:q + 1, :], (d.sub, d.prod)), 0.0)
                    kw[s, c, t, q * d.sub:(q + 1) * d.sub, :] = full.astype(jnp.bfloat16)
        return carry

    lax.fori_loop(0, CHIPS, spread_pair, 0)
    vprev[...] = jnp.zeros_like(vprev)
    for copy in first_out:
        copy.wait()

    def right_product(grp, ch, qb, to):
        r_all = rv[pl.ds(grp * 4, 4)].reshape(d.group_terms * d.slab, d.bond)
        y = jnp.dot(r_all, uv[ch, qb], preferred_element_type=jnp.float32).astype(jnp.bfloat16)
        y = y.reshape(d.group_terms, 2, d.sub, 2 * d.chunk)
        for q2 in range(2):
            for bh in range(2):
                yst[pl.ds(to * d.group_terms, d.group_terms), qb * 2 + q2, :, bh * d.chunk:(bh + 1) * d.chunk] = \
                    y[:, bh, :, q2 * d.chunk:(q2 + 1) * d.chunk]

    def right_of_piece(ch, part):
        for qb in range(2):
            for grp in range(GROUPS):
                right_product(grp, ch, part * 2 + qb, grp)

    def right_of_group(grp, ch, to):
        for qb in range(d.pair // 2):
            right_product(grp, ch, qb, to)

    def left_products(ch, grp, at=None):
        for k in range(d.group_terms):
            w = kw[grp * 4 + k // 4, k // 2 % 2, k % 2]
            z = jnp.dot(w, yst[(grp if at is None else at) * d.group_terms + k].reshape(d.prod, 2 * d.chunk), preferred_element_type=jnp.float32).astype(jnp.bfloat16)
            for bh in range(2):
                zst[bh * d.prod:(bh + 1) * d.prod, k * d.chunk:(k + 1) * d.chunk] = z[:, bh * d.chunk:(bh + 1) * d.chunk]
        l_all = lv[ch, pl.ds(grp * 4, 4)].reshape(d.group_terms * d.chunk, d.bond)
        sig[...] += jnp.dot(zst[...], l_all, preferred_element_type=jnp.float32)

    def first_right(grp, carry):
        right_of_group(grp, 0, grp)

        @pl.when(grp == 1)
        def _():
            l_event(4)
        return carry

    def first_group(n, carry):
        own, third = xpos * 2 + ypos, x_three * 2 + y_three
        grp = jnp.where(n == 0, own, jnp.where(n == 1, x_two * 2 + y_two, jnp.where(n == 2, third, 3 - own)))
        spare = jnp.where(n == 3, own, grp)

        @pl.when(n == 1)
        def _():
            l_event(6)
            l_last(False)

        @pl.when(n == 3)
        def _():
            right_of_group(grp, 1, spare)
            l_last(True)

        def fill(z, carry):
            l_fill(grp * 4 + z)
            return carry

        lax.fori_loop(0, 4, fill, 0)

        def chunk_products(ch, carry):
            left_products(ch, grp, (1 - ch) * grp + ch * spare)

            @pl.when((ch == 0) & (n < 3))
            def _():
                right_of_group(grp, 1, spare)
            return carry

        lax.fori_loop(0, CHUNKS, chunk_products, 0)
        return carry

    def turn_result(j, vector):
        for n in range(d.pair // TILE_PARTS):
            rows = [vector[(bh * d.pair + q) * d.sub:(bh * d.pair + q + 1) * d.sub, :d.half]
                    for q in range(n * TILE_PARTS, (n + 1) * TILE_PARTS) for bh in range(2)]
            tbuf[j, n] = jnp.concatenate(rows, axis=0).T

    def hand_out(j, begin, end):
        for n in range(begin, end):
            to = core * CHIPS + n
            block = tbuf.at[j, :, pl.ds(n * d.out_rows, d.out_rows), :]

            @pl.when(to != me)
            def _():
                remote(block, gbuf.at[j, slot], k_send.at[j], k_recv.at[j], to).start()

            @pl.when(to == me)
            def _():
                gbuf[j, slot] = block[...]

    sends_self = me // CHIPS == core
    lanes = lax.broadcasted_iota(jnp.int32, (d.out_rows, d.wide), 1) // d.slab

    def put_out(j, finish=None):
        @pl.when(sends_self)
        def _():
            some = gbuf.at[j, pl.ds(0, CHIPS - 1)]
            remote(some, some, k_send.at[j], k_recv.at[j], me).wait()

        @pl.when(jnp.logical_not(sends_self))
        def _():
            remote(gbuf.at[j], gbuf.at[j], k_send.at[j], k_recv.at[j], me).wait()

        for ct in range(CHIPS // TILE_PARTS):
            for qt in range(d.pair // TILE_PARTS):
                src = [gbuf[j, ct * TILE_PARTS + c, qt] for c in range(TILE_PARTS)]
                if finish is not None:
                    src = [finish(x, gbuf[j - 1, ct * TILE_PARTS + c, qt], ct * TILE_PARTS + c) for c, x in enumerate(src)]
                for q in range(TILE_PARTS):
                    tile = jnp.zeros((d.out_rows, d.wide), jnp.float32)
                    for c in range(TILE_PARTS):
                        shift = (c - q) % TILE_PARTS * d.slab
                        moved = pltpu.roll(src[c], shift, 1) if shift else src[c]
                        tile = jnp.where(lanes == c, moved, tile)
                    tbuf[j, ct, pl.ds(qt * TILE_PARTS + q, d.out_rows, stride=d.pair), :] = tile
            pltpu.make_async_copy(tbuf.at[j, ct], out.at[j, :, pl.ds(ct * d.wide, d.wide)], o_sem.at[j, ct]).start()

    def step(j, carried):
        beta_prev = carried[0]
        sig[...] = jnp.zeros_like(sig)

        def slot_step(t, carry):
            done_right = sum((t > r).astype(jnp.int32) for r in RIGHT_SLOTS)
            done_left = t - done_right
            is_right = sum((t == r).astype(jnp.int32) for r in RIGHT_SLOTS)
            for four in range(0, len(SLOTS), 4):
                @pl.when((t >= four) & (t < four + 4))
                def _():
                    for at in range(four, four + 4):
                        if not SLOTS[at]:
                            continue

                        @pl.when(t == at)
                        def _():
                            for kind, i, p in SLOTS[at]:
                                act(kind, i, p, j)

            @pl.when(is_right == 1)
            def _():
                right_of_piece(done_right // QUARTERS, done_right % QUARTERS)

            @pl.when(is_right == 0)
            def _():
                left_products(done_left // GROUPS, done_left % GROUPS)
            return carry

        @pl.when(j == 0)
        def _():
            lax.fori_loop(0, GROUPS, first_right, 0)
            l_event(5)
            lax.fori_loop(0, GROUPS, first_group, 0)

        @pl.when(j > 0)
        def _():
            lax.fori_loop(0, len(SLOTS), slot_step, 0)
            for p in range(PIECES):
                sent = uv.at[p // QUARTERS, pl.ds(0, 2), pl.ds(0, 15 * d.slab), :]
                remote(sent, sent, u_send.at[p], u_recv.at[p, 0], me).wait_send()

        other = sig.at[:, pl.ds(d.half, d.half)]
        to_other = remote(other, part, p_send, p_recv, partner)
        to_other.start()
        to_other.wait()
        s = sig[:, :d.half] + part[...]
        v = vcur[...]
        w = s - beta_prev * vprev[...]
        sv = jnp.sum(s * v, keepdims=True)
        wv_sum = jnp.sum(w * v, keepdims=True)
        vv = jnp.sum(v * v, keepdims=True)
        guess = jnp.where(vv > 0.0, wv_sum / jnp.where(vv > 0.0, vv, 1.0), 0.0)
        t = w - guess * v
        sig[:, :d.half] = t
        tt = jnp.sum(t * t, keepdims=True)
        tv = jnp.sum(t * v, keepdims=True)
        at_lane = lax.broadcasted_iota(jnp.int32, (1, 128), 1)
        line = jnp.zeros((1, 128), jnp.float32)
        for n, value in enumerate((sv, vv, tt, tv, guess)):
            line = jnp.where(at_lane == n, value, line)
        scs[...] = line
        scr[me] = line

        def tell(n, carry):
            remote(scs, scr.at[me], s_send, s_recv, (me + n) % DEVS).start()
            return carry

        lax.fori_loop(1, DEVS, tell, 0)

        @pl.when(j > 0)
        def _():
            hand_out(j - 1, RESULT_EARLY, CHIPS)

        @pl.when(j == LANCZOS_STEPS - 1)
        def _():
            turn_result(LANCZOS_STEPS - 1, sig)
            hand_out(LANCZOS_STEPS - 1, 0, CHIPS)

        heard = scr.at[pl.ds(0, DEVS - 1)]
        remote(heard, heard, s_send, s_recv, me).wait()
        told = scr[:, 0, :]
        alpha = jnp.sum(told[:, 0:1], axis=0, keepdims=True) / d.vec_size
        off = alpha - told[:, 4:5]
        square = told[:, 2:3] - 2.0 * off * told[:, 3:4] + off * off * told[:, 1:2]
        beta = jnp.sqrt(jnp.sum(square, axis=0, keepdims=True) / d.vec_size)
        vnew = (sig[:, :d.half] - (alpha - guess) * vcur[...]) / beta
        vprev[...] = vcur[...]
        vcur[...] = vnew
        vb = vnew.astype(jnp.bfloat16)

        @pl.when(j < LANCZOS_STEPS - 1)
        def _():
            for ch in range(CHUNKS):
                for bh in range(2):
                    at = pl.ds(pl.multiple_of(slot * d.slab + bh * d.sub, d.sub), d.sub)
                    for q in range(d.pair):
                        uv[ch, q // 2, at, q % 2 * d.chunk:(q % 2 + 1) * d.chunk] = \
                            vb[(bh * d.pair + q) * d.sub:(bh * d.pair + q + 1) * d.sub, ch * d.chunk:(ch + 1) * d.chunk]
        alphas[j] = alpha[0, 0]
        betas[j] = beta[0, 0]
        return beta, alpha


    zero = jnp.zeros((1, 1), jnp.float32)
    last_beta, last_alpha = lax.fori_loop(0, LANCZOS_STEPS, step, (zero, zero))

    for n, part in enumerate((lv.at[0, pl.ds(0, 15), :, 0], lv.at[1, pl.ds(0, 15), :, 0, :, pl.ds(edge, d.bond - edge)],
                              lv.at[0, pl.ds(0, 15), :, 0, :, pl.ds(0, d.half)], lv.at[1, pl.ds(0, 15), :, 0, :, pl.ds(edge, d.half - edge)])):
        remote(part, part, l_send.at[n], l_recv.at[n, 0], me).wait_send()
    swapped = lv.at[:, pl.ds(0, 15), :, 0, :, pl.ds(d.half, d.half)]
    remote(swapped, swapped, f_send, f_recv.at[0], me).wait_send()
    for ch in range(CHUNKS):
        for h in range(2):
            theirs = left.at[:, pl.ds(0, d.chunk), pl.ds(0, d.half)]
            remote(theirs, lv.at[ch, slot, core, :, :, pl.ds(h * d.half, d.half)], d2d_sem.at[ch, h], d2d_recv.at[ch, h], partner).wait_send()
    put_out(LANCZOS_STEPS - 2)

    def finish(block, before, s):
        owner = device(s % 4, s // 4 % 2, s // 8, me // CHIPS)
        return (block - (last_alpha - scr[owner][:, 4:5]) * before) / last_beta

    put_out(LANCZOS_STEPS - 1, finish)
    for j in range(LANCZOS_STEPS):
        for c in range(d.bond // d.wide):
            pltpu.make_async_copy(tbuf.at[j, c], out.at[j, :, pl.ds(c * d.wide, d.wide)], o_sem.at[j, c]).wait()


def solution(mesh):
    def device_body(wavefunction, left_loc, pair_loc, right_loc, flag_loc):
        bond, pair = wavefunction.shape[0], wavefunction.shape[1]
        d = Dims(bond, pair, left_loc.shape[0])
        bf16, f32 = jnp.bfloat16, jnp.float32
        dma = pltpu.SemaphoreType.DMA
        any_space = pl.BlockSpec(memory_space=pl.ANY)
        smem = pl.BlockSpec(memory_space=pltpu.SMEM)
        scalars = jax.ShapeDtypeStruct((LANCZOS_STEPS,), f32)
        later, first, alphas, betas = pl.pallas_call(
            functools.partial(lanczos_kernel, d),
            out_shape=(jax.ShapeDtypeStruct((LANCZOS_STEPS, d.out_rows * pair, bond), f32),
                       jax.ShapeDtypeStruct((d.out_rows * pair, bond), f32), scalars, scalars),
            in_specs=[any_space] * 3 + [pl.BlockSpec(memory_space=pltpu.VMEM), smem],
            out_specs=(any_space, any_space, smem, smem),
            scratch_shapes=[
                pltpu.VMEM((CHUNKS, CHIPS, CORES, d.terms_dev, d.chunk, bond), bf16),
                pltpu.VMEM((CHIPS, CORES, d.terms_dev, d.slab, bond), bf16),
                pltpu.VMEM((d.terms_dev, bond, bond), bf16),
                pltpu.VMEM((CHIPS, CORES, d.terms_dev, pair, d.prod), bf16),
                pltpu.VMEM((CHIPS, CORES, d.terms_dev, d.prod, d.prod), bf16),
                pltpu.VMEM((CHUNKS, pair // 2, bond, 2 * d.chunk), bf16),
                pltpu.VMEM((d.lane_tiles, d.half * pair, d.lane), f32),
                pltpu.VMEM((CHIPS * CORES * d.terms_dev, pair, d.sub, 2 * d.chunk), bf16),
                pltpu.VMEM((d.rows, d.group_terms * d.chunk), bf16),
                pltpu.VMEM((d.rows, bond), f32),
                pltpu.VMEM((d.rows, d.half), f32),
                pltpu.VMEM((d.rows, d.half), f32),
                pltpu.VMEM((d.rows, d.half), f32),
                pltpu.VMEM((LANCZOS_STEPS, bond // d.wide, d.half, d.wide), f32),
                pltpu.VMEM((LANCZOS_STEPS, CHIPS, bond // d.wide, d.out_rows, d.wide), f32),
                pltpu.VMEM((1, 128), f32),
                pltpu.VMEM((DEVS, 1, 128), f32),
                pltpu.VMEM((2, 8, 128), f32),
                dma((3, 2)), dma((8, d.lane_tiles)), dma((CHUNKS, 2)), dma((CHUNKS, 2)), dma((2,)), dma((2,)), dma((2,)), dma((2,)),
                dma((4,)), dma((4, CHIPS)), dma, dma((CHIPS,)), dma((PIECES,)), dma((PIECES, CHIPS)),
                dma, dma, dma, dma, dma((LANCZOS_STEPS,)), dma((LANCZOS_STEPS,)), dma, dma, dma((LANCZOS_STEPS, bond // d.wide)), dma((bond // d.wide,)),
            ],
            compiler_params=pltpu.CompilerParams(has_side_effects=True, collective_id=0, vmem_limit_bytes=67043328),
            name='lanczos',
        )(wavefunction.reshape(bond * pair, bond), left_loc, right_loc, pair_loc, flag_loc)
        krylov = jnp.concatenate([first[None], later])
        return krylov.reshape(LANCZOS_STEPS + 1, d.out_rows, pair, bond), alphas, betas

    return jax.shard_map(device_body, mesh=mesh, in_specs=(P(), P(AXIS_NAME), P(AXIS_NAME), P(AXIS_NAME), P(AXIS_NAME)),
                         out_specs=(P(None, AXIS_NAME), P(), P()), check_vma=False)
```

```python
import functools

import jax
import jax.numpy as jnp
from jax import lax
from jax.experimental import pallas as pl
from jax.experimental.pallas import tpu as pltpu
from jax.sharding import PartitionSpec as P

LANCZOS_STEPS = 6
AXIS_NAME = 'terms'
MESH = pl.DeviceIdType.MESH

CHIPS = 16
CORES = 2
DEVS = 32
CHUNKS = 2
GROUPS = 4
TILE_PARTS = 4
QUARTERS = 4
PIECES = CHUNKS * QUARTERS

ALONG, ACROSS, FROM_COLUMN, FROM_SECOND, THIRD, DIAGONAL, RESULT, RESULT_OUT, RESULT_PUT = range(9)
RIGHT_SLOTS = (0, 1, 2, 3, 8, 9, 10, 11)
SLOTS = (
    ((0, 1, 0), (0, 1, 1), (1, 0, 2), (0, 2, 0), (1, 0, 5), (1, 0, 3), (1, 0, 6), (1, 0, 0), (0, 3, 0), (3, 0, 2), (0, 2, 1), (0, 1, 3), (1, 0, 4), (0, 3, 1), (1, 0, 7), (0, 1, 2), (1, 0, 1), (0, 3, 3), (2, 1, 0), (2, 2, 0), (0, 2, 3), (0, 3, 2), (2, 1, 1), (3, 0, 0), (2, 3, 0), (3, 1, 0), (2, 2, 1), (0, 2, 2), (0, 1, 4), (3, 0, 1), (2, 1, 3), (3, 2, 0), (2, 3, 1), (2, 2, 2), (2, 2, 3), (2, 1, 2), (4, 0, 0), (0, 2, 5), (0, 3, 4), (0, 2, 4), (0, 1, 5), (0, 1, 6), (0, 1, 7), (3, 3, 0), (2, 3, 3), (3, 1, 1), (3, 2, 1), (0, 2, 6), (2, 3, 2), (4, 0, 1), (3, 3, 1), (0, 3, 6), (3, 2, 2), (3, 1, 2), (0, 3, 5), (0, 2, 7), (0, 3, 7), (3, 2, 3), (3, 3, 2), (3, 0, 3), (5, 0, 0), (3, 3, 3), (4, 0, 3), (3, 1, 3), (3, 0, 4),),
    ((6, 0, 0), (2, 2, 4), (5, 0, 1), (3, 0, 6), (2, 1, 4), (4, 0, 2),),
    ((2, 2, 6), (5, 0, 2), (2, 1, 6),),
    ((2, 2, 5), (5, 0, 3), (3, 2, 4), (2, 3, 4),),
    ((2, 1, 5), (3, 0, 5), (3, 1, 4),),
    ((2, 3, 5), (3, 2, 5), (2, 3, 6),),
    ((2, 2, 7), (3, 3, 4), (2, 1, 7), (3, 1, 5), (8, 0, 0),),
    ((3, 3, 5), (2, 3, 7), (3, 2, 6), (3, 1, 6), (3, 3, 6),),
    ((3, 0, 7), (3, 1, 7), (3, 2, 7), (4, 0, 5), (5, 0, 4), (4, 0, 4),),
    ((3, 3, 7), (5, 0, 5),),
    ((4, 0, 6), (5, 0, 6),),
    ((4, 0, 7), (5, 0, 7), (7, 0, 0),),
    (),
    (),
    (),
    (),
)
RESULT_EARLY = 12


class Dims:
    def __init__(self, bond, pair, terms_dev):
        self.bond = bond
        self.pair = pair
        self.terms_dev = terms_dev
        self.slab = bond // CHIPS
        self.sub = self.slab // 2
        self.half = bond // CORES
        self.chunk = self.half // CHUNKS
        self.rows = self.slab * pair
        self.prod = self.sub * pair
        self.out_rows = bond // DEVS
        self.group_terms = 4 * CORES * terms_dev
        self.vec_size = bond * pair * bond
        self.lane = min(bond, 128)
        self.wide = TILE_PARTS * self.slab
        self.lane_tiles = bond // self.lane


def lanczos_kernel(d, psi, left, right, pair_ops, flags, out, first, alphas, betas, lv, rv, rs, wv, kw, uv, ps, yst, zst, sig, part, vcur, vprev, tbuf, gbuf,
                   scs, scr, nbuf,
                   loc_sem, psi_sem, d2d_sem, d2d_recv, rw_send, rw_recv, fw_send, fw_recv, l_send, l_recv, f_send, f_recv, u_send, u_recv,
                   p_send, p_recv, s_send, s_recv, k_send, k_recv, n_send, n_recv, o_sem, first_sem):
    me = lax.axis_index(AXIS_NAME)
    core = me % 2
    xpos = (me // 2) % 2
    ypos = (me // 4) % 2
    zpos = me // 8

    def device(z, y, x, c):
        return ((z * 2 + y) * 2 + x) * 2 + c

    def chip_slot(z, y, x):
        return (x * 2 + y) * 4 + z

    partner = device(zpos, ypos, xpos, 1 - core)
    slot = chip_slot(zpos, ypos, xpos)
    zs = (zpos, zpos + 1 - 2 * (zpos % 2), (zpos + 2) % 4, 3 - zpos)
    inner = (zpos + 1) // 2 % 2
    zn = (zpos, (1 - inner) * (zpos + 1 - zpos // 3 * 2) + inner * (zpos - 1), (1 - inner) * ((zpos + 2) % 4) + inner * (zpos + 1),
          (1 - inner) * (3 - zpos) + inner * ((zpos + 2) % 4))
    y_two = ypos + (1 - core) * (1 - 2 * ypos)
    x_two = xpos + core * (1 - 2 * xpos)
    y_three = ypos + core * (1 - 2 * ypos)
    x_three = xpos + (1 - core) * (1 - 2 * xpos)
    two = device(zpos, y_two, x_two, core)
    three = device(zpos, y_three, x_three, core)

    def remote(src, dst, send, recv, dev):
        return pltpu.make_async_remote_copy(src_ref=src, dst_ref=dst, send_sem=send, recv_sem=recv, device_id=(dev,), device_id_type=MESH)

    class Gather:
        def __init__(self, block, send, recv):
            self.block, self.send_sem, self.recv_sem = block, send, recv

        def send(self, which, dev):
            remote(self.block(which), self.block(which), self.send_sem, self.recv_sem(which), dev).start()

        def wait(self, which):
            remote(self.block(which), self.block(which), self.send_sem, self.recv_sem(which), me).wait_recv()

        def own_along(self):
            for i in (1, 2, 3):
                self.send(slot, device(zs[i], ypos, xpos, core))

        def own_across(self):
            self.send(slot, three)
            self.send(slot, two)

        def event(self, n):
            i = (n + 1) // 2
            if n % 2:
                which = chip_slot(zs[i], ypos, xpos)
                self.wait(which)
                self.send(which, three)
                self.send(which, two)
            else:
                which = chip_slot(zs[i], y_two, x_two)
                self.wait(which)
                self.send(which, three)

        def last(self, diagonal):
            for i in range(4):
                self.wait(chip_slot(zs[i], 1 - ypos, 1 - xpos) if diagonal else chip_slot(zs[i], y_three, x_three))

    edge = d.chunk
    l_parts = (
        (lambda s: lv.at[0, s, :, core], 0),
        (lambda s: lv.at[1, s, :, core, :, pl.ds(edge, d.bond - edge)], 1),
        (lambda s: lv.at[0, s, :, 1 - core, :, pl.ds(0, d.half)], 2),
        (lambda s: lv.at[1, s, :, 1 - core, :, pl.ds(edge, d.half - edge)], 3),
    )
    l_gathers = [Gather(block, l_send.at[n], lambda s, n=n: l_recv.at[n, s]) for block, n in l_parts]

    def l_swap(s, term):
        part = lv.at[:, s, :, term, :, pl.ds(d.half, d.half)]
        return remote(part, part, f_send, f_recv.at[s], partner)

    def l_event(n):
        i = (n + 1) // 2
        for g in l_gathers:
            g.event(n)
        l_swap(chip_slot(zs[i], ypos, xpos) if n % 2 else chip_slot(zs[i], y_two, x_two), core).start()

    def l_last(diagonal):
        for i in range(4):
            which = chip_slot(zs[i], 1 - ypos, 1 - xpos) if diagonal else chip_slot(zs[i], y_three, x_three)
            for g in l_gathers:
                g.wait(which)
            l_swap(which, core).start()

    def l_fill(s):
        @pl.when(s != slot)
        def _():
            l_swap(s, 1 - core).wait_recv()
            for c in range(CORES):
                tile = lv[:, s, c, 1 - core, :, d.half:].reshape(d.half, d.half).T
                lv[:, s, c, 1 - core, :, d.half:] = tile.reshape(CHUNKS, d.chunk, d.half)
                for t in range(d.terms_dev):
                    lv[1, s, c, t, :, :edge] = lv[0, s, c, t, :, edge:d.half].T

    def l_along():
        for i in (1, 2, 3):
            for g in l_gathers:
                g.send(slot, device(zs[i], ypos, xpos, core))

    def u_block(p):
        return lambda s: uv.at[p // QUARTERS, pl.ds(p % QUARTERS * 2, 2), pl.ds(pl.multiple_of(s * d.slab, d.slab), d.slab), :]

    u_gathers = [Gather(u_block(p), u_send.at[p], lambda s, p=p: u_recv.at[p, s]) for p in range(PIECES)]

    def act(kind, i, p, j):
        g = u_gathers[p]
        if kind == ALONG:
            g.send(slot, device(zn[i], ypos, xpos, core))
        elif kind == ACROSS:
            g.own_across()
        elif kind == FROM_COLUMN:
            which = chip_slot(zn[i], ypos, xpos)
            g.wait(which)
            g.send(which, three)
            g.send(which, two)
        elif kind == FROM_SECOND:
            which = chip_slot(zn[i], y_two, x_two)
            g.wait(which)
            g.send(which, three)
        elif kind == THIRD:
            g.last(False)
        elif kind == DIAGONAL:
            g.last(True)
        elif kind == RESULT:
            turn_result(j - 1, vcur)
        elif kind == RESULT_OUT:
            hand_out(j - 1, 0, RESULT_EARLY)
        elif kind == RESULT_PUT:
            @pl.when(j > 1)
            def _():
                put_out(j - 2)

    all_right = pltpu.make_async_copy(right, rs, loc_sem.at[2, 0])
    all_right.start()

    barrier = pltpu.get_barrier_semaphore()

    def knock(n, carry):
        pl.semaphore_signal(barrier, inc=1, device_id=((me + n) % DEVS,), device_id_type=MESH)
        return carry

    lax.fori_loop(1, DEVS, knock, 0)

    for ch in range(CHUNKS):
        for h in range(2):
            mine = left.at[:, pl.ds(pl.multiple_of(core * d.half + ch * d.chunk, d.chunk), d.chunk),
                           pl.ds(pl.multiple_of((core + h) % 2 * d.half, d.half), d.half)]
            pltpu.make_async_copy(mine, lv.at[ch, slot, core, :, :, pl.ds(h * d.half, d.half)], loc_sem.at[ch, h]).start()

    psi_rows = d.half * d.pair // 8
    psi_copies = [pltpu.make_async_copy(psi.at[pl.ds(pl.multiple_of(core * d.half * d.pair + n * psi_rows, psi_rows), psi_rows),
                                               pl.ds(c * d.lane, d.lane)],
                                        ps.at[c, pl.ds(n * psi_rows, psi_rows), :], psi_sem.at[n, c])
                  for n in range(8) for c in range(d.lane_tiles)]
    for copy in psi_copies:
        copy.start()

    first_rows = d.out_rows * d.pair
    first_copies = [pltpu.make_async_copy(psi.at[pl.ds(pl.multiple_of(me * first_rows, first_rows), first_rows), pl.ds(c * d.wide, d.wide)],
                                          tbuf.at[LANCZOS_STEPS - 1, c], first_sem.at[c]) for c in range(d.bond // d.wide)]
    for copy in first_copies:
        copy.start()

    side_by_side = jnp.zeros((d.pair, 128), jnp.float32)
    for t in range(d.terms_dev):
        place_of = lax.broadcasted_iota(jnp.int32, (d.pair, 128), 1) == lax.broadcasted_iota(jnp.int32, (d.pair, 128), 0) + t * d.pair
        place_of = jnp.where(place_of, 1.0, 0.0).astype(jnp.bfloat16)
        side_by_side += jnp.dot(pair_ops[t], place_of, preferred_element_type=jnp.float32)
    wv[slot, core] = side_by_side.astype(jnp.bfloat16)
    all_right.wait()
    some_rows = d.bond // 8

    def one_sided(i, carry):
        at = pl.ds(pl.multiple_of(i * some_rows, some_rows), some_rows)
        row = lax.broadcasted_iota(jnp.int32, (some_rows, d.bond), 0) + i * some_rows
        one = jnp.where(row == lax.broadcasted_iota(jnp.int32, (some_rows, d.bond), 1), 1.0, 0.0)
        for t in range(d.terms_dev):
            rs[t, at, :] = jnp.where(flags[t] == 1, rs[t, at, :].astype(jnp.float32), one).astype(jnp.bfloat16)
        return carry

    lax.fori_loop(0, 8, one_sided, 0)

    def right_rows(s):
        return rs.at[:, pl.ds(pl.multiple_of(s * d.slab, d.slab), d.slab), :]

    rv[slot, core] = rs[:, pl.ds(pl.multiple_of(slot * d.slab, d.slab), d.slab), :]

    pl.semaphore_wait(barrier, DEVS - 1)
    for ch in range(CHUNKS):
        for h in range(2):
            theirs = left.at[:, pl.ds(pl.multiple_of((1 - core) * d.half + ch * d.chunk, d.chunk), d.chunk),
                             pl.ds(pl.multiple_of((1 - core + h) % 2 * d.half, d.half), d.half)]
            remote(theirs, lv.at[ch, slot, core, :, :, pl.ds(h * d.half, d.half)], d2d_sem.at[ch, h], d2d_recv.at[ch, h], partner).start()
    for n in range(1, CHIPS):
        chip = (me // 2 + n) % CHIPS
        to = chip_slot(chip // 4, chip // 2 % 2, chip % 2)
        remote(right_rows(to), rv.at[slot, core], rw_send.at[0], rw_recv.at[0], chip * 2 + core).start()
        remote(wv.at[slot, core], wv.at[slot, core], rw_send.at[1], rw_recv.at[1], chip * 2 + core).start()

    for ch in range(CHUNKS):
        for h in range(2):
            pltpu.make_async_copy(lv.at[ch, slot, core, :, :, pl.ds(h * d.half, d.half)], lv.at[ch, slot, core, :, :, pl.ds(h * d.half, d.half)], loc_sem.at[ch, h]).wait()
            back = remote(lv.at[ch, slot, 1 - core, :, :, pl.ds(h * d.half, d.half)], lv.at[ch, slot, 1 - core, :, :, pl.ds(h * d.half, d.half)], d2d_sem.at[ch, h], d2d_recv.at[ch, h], partner)
            back.wait_recv()
    l_along()
    for g in l_gathers:
        g.own_across()

    total = jnp.zeros((8, d.lane), jnp.float32)
    for n in range(8):
        for copy in psi_copies[n * d.lane_tiles:(n + 1) * d.lane_tiles]:
            copy.wait()

        def add_rows(i, acc, n=n):
            x = ps[:, pl.ds(pl.multiple_of(n * psi_rows + i * (psi_rows // 8), 8), psi_rows // 8), :]
            return acc + jnp.sum((x * x).reshape(d.lane_tiles * psi_rows // 64, 8, d.lane), axis=0)

        total = lax.fori_loop(0, 8, add_rows, total)
    nbuf[0] = jnp.broadcast_to(jnp.sum(total, keepdims=True), (8, 128))
    to_partner = remote(nbuf.at[0], nbuf.at[1], n_send, n_recv, partner)
    to_partner.start()
    to_partner.wait()
    norm = jnp.sqrt((nbuf[0] + nbuf[1])[0:1, :] / d.vec_size)
    norm_one = norm[:, 0:1]
    for copy in first_copies:
        copy.wait()
    tbuf[LANCZOS_STEPS - 1] = tbuf[LANCZOS_STEPS - 1] / norm_one[None]
    first_out = [pltpu.make_async_copy(tbuf.at[LANCZOS_STEPS - 1, c], first.at[:, pl.ds(c * d.wide, d.wide)], first_sem.at[c])
                 for c in range(d.bond // d.wide)]
    for copy in first_out:
        copy.start()

    def place(q):
        tiles = [(ps[c, pl.ds(q, d.half, stride=d.pair), :] / norm_one).T for c in range(d.lane_tiles)]
        xt = jnp.concatenate(tiles, axis=0)
        vprev[...] = xt
        return xt.astype(jnp.bfloat16)

    def start_vector(qb, carry):
        for q2 in range(2):
            q = qb * 2 + q2
            xb = place(q)
            for ch in range(CHUNKS):
                uv[ch, qb, :, q2 * d.chunk:(q2 + 1) * d.chunk] = xb[:, ch * d.chunk:(ch + 1) * d.chunk]
            for bh in range(2):
                rows = vprev[pl.ds(pl.multiple_of(slot * d.slab + bh * d.sub, d.sub), d.sub), :]
                vcur[pl.ds(pl.multiple_of((bh * d.pair + q) * d.sub, d.sub), d.sub), :] = rows
        return carry

    lax.fori_loop(0, d.pair // 4, start_vector, 0)
    fifteen = rv.at[pl.ds(0, CHIPS - 1), 0]
    fifteen_w = wv.at[pl.ds(0, CHIPS - 1), 0]
    remote(fifteen, fifteen, rw_send.at[0], rw_recv.at[0], me).wait()
    remote(fifteen_w, fifteen_w, rw_send.at[1], rw_recv.at[1], me).wait()
    fw_right = remote(rv.at[:, core], rv.at[:, core], fw_send.at[0], fw_recv.at[0], partner)
    fw_pair = remote(wv.at[:, core], wv.at[:, core], fw_send.at[1], fw_recv.at[1], partner)
    fw_right.start()
    fw_pair.start()
    l_event(0)
    l_event(1)
    lax.fori_loop(d.pair // 4, d.pair // 2, start_vector, 0)
    l_event(2)
    l_event(3)
    fw_right.wait()
    fw_pair.wait()
    lane = lax.broadcasted_iota(jnp.int32, (d.sub, d.prod), 1)
    row = lax.broadcasted_iota(jnp.int32, (d.sub, d.prod), 0)
    diagonal = lane % d.sub == row

    for t in range(d.terms_dev):
        at_row = lax.broadcasted_iota(jnp.int32, (128, d.prod), 0)
        wide = jnp.where(at_row == lax.broadcasted_iota(jnp.int32, (128, d.prod), 1) // d.sub + t * d.pair, 1.0, 0.0).astype(jnp.bfloat16)
        spread = jnp.dot(wv[...].reshape(CHIPS * CORES * d.pair, 128), wide, preferred_element_type=jnp.float32)
        zst[:, t * d.prod:(t + 1) * d.prod] = spread.astype(jnp.bfloat16)

    def spread_pair(s, carry):
        for c in range(2):
            for t in range(d.terms_dev):
                w = zst[pl.ds(pl.multiple_of((s * CORES + c) * d.pair, d.pair), d.pair), t * d.prod:(t + 1) * d.prod].astype(jnp.float32)
                for q in range(d.pair):
                    full = jnp.where(diagonal, jnp.broadcast_to(w[q:q + 1, :], (d.sub, d.prod)), 0.0)
                    kw[s, c, t, q * d.sub:(q + 1) * d.sub, :] = full.astype(jnp.bfloat16)
        return carry

    lax.fori_loop(0, CHIPS, spread_pair, 0)
    vprev[...] = jnp.zeros_like(vprev)
    for copy in first_out:
        copy.wait()

    def right_product(grp, ch, qb, to):
        r_all = rv[pl.ds(grp * 4, 4)].reshape(d.group_terms * d.slab, d.bond)
        y = jnp.dot(r_all, uv[ch, qb], preferred_element_type=jnp.float32).astype(jnp.bfloat16)
        y = y.reshape(d.group_terms, 2, d.sub, 2 * d.chunk)
        for q2 in range(2):
            for bh in range(2):
                yst[pl.ds(to * d.group_terms, d.group_terms), qb * 2 + q2, :, bh * d.chunk:(bh + 1) * d.chunk] = \
                    y[:, bh, :, q2 * d.chunk:(q2 + 1) * d.chunk]

    def right_of_piece(ch, part):
        for qb in range(2):
            for grp in range(GROUPS):
                right_product(grp, ch, part * 2 + qb, grp)

    def right_of_group(grp, ch, to):
        for qb in range(d.pair // 2):
            right_product(grp, ch, qb, to)

    def left_products(ch, grp, at=None):
        for k in range(d.group_terms):
            w = kw[grp * 4 + k // 4, k // 2 % 2, k % 2]
            z = jnp.dot(w, yst[(grp if at is None else at) * d.group_terms + k].reshape(d.prod, 2 * d.chunk), preferred_element_type=jnp.float32).astype(jnp.bfloat16)
            for bh in range(2):
                zst[bh * d.prod:(bh + 1) * d.prod, k * d.chunk:(k + 1) * d.chunk] = z[:, bh * d.chunk:(bh + 1) * d.chunk]
        l_all = lv[ch, pl.ds(grp * 4, 4)].reshape(d.group_terms * d.chunk, d.bond)
        sig[...] += jnp.dot(zst[...], l_all, preferred_element_type=jnp.float32)

    def first_right(grp, carry):
        right_of_group(grp, 0, grp)

        @pl.when(grp == 1)
        def _():
            l_event(4)
        return carry

    def first_group(n, carry):
        own, third = xpos * 2 + ypos, x_three * 2 + y_three
        grp = jnp.where(n == 0, own, jnp.where(n == 1, x_two * 2 + y_two, jnp.where(n == 2, third, 3 - own)))
        spare = jnp.where(n == 3, own, grp)

        @pl.when(n == 1)
        def _():
            l_event(6)
            l_last(False)

        @pl.when(n == 3)
        def _():
            right_of_group(grp, 1, spare)
            l_last(True)

        def fill(z, carry):
            l_fill(grp * 4 + z)
            return carry

        lax.fori_loop(0, 4, fill, 0)

        def chunk_products(ch, carry):
            left_products(ch, grp, (1 - ch) * grp + ch * spare)

            @pl.when((ch == 0) & (n < 3))
            def _():
                right_of_group(grp, 1, spare)
            return carry

        lax.fori_loop(0, CHUNKS, chunk_products, 0)
        return carry

    def turn_result(j, vector):
        for n in range(d.pair // TILE_PARTS):
            rows = [vector[(bh * d.pair + q) * d.sub:(bh * d.pair + q + 1) * d.sub, :d.half]
                    for q in range(n * TILE_PARTS, (n + 1) * TILE_PARTS) for bh in range(2)]
            tbuf[j, n] = jnp.concatenate(rows, axis=0).T

    def hand_out(j, begin, end):
        for n in range(begin, end):
            to = core * CHIPS + n
            block = tbuf.at[j, :, pl.ds(n * d.out_rows, d.out_rows), :]

            @pl.when(to != me)
            def _():
                remote(block, gbuf.at[j, slot], k_send.at[j], k_recv.at[j], to).start()

            @pl.when(to == me)
            def _():
                gbuf[j, slot] = block[...]

    sends_self = me // CHIPS == core
    lanes = lax.broadcasted_iota(jnp.int32, (d.out_rows, d.wide), 1) // d.slab

    def put_out(j, finish=None):
        @pl.when(sends_self)
        def _():
            some = gbuf.at[j, pl.ds(0, CHIPS - 1)]
            remote(some, some, k_send.at[j], k_recv.at[j], me).wait()

        @pl.when(jnp.logical_not(sends_self))
        def _():
            remote(gbuf.at[j], gbuf.at[j], k_send.at[j], k_recv.at[j], me).wait()

        for ct in range(CHIPS // TILE_PARTS):
            for qt in range(d.pair // TILE_PARTS):
                src = [gbuf[j, ct * TILE_PARTS + c, qt] for c in range(TILE_PARTS)]
                if finish is not None:
                    src = [finish(x, gbuf[j - 1, ct * TILE_PARTS + c, qt], ct * TILE_PARTS + c) for c, x in enumerate(src)]
                for q in range(TILE_PARTS):
                    tile = jnp.zeros((d.out_rows, d.wide), jnp.float32)
                    for c in range(TILE_PARTS):
                        shift = (c - q) % TILE_PARTS * d.slab
                        moved = pltpu.roll(src[c], shift, 1) if shift else src[c]
                        tile = jnp.where(lanes == c, moved, tile)
                    tbuf[j, ct, pl.ds(qt * TILE_PARTS + q, d.out_rows, stride=d.pair), :] = tile
            pltpu.make_async_copy(tbuf.at[j, ct], out.at[j, :, pl.ds(ct * d.wide, d.wide)], o_sem.at[j, ct]).start()

    def step(j, carried):
        beta_prev = carried[0]
        sig[...] = jnp.zeros_like(sig)

        def slot_step(t, carry):
            done_right = sum((t > r).astype(jnp.int32) for r in RIGHT_SLOTS)
            done_left = t - done_right
            is_right = sum((t == r).astype(jnp.int32) for r in RIGHT_SLOTS)
            for four in range(0, len(SLOTS), 4):
                @pl.when((t >= four) & (t < four + 4))
                def _():
                    for at in range(four, four + 4):
                        if not SLOTS[at]:
                            continue

                        @pl.when(t == at)
                        def _():
                            for kind, i, p in SLOTS[at]:
                                act(kind, i, p, j)

            @pl.when(is_right == 1)
            def _():
                right_of_piece(done_right // QUARTERS, done_right % QUARTERS)

            @pl.when(is_right == 0)
            def _():
                left_products(done_left // GROUPS, done_left % GROUPS)
            return carry

        @pl.when(j == 0)
        def _():
            lax.fori_loop(0, GROUPS, first_right, 0)
            l_event(5)
            lax.fori_loop(0, GROUPS, first_group, 0)

        @pl.when(j > 0)
        def _():
            lax.fori_loop(0, len(SLOTS), slot_step, 0)
            for p in range(PIECES):
                sent = uv.at[p // QUARTERS, pl.ds(0, 2), pl.ds(0, 15 * d.slab), :]
                remote(sent, sent, u_send.at[p], u_recv.at[p, 0], me).wait_send()

        other = sig.at[:, pl.ds(d.half, d.half)]
        to_other = remote(other, part, p_send, p_recv, partner)
        to_other.start()
        to_other.wait()
        s = sig[:, :d.half] + part[...]
        v = vcur[...]
        w = s - beta_prev * vprev[...]
        sv = jnp.sum(s * v, keepdims=True)
        wv_sum = jnp.sum(w * v, keepdims=True)
        vv = jnp.sum(v * v, keepdims=True)
        guess = jnp.where(vv > 0.0, wv_sum / jnp.where(vv > 0.0, vv, 1.0), 0.0)
        t = w - guess * v
        sig[:, :d.half] = t
        tt = jnp.sum(t * t, keepdims=True)
        tv = jnp.sum(t * v, keepdims=True)
        at_lane = lax.broadcasted_iota(jnp.int32, (1, 128), 1)
        line = jnp.zeros((1, 128), jnp.float32)
        for n, value in enumerate((sv, vv, tt, tv, guess)):
            line = jnp.where(at_lane == n, value, line)
        scs[...] = line
        scr[me] = line

        def tell(n, carry):
            remote(scs, scr.at[me], s_send, s_recv, (me + n) % DEVS).start()
            return carry

        lax.fori_loop(1, DEVS, tell, 0)

        @pl.when(j > 0)
        def _():
            hand_out(j - 1, RESULT_EARLY, CHIPS)

        @pl.when(j == LANCZOS_STEPS - 1)
        def _():
            turn_result(LANCZOS_STEPS - 1, sig)
            hand_out(LANCZOS_STEPS - 1, 0, CHIPS)

        heard = scr.at[pl.ds(0, DEVS - 1)]
        remote(heard, heard, s_send, s_recv, me).wait()
        told = scr[:, 0, :]
        alpha = jnp.sum(told[:, 0:1], axis=0, keepdims=True) / d.vec_size
        off = alpha - told[:, 4:5]
        square = told[:, 2:3] - 2.0 * off * told[:, 3:4] + off * off * told[:, 1:2]
        beta = jnp.sqrt(jnp.sum(square, axis=0, keepdims=True) / d.vec_size)
        vnew = (sig[:, :d.half] - (alpha - guess) * vcur[...]) / beta
        vprev[...] = vcur[...]
        vcur[...] = vnew
        vb = vnew.astype(jnp.bfloat16)

        @pl.when(j < LANCZOS_STEPS - 1)
        def _():
            for ch in range(CHUNKS):
                for bh in range(2):
                    at = pl.ds(pl.multiple_of(slot * d.slab + bh * d.sub, d.sub), d.sub)
                    for q in range(d.pair):
                        uv[ch, q // 2, at, q % 2 * d.chunk:(q % 2 + 1) * d.chunk] = \
                            vb[(bh * d.pair + q) * d.sub:(bh * d.pair + q + 1) * d.sub, ch * d.chunk:(ch + 1) * d.chunk]
        alphas[j] = alpha[0, 0]
        betas[j] = beta[0, 0]
        return beta, alpha


    zero = jnp.zeros((1, 1), jnp.float32)
    last_beta, last_alpha = lax.fori_loop(0, LANCZOS_STEPS, step, (zero, zero))

    for n, part in enumerate((lv.at[0, pl.ds(0, 15), :, 0], lv.at[1, pl.ds(0, 15), :, 0, :, pl.ds(edge, d.bond - edge)],
                              lv.at[0, pl.ds(0, 15), :, 0, :, pl.ds(0, d.half)], lv.at[1, pl.ds(0, 15), :, 0, :, pl.ds(edge, d.half - edge)])):
        remote(part, part, l_send.at[n], l_recv.at[n, 0], me).wait_send()
    swapped = lv.at[:, pl.ds(0, 15), :, 0, :, pl.ds(d.half, d.half)]
    remote(swapped, swapped, f_send, f_recv.at[0], me).wait_send()
    for ch in range(CHUNKS):
        for h in range(2):
            theirs = left.at[:, pl.ds(0, d.chunk), pl.ds(0, d.half)]
            remote(theirs, lv.at[ch, slot, core, :, :, pl.ds(h * d.half, d.half)], d2d_sem.at[ch, h], d2d_recv.at[ch, h], partner).wait_send()
    put_out(LANCZOS_STEPS - 2)

    def finish(block, before, s):
        owner = device(s % 4, s // 4 % 2, s // 8, me // CHIPS)
        return (block - (last_alpha - scr[owner][:, 4:5]) * before) / last_beta

    put_out(LANCZOS_STEPS - 1, finish)
    for j in range(LANCZOS_STEPS):
        for c in range(d.bond // d.wide):
            pltpu.make_async_copy(tbuf.at[j, c], out.at[j, :, pl.ds(c * d.wide, d.wide)], o_sem.at[j, c]).wait()


def solution(mesh):
    def device_body(wavefunction, left_loc, pair_loc, right_loc, flag_loc):
        bond, pair = wavefunction.shape[0], wavefunction.shape[1]
        d = Dims(bond, pair, left_loc.shape[0])
        bf16, f32 = jnp.bfloat16, jnp.float32
        dma = pltpu.SemaphoreType.DMA
        any_space = pl.BlockSpec(memory_space=pl.ANY)
        smem = pl.BlockSpec(memory_space=pltpu.SMEM)
        scalars = jax.ShapeDtypeStruct((LANCZOS_STEPS,), f32)
        later, first, alphas, betas = pl.pallas_call(
            functools.partial(lanczos_kernel, d),
            out_shape=(jax.ShapeDtypeStruct((LANCZOS_STEPS, d.out_rows * pair, bond), f32),
                       jax.ShapeDtypeStruct((d.out_rows * pair, bond), f32), scalars, scalars),
            in_specs=[any_space] * 3 + [pl.BlockSpec(memory_space=pltpu.VMEM), smem],
            out_specs=(any_space, any_space, smem, smem),
            scratch_shapes=[
                pltpu.VMEM((CHUNKS, CHIPS, CORES, d.terms_dev, d.chunk, bond), bf16),
                pltpu.VMEM((CHIPS, CORES, d.terms_dev, d.slab, bond), bf16),
                pltpu.VMEM((d.terms_dev, bond, bond), bf16),
                pltpu.VMEM((CHIPS, CORES, pair, 128), bf16),
                pltpu.VMEM((CHIPS, CORES, d.terms_dev, d.prod, d.prod), bf16),
                pltpu.VMEM((CHUNKS, pair // 2, bond, 2 * d.chunk), bf16),
                pltpu.VMEM((d.lane_tiles, d.half * pair, d.lane), f32),
                pltpu.VMEM((CHIPS * CORES * d.terms_dev, pair, d.sub, 2 * d.chunk), bf16),
                pltpu.VMEM((d.rows, d.group_terms * d.chunk), bf16),
                pltpu.VMEM((d.rows, bond), f32),
                pltpu.VMEM((d.rows, d.half), f32),
                pltpu.VMEM((d.rows, d.half), f32),
                pltpu.VMEM((d.rows, d.half), f32),
                pltpu.VMEM((LANCZOS_STEPS, bond // d.wide, d.half, d.wide), f32),
                pltpu.VMEM((LANCZOS_STEPS, CHIPS, bond // d.wide, d.out_rows, d.wide), f32),
                pltpu.VMEM((1, 128), f32),
                pltpu.VMEM((DEVS, 1, 128), f32),
                pltpu.VMEM((2, 8, 128), f32),
                dma((3, 2)), dma((8, d.lane_tiles)), dma((CHUNKS, 2)), dma((CHUNKS, 2)), dma((2,)), dma((2,)), dma((2,)), dma((2,)),
                dma((4,)), dma((4, CHIPS)), dma, dma((CHIPS,)), dma((PIECES,)), dma((PIECES, CHIPS)),
                dma, dma, dma, dma, dma((LANCZOS_STEPS,)), dma((LANCZOS_STEPS,)), dma, dma, dma((LANCZOS_STEPS, bond // d.wide)), dma((bond // d.wide,)),
            ],
            compiler_params=pltpu.CompilerParams(has_side_effects=True, collective_id=0, vmem_limit_bytes=67043328),
            name='lanczos',
        )(wavefunction.reshape(bond * pair, bond), left_loc, right_loc, pair_loc, flag_loc)
        krylov = jnp.concatenate([first[None], later])
        return krylov.reshape(LANCZOS_STEPS + 1, d.out_rows, pair, bond), alphas, betas

    return jax.shard_map(device_body, mesh=mesh, in_specs=(P(), P(AXIS_NAME), P(AXIS_NAME), P(AXIS_NAME), P(AXIS_NAME)),
                         out_specs=(P(None, AXIS_NAME), P(), P()), check_vma=False)
```

```python
import functools

import jax
import jax.numpy as jnp
from jax import lax
from jax.experimental import pallas as pl
from jax.experimental.pallas import tpu as pltpu
from jax.sharding import PartitionSpec as P

LANCZOS_STEPS = 6
AXIS_NAME = 'terms'
MESH = pl.DeviceIdType.MESH

CHIPS = 16
CORES = 2
DEVS = 32
CHUNKS = 2
GROUPS = 4
TILE_PARTS = 4
QUARTERS = 4
PIECES = CHUNKS * QUARTERS

ALONG, ACROSS, FROM_COLUMN, FROM_SECOND, THIRD, DIAGONAL, RESULT, RESULT_OUT, RESULT_PUT = range(9)
RIGHT_SLOTS = (0, 1, 2, 3, 8, 9, 10, 11)
SLOTS = (
    ((0, 1, 0), (0, 1, 1), (1, 0, 2), (0, 2, 0), (1, 0, 5), (1, 0, 3), (1, 0, 6), (1, 0, 0), (0, 3, 0), (3, 0, 2), (0, 2, 1), (0, 1, 3), (1, 0, 4), (0, 3, 1), (1, 0, 7), (0, 1, 2), (1, 0, 1), (0, 3, 3), (2, 1, 0), (2, 2, 0), (0, 2, 3), (0, 3, 2), (2, 1, 1), (3, 0, 0), (2, 3, 0), (3, 1, 0), (2, 2, 1), (0, 2, 2), (0, 1, 4), (3, 0, 1), (2, 1, 3), (3, 2, 0), (2, 3, 1), (2, 2, 2), (2, 2, 3), (2, 1, 2), (4, 0, 0), (0, 2, 5), (0, 3, 4), (0, 2, 4), (0, 1, 5), (0, 1, 6), (0, 1, 7), (3, 3, 0), (2, 3, 3), (3, 1, 1), (3, 2, 1), (0, 2, 6), (2, 3, 2), (4, 0, 1), (3, 3, 1), (0, 3, 6), (3, 2, 2), (3, 1, 2), (0, 3, 5), (0, 2, 7), (0, 3, 7), (3, 2, 3), (3, 3, 2), (3, 0, 3), (5, 0, 0), (3, 3, 3), (4, 0, 3), (3, 1, 3), (3, 0, 4),),
    ((6, 0, 0), (2, 2, 4), (5, 0, 1), (3, 0, 6), (2, 1, 4), (4, 0, 2),),
    ((2, 2, 6), (5, 0, 2), (2, 1, 6),),
    ((2, 2, 5), (5, 0, 3), (3, 2, 4), (2, 3, 4),),
    ((2, 1, 5), (3, 0, 5), (3, 1, 4),),
    ((2, 3, 5), (3, 2, 5), (2, 3, 6),),
    ((2, 2, 7), (3, 3, 4), (2, 1, 7), (3, 1, 5), (8, 0, 0),),
    ((3, 3, 5), (2, 3, 7), (3, 2, 6), (3, 1, 6), (3, 3, 6),),
    ((3, 0, 7), (3, 1, 7), (3, 2, 7), (4, 0, 5), (5, 0, 4), (4, 0, 4),),
    ((3, 3, 7), (5, 0, 5),),
    ((4, 0, 6), (5, 0, 6),),
    ((4, 0, 7), (5, 0, 7), (7, 0, 0),),
)
RESULT_EARLY = 12


class Dims:
    def __init__(self, bond, pair, terms_dev):
        self.bond = bond
        self.pair = pair
        self.terms_dev = terms_dev
        self.slab = bond // CHIPS
        self.sub = self.slab // 2
        self.half = bond // CORES
        self.chunk = self.half // CHUNKS
        self.rows = self.slab * pair
        self.prod = self.sub * pair
        self.out_rows = bond // DEVS
        self.group_terms = 4 * CORES * terms_dev
        self.vec_size = bond * pair * bond
        self.lane = min(bond, 128)
        self.wide = TILE_PARTS * self.slab
        self.lane_tiles = bond // self.lane


def lanczos_kernel(d, psi, left, right, pair_ops, flags, out, first, alphas, betas, lv, rv, rs, wv, kw, uv, ps, yst, zst, sig, part, vcur, vprev, tbuf, gbuf,
                   scs, scr, nbuf,
                   loc_sem, psi_sem, d2d_sem, d2d_recv, rw_send, rw_recv, fw_send, fw_recv, l_send, l_recv, f_send, f_recv, u_send, u_recv,
                   p_send, p_recv, s_send, s_recv, k_send, k_recv, n_send, n_recv, o_sem, first_sem):
    me = lax.axis_index(AXIS_NAME)
    core = me % 2
    xpos = (me // 2) % 2
    ypos = (me // 4) % 2
    zpos = me // 8

    def device(z, y, x, c):
        return ((z * 2 + y) * 2 + x) * 2 + c

    def chip_slot(z, y, x):
        return (x * 2 + y) * 4 + z

    partner = device(zpos, ypos, xpos, 1 - core)
    slot = chip_slot(zpos, ypos, xpos)
    zs = (zpos, zpos + 1 - 2 * (zpos % 2), (zpos + 2) % 4, 3 - zpos)
    inner = (zpos + 1) // 2 % 2
    zn = (zpos, (1 - inner) * (zpos + 1 - zpos // 3 * 2) + inner * (zpos - 1), (1 - inner) * ((zpos + 2) % 4) + inner * (zpos + 1),
          (1 - inner) * (3 - zpos) + inner * ((zpos + 2) % 4))
    y_two = ypos + (1 - core) * (1 - 2 * ypos)
    x_two = xpos + core * (1 - 2 * xpos)
    y_three = ypos + core * (1 - 2 * ypos)
    x_three = xpos + (1 - core) * (1 - 2 * xpos)
    two = device(zpos, y_two, x_two, core)
    three = device(zpos, y_three, x_three, core)

    def remote(src, dst, send, recv, dev):
        return pltpu.make_async_remote_copy(src_ref=src, dst_ref=dst, send_sem=send, recv_sem=recv, device_id=(dev,), device_id_type=MESH)

    class Gather:
        def __init__(self, block, send, recv):
            self.block, self.send_sem, self.recv_sem = block, send, recv

        def send(self, which, dev):
            remote(self.block(which), self.block(which), self.send_sem, self.recv_sem(which), dev).start()

        def wait(self, which):
            remote(self.block(which), self.block(which), self.send_sem, self.recv_sem(which), me).wait_recv()

        def own_along(self):
            for i in (1, 2, 3):
                self.send(slot, device(zs[i], ypos, xpos, core))

        def own_across(self):
            self.send(slot, three)
            self.send(slot, two)

        def event(self, n):
            i = (n + 1) // 2
            if n % 2:
                which = chip_slot(zs[i], ypos, xpos)
                self.wait(which)
                self.send(which, three)
                self.send(which, two)
            else:
                which = chip_slot(zs[i], y_two, x_two)
                self.wait(which)
                self.send(which, three)

        def last(self, diagonal):
            for i in range(4):
                self.wait(chip_slot(zs[i], 1 - ypos, 1 - xpos) if diagonal else chip_slot(zs[i], y_three, x_three))

    edge = d.chunk
    l_parts = (
        (lambda s: lv.at[0, s, :, core], 0),
        (lambda s: lv.at[1, s, :, core, :, pl.ds(edge, d.bond - edge)], 1),
        (lambda s: lv.at[0, s, :, 1 - core, :, pl.ds(0, d.half)], 2),
        (lambda s: lv.at[1, s, :, 1 - core, :, pl.ds(edge, d.half - edge)], 3),
    )
    l_gathers = [Gather(block, l_send.at[n], lambda s, n=n: l_recv.at[n, s]) for block, n in l_parts]

    def l_swap(s, term):
        part = lv.at[:, s, :, term, :, pl.ds(d.half, d.half)]
        return remote(part, part, f_send, f_recv.at[s], partner)

    def l_event(n):
        i = (n + 1) // 2
        for g in l_gathers:
            g.event(n)
        l_swap(chip_slot(zs[i], ypos, xpos) if n % 2 else chip_slot(zs[i], y_two, x_two), core).start()

    def l_last(diagonal):
        for i in range(4):
            which = chip_slot(zs[i], 1 - ypos, 1 - xpos) if diagonal else chip_slot(zs[i], y_three, x_three)
            for g in l_gathers:
                g.wait(which)
            l_swap(which, core).start()

    def l_fill(s):
        @pl.when(s != slot)
        def _():
            l_swap(s, 1 - core).wait_recv()
            for c in range(CORES):
                tile = lv[:, s, c, 1 - core, :, d.half:].reshape(d.half, d.half).T
                lv[:, s, c, 1 - core, :, d.half:] = tile.reshape(CHUNKS, d.chunk, d.half)
                for t in range(d.terms_dev):
                    lv[1, s, c, t, :, :edge] = lv[0, s, c, t, :, edge:d.half].T

    def l_along():
        for i in (1, 2, 3):
            for g in l_gathers:
                g.send(slot, device(zs[i], ypos, xpos, core))

    def u_block(p):
        return lambda s: uv.at[p // QUARTERS, pl.ds(p % QUARTERS * 2, 2), pl.ds(pl.multiple_of(s * d.slab, d.slab), d.slab), :]

    u_gathers = [Gather(u_block(p), u_send.at[p], lambda s, p=p: u_recv.at[p, s]) for p in range(PIECES)]

    def act(kind, i, p, j):
        g = u_gathers[p]
        if kind == ALONG:
            g.send(slot, device(zn[i], ypos, xpos, core))
        elif kind == ACROSS:
            g.own_across()
        elif kind == FROM_COLUMN:
            which = chip_slot(zn[i], ypos, xpos)
            g.wait(which)
            g.send(which, three)
            g.send(which, two)
        elif kind == FROM_SECOND:
            which = chip_slot(zn[i], y_two, x_two)
            g.wait(which)
            g.send(which, three)
        elif kind == THIRD:
            g.last(False)
        elif kind == DIAGONAL:
            g.last(True)
        elif kind == RESULT:
            turn_result(j - 1, vcur)
        elif kind == RESULT_OUT:
            hand_out(j - 1, 0, RESULT_EARLY)
        elif kind == RESULT_PUT:
            @pl.when(j > 1)
            def _():
                put_out(j - 2)

    all_right = pltpu.make_async_copy(right, rs, loc_sem.at[2, 0])
    all_right.start()

    barrier = pltpu.get_barrier_semaphore()

    def knock(n, carry):
        pl.semaphore_signal(barrier, inc=1, device_id=((me + n) % DEVS,), device_id_type=MESH)
        return carry

    lax.fori_loop(1, DEVS, knock, 0)

    for ch in range(CHUNKS):
        for h in range(2):
            mine = left.at[:, pl.ds(pl.multiple_of(core * d.half + ch * d.chunk, d.chunk), d.chunk),
                           pl.ds(pl.multiple_of((core + h) % 2 * d.half, d.half), d.half)]
            pltpu.make_async_copy(mine, lv.at[ch, slot, core, :, :, pl.ds(h * d.half, d.half)], loc_sem.at[ch, h]).start()

    psi_rows = d.half * d.pair // 8
    psi_copies = [pltpu.make_async_copy(psi.at[pl.ds(pl.multiple_of(core * d.half * d.pair + n * psi_rows, psi_rows), psi_rows),
                                               pl.ds(c * d.lane, d.lane)],
                                        ps.at[c, pl.ds(n * psi_rows, psi_rows), :], psi_sem.at[n, c])
                  for n in range(8) for c in range(d.lane_tiles)]
    for copy in psi_copies:
        copy.start()

    first_rows = d.out_rows * d.pair
    first_copies = [pltpu.make_async_copy(psi.at[pl.ds(pl.multiple_of(me * first_rows, first_rows), first_rows), pl.ds(c * d.wide, d.wide)],
                                          tbuf.at[LANCZOS_STEPS - 1, c], first_sem.at[c]) for c in range(d.bond // d.wide)]
    for copy in first_copies:
        copy.start()

    side_by_side = jnp.zeros((d.pair, 128), jnp.float32)
    for t in range(d.terms_dev):
        place_of = lax.broadcasted_iota(jnp.int32, (d.pair, 128), 1) == lax.broadcasted_iota(jnp.int32, (d.pair, 128), 0) + t * d.pair
        place_of = jnp.where(place_of, 1.0, 0.0).astype(jnp.bfloat16)
        side_by_side += jnp.dot(pair_ops[t], place_of, preferred_element_type=jnp.float32)
    wv[slot, core] = side_by_side.astype(jnp.bfloat16)
    all_right.wait()
    some_rows = d.bond // 8

    def one_sided(i, carry):
        at = pl.ds(pl.multiple_of(i * some_rows, some_rows), some_rows)
        row = lax.broadcasted_iota(jnp.int32, (some_rows, d.bond), 0) + i * some_rows
        one = jnp.where(row == lax.broadcasted_iota(jnp.int32, (some_rows, d.bond), 1), 1.0, 0.0)
        for t in range(d.terms_dev):
            rs[t, at, :] = jnp.where(flags[t] == 1, rs[t, at, :].astype(jnp.float32), one).astype(jnp.bfloat16)
        return carry

    lax.fori_loop(0, 8, one_sided, 0)

    def right_rows(s):
        return rs.at[:, pl.ds(pl.multiple_of(s * d.slab, d.slab), d.slab), :]

    rv[slot, core] = rs[:, pl.ds(pl.multiple_of(slot * d.slab, d.slab), d.slab), :]

    pl.semaphore_wait(barrier, DEVS - 1)
    for ch in range(CHUNKS):
        for h in range(2):
            theirs = left.at[:, pl.ds(pl.multiple_of((1 - core) * d.half + ch * d.chunk, d.chunk), d.chunk),
                             pl.ds(pl.multiple_of((1 - core + h) % 2 * d.half, d.half), d.half)]
            remote(theirs, lv.at[ch, slot, core, :, :, pl.ds(h * d.half, d.half)], d2d_sem.at[ch, h], d2d_recv.at[ch, h], partner).start()
    for n in range(1, CHIPS):
        chip = (me // 2 + n) % CHIPS
        to = chip_slot(chip // 4, chip // 2 % 2, chip % 2)
        remote(right_rows(to), rv.at[slot, core], rw_send.at[0], rw_recv.at[0], chip * 2 + core).start()
        remote(wv.at[slot, core], wv.at[slot, core], rw_send.at[1], rw_recv.at[1], chip * 2 + core).start()

    for ch in range(CHUNKS):
        for h in range(2):
            pltpu.make_async_copy(lv.at[ch, slot, core, :, :, pl.ds(h * d.half, d.half)], lv.at[ch, slot, core, :, :, pl.ds(h * d.half, d.half)], loc_sem.at[ch, h]).wait()
            back = remote(lv.at[ch, slot, 1 - core, :, :, pl.ds(h * d.half, d.half)], lv.at[ch, slot, 1 - core, :, :, pl.ds(h * d.half, d.half)], d2d_sem.at[ch, h], d2d_recv.at[ch, h], partner)
            back.wait_recv()
    l_along()
    for g in l_gathers:
        g.own_across()

    total = jnp.zeros((8, d.lane), jnp.float32)
    for n in range(8):
        for copy in psi_copies[n * d.lane_tiles:(n + 1) * d.lane_tiles]:
            copy.wait()

        def add_rows(i, acc, n=n):
            x = ps[:, pl.ds(pl.multiple_of(n * psi_rows + i * (psi_rows // 8), 8), psi_rows // 8), :]
            return acc + jnp.sum((x * x).reshape(d.lane_tiles * psi_rows // 64, 8, d.lane), axis=0)

        total = lax.fori_loop(0, 8, add_rows, total)
    nbuf[0] = jnp.broadcast_to(jnp.sum(total, keepdims=True), (8, 128))
    to_partner = remote(nbuf.at[0], nbuf.at[1], n_send, n_recv, partner)
    to_partner.start()
    to_partner.wait()
    norm = jnp.sqrt((nbuf[0] + nbuf[1])[0:1, :] / d.vec_size)
    norm_one = norm[:, 0:1]
    for copy in first_copies:
        copy.wait()
    tbuf[LANCZOS_STEPS - 1] = tbuf[LANCZOS_STEPS - 1] / norm_one[None]
    first_out = [pltpu.make_async_copy(tbuf.at[LANCZOS_STEPS - 1, c], first.at[:, pl.ds(c * d.wide, d.wide)], first_sem.at[c])
                 for c in range(d.bond // d.wide)]
    for copy in first_out:
        copy.start()

    def place(q):
        tiles = [(ps[c, pl.ds(q, d.half, stride=d.pair), :] / norm_one).T for c in range(d.lane_tiles)]
        xt = jnp.concatenate(tiles, axis=0)
        vprev[...] = xt
        return xt.astype(jnp.bfloat16)

    def start_vector(qb, carry):
        for q2 in range(2):
            q = qb * 2 + q2
            xb = place(q)
            for ch in range(CHUNKS):
                uv[ch, qb, :, q2 * d.chunk:(q2 + 1) * d.chunk] = xb[:, ch * d.chunk:(ch + 1) * d.chunk]
            for bh in range(2):
                rows = vprev[pl.ds(pl.multiple_of(slot * d.slab + bh * d.sub, d.sub), d.sub), :]
                vcur[pl.ds(pl.multiple_of((bh * d.pair + q) * d.sub, d.sub), d.sub), :] = rows
        return carry

    lax.fori_loop(0, d.pair // 4, start_vector, 0)
    fifteen = rv.at[pl.ds(0, CHIPS - 1), 0]
    fifteen_w = wv.at[pl.ds(0, CHIPS - 1), 0]
    remote(fifteen, fifteen, rw_send.at[0], rw_recv.at[0], me).wait()
    remote(fifteen_w, fifteen_w, rw_send.at[1], rw_recv.at[1], me).wait()
    fw_right = remote(rv.at[:, core], rv.at[:, core], fw_send.at[0], fw_recv.at[0], partner)
    fw_pair = remote(wv.at[:, core], wv.at[:, core], fw_send.at[1], fw_recv.at[1], partner)
    fw_right.start()
    fw_pair.start()
    l_event(0)
    l_event(1)
    lax.fori_loop(d.pair // 4, d.pair // 2, start_vector, 0)
    l_event(2)
    l_event(3)
    fw_right.wait()
    fw_pair.wait()
    lane = lax.broadcasted_iota(jnp.int32, (d.sub, d.prod), 1)
    row = lax.broadcasted_iota(jnp.int32, (d.sub, d.prod), 0)
    diagonal = lane % d.sub == row

    for t in range(d.terms_dev):
        at_row = lax.broadcasted_iota(jnp.int32, (128, d.prod), 0)
        wide = jnp.where(at_row == lax.broadcasted_iota(jnp.int32, (128, d.prod), 1) // d.sub + t * d.pair, 1.0, 0.0).astype(jnp.bfloat16)
        spread = jnp.dot(wv[...].reshape(CHIPS * CORES * d.pair, 128), wide, preferred_element_type=jnp.float32)
        zst[0, :, t * d.prod:(t + 1) * d.prod] = spread.astype(jnp.bfloat16)

    def spread_pair(s, carry):
        for c in range(2):
            for t in range(d.terms_dev):
                w = zst[0, pl.ds(pl.multiple_of((s * CORES + c) * d.pair, d.pair), d.pair), t * d.prod:(t + 1) * d.prod].astype(jnp.float32)
                for q in range(d.pair):
                    full = jnp.where(diagonal, jnp.broadcast_to(w[q:q + 1, :], (d.sub, d.prod)), 0.0)
                    kw[s, c, t, q * d.sub:(q + 1) * d.sub, :] = full.astype(jnp.bfloat16)
        return carry

    lax.fori_loop(0, CHIPS, spread_pair, 0)
    vprev[...] = jnp.zeros_like(vprev)
    for copy in first_out:
        copy.wait()

    def right_product(grp, ch, qb, to):
        r_all = rv[pl.ds(grp * 4, 4)].reshape(d.group_terms * d.slab, d.bond)
        y = jnp.dot(r_all, uv[ch, qb], preferred_element_type=jnp.float32).astype(jnp.bfloat16)
        y = y.reshape(d.group_terms, 2, d.sub, 2 * d.chunk)
        for q2 in range(2):
            for bh in range(2):
                yst[pl.ds(to * d.group_terms, d.group_terms), qb * 2 + q2, :, bh * d.chunk:(bh + 1) * d.chunk] = \
                    y[:, bh, :, q2 * d.chunk:(q2 + 1) * d.chunk]

    def right_of_piece(ch, part):
        for qb in range(2):
            for grp in range(GROUPS):
                right_product(grp, ch, part * 2 + qb, grp)

    def right_of_group(grp, ch, to):
        for qb in range(d.pair // 2):
            right_product(grp, ch, qb, to)

    def pair_products(grp, at, side):
        for k in range(d.group_terms):
            w = kw[grp * 4 + k // 4, k // 2 % 2, k % 2]
            z = jnp.dot(w, yst[at * d.group_terms + k].reshape(d.prod, 2 * d.chunk), preferred_element_type=jnp.float32).astype(jnp.bfloat16)
            for bh in range(2):
                zst[side, bh * d.prod:(bh + 1) * d.prod, k * d.chunk:(k + 1) * d.chunk] = z[:, bh * d.chunk:(bh + 1) * d.chunk]

    def sum_left(ch, grp, side):
        l_all = lv[ch, pl.ds(grp * 4, 4)].reshape(d.group_terms * d.chunk, d.bond)
        sig[...] += jnp.dot(zst[side], l_all, preferred_element_type=jnp.float32)

    def left_products(ch, grp, at=None):
        pair_products(grp, grp if at is None else at, 0)
        sum_left(ch, grp, 0)

    def last_products():
        pair_products(0, 0, 0)

        def both(grp, carry):
            sum_left(CHUNKS - 1, grp - 1, (grp - 1) % 2)
            pair_products(grp, grp, grp % 2)
            return carry

        lax.fori_loop(1, GROUPS, both, 0)
        sum_left(CHUNKS - 1, GROUPS - 1, (GROUPS - 1) % 2)

    def first_right(grp, carry):
        right_of_group(grp, 0, grp)

        @pl.when(grp == 1)
        def _():
            l_event(4)
        return carry

    def first_group(n, carry):
        own, third = xpos * 2 + ypos, x_three * 2 + y_three
        grp = jnp.where(n == 0, own, jnp.where(n == 1, x_two * 2 + y_two, jnp.where(n == 2, third, 3 - own)))
        spare = jnp.where(n == 3, own, grp)

        @pl.when(n == 1)
        def _():
            l_event(6)
            l_last(False)

        @pl.when(n == 3)
        def _():
            right_of_group(grp, 1, spare)
            l_last(True)

        def fill(z, carry):
            l_fill(grp * 4 + z)
            return carry

        lax.fori_loop(0, 4, fill, 0)

        def chunk_products(ch, carry):
            left_products(ch, grp, (1 - ch) * grp + ch * spare)

            @pl.when((ch == 0) & (n < 3))
            def _():
                right_of_group(grp, 1, spare)
            return carry

        lax.fori_loop(0, CHUNKS, chunk_products, 0)
        return carry

    def turn_result(j, vector):
        for n in range(d.pair // TILE_PARTS):
            rows = [vector[(bh * d.pair + q) * d.sub:(bh * d.pair + q + 1) * d.sub, :d.half]
                    for q in range(n * TILE_PARTS, (n + 1) * TILE_PARTS) for bh in range(2)]
            tbuf[j, n] = jnp.concatenate(rows, axis=0).T

    def hand_out(j, begin, end):
        for n in range(begin, end):
            to = core * CHIPS + n
            block = tbuf.at[j, :, pl.ds(n * d.out_rows, d.out_rows), :]

            @pl.when(to != me)
            def _():
                remote(block, gbuf.at[j, slot], k_send.at[j], k_recv.at[j], to).start()

            @pl.when(to == me)
            def _():
                gbuf[j, slot] = block[...]

    sends_self = me // CHIPS == core
    lanes = lax.broadcasted_iota(jnp.int32, (d.out_rows, d.wide), 1) // d.slab

    def put_out(j, finish=None):
        @pl.when(sends_self)
        def _():
            some = gbuf.at[j, pl.ds(0, CHIPS - 1)]
            remote(some, some, k_send.at[j], k_recv.at[j], me).wait()

        @pl.when(jnp.logical_not(sends_self))
        def _():
            remote(gbuf.at[j], gbuf.at[j], k_send.at[j], k_recv.at[j], me).wait()

        for ct in range(CHIPS // TILE_PARTS):
            for qt in range(d.pair // TILE_PARTS):
                src = [gbuf[j, ct * TILE_PARTS + c, qt] for c in range(TILE_PARTS)]
                if finish is not None:
                    src = [finish(x, gbuf[j - 1, ct * TILE_PARTS + c, qt], ct * TILE_PARTS + c) for c, x in enumerate(src)]
                for q in range(TILE_PARTS):
                    tile = jnp.zeros((d.out_rows, d.wide), jnp.float32)
                    for c in range(TILE_PARTS):
                        shift = (c - q) % TILE_PARTS * d.slab
                        moved = pltpu.roll(src[c], shift, 1) if shift else src[c]
                        tile = jnp.where(lanes == c, moved, tile)
                    tbuf[j, ct, pl.ds(qt * TILE_PARTS + q, d.out_rows, stride=d.pair), :] = tile
            pltpu.make_async_copy(tbuf.at[j, ct], out.at[j, :, pl.ds(ct * d.wide, d.wide)], o_sem.at[j, ct]).start()

    def step(j, carried):
        beta_prev = carried[0]
        sig[...] = jnp.zeros_like(sig)

        def slot_step(t, carry):
            done_right = sum((t > r).astype(jnp.int32) for r in RIGHT_SLOTS)
            done_left = t - done_right
            is_right = sum((t == r).astype(jnp.int32) for r in RIGHT_SLOTS)
            for four in range(0, len(SLOTS), 4):
                @pl.when((t >= four) & (t < four + 4))
                def _():
                    for at in range(four, min(four + 4, len(SLOTS))):
                        if not SLOTS[at]:
                            continue

                        @pl.when(t == at)
                        def _():
                            for kind, i, p in SLOTS[at]:
                                act(kind, i, p, j)

            @pl.when(is_right == 1)
            def _():
                right_of_piece(done_right // QUARTERS, done_right % QUARTERS)

            @pl.when((is_right == 0) & (done_left < GROUPS))
            def _():
                left_products(0, done_left)

            return carry

        @pl.when(j == 0)
        def _():
            lax.fori_loop(0, GROUPS, first_right, 0)
            l_event(5)
            lax.fori_loop(0, GROUPS, first_group, 0)

        @pl.when(j > 0)
        def _():
            lax.fori_loop(0, len(SLOTS), slot_step, 0)
            last_products()
            for p in range(PIECES):
                sent = uv.at[p // QUARTERS, pl.ds(0, 2), pl.ds(0, 15 * d.slab), :]
                remote(sent, sent, u_send.at[p], u_recv.at[p, 0], me).wait_send()

        other = sig.at[:, pl.ds(d.half, d.half)]
        to_other = remote(other, part, p_send, p_recv, partner)
        to_other.start()
        to_other.wait()
        s = sig[:, :d.half] + part[...]
        v = vcur[...]
        w = s - beta_prev * vprev[...]
        sv = jnp.sum(s * v, keepdims=True)
        wv_sum = jnp.sum(w * v, keepdims=True)
        vv = jnp.sum(v * v, keepdims=True)
        guess = jnp.where(vv > 0.0, wv_sum / jnp.where(vv > 0.0, vv, 1.0), 0.0)
        t = w - guess * v
        sig[:, :d.half] = t
        tt = jnp.sum(t * t, keepdims=True)
        tv = jnp.sum(t * v, keepdims=True)
        at_lane = lax.broadcasted_iota(jnp.int32, (1, 128), 1)
        line = jnp.zeros((1, 128), jnp.float32)
        for n, value in enumerate((sv, vv, tt, tv, guess)):
            line = jnp.where(at_lane == n, value, line)
        scs[...] = line
        scr[me] = line

        def tell(n, carry):
            remote(scs, scr.at[me], s_send, s_recv, (me + n) % DEVS).start()
            return carry

        lax.fori_loop(1, DEVS, tell, 0)

        @pl.when(j > 0)
        def _():
            hand_out(j - 1, RESULT_EARLY, CHIPS)

        @pl.when(j == LANCZOS_STEPS - 1)
        def _():
            turn_result(LANCZOS_STEPS - 1, sig)
            hand_out(LANCZOS_STEPS - 1, 0, CHIPS)

        heard = scr.at[pl.ds(0, DEVS - 1)]
        remote(heard, heard, s_send, s_recv, me).wait()
        told = scr[:, 0, :]
        alpha = jnp.sum(told[:, 0:1], axis=0, keepdims=True) / d.vec_size
        off = alpha - told[:, 4:5]
        square = told[:, 2:3] - 2.0 * off * told[:, 3:4] + off * off * told[:, 1:2]
        beta = jnp.sqrt(jnp.sum(square, axis=0, keepdims=True) / d.vec_size)
        vnew = (sig[:, :d.half] - (alpha - guess) * vcur[...]) / beta
        vprev[...] = vcur[...]
        vcur[...] = vnew
        vb = vnew.astype(jnp.bfloat16)

        @pl.when(j < LANCZOS_STEPS - 1)
        def _():
            for ch in range(CHUNKS):
                for bh in range(2):
                    at = pl.ds(pl.multiple_of(slot * d.slab + bh * d.sub, d.sub), d.sub)
                    for q in range(d.pair):
                        uv[ch, q // 2, at, q % 2 * d.chunk:(q % 2 + 1) * d.chunk] = \
                            vb[(bh * d.pair + q) * d.sub:(bh * d.pair + q + 1) * d.sub, ch * d.chunk:(ch + 1) * d.chunk]
        alphas[j] = alpha[0, 0]
        betas[j] = beta[0, 0]
        return beta, alpha


    zero = jnp.zeros((1, 1), jnp.float32)
    last_beta, last_alpha = lax.fori_loop(0, LANCZOS_STEPS, step, (zero, zero))

    for n, part in enumerate((lv.at[0, pl.ds(0, 15), :, 0], lv.at[1, pl.ds(0, 15), :, 0, :, pl.ds(edge, d.bond - edge)],
                              lv.at[0, pl.ds(0, 15), :, 0, :, pl.ds(0, d.half)], lv.at[1, pl.ds(0, 15), :, 0, :, pl.ds(edge, d.half - edge)])):
        remote(part, part, l_send.at[n], l_recv.at[n, 0], me).wait_send()
    swapped = lv.at[:, pl.ds(0, 15), :, 0, :, pl.ds(d.half, d.half)]
    remote(swapped, swapped, f_send, f_recv.at[0], me).wait_send()
    for ch in range(CHUNKS):
        for h in range(2):
            theirs = left.at[:, pl.ds(0, d.chunk), pl.ds(0, d.half)]
            remote(theirs, lv.at[ch, slot, core, :, :, pl.ds(h * d.half, d.half)], d2d_sem.at[ch, h], d2d_recv.at[ch, h], partner).wait_send()
    put_out(LANCZOS_STEPS - 2)

    def finish(block, before, s):
        owner = device(s % 4, s // 4 % 2, s // 8, me // CHIPS)
        return (block - (last_alpha - scr[owner][:, 4:5]) * before) / last_beta

    put_out(LANCZOS_STEPS - 1, finish)
    for j in range(LANCZOS_STEPS):
        for c in range(d.bond // d.wide):
            pltpu.make_async_copy(tbuf.at[j, c], out.at[j, :, pl.ds(c * d.wide, d.wide)], o_sem.at[j, c]).wait()


def join_kernel(first, later, out):
    @pl.when(pl.program_id(0) == 0)
    def _():
        out[0] = first[...]

    @pl.when(pl.program_id(0) > 0)
    def _():
        out[...] = later[...]


def solution(mesh):
    def device_body(wavefunction, left_loc, pair_loc, right_loc, flag_loc):
        bond, pair = wavefunction.shape[0], wavefunction.shape[1]
        d = Dims(bond, pair, left_loc.shape[0])
        bf16, f32 = jnp.bfloat16, jnp.float32
        dma = pltpu.SemaphoreType.DMA
        any_space = pl.BlockSpec(memory_space=pl.ANY)
        smem = pl.BlockSpec(memory_space=pltpu.SMEM)
        scalars = jax.ShapeDtypeStruct((LANCZOS_STEPS,), f32)
        later, first, alphas, betas = pl.pallas_call(
            functools.partial(lanczos_kernel, d),
            out_shape=(jax.ShapeDtypeStruct((LANCZOS_STEPS, d.out_rows * pair, bond), f32),
                       jax.ShapeDtypeStruct((d.out_rows * pair, bond), f32), scalars, scalars),
            in_specs=[any_space] * 3 + [pl.BlockSpec(memory_space=pltpu.VMEM), smem],
            out_specs=(any_space, any_space, smem, smem),
            scratch_shapes=[
                pltpu.VMEM((CHUNKS, CHIPS, CORES, d.terms_dev, d.chunk, bond), bf16),
                pltpu.VMEM((CHIPS, CORES, d.terms_dev, d.slab, bond), bf16),
                pltpu.VMEM((d.terms_dev, bond, bond), bf16),
                pltpu.VMEM((CHIPS, CORES, pair, 128), bf16),
                pltpu.VMEM((CHIPS, CORES, d.terms_dev, d.prod, d.prod), bf16),
                pltpu.VMEM((CHUNKS, pair // 2, bond, 2 * d.chunk), bf16),
                pltpu.VMEM((d.lane_tiles, d.half * pair, d.lane), f32),
                pltpu.VMEM((CHIPS * CORES * d.terms_dev, pair, d.sub, 2 * d.chunk), bf16),
                pltpu.VMEM((2, d.rows, d.group_terms * d.chunk), bf16),
                pltpu.VMEM((d.rows, bond), f32),
                pltpu.VMEM((d.rows, d.half), f32),
                pltpu.VMEM((d.rows, d.half), f32),
                pltpu.VMEM((d.rows, d.half), f32),
                pltpu.VMEM((LANCZOS_STEPS, bond // d.wide, d.half, d.wide), f32),
                pltpu.VMEM((LANCZOS_STEPS, CHIPS, bond // d.wide, d.out_rows, d.wide), f32),
                pltpu.VMEM((1, 128), f32),
                pltpu.VMEM((DEVS, 1, 128), f32),
                pltpu.VMEM((2, 8, 128), f32),
                dma((3, 2)), dma((8, d.lane_tiles)), dma((CHUNKS, 2)), dma((CHUNKS, 2)), dma((2,)), dma((2,)), dma((2,)), dma((2,)),
                dma((4,)), dma((4, CHIPS)), dma, dma((CHIPS,)), dma((PIECES,)), dma((PIECES, CHIPS)),
                dma, dma, dma, dma, dma((LANCZOS_STEPS,)), dma((LANCZOS_STEPS,)), dma, dma, dma((LANCZOS_STEPS, bond // d.wide)), dma((bond // d.wide,)),
            ],
            compiler_params=pltpu.CompilerParams(has_side_effects=True, collective_id=0, vmem_limit_bytes=67043328),
            name='lanczos',
        )(wavefunction.reshape(bond * pair, bond), left_loc, right_loc, pair_loc, flag_loc)
        block = (1, d.out_rows * pair, bond)
        krylov = pl.pallas_call(
            join_kernel,
            out_shape=jax.ShapeDtypeStruct((LANCZOS_STEPS + 1,) + block[1:], f32),
            grid=(LANCZOS_STEPS + 1,),
            in_specs=[pl.BlockSpec(block[1:], lambda i: (0, 0)), pl.BlockSpec(block, lambda i: (jnp.maximum(i - 1, 0), 0, 0))],
            out_specs=pl.BlockSpec(block, lambda i: (i, 0, 0)),
            compiler_params=pltpu.CompilerParams(vmem_limit_bytes=8 * 1024 * 1024),
            name='join',
        )(first, later)
        return krylov.reshape(LANCZOS_STEPS + 1, d.out_rows, pair, bond), alphas, betas

    return jax.shard_map(device_body, mesh=mesh, in_specs=(P(), P(AXIS_NAME), P(AXIS_NAME), P(AXIS_NAME), P(AXIS_NAME)),
                         out_specs=(P(None, AXIS_NAME), P(), P()), check_vma=False)
```

```python
import functools

import jax
import jax.numpy as jnp
from jax import lax
from jax.experimental import pallas as pl
from jax.experimental.pallas import tpu as pltpu
from jax.sharding import PartitionSpec as P

LANCZOS_STEPS = 6
AXIS_NAME = 'terms'
MESH = pl.DeviceIdType.MESH

CHIPS = 16
CORES = 2
DEVS = 32
CHUNKS = 2
GROUPS = 4
TILE_PARTS = 4
QUARTERS = 4
PIECES = CHUNKS * QUARTERS

ALONG, ACROSS, FROM_COLUMN, FROM_SECOND, THIRD, DIAGONAL, RESULT, RESULT_OUT, RESULT_PUT = range(9)
RIGHT_SLOTS = (0, 1, 2, 3, 8, 9, 10, 11)
SLOTS = (
    ((0, 1, 0), (0, 1, 1), (1, 0, 2), (0, 2, 0), (1, 0, 5), (1, 0, 3), (1, 0, 6), (1, 0, 0), (0, 3, 0), (3, 0, 2), (0, 2, 1), (0, 1, 3), (1, 0, 4), (0, 3, 1), (1, 0, 7), (0, 1, 2), (1, 0, 1), (0, 3, 3), (2, 1, 0), (2, 2, 0), (0, 2, 3), (0, 3, 2), (2, 1, 1), (3, 0, 0), (2, 3, 0), (3, 1, 0), (2, 2, 1), (0, 2, 2), (0, 1, 4), (3, 0, 1), (2, 1, 3), (3, 2, 0), (2, 3, 1), (2, 2, 2), (2, 2, 3), (2, 1, 2), (4, 0, 0), (0, 2, 5), (0, 3, 4), (0, 2, 4), (0, 1, 5), (0, 1, 6), (0, 1, 7), (3, 3, 0), (2, 3, 3), (3, 1, 1), (3, 2, 1), (0, 2, 6), (2, 3, 2), (4, 0, 1), (3, 3, 1), (0, 3, 6), (3, 2, 2), (3, 1, 2), (0, 3, 5), (0, 2, 7), (0, 3, 7), (3, 2, 3), (3, 3, 2), (3, 0, 3), (5, 0, 0), (3, 3, 3), (4, 0, 3), (3, 1, 3), (3, 0, 4),),
    ((6, 0, 0), (2, 2, 4), (5, 0, 1), (3, 0, 6), (2, 1, 4), (4, 0, 2),),
    ((2, 2, 6), (5, 0, 2), (2, 1, 6),),
    ((2, 2, 5), (5, 0, 3), (3, 2, 4), (2, 3, 4),),
    ((2, 1, 5), (3, 0, 5), (3, 1, 4),),
    ((2, 3, 5), (3, 2, 5), (2, 3, 6),),
    ((2, 2, 7), (3, 3, 4), (2, 1, 7), (3, 1, 5), (8, 0, 0),),
    ((3, 3, 5), (2, 3, 7), (3, 2, 6), (3, 1, 6), (3, 3, 6),),
    ((3, 0, 7), (3, 1, 7), (3, 2, 7), (4, 0, 5), (5, 0, 4), (4, 0, 4), (7, 0, 0),),
    ((3, 3, 7), (5, 0, 5),),
    ((4, 0, 6), (5, 0, 6),),
    ((4, 0, 7), (5, 0, 7), (7, 1, 0),),
    (),
    (),
    (),
    (),
)
RESULT_PARTS = ((0, 4), (4, 12), (12, 16))


class Dims:
    def __init__(self, bond, pair, terms_dev):
        self.bond = bond
        self.pair = pair
        self.terms_dev = terms_dev
        self.slab = bond // CHIPS
        self.sub = self.slab // 2
        self.half = bond // CORES
        self.chunk = self.half // CHUNKS
        self.rows = self.slab * pair
        self.prod = self.sub * pair
        self.out_rows = bond // DEVS
        self.group_terms = 4 * CORES * terms_dev
        self.vec_size = bond * pair * bond
        self.lane = min(bond, 128)
        self.wide = TILE_PARTS * self.slab
        self.lane_tiles = bond // self.lane


def lanczos_kernel(d, psi, left, right, pair_ops, flags, out, first, alphas, betas, lv, rv, rs, wv, kw, uv, ps, yst, zst, sig, part, vcur, vprev, tbuf, gbuf,
                   scs, scr, nbuf,
                   loc_sem, psi_sem, d2d_sem, d2d_recv, rw_send, rw_recv, fw_send, fw_recv, l_send, l_recv, f_send, f_recv, u_send, u_recv,
                   p_send, p_recv, s_send, s_recv, k_send, k_recv, n_send, n_recv, o_sem, first_sem):
    me = lax.axis_index(AXIS_NAME)
    core = me % 2
    xpos = (me // 2) % 2
    ypos = (me // 4) % 2
    zpos = me // 8

    def device(z, y, x, c):
        return ((z * 2 + y) * 2 + x) * 2 + c

    def chip_slot(z, y, x):
        return (x * 2 + y) * 4 + z

    partner = device(zpos, ypos, xpos, 1 - core)
    slot = chip_slot(zpos, ypos, xpos)
    zs = (zpos, zpos + 1 - 2 * (zpos % 2), (zpos + 2) % 4, 3 - zpos)
    inner = (zpos + 1) // 2 % 2
    zn = (zpos, (1 - inner) * (zpos + 1 - zpos // 3 * 2) + inner * (zpos - 1), (1 - inner) * ((zpos + 2) % 4) + inner * (zpos + 1),
          (1 - inner) * (3 - zpos) + inner * ((zpos + 2) % 4))
    y_two = ypos + (1 - core) * (1 - 2 * ypos)
    x_two = xpos + core * (1 - 2 * xpos)
    y_three = ypos + core * (1 - 2 * ypos)
    x_three = xpos + (1 - core) * (1 - 2 * xpos)
    two = device(zpos, y_two, x_two, core)
    three = device(zpos, y_three, x_three, core)

    def remote(src, dst, send, recv, dev):
        return pltpu.make_async_remote_copy(src_ref=src, dst_ref=dst, send_sem=send, recv_sem=recv, device_id=(dev,), device_id_type=MESH)

    class Gather:
        def __init__(self, block, send, recv):
            self.block, self.send_sem, self.recv_sem = block, send, recv

        def send(self, which, dev):
            remote(self.block(which), self.block(which), self.send_sem, self.recv_sem(which), dev).start()

        def wait(self, which):
            remote(self.block(which), self.block(which), self.send_sem, self.recv_sem(which), me).wait_recv()

        def own_along(self):
            for i in (1, 2, 3):
                self.send(slot, device(zs[i], ypos, xpos, core))

        def own_across(self):
            self.send(slot, three)
            self.send(slot, two)

        def event(self, n):
            i = (n + 1) // 2
            if n % 2:
                which = chip_slot(zs[i], ypos, xpos)
                self.wait(which)
                self.send(which, three)
                self.send(which, two)
            else:
                which = chip_slot(zs[i], y_two, x_two)
                self.wait(which)
                self.send(which, three)

        def last(self, diagonal):
            for i in range(4):
                self.wait(chip_slot(zs[i], 1 - ypos, 1 - xpos) if diagonal else chip_slot(zs[i], y_three, x_three))

    edge = d.chunk
    l_parts = (
        (lambda s: lv.at[0, s, :, core], 0),
        (lambda s: lv.at[1, s, :, core, :, pl.ds(edge, d.bond - edge)], 1),
        (lambda s: lv.at[0, s, :, 1 - core, :, pl.ds(0, d.half)], 2),
        (lambda s: lv.at[1, s, :, 1 - core, :, pl.ds(edge, d.half - edge)], 3),
    )
    l_gathers = [Gather(block, l_send.at[n], lambda s, n=n: l_recv.at[n, s]) for block, n in l_parts]

    def l_swap(s, term):
        part = lv.at[:, s, :, term, :, pl.ds(d.half, d.half)]
        return remote(part, part, f_send, f_recv.at[s], partner)

    def l_event(n):
        i = (n + 1) // 2
        for g in l_gathers:
            g.event(n)
        l_swap(chip_slot(zs[i], ypos, xpos) if n % 2 else chip_slot(zs[i], y_two, x_two), core).start()

    def l_last(diagonal):
        for i in range(4):
            which = chip_slot(zs[i], 1 - ypos, 1 - xpos) if diagonal else chip_slot(zs[i], y_three, x_three)
            for g in l_gathers:
                g.wait(which)
            l_swap(which, core).start()

    def l_fill(s):
        @pl.when(s != slot)
        def _():
            l_swap(s, 1 - core).wait_recv()
            for c in range(CORES):
                tile = lv[:, s, c, 1 - core, :, d.half:].reshape(d.half, d.half).T
                lv[:, s, c, 1 - core, :, d.half:] = tile.reshape(CHUNKS, d.chunk, d.half)
                for t in range(d.terms_dev):
                    lv[1, s, c, t, :, :edge] = lv[0, s, c, t, :, edge:d.half].T

    def l_along():
        for i in (1, 2, 3):
            for g in l_gathers:
                g.send(slot, device(zs[i], ypos, xpos, core))

    def u_block(p):
        return lambda s: uv.at[p // QUARTERS, pl.ds(p % QUARTERS * 2, 2), pl.ds(pl.multiple_of(s * d.slab, d.slab), d.slab), :]

    u_gathers = [Gather(u_block(p), u_send.at[p], lambda s, p=p: u_recv.at[p, s]) for p in range(PIECES)]

    def act(kind, i, p, j):
        g = u_gathers[p]
        if kind == ALONG:
            g.send(slot, device(zn[i], ypos, xpos, core))
        elif kind == ACROSS:
            g.own_across()
        elif kind == FROM_COLUMN:
            which = chip_slot(zn[i], ypos, xpos)
            g.wait(which)
            g.send(which, three)
            g.send(which, two)
        elif kind == FROM_SECOND:
            which = chip_slot(zn[i], y_two, x_two)
            g.wait(which)
            g.send(which, three)
        elif kind == THIRD:
            g.last(False)
        elif kind == DIAGONAL:
            g.last(True)
        elif kind == RESULT:
            turn_result(j - 1, vcur)
        elif kind == RESULT_OUT:
            hand_out(j - 1, *RESULT_PARTS[i])
        elif kind == RESULT_PUT:
            @pl.when(j > 1)
            def _():
                put_out(j - 2)

    all_right = pltpu.make_async_copy(right, rs, loc_sem.at[2, 0])
    all_right.start()

    barrier = pltpu.get_barrier_semaphore()

    def knock(n, carry):
        pl.semaphore_signal(barrier, inc=1, device_id=((me + n) % DEVS,), device_id_type=MESH)
        return carry

    lax.fori_loop(1, DEVS, knock, 0)

    for ch in range(CHUNKS):
        for h in range(2):
            mine = left.at[:, pl.ds(pl.multiple_of(core * d.half + ch * d.chunk, d.chunk), d.chunk),
                           pl.ds(pl.multiple_of((core + h) % 2 * d.half, d.half), d.half)]
            pltpu.make_async_copy(mine, lv.at[ch, slot, core, :, :, pl.ds(h * d.half, d.half)], loc_sem.at[ch, h]).start()

    psi_rows = d.half * d.pair // 8
    psi_copies = [pltpu.make_async_copy(psi.at[pl.ds(pl.multiple_of(core * d.half * d.pair + n * psi_rows, psi_rows), psi_rows),
                                               pl.ds(c * d.lane, d.lane)],
                                        ps.at[c, pl.ds(n * psi_rows, psi_rows), :], psi_sem.at[n, c])
                  for n in range(8) for c in range(d.lane_tiles)]
    for copy in psi_copies:
        copy.start()

    first_rows = d.out_rows * d.pair
    first_copies = [pltpu.make_async_copy(psi.at[pl.ds(pl.multiple_of(me * first_rows, first_rows), first_rows), pl.ds(c * d.wide, d.wide)],
                                          tbuf.at[LANCZOS_STEPS - 1, c], first_sem.at[c]) for c in range(d.bond // d.wide)]
    for copy in first_copies:
        copy.start()

    side_by_side = jnp.zeros((d.pair, 128), jnp.float32)
    for t in range(d.terms_dev):
        place_of = lax.broadcasted_iota(jnp.int32, (d.pair, 128), 1) == lax.broadcasted_iota(jnp.int32, (d.pair, 128), 0) + t * d.pair
        place_of = jnp.where(place_of, 1.0, 0.0).astype(jnp.bfloat16)
        side_by_side += jnp.dot(pair_ops[t], place_of, preferred_element_type=jnp.float32)
    wv[slot, core] = side_by_side.astype(jnp.bfloat16)
    all_right.wait()
    some_rows = d.bond // 8

    def one_sided(i, carry):
        at = pl.ds(pl.multiple_of(i * some_rows, some_rows), some_rows)
        row = lax.broadcasted_iota(jnp.int32, (some_rows, d.bond), 0) + i * some_rows
        one = jnp.where(row == lax.broadcasted_iota(jnp.int32, (some_rows, d.bond), 1), 1.0, 0.0)
        for t in range(d.terms_dev):
            rs[t, at, :] = jnp.where(flags[t] == 1, rs[t, at, :].astype(jnp.float32), one).astype(jnp.bfloat16)
        return carry

    lax.fori_loop(0, 8, one_sided, 0)

    def right_rows(s):
        return rs.at[:, pl.ds(pl.multiple_of(s * d.slab, d.slab), d.slab), :]

    rv[slot, core] = rs[:, pl.ds(pl.multiple_of(slot * d.slab, d.slab), d.slab), :]

    pl.semaphore_wait(barrier, DEVS - 1)
    for ch in range(CHUNKS):
        for h in range(2):
            theirs = left.at[:, pl.ds(pl.multiple_of((1 - core) * d.half + ch * d.chunk, d.chunk), d.chunk),
                             pl.ds(pl.multiple_of((1 - core + h) % 2 * d.half, d.half), d.half)]
            remote(theirs, lv.at[ch, slot, core, :, :, pl.ds(h * d.half, d.half)], d2d_sem.at[ch, h], d2d_recv.at[ch, h], partner).start()
    for n in range(1, CHIPS):
        chip = (me // 2 + n) % CHIPS
        to = chip_slot(chip // 4, chip // 2 % 2, chip % 2)
        remote(right_rows(to), rv.at[slot, core], rw_send.at[0], rw_recv.at[0], chip * 2 + core).start()
        remote(wv.at[slot, core], wv.at[slot, core], rw_send.at[1], rw_recv.at[1], chip * 2 + core).start()

    for ch in range(CHUNKS):
        for h in range(2):
            pltpu.make_async_copy(lv.at[ch, slot, core, :, :, pl.ds(h * d.half, d.half)], lv.at[ch, slot, core, :, :, pl.ds(h * d.half, d.half)], loc_sem.at[ch, h]).wait()
            back = remote(lv.at[ch, slot, 1 - core, :, :, pl.ds(h * d.half, d.half)], lv.at[ch, slot, 1 - core, :, :, pl.ds(h * d.half, d.half)], d2d_sem.at[ch, h], d2d_recv.at[ch, h], partner)
            back.wait_recv()
    l_along()
    for g in l_gathers:
        g.own_across()

    total = jnp.zeros((8, d.lane), jnp.float32)
    for n in range(8):
        for copy in psi_copies[n * d.lane_tiles:(n + 1) * d.lane_tiles]:
            copy.wait()

        def add_rows(i, acc, n=n):
            x = ps[:, pl.ds(pl.multiple_of(n * psi_rows + i * (psi_rows // 8), 8), psi_rows // 8), :]
            return acc + jnp.sum((x * x).reshape(d.lane_tiles * psi_rows // 64, 8, d.lane), axis=0)

        total = lax.fori_loop(0, 8, add_rows, total)
    nbuf[0] = jnp.broadcast_to(jnp.sum(total, keepdims=True), (8, 128))
    to_partner = remote(nbuf.at[0], nbuf.at[1], n_send, n_recv, partner)
    to_partner.start()
    to_partner.wait()
    norm = jnp.sqrt((nbuf[0] + nbuf[1])[0:1, :] / d.vec_size)
    norm_one = norm[:, 0:1]
    for copy in first_copies:
        copy.wait()
    tbuf[LANCZOS_STEPS - 1] = tbuf[LANCZOS_STEPS - 1] / norm_one[None]
    first_out = [pltpu.make_async_copy(tbuf.at[LANCZOS_STEPS - 1, c], first.at[:, pl.ds(c * d.wide, d.wide)], first_sem.at[c])
                 for c in range(d.bond // d.wide)]
    for copy in first_out:
        copy.start()

    def place(q):
        tiles = [(ps[c, pl.ds(q, d.half, stride=d.pair), :] / norm_one).T for c in range(d.lane_tiles)]
        xt = jnp.concatenate(tiles, axis=0)
        vprev[...] = xt
        return xt.astype(jnp.bfloat16)

    def start_vector(qb, carry):
        for q2 in range(2):
            q = qb * 2 + q2
            xb = place(q)
            for ch in range(CHUNKS):
                uv[ch, qb, :, q2 * d.chunk:(q2 + 1) * d.chunk] = xb[:, ch * d.chunk:(ch + 1) * d.chunk]
            for bh in range(2):
                rows = vprev[pl.ds(pl.multiple_of(slot * d.slab + bh * d.sub, d.sub), d.sub), :]
                vcur[pl.ds(pl.multiple_of((bh * d.pair + q) * d.sub, d.sub), d.sub), :] = rows
        return carry

    lax.fori_loop(0, d.pair // 4, start_vector, 0)
    fifteen = rv.at[pl.ds(0, CHIPS - 1), 0]
    fifteen_w = wv.at[pl.ds(0, CHIPS - 1), 0]
    remote(fifteen, fifteen, rw_send.at[0], rw_recv.at[0], me).wait()
    remote(fifteen_w, fifteen_w, rw_send.at[1], rw_recv.at[1], me).wait()
    fw_right = remote(rv.at[:, core], rv.at[:, core], fw_send.at[0], fw_recv.at[0], partner)
    fw_pair = remote(wv.at[:, core], wv.at[:, core], fw_send.at[1], fw_recv.at[1], partner)
    fw_right.start()
    fw_pair.start()
    l_event(0)
    l_event(1)
    lax.fori_loop(d.pair // 4, d.pair // 2, start_vector, 0)
    l_event(2)
    l_event(3)
    fw_right.wait()
    fw_pair.wait()
    lane = lax.broadcasted_iota(jnp.int32, (d.sub, d.prod), 1)
    row = lax.broadcasted_iota(jnp.int32, (d.sub, d.prod), 0)
    diagonal = lane % d.sub == row

    for t in range(d.terms_dev):
        at_row = lax.broadcasted_iota(jnp.int32, (128, d.prod), 0)
        wide = jnp.where(at_row == lax.broadcasted_iota(jnp.int32, (128, d.prod), 1) // d.sub + t * d.pair, 1.0, 0.0).astype(jnp.bfloat16)
        spread = jnp.dot(wv[...].reshape(CHIPS * CORES * d.pair, 128), wide, preferred_element_type=jnp.float32)
        zst[:, t * d.prod:(t + 1) * d.prod] = spread.astype(jnp.bfloat16)

    def spread_pair(s, carry):
        for c in range(2):
            for t in range(d.terms_dev):
                w = zst[pl.ds(pl.multiple_of((s * CORES + c) * d.pair, d.pair), d.pair), t * d.prod:(t + 1) * d.prod].astype(jnp.float32)
                for q in range(d.pair):
                    full = jnp.where(diagonal, jnp.broadcast_to(w[q:q + 1, :], (d.sub, d.prod)), 0.0)
                    kw[s, c, t, q * d.sub:(q + 1) * d.sub, :] = full.astype(jnp.bfloat16)
        return carry

    lax.fori_loop(0, CHIPS, spread_pair, 0)
    vprev[...] = jnp.zeros_like(vprev)
    for copy in first_out:
        copy.wait()

    def right_product(grp, ch, qb, to):
        r_all = rv[pl.ds(grp * 4, 4)].reshape(d.group_terms * d.slab, d.bond)
        y = jnp.dot(r_all, uv[ch, qb], preferred_element_type=jnp.float32).astype(jnp.bfloat16)
        y = y.reshape(d.group_terms, 2, d.sub, 2 * d.chunk)
        for q2 in range(2):
            for bh in range(2):
                yst[pl.ds(to * d.group_terms, d.group_terms), qb * 2 + q2, :, bh * d.chunk:(bh + 1) * d.chunk] = \
                    y[:, bh, :, q2 * d.chunk:(q2 + 1) * d.chunk]

    def right_of_piece(ch, part):
        for qb in range(2):
            for grp in range(GROUPS):
                right_product(grp, ch, part * 2 + qb, grp)

    def right_of_group(grp, ch, to):
        for qb in range(d.pair // 2):
            right_product(grp, ch, qb, to)

    def left_products(ch, grp, at=None):
        for k in range(d.group_terms):
            w = kw[grp * 4 + k // 4, k // 2 % 2, k % 2]
            z = jnp.dot(w, yst[(grp if at is None else at) * d.group_terms + k].reshape(d.prod, 2 * d.chunk), preferred_element_type=jnp.float32).astype(jnp.bfloat16)
            for bh in range(2):
                zst[bh * d.prod:(bh + 1) * d.prod, k * d.chunk:(k + 1) * d.chunk] = z[:, bh * d.chunk:(bh + 1) * d.chunk]
        l_all = lv[ch, pl.ds(grp * 4, 4)].reshape(d.group_terms * d.chunk, d.bond)
        sig[...] += jnp.dot(zst[...], l_all, preferred_element_type=jnp.float32)

    def first_right(grp, carry):
        right_of_group(grp, 0, grp)

        @pl.when(grp == 1)
        def _():
            l_event(4)
        return carry

    def first_group(n, carry):
        own, third = xpos * 2 + ypos, x_three * 2 + y_three
        grp = jnp.where(n == 0, own, jnp.where(n == 1, x_two * 2 + y_two, jnp.where(n == 2, third, 3 - own)))
        spare = jnp.where(n == 3, own, grp)

        @pl.when(n == 1)
        def _():
            l_event(6)
            l_last(False)

        @pl.when(n == 3)
        def _():
            right_of_group(grp, 1, spare)
            l_last(True)

        def fill(z, carry):
            l_fill(grp * 4 + z)
            return carry

        lax.fori_loop(0, 4, fill, 0)

        def chunk_products(ch, carry):
            left_products(ch, grp, (1 - ch) * grp + ch * spare)

            @pl.when((ch == 0) & (n < 3))
            def _():
                right_of_group(grp, 1, spare)
            return carry

        lax.fori_loop(0, CHUNKS, chunk_products, 0)
        return carry

    def turn_result(j, vector):
        for n in range(d.pair // TILE_PARTS):
            rows = [vector[(bh * d.pair + q) * d.sub:(bh * d.pair + q + 1) * d.sub, :d.half]
                    for q in range(n * TILE_PARTS, (n + 1) * TILE_PARTS) for bh in range(2)]
            tbuf[j, n] = jnp.concatenate(rows, axis=0).T

    def hand_out(j, begin, end):
        for n in range(begin, end):
            to = core * CHIPS + n
            block = tbuf.at[j, :, pl.ds(n * d.out_rows, d.out_rows), :]

            @pl.when(to != me)
            def _():
                remote(block, gbuf.at[j, slot], k_send.at[j], k_recv.at[j], to).start()

            @pl.when(to == me)
            def _():
                gbuf[j, slot] = block[...]

    sends_self = me // CHIPS == core
    lanes = lax.broadcasted_iota(jnp.int32, (d.out_rows, d.wide), 1) // d.slab

    def put_out(j, finish=None):
        @pl.when(sends_self)
        def _():
            some = gbuf.at[j, pl.ds(0, CHIPS - 1)]
            remote(some, some, k_send.at[j], k_recv.at[j], me).wait()

        @pl.when(jnp.logical_not(sends_self))
        def _():
            remote(gbuf.at[j], gbuf.at[j], k_send.at[j], k_recv.at[j], me).wait()

        for ct in range(CHIPS // TILE_PARTS):
            for qt in range(d.pair // TILE_PARTS):
                src = [gbuf[j, ct * TILE_PARTS + c, qt] for c in range(TILE_PARTS)]
                if finish is not None:
                    src = [finish(x, gbuf[j - 1, ct * TILE_PARTS + c, qt], ct * TILE_PARTS + c) for c, x in enumerate(src)]
                for q in range(TILE_PARTS):
                    tile = jnp.zeros((d.out_rows, d.wide), jnp.float32)
                    for c in range(TILE_PARTS):
                        shift = (c - q) % TILE_PARTS * d.slab
                        moved = pltpu.roll(src[c], shift, 1) if shift else src[c]
                        tile = jnp.where(lanes == c, moved, tile)
                    tbuf[j, ct, pl.ds(qt * TILE_PARTS + q, d.out_rows, stride=d.pair), :] = tile
            pltpu.make_async_copy(tbuf.at[j, ct], out.at[j, :, pl.ds(ct * d.wide, d.wide)], o_sem.at[j, ct]).start()

    def step(j, carried):
        beta_prev = carried[0]
        sig[...] = jnp.zeros_like(sig)

        def slot_step(t, carry):
            done_right = sum((t > r).astype(jnp.int32) for r in RIGHT_SLOTS)
            done_left = t - done_right
            is_right = sum((t == r).astype(jnp.int32) for r in RIGHT_SLOTS)
            for four in range(0, len(SLOTS), 4):
                @pl.when((t >= four) & (t < four + 4))
                def _():
                    for at in range(four, four + 4):
                        if not SLOTS[at]:
                            continue

                        @pl.when(t == at)
                        def _():
                            for kind, i, p in SLOTS[at]:
                                act(kind, i, p, j)

            @pl.when(is_right == 1)
            def _():
                right_of_piece(done_right // QUARTERS, done_right % QUARTERS)

            @pl.when(is_right == 0)
            def _():
                left_products(done_left // GROUPS, done_left % GROUPS)
            return carry

        @pl.when(j == 0)
        def _():
            lax.fori_loop(0, GROUPS, first_right, 0)
            l_event(5)
            lax.fori_loop(0, GROUPS, first_group, 0)

        @pl.when(j > 0)
        def _():
            lax.fori_loop(0, len(SLOTS), slot_step, 0)
            for p in range(PIECES):
                sent = uv.at[p // QUARTERS, pl.ds(0, 2), pl.ds(0, 15 * d.slab), :]
                remote(sent, sent, u_send.at[p], u_recv.at[p, 0], me).wait_send()

        other = sig.at[:, pl.ds(d.half, d.half)]
        to_other = remote(other, part, p_send, p_recv, partner)
        to_other.start()
        to_other.wait()
        s = sig[:, :d.half] + part[...]
        v = vcur[...]
        w = s - beta_prev * vprev[...]
        sv = jnp.sum(s * v, keepdims=True)
        wv_sum = jnp.sum(w * v, keepdims=True)
        vv = jnp.sum(v * v, keepdims=True)
        guess = jnp.where(vv > 0.0, wv_sum / jnp.where(vv > 0.0, vv, 1.0), 0.0)
        t = w - guess * v
        sig[:, :d.half] = t
        tt = jnp.sum(t * t, keepdims=True)
        tv = jnp.sum(t * v, keepdims=True)
        at_lane = lax.broadcasted_iota(jnp.int32, (1, 128), 1)
        line = jnp.zeros((1, 128), jnp.float32)
        for n, value in enumerate((sv, vv, tt, tv, guess)):
            line = jnp.where(at_lane == n, value, line)
        scs[...] = line
        scr[me] = line

        def tell(n, carry):
            remote(scs, scr.at[me], s_send, s_recv, (me + n) % DEVS).start()
            return carry

        lax.fori_loop(1, DEVS, tell, 0)

        @pl.when(j > 0)
        def _():
            hand_out(j - 1, *RESULT_PARTS[2])

        @pl.when(j == LANCZOS_STEPS - 1)
        def _():
            turn_result(LANCZOS_STEPS - 1, sig)
            hand_out(LANCZOS_STEPS - 1, 0, CHIPS)

        heard = scr.at[pl.ds(0, DEVS - 1)]
        remote(heard, heard, s_send, s_recv, me).wait()
        told = scr[:, 0, :]
        alpha = jnp.sum(told[:, 0:1], axis=0, keepdims=True) / d.vec_size
        off = alpha - told[:, 4:5]
        square = told[:, 2:3] - 2.0 * off * told[:, 3:4] + off * off * told[:, 1:2]
        beta = jnp.sqrt(jnp.sum(square, axis=0, keepdims=True) / d.vec_size)
        vnew = (sig[:, :d.half] - (alpha - guess) * vcur[...]) / beta
        vprev[...] = vcur[...]
        vcur[...] = vnew
        vb = vnew.astype(jnp.bfloat16)

        @pl.when(j < LANCZOS_STEPS - 1)
        def _():
            for ch in range(CHUNKS):
                for bh in range(2):
                    at = pl.ds(pl.multiple_of(slot * d.slab + bh * d.sub, d.sub), d.sub)
                    for q in range(d.pair):
                        uv[ch, q // 2, at, q % 2 * d.chunk:(q % 2 + 1) * d.chunk] = \
                            vb[(bh * d.pair + q) * d.sub:(bh * d.pair + q + 1) * d.sub, ch * d.chunk:(ch + 1) * d.chunk]
        alphas[j] = alpha[0, 0]
        betas[j] = beta[0, 0]
        return beta, alpha


    zero = jnp.zeros((1, 1), jnp.float32)
    last_beta, last_alpha = lax.fori_loop(0, LANCZOS_STEPS, step, (zero, zero))

    for n, part in enumerate((lv.at[0, pl.ds(0, 15), :, 0], lv.at[1, pl.ds(0, 15), :, 0, :, pl.ds(edge, d.bond - edge)],
                              lv.at[0, pl.ds(0, 15), :, 0, :, pl.ds(0, d.half)], lv.at[1, pl.ds(0, 15), :, 0, :, pl.ds(edge, d.half - edge)])):
        remote(part, part, l_send.at[n], l_recv.at[n, 0], me).wait_send()
    swapped = lv.at[:, pl.ds(0, 15), :, 0, :, pl.ds(d.half, d.half)]
    remote(swapped, swapped, f_send, f_recv.at[0], me).wait_send()
    for ch in range(CHUNKS):
        for h in range(2):
            theirs = left.at[:, pl.ds(0, d.chunk), pl.ds(0, d.half)]
            remote(theirs, lv.at[ch, slot, core, :, :, pl.ds(h * d.half, d.half)], d2d_sem.at[ch, h], d2d_recv.at[ch, h], partner).wait_send()
    put_out(LANCZOS_STEPS - 2)

    def finish(block, before, s):
        owner = device(s % 4, s // 4 % 2, s // 8, me // CHIPS)
        return (block - (last_alpha - scr[owner][:, 4:5]) * before) / last_beta

    put_out(LANCZOS_STEPS - 1, finish)
    for j in range(LANCZOS_STEPS):
        for c in range(d.bond // d.wide):
            pltpu.make_async_copy(tbuf.at[j, c], out.at[j, :, pl.ds(c * d.wide, d.wide)], o_sem.at[j, c]).wait()


def solution(mesh):
    def device_body(wavefunction, left_loc, pair_loc, right_loc, flag_loc):
        bond, pair = wavefunction.shape[0], wavefunction.shape[1]
        d = Dims(bond, pair, left_loc.shape[0])
        bf16, f32 = jnp.bfloat16, jnp.float32
        dma = pltpu.SemaphoreType.DMA
        any_space = pl.BlockSpec(memory_space=pl.ANY)
        smem = pl.BlockSpec(memory_space=pltpu.SMEM)
        scalars = jax.ShapeDtypeStruct((LANCZOS_STEPS,), f32)
        later, first, alphas, betas = pl.pallas_call(
            functools.partial(lanczos_kernel, d),
            out_shape=(jax.ShapeDtypeStruct((LANCZOS_STEPS, d.out_rows * pair, bond), f32),
                       jax.ShapeDtypeStruct((d.out_rows * pair, bond), f32), scalars, scalars),
            in_specs=[any_space] * 3 + [pl.BlockSpec(memory_space=pltpu.VMEM), smem],
            out_specs=(any_space, any_space, smem, smem),
            scratch_shapes=[
                pltpu.VMEM((CHUNKS, CHIPS, CORES, d.terms_dev, d.chunk, bond), bf16),
                pltpu.VMEM((CHIPS, CORES, d.terms_dev, d.slab, bond), bf16),
                pltpu.VMEM((d.terms_dev, bond, bond), bf16),
                pltpu.VMEM((CHIPS, CORES, pair, 128), bf16),
                pltpu.VMEM((CHIPS, CORES, d.terms_dev, d.prod, d.prod), bf16),
                pltpu.VMEM((CHUNKS, pair // 2, bond, 2 * d.chunk), bf16),
                pltpu.VMEM((d.lane_tiles, d.half * pair, d.lane), f32),
                pltpu.VMEM((CHIPS * CORES * d.terms_dev, pair, d.sub, 2 * d.chunk), bf16),
                pltpu.VMEM((d.rows, d.group_terms * d.chunk), bf16),
                pltpu.VMEM((d.rows, bond), f32),
                pltpu.VMEM((d.rows, d.half), f32),
                pltpu.VMEM((d.rows, d.half), f32),
                pltpu.VMEM((d.rows, d.half), f32),
                pltpu.VMEM((LANCZOS_STEPS, bond // d.wide, d.half, d.wide), f32),
                pltpu.VMEM((LANCZOS_STEPS, CHIPS, bond // d.wide, d.out_rows, d.wide), f32),
                pltpu.VMEM((1, 128), f32),
                pltpu.VMEM((DEVS, 1, 128), f32),
                pltpu.VMEM((2, 8, 128), f32),
                dma((3, 2)), dma((8, d.lane_tiles)), dma((CHUNKS, 2)), dma((CHUNKS, 2)), dma((2,)), dma((2,)), dma((2,)), dma((2,)),
                dma((4,)), dma((4, CHIPS)), dma, dma((CHIPS,)), dma((PIECES,)), dma((PIECES, CHIPS)),
                dma, dma, dma, dma, dma((LANCZOS_STEPS,)), dma((LANCZOS_STEPS,)), dma, dma, dma((LANCZOS_STEPS, bond // d.wide)), dma((bond // d.wide,)),
            ],
            compiler_params=pltpu.CompilerParams(has_side_effects=True, collective_id=0, vmem_limit_bytes=67043328),
            name='lanczos',
        )(wavefunction.reshape(bond * pair, bond), left_loc, right_loc, pair_loc, flag_loc)
        krylov = jnp.concatenate([first[None], later])
        return krylov.reshape(LANCZOS_STEPS + 1, d.out_rows, pair, bond), alphas, betas

    return jax.shard_map(device_body, mesh=mesh, in_specs=(P(), P(AXIS_NAME), P(AXIS_NAME), P(AXIS_NAME), P(AXIS_NAME)),
                         out_specs=(P(None, AXIS_NAME), P(), P()), check_vma=False)
```

```python
import functools

import jax
import jax.numpy as jnp
from jax import lax
from jax.experimental import pallas as pl
from jax.experimental.pallas import tpu as pltpu
from jax.sharding import PartitionSpec as P

LANCZOS_STEPS = 6
AXIS_NAME = 'terms'
MESH = pl.DeviceIdType.MESH

CHIPS = 16
CORES = 2
DEVS = 32
CHUNKS = 2
GROUPS = 4
TILE_PARTS = 4
QUARTERS = 4
PIECES = CHUNKS * QUARTERS

ALONG, ACROSS, FROM_COLUMN, FROM_SECOND, THIRD, DIAGONAL, RESULT, RESULT_OUT, RESULT_PUT = range(9)
RIGHT_SLOTS = (0, 1, 2, 3, 8, 9, 10, 11)
SLOTS = (
    ((0, 1, 0), (0, 1, 1), (1, 0, 2), (0, 2, 0), (1, 0, 5), (1, 0, 3), (1, 0, 6), (1, 0, 0), (0, 3, 0), (3, 0, 2), (0, 2, 1), (0, 1, 3), (1, 0, 4), (0, 3, 1), (1, 0, 7), (0, 1, 2), (1, 0, 1), (0, 3, 3), (2, 1, 0), (2, 2, 0), (0, 2, 3), (0, 3, 2), (2, 1, 1), (3, 0, 0), (2, 3, 0), (3, 1, 0), (2, 2, 1), (0, 2, 2), (0, 1, 4), (3, 0, 1), (2, 1, 3), (3, 2, 0), (2, 3, 1), (2, 2, 2), (2, 2, 3), (2, 1, 2), (4, 0, 0), (0, 2, 5), (0, 3, 4), (0, 2, 4), (0, 1, 5), (0, 1, 6), (0, 1, 7), (3, 3, 0), (2, 3, 3), (3, 1, 1), (3, 2, 1), (0, 2, 6), (2, 3, 2), (4, 0, 1), (3, 3, 1), (0, 3, 6), (3, 2, 2), (3, 1, 2), (0, 3, 5), (0, 2, 7), (0, 3, 7), (3, 2, 3), (3, 3, 2), (3, 0, 3), (5, 0, 0), (3, 3, 3), (4, 0, 3), (3, 1, 3), (3, 0, 4),),
    ((6, 0, 0), (2, 2, 4), (5, 0, 1), (3, 0, 6), (2, 1, 4), (4, 0, 2),),
    ((2, 2, 6), (5, 0, 2), (2, 1, 6),),
    ((2, 2, 5), (5, 0, 3), (3, 2, 4), (2, 3, 4),),
    ((2, 1, 5), (3, 0, 5), (3, 1, 4),),
    ((2, 3, 5), (3, 2, 5), (2, 3, 6),),
    ((2, 2, 7), (3, 3, 4), (2, 1, 7), (3, 1, 5), (8, 0, 0),),
    ((3, 3, 5), (2, 3, 7), (3, 2, 6), (3, 1, 6), (3, 3, 6),),
    ((3, 0, 7), (3, 1, 7), (3, 2, 7), (4, 0, 5), (5, 0, 4), (4, 0, 4),),
    ((3, 3, 7), (5, 0, 5),),
    ((4, 0, 6), (5, 0, 6),),
    ((4, 0, 7), (5, 0, 7),),
    ((7, 0, 0),),
    (),
    (),
    (),
)
RESULT_EARLY = 12


class Dims:
    def __init__(self, bond, pair, terms_dev):
        self.bond = bond
        self.pair = pair
        self.terms_dev = terms_dev
        self.slab = bond // CHIPS
        self.sub = self.slab // 2
        self.half = bond // CORES
        self.chunk = self.half // CHUNKS
        self.rows = self.slab * pair
        self.prod = self.sub * pair
        self.out_rows = bond // DEVS
        self.group_terms = 4 * CORES * terms_dev
        self.vec_size = bond * pair * bond
        self.lane = min(bond, 128)
        self.wide = TILE_PARTS * self.slab
        self.lane_tiles = bond // self.lane


def lanczos_kernel(d, psi, left, right, pair_ops, flags, out, first, alphas, betas, lv, rv, rs, wv, kw, uv, ps, yst, zst, sig, part, vcur, vprev, tbuf, gbuf,
                   scs, scr, nbuf,
                   loc_sem, psi_sem, d2d_sem, d2d_recv, rw_send, rw_recv, fw_send, fw_recv, l_send, l_recv, f_send, f_recv, u_send, u_recv,
                   p_send, p_recv, s_send, s_recv, k_send, k_recv, n_send, n_recv, o_sem, first_sem):
    me = lax.axis_index(AXIS_NAME)
    core = me % 2
    xpos = (me // 2) % 2
    ypos = (me // 4) % 2
    zpos = me // 8

    def device(z, y, x, c):
        return ((z * 2 + y) * 2 + x) * 2 + c

    def chip_slot(z, y, x):
        return (x * 2 + y) * 4 + z

    partner = device(zpos, ypos, xpos, 1 - core)
    slot = chip_slot(zpos, ypos, xpos)
    zs = (zpos, zpos + 1 - 2 * (zpos % 2), (zpos + 2) % 4, 3 - zpos)
    inner = (zpos + 1) // 2 % 2
    zn = (zpos, (1 - inner) * (zpos + 1 - zpos // 3 * 2) + inner * (zpos - 1), (1 - inner) * ((zpos + 2) % 4) + inner * (zpos + 1),
          (1 - inner) * (3 - zpos) + inner * ((zpos + 2) % 4))
    y_two = ypos + (1 - core) * (1 - 2 * ypos)
    x_two = xpos + core * (1 - 2 * xpos)
    y_three = ypos + core * (1 - 2 * ypos)
    x_three = xpos + (1 - core) * (1 - 2 * xpos)
    two = device(zpos, y_two, x_two, core)
    three = device(zpos, y_three, x_three, core)

    def remote(src, dst, send, recv, dev):
        return pltpu.make_async_remote_copy(src_ref=src, dst_ref=dst, send_sem=send, recv_sem=recv, device_id=(dev,), device_id_type=MESH)

    class Gather:
        def __init__(self, block, send, recv):
            self.block, self.send_sem, self.recv_sem = block, send, recv

        def send(self, which, dev):
            remote(self.block(which), self.block(which), self.send_sem, self.recv_sem(which), dev).start()

        def wait(self, which):
            remote(self.block(which), self.block(which), self.send_sem, self.recv_sem(which), me).wait_recv()

        def own_along(self):
            for i in (1, 2, 3):
                self.send(slot, device(zs[i], ypos, xpos, core))

        def own_across(self):
            self.send(slot, three)
            self.send(slot, two)

        def event(self, n):
            i = (n + 1) // 2
            if n % 2:
                which = chip_slot(zs[i], ypos, xpos)
                self.wait(which)
                self.send(which, three)
                self.send(which, two)
            else:
                which = chip_slot(zs[i], y_two, x_two)
                self.wait(which)
                self.send(which, three)

        def last(self, diagonal):
            for i in range(4):
                self.wait(chip_slot(zs[i], 1 - ypos, 1 - xpos) if diagonal else chip_slot(zs[i], y_three, x_three))

    edge = d.chunk
    l_parts = (
        (lambda s: lv.at[0, s, :, core], 0),
        (lambda s: lv.at[1, s, :, core, :, pl.ds(edge, d.bond - edge)], 1),
        (lambda s: lv.at[0, s, :, 1 - core, :, pl.ds(0, d.half)], 2),
        (lambda s: lv.at[1, s, :, 1 - core, :, pl.ds(edge, d.half - edge)], 3),
    )
    l_gathers = [Gather(block, l_send.at[n], lambda s, n=n: l_recv.at[n, s]) for block, n in l_parts]

    def l_swap(s, term):
        part = lv.at[:, s, :, term, :, pl.ds(d.half, d.half)]
        return remote(part, part, f_send, f_recv.at[s], partner)

    def l_event(n):
        i = (n + 1) // 2
        for g in l_gathers:
            g.event(n)
        l_swap(chip_slot(zs[i], ypos, xpos) if n % 2 else chip_slot(zs[i], y_two, x_two), core).start()

    def l_last(diagonal):
        for i in range(4):
            which = chip_slot(zs[i], 1 - ypos, 1 - xpos) if diagonal else chip_slot(zs[i], y_three, x_three)
            for g in l_gathers:
                g.wait(which)
            l_swap(which, core).start()

    def l_fill(s):
        @pl.when(s != slot)
        def _():
            l_swap(s, 1 - core).wait_recv()
            for c in range(CORES):
                tile = lv[:, s, c, 1 - core, :, d.half:].reshape(d.half, d.half).T
                lv[:, s, c, 1 - core, :, d.half:] = tile.reshape(CHUNKS, d.chunk, d.half)
                for t in range(d.terms_dev):
                    lv[1, s, c, t, :, :edge] = lv[0, s, c, t, :, edge:d.half].T

    def l_along():
        for i in (1, 2, 3):
            for g in l_gathers:
                g.send(slot, device(zs[i], ypos, xpos, core))

    def u_block(p):
        return lambda s: uv.at[p // QUARTERS, pl.ds(p % QUARTERS * 2, 2), pl.ds(pl.multiple_of(s * d.slab, d.slab), d.slab), :]

    u_gathers = [Gather(u_block(p), u_send.at[p], lambda s, p=p: u_recv.at[p, s]) for p in range(PIECES)]

    def act(kind, i, p, j):
        g = u_gathers[p]
        if kind == ALONG:
            g.send(slot, device(zn[i], ypos, xpos, core))
        elif kind == ACROSS:
            g.own_across()
        elif kind == FROM_COLUMN:
            which = chip_slot(zn[i], ypos, xpos)
            g.wait(which)
            g.send(which, three)
            g.send(which, two)
        elif kind == FROM_SECOND:
            which = chip_slot(zn[i], y_two, x_two)
            g.wait(which)
            g.send(which, three)
        elif kind == THIRD:
            g.last(False)
        elif kind == DIAGONAL:
            g.last(True)
        elif kind == RESULT:
            turn_result(j - 1, vcur)
        elif kind == RESULT_OUT:
            hand_out(j - 1, 0, RESULT_EARLY)
        elif kind == RESULT_PUT:
            @pl.when(j > 1)
            def _():
                put_out(j - 2)

    all_right = pltpu.make_async_copy(right, rs, loc_sem.at[2, 0])
    all_right.start()

    barrier = pltpu.get_barrier_semaphore()

    def knock(n, carry):
        pl.semaphore_signal(barrier, inc=1, device_id=((me + n) % DEVS,), device_id_type=MESH)
        return carry

    lax.fori_loop(1, DEVS, knock, 0)

    for ch in range(CHUNKS):
        for h in range(2):
            mine = left.at[:, pl.ds(pl.multiple_of(core * d.half + ch * d.chunk, d.chunk), d.chunk),
                           pl.ds(pl.multiple_of((core + h) % 2 * d.half, d.half), d.half)]
            pltpu.make_async_copy(mine, lv.at[ch, slot, core, :, :, pl.ds(h * d.half, d.half)], loc_sem.at[ch, h]).start()

    psi_rows = d.half * d.pair // 8
    psi_copies = [pltpu.make_async_copy(psi.at[pl.ds(pl.multiple_of(core * d.half * d.pair + n * psi_rows, psi_rows), psi_rows),
                                               pl.ds(c * d.lane, d.lane)],
                                        ps.at[c, pl.ds(n * psi_rows, psi_rows), :], psi_sem.at[n, c])
                  for n in range(8) for c in range(d.lane_tiles)]
    for copy in psi_copies:
        copy.start()

    first_rows = d.out_rows * d.pair
    first_copies = [pltpu.make_async_copy(psi.at[pl.ds(pl.multiple_of(me * first_rows, first_rows), first_rows), pl.ds(c * d.wide, d.wide)],
                                          tbuf.at[LANCZOS_STEPS - 1, c], first_sem.at[c]) for c in range(d.bond // d.wide)]
    for copy in first_copies:
        copy.start()

    side_by_side = jnp.zeros((d.pair, 128), jnp.float32)
    for t in range(d.terms_dev):
        place_of = lax.broadcasted_iota(jnp.int32, (d.pair, 128), 1) == lax.broadcasted_iota(jnp.int32, (d.pair, 128), 0) + t * d.pair
        place_of = jnp.where(place_of, 1.0, 0.0).astype(jnp.bfloat16)
        side_by_side += jnp.dot(pair_ops[t], place_of, preferred_element_type=jnp.float32)
    wv[slot, core] = side_by_side.astype(jnp.bfloat16)
    all_right.wait()
    some_rows = d.bond // 8

    def one_sided(i, carry):
        at = pl.ds(pl.multiple_of(i * some_rows, some_rows), some_rows)
        row = lax.broadcasted_iota(jnp.int32, (some_rows, d.bond), 0) + i * some_rows
        one = jnp.where(row == lax.broadcasted_iota(jnp.int32, (some_rows, d.bond), 1), 1.0, 0.0)
        for t in range(d.terms_dev):
            rs[t, at, :] = jnp.where(flags[t] == 1, rs[t, at, :].astype(jnp.float32), one).astype(jnp.bfloat16)
        return carry

    lax.fori_loop(0, 8, one_sided, 0)

    def right_rows(s):
        return rs.at[:, pl.ds(pl.multiple_of(s * d.slab, d.slab), d.slab), :]

    rv[slot, core] = rs[:, pl.ds(pl.multiple_of(slot * d.slab, d.slab), d.slab), :]

    pl.semaphore_wait(barrier, DEVS - 1)
    for ch in range(CHUNKS):
        for h in range(2):
            theirs = left.at[:, pl.ds(pl.multiple_of((1 - core) * d.half + ch * d.chunk, d.chunk), d.chunk),
                             pl.ds(pl.multiple_of((1 - core + h) % 2 * d.half, d.half), d.half)]
            remote(theirs, lv.at[ch, slot, core, :, :, pl.ds(h * d.half, d.half)], d2d_sem.at[ch, h], d2d_recv.at[ch, h], partner).start()
    for n in range(1, CHIPS):
        chip = (me // 2 + n) % CHIPS
        to = chip_slot(chip // 4, chip // 2 % 2, chip % 2)
        remote(right_rows(to), rv.at[slot, core], rw_send.at[0], rw_recv.at[0], chip * 2 + core).start()
        remote(wv.at[slot, core], wv.at[slot, core], rw_send.at[1], rw_recv.at[1], chip * 2 + core).start()

    for ch in range(CHUNKS):
        for h in range(2):
            pltpu.make_async_copy(lv.at[ch, slot, core, :, :, pl.ds(h * d.half, d.half)], lv.at[ch, slot, core, :, :, pl.ds(h * d.half, d.half)], loc_sem.at[ch, h]).wait()
            back = remote(lv.at[ch, slot, 1 - core, :, :, pl.ds(h * d.half, d.half)], lv.at[ch, slot, 1 - core, :, :, pl.ds(h * d.half, d.half)], d2d_sem.at[ch, h], d2d_recv.at[ch, h], partner)
            back.wait_recv()
    l_along()
    for g in l_gathers:
        g.own_across()

    total = jnp.zeros((8, d.lane), jnp.float32)
    for n in range(8):
        for copy in psi_copies[n * d.lane_tiles:(n + 1) * d.lane_tiles]:
            copy.wait()

        def add_rows(i, acc, n=n):
            x = ps[:, pl.ds(pl.multiple_of(n * psi_rows + i * (psi_rows // 8), 8), psi_rows // 8), :]
            return acc + jnp.sum((x * x).reshape(d.lane_tiles * psi_rows // 64, 8, d.lane), axis=0)

        total = lax.fori_loop(0, 8, add_rows, total)
    nbuf[0] = jnp.broadcast_to(jnp.sum(total, keepdims=True), (8, 128))
    to_partner = remote(nbuf.at[0], nbuf.at[1], n_send, n_recv, partner)
    to_partner.start()
    to_partner.wait()
    norm = jnp.sqrt((nbuf[0] + nbuf[1])[0:1, :] / d.vec_size)
    norm_one = norm[:, 0:1]
    for copy in first_copies:
        copy.wait()
    tbuf[LANCZOS_STEPS - 1] = tbuf[LANCZOS_STEPS - 1] / norm_one[None]
    first_out = [pltpu.make_async_copy(tbuf.at[LANCZOS_STEPS - 1, c], first.at[:, pl.ds(c * d.wide, d.wide)], first_sem.at[c])
                 for c in range(d.bond // d.wide)]
    for copy in first_out:
        copy.start()

    def place(q):
        tiles = [(ps[c, pl.ds(q, d.half, stride=d.pair), :] / norm_one).T for c in range(d.lane_tiles)]
        xt = jnp.concatenate(tiles, axis=0)
        vprev[...] = xt
        return xt.astype(jnp.bfloat16)

    def start_vector(qb, carry):
        for q2 in range(2):
            q = qb * 2 + q2
            xb = place(q)
            for ch in range(CHUNKS):
                uv[ch, qb, :, q2 * d.chunk:(q2 + 1) * d.chunk] = xb[:, ch * d.chunk:(ch + 1) * d.chunk]
            for bh in range(2):
                rows = vprev[pl.ds(pl.multiple_of(slot * d.slab + bh * d.sub, d.sub), d.sub), :]
                vcur[pl.ds(pl.multiple_of((bh * d.pair + q) * d.sub, d.sub), d.sub), :] = rows
        return carry

    lax.fori_loop(0, d.pair // 4, start_vector, 0)
    fifteen = rv.at[pl.ds(0, CHIPS - 1), 0]
    fifteen_w = wv.at[pl.ds(0, CHIPS - 1), 0]
    remote(fifteen, fifteen, rw_send.at[0], rw_recv.at[0], me).wait()
    remote(fifteen_w, fifteen_w, rw_send.at[1], rw_recv.at[1], me).wait()
    fw_right = remote(rv.at[:, core], rv.at[:, core], fw_send.at[0], fw_recv.at[0], partner)
    fw_pair = remote(wv.at[:, core], wv.at[:, core], fw_send.at[1], fw_recv.at[1], partner)
    fw_right.start()
    fw_pair.start()
    l_event(0)
    l_event(1)
    lax.fori_loop(d.pair // 4, d.pair // 2, start_vector, 0)
    l_event(2)
    l_event(3)
    fw_right.wait()
    fw_pair.wait()
    lane = lax.broadcasted_iota(jnp.int32, (d.sub, d.prod), 1)
    row = lax.broadcasted_iota(jnp.int32, (d.sub, d.prod), 0)
    diagonal = lane % d.sub == row

    for t in range(d.terms_dev):
        at_row = lax.broadcasted_iota(jnp.int32, (128, d.prod), 0)
        wide = jnp.where(at_row == lax.broadcasted_iota(jnp.int32, (128, d.prod), 1) // d.sub + t * d.pair, 1.0, 0.0).astype(jnp.bfloat16)
        spread = jnp.dot(wv[...].reshape(CHIPS * CORES * d.pair, 128), wide, preferred_element_type=jnp.float32)
        zst[:, t * d.prod:(t + 1) * d.prod] = spread.astype(jnp.bfloat16)

    def spread_pair(s, carry):
        for c in range(2):
            for t in range(d.terms_dev):
                w = zst[pl.ds(pl.multiple_of((s * CORES + c) * d.pair, d.pair), d.pair), t * d.prod:(t + 1) * d.prod].astype(jnp.float32)
                for q in range(d.pair):
                    full = jnp.where(diagonal, jnp.broadcast_to(w[q:q + 1, :], (d.sub, d.prod)), 0.0)
                    kw[s, c, t, q * d.sub:(q + 1) * d.sub, :] = full.astype(jnp.bfloat16)
        return carry

    lax.fori_loop(0, CHIPS, spread_pair, 0)
    vprev[...] = jnp.zeros_like(vprev)
    for copy in first_out:
        copy.wait()

    def right_product(grp, ch, qb, to):
        r_all = rv[pl.ds(grp * 4, 4)].reshape(d.group_terms * d.slab, d.bond)
        y = jnp.dot(r_all, uv[ch, qb], preferred_element_type=jnp.float32).astype(jnp.bfloat16)
        y = y.reshape(d.group_terms, 2, d.sub, 2 * d.chunk)
        for q2 in range(2):
            for bh in range(2):
                yst[pl.ds(to * d.group_terms, d.group_terms), qb * 2 + q2, :, bh * d.chunk:(bh + 1) * d.chunk] = \
                    y[:, bh, :, q2 * d.chunk:(q2 + 1) * d.chunk]

    def right_of_piece(ch, part):
        for qb in range(2):
            for grp in range(GROUPS):
                right_product(grp, ch, part * 2 + qb, grp)

    def right_of_group(grp, ch, to):
        for qb in range(d.pair // 2):
            right_product(grp, ch, qb, to)

    def left_products(ch, grp, at=None):
        for k in range(d.group_terms):
            w = kw[grp * 4 + k // 4, k // 2 % 2, k % 2]
            z = jnp.dot(w, yst[(grp if at is None else at) * d.group_terms + k].reshape(d.prod, 2 * d.chunk), preferred_element_type=jnp.float32).astype(jnp.bfloat16)
            for bh in range(2):
                zst[bh * d.prod:(bh + 1) * d.prod, k * d.chunk:(k + 1) * d.chunk] = z[:, bh * d.chunk:(bh + 1) * d.chunk]
        l_all = lv[ch, pl.ds(grp * 4, 4)].reshape(d.group_terms * d.chunk, d.bond)
        sig[...] += jnp.dot(zst[...], l_all, preferred_element_type=jnp.float32)

    def first_right(grp, carry):
        right_of_group(grp, 0, grp)

        @pl.when(grp == 1)
        def _():
            l_event(4)
        return carry

    def first_group(n, carry):
        own, third = xpos * 2 + ypos, x_three * 2 + y_three
        grp = jnp.where(n == 0, own, jnp.where(n == 1, x_two * 2 + y_two, jnp.where(n == 2, third, 3 - own)))
        spare = jnp.where(n == 3, own, grp)

        @pl.when(n == 1)
        def _():
            l_event(6)
            l_last(False)

        @pl.when(n == 3)
        def _():
            right_of_group(grp, 1, spare)
            l_last(True)

        def fill(z, carry):
            l_fill(grp * 4 + z)
            return carry

        lax.fori_loop(0, 4, fill, 0)

        def chunk_products(ch, carry):
            left_products(ch, grp, (1 - ch) * grp + ch * spare)

            @pl.when((ch == 0) & (n < 3))
            def _():
                right_of_group(grp, 1, spare)
            return carry

        lax.fori_loop(0, CHUNKS, chunk_products, 0)
        return carry

    def turn_result(j, vector):
        for n in range(d.pair // TILE_PARTS):
            rows = [vector[(bh * d.pair + q) * d.sub:(bh * d.pair + q + 1) * d.sub, :d.half]
                    for q in range(n * TILE_PARTS, (n + 1) * TILE_PARTS) for bh in range(2)]
            tbuf[j, n] = jnp.concatenate(rows, axis=0).T

    def hand_out(j, begin, end):
        for n in range(begin, end):
            to = core * CHIPS + n
            block = tbuf.at[j, :, pl.ds(n * d.out_rows, d.out_rows), :]

            @pl.when(to != me)
            def _():
                remote(block, gbuf.at[j, slot], k_send.at[j], k_recv.at[j], to).start()

            @pl.when(to == me)
            def _():
                gbuf[j, slot] = block[...]

    sends_self = me // CHIPS == core
    lanes = lax.broadcasted_iota(jnp.int32, (d.out_rows, d.wide), 1) // d.slab

    def put_out(j, finish=None):
        @pl.when(sends_self)
        def _():
            some = gbuf.at[j, pl.ds(0, CHIPS - 1)]
            remote(some, some, k_send.at[j], k_recv.at[j], me).wait()

        @pl.when(jnp.logical_not(sends_self))
        def _():
            remote(gbuf.at[j], gbuf.at[j], k_send.at[j], k_recv.at[j], me).wait()

        for ct in range(CHIPS // TILE_PARTS):
            for qt in range(d.pair // TILE_PARTS):
                src = [gbuf[j, ct * TILE_PARTS + c, qt] for c in range(TILE_PARTS)]
                if finish is not None:
                    src = [finish(x, gbuf[j - 1, ct * TILE_PARTS + c, qt], ct * TILE_PARTS + c) for c, x in enumerate(src)]
                for q in range(TILE_PARTS):
                    tile = jnp.zeros((d.out_rows, d.wide), jnp.float32)
                    for c in range(TILE_PARTS):
                        shift = (c - q) % TILE_PARTS * d.slab
                        moved = pltpu.roll(src[c], shift, 1) if shift else src[c]
                        tile = jnp.where(lanes == c, moved, tile)
                    tbuf[j, ct, pl.ds(qt * TILE_PARTS + q, d.out_rows, stride=d.pair), :] = tile
            pltpu.make_async_copy(tbuf.at[j, ct], out.at[j, :, pl.ds(ct * d.wide, d.wide)], o_sem.at[j, ct]).start()

    def step(j, carried):
        beta_prev = carried[0]
        sig[...] = jnp.zeros_like(sig)

        def slot_step(t, carry):
            done_right = sum((t > r).astype(jnp.int32) for r in RIGHT_SLOTS)
            done_left = t - done_right
            is_right = sum((t == r).astype(jnp.int32) for r in RIGHT_SLOTS)
            for four in range(0, len(SLOTS), 4):
                @pl.when((t >= four) & (t < four + 4))
                def _():
                    for at in range(four, four + 4):
                        if not SLOTS[at]:
                            continue

                        @pl.when(t == at)
                        def _():
                            for kind, i, p in SLOTS[at]:
                                act(kind, i, p, j)

            @pl.when(is_right == 1)
            def _():
                right_of_piece(done_right // QUARTERS, done_right % QUARTERS)

            @pl.when(is_right == 0)
            def _():
                left_products(done_left // GROUPS, done_left % GROUPS)
            return carry

        @pl.when(j == 0)
        def _():
            lax.fori_loop(0, GROUPS, first_right, 0)
            l_event(5)
            lax.fori_loop(0, GROUPS, first_group, 0)

        @pl.when(j > 0)
        def _():
            lax.fori_loop(0, len(SLOTS), slot_step, 0)
            for p in range(PIECES):
                sent = uv.at[p // QUARTERS, pl.ds(0, 2), pl.ds(0, 15 * d.slab), :]
                remote(sent, sent, u_send.at[p], u_recv.at[p, 0], me).wait_send()

        other = sig.at[:, pl.ds(d.half, d.half)]
        to_other = remote(other, part, p_send, p_recv, partner)
        to_other.start()
        to_other.wait()
        s = sig[:, :d.half] + part[...]
        v = vcur[...]
        w = s - beta_prev * vprev[...]
        sv = jnp.sum(s * v, keepdims=True)
        wv_sum = jnp.sum(w * v, keepdims=True)
        vv = jnp.sum(v * v, keepdims=True)
        guess = jnp.where(vv > 0.0, wv_sum / jnp.where(vv > 0.0, vv, 1.0), 0.0)
        t = w - guess * v
        sig[:, :d.half] = t
        tt = jnp.sum(t * t, keepdims=True)
        tv = jnp.sum(t * v, keepdims=True)
        at_lane = lax.broadcasted_iota(jnp.int32, (1, 128), 1)
        line = jnp.zeros((1, 128), jnp.float32)
        for n, value in enumerate((sv, vv, tt, tv, guess)):
            line = jnp.where(at_lane == n, value, line)
        scs[...] = line
        scr[me] = line

        def tell(n, carry):
            remote(scs, scr.at[me], s_send, s_recv, (me + n) % DEVS).start()
            return carry

        lax.fori_loop(1, DEVS, tell, 0)

        @pl.when(j > 0)
        def _():
            hand_out(j - 1, RESULT_EARLY, CHIPS)

        @pl.when(j == LANCZOS_STEPS - 1)
        def _():
            turn_result(LANCZOS_STEPS - 1, sig)
            hand_out(LANCZOS_STEPS - 1, 0, CHIPS)

        heard = scr.at[pl.ds(0, DEVS - 1)]
        remote(heard, heard, s_send, s_recv, me).wait()
        told = scr[:, 0, :]
        alpha = jnp.sum(told[:, 0:1], axis=0, keepdims=True) / d.vec_size
        off = alpha - told[:, 4:5]
        square = told[:, 2:3] - 2.0 * off * told[:, 3:4] + off * off * told[:, 1:2]
        beta = jnp.sqrt(jnp.sum(square, axis=0, keepdims=True) / d.vec_size)
        vnew = (sig[:, :d.half] - (alpha - guess) * vcur[...]) / beta
        vprev[...] = vcur[...]
        vcur[...] = vnew
        vb = vnew.astype(jnp.bfloat16)

        @pl.when(j < LANCZOS_STEPS - 1)
        def _():
            for ch in range(CHUNKS):
                for bh in range(2):
                    at = pl.ds(pl.multiple_of(slot * d.slab + bh * d.sub, d.sub), d.sub)
                    for q in range(d.pair):
                        uv[ch, q // 2, at, q % 2 * d.chunk:(q % 2 + 1) * d.chunk] = \
                            vb[(bh * d.pair + q) * d.sub:(bh * d.pair + q + 1) * d.sub, ch * d.chunk:(ch + 1) * d.chunk]
        alphas[j] = alpha[0, 0]
        betas[j] = beta[0, 0]
        return beta, alpha


    zero = jnp.zeros((1, 1), jnp.float32)
    last_beta, last_alpha = lax.fori_loop(0, LANCZOS_STEPS, step, (zero, zero))

    for n, part in enumerate((lv.at[0, pl.ds(0, 15), :, 0], lv.at[1, pl.ds(0, 15), :, 0, :, pl.ds(edge, d.bond - edge)],
                              lv.at[0, pl.ds(0, 15), :, 0, :, pl.ds(0, d.half)], lv.at[1, pl.ds(0, 15), :, 0, :, pl.ds(edge, d.half - edge)])):
        remote(part, part, l_send.at[n], l_recv.at[n, 0], me).wait_send()
    swapped = lv.at[:, pl.ds(0, 15), :, 0, :, pl.ds(d.half, d.half)]
    remote(swapped, swapped, f_send, f_recv.at[0], me).wait_send()
    for ch in range(CHUNKS):
        for h in range(2):
            theirs = left.at[:, pl.ds(0, d.chunk), pl.ds(0, d.half)]
            remote(theirs, lv.at[ch, slot, core, :, :, pl.ds(h * d.half, d.half)], d2d_sem.at[ch, h], d2d_recv.at[ch, h], partner).wait_send()
    put_out(LANCZOS_STEPS - 2)

    def finish(block, before, s):
        owner = device(s % 4, s // 4 % 2, s // 8, me // CHIPS)
        return (block - (last_alpha - scr[owner][:, 4:5]) * before) / last_beta

    put_out(LANCZOS_STEPS - 1, finish)
    for j in range(LANCZOS_STEPS):
        for c in range(d.bond // d.wide):
            pltpu.make_async_copy(tbuf.at[j, c], out.at[j, :, pl.ds(c * d.wide, d.wide)], o_sem.at[j, c]).wait()


def solution(mesh):
    def device_body(wavefunction, left_loc, pair_loc, right_loc, flag_loc):
        bond, pair = wavefunction.shape[0], wavefunction.shape[1]
        d = Dims(bond, pair, left_loc.shape[0])
        bf16, f32 = jnp.bfloat16, jnp.float32
        dma = pltpu.SemaphoreType.DMA
        any_space = pl.BlockSpec(memory_space=pl.ANY)
        smem = pl.BlockSpec(memory_space=pltpu.SMEM)
        scalars = jax.ShapeDtypeStruct((LANCZOS_STEPS,), f32)
        later, first, alphas, betas = pl.pallas_call(
            functools.partial(lanczos_kernel, d),
            out_shape=(jax.ShapeDtypeStruct((LANCZOS_STEPS, d.out_rows * pair, bond), f32),
                       jax.ShapeDtypeStruct((d.out_rows * pair, bond), f32), scalars, scalars),
            in_specs=[any_space] * 3 + [pl.BlockSpec(memory_space=pltpu.VMEM), smem],
            out_specs=(any_space, any_space, smem, smem),
            scratch_shapes=[
                pltpu.VMEM((CHUNKS, CHIPS, CORES, d.terms_dev, d.chunk, bond), bf16),
                pltpu.VMEM((CHIPS, CORES, d.terms_dev, d.slab, bond), bf16),
                pltpu.VMEM((d.terms_dev, bond, bond), bf16),
                pltpu.VMEM((CHIPS, CORES, pair, 128), bf16),
                pltpu.VMEM((CHIPS, CORES, d.terms_dev, d.prod, d.prod), bf16),
                pltpu.VMEM((CHUNKS, pair // 2, bond, 2 * d.chunk), bf16),
                pltpu.VMEM((d.lane_tiles, d.half * pair, d.lane), f32),
                pltpu.VMEM((CHIPS * CORES * d.terms_dev, pair, d.sub, 2 * d.chunk), bf16),
                pltpu.VMEM((d.rows, d.group_terms * d.chunk), bf16),
                pltpu.VMEM((d.rows, bond), f32),
                pltpu.VMEM((d.rows, d.half), f32),
                pltpu.VMEM((d.rows, d.half), f32),
                pltpu.VMEM((d.rows, d.half), f32),
                pltpu.VMEM((LANCZOS_STEPS, bond // d.wide, d.half, d.wide), f32),
                pltpu.VMEM((LANCZOS_STEPS, CHIPS, bond // d.wide, d.out_rows, d.wide), f32),
                pltpu.VMEM((1, 128), f32),
                pltpu.VMEM((DEVS, 1, 128), f32),
                pltpu.VMEM((2, 8, 128), f32),
                dma((3, 2)), dma((8, d.lane_tiles)), dma((CHUNKS, 2)), dma((CHUNKS, 2)), dma((2,)), dma((2,)), dma((2,)), dma((2,)),
                dma((4,)), dma((4, CHIPS)), dma, dma((CHIPS,)), dma((PIECES,)), dma((PIECES, CHIPS)),
                dma, dma, dma, dma, dma((LANCZOS_STEPS,)), dma((LANCZOS_STEPS,)), dma, dma, dma((LANCZOS_STEPS, bond // d.wide)), dma((bond // d.wide,)),
            ],
            compiler_params=pltpu.CompilerParams(has_side_effects=True, collective_id=0, vmem_limit_bytes=67043328),
            name='lanczos',
        )(wavefunction.reshape(bond * pair, bond), left_loc, right_loc, pair_loc, flag_loc)
        krylov = jnp.concatenate([first[None], later])
        return krylov.reshape(LANCZOS_STEPS + 1, d.out_rows, pair, bond), alphas, betas

    return jax.shard_map(device_body, mesh=mesh, in_specs=(P(), P(AXIS_NAME), P(AXIS_NAME), P(AXIS_NAME), P(AXIS_NAME)),
                         out_specs=(P(None, AXIS_NAME), P(), P()), check_vma=False)
```
